32 devices in a mesh: section: 2 (over core), dp: 4 (over z), tensor: 4 (over y, x).
Axes of the slice: x: 2, y: 2, z: 4, core: 2. Of those that a mesh axis runs over, the one named last changes fastest.
Arguments:
- inputs: bfloat16 [2, 4, 2048, 768], P(None, 'dp', 'tensor'), may hold values from -6 to 6
- cotangent: bfloat16 [2, 4, 2048, 768], P(None, 'dp', 'tensor'), may hold values from -6 to 6
- segments: int32 [2, 4, 2048], P(None, 'dp'), may hold values from 0 to 3, never falling along the last dimension, each value on 1 to 1024 neighbouring positions
- live_blocks: int32 [2, 4], P(None, 'dp'), may hold values from 8 to 16
- ln1_gain: bfloat16 [2, 768], P('section', ('dp', 'tensor')), may hold values from 0.25 to 1.75
- ln1_bias: bfloat16 [2, 768], P('section', ('dp', 'tensor')), may hold values from -3 to 3
- qkv_weight: bfloat16 [2, 768, 2304], P('section', 'dp', 'tensor'), may hold values from -0.21875 to 0.21875
- qkv_bias: bfloat16 [2, 12, 192], P('section', 'tensor', 'dp'), may hold values from -2 to 2
- out_weight: bfloat16 [2, 768, 768], P('section', 'tensor', 'dp'), may hold values from -0.875 to 0.875
- out_bias: bfloat16 [2, 768], P('section', ('dp', 'tensor')), may hold values from -3 to 3
- ln2_gain: bfloat16 [2, 768], P('section', ('dp', 'tensor')), may hold values from 0.25 to 1.75
- ln2_bias: bfloat16 [2, 768], P('section', ('dp', 'tensor')), may hold values from -3 to 3
- fc1_weight: bfloat16 [2, 768, 3072], P('section', 'dp', 'tensor'), may hold values from -0.21875 to 0.21875
- fc1_bias: bfloat16 [2, 12, 256], P('section', 'tensor', 'dp'), may hold values from -3 to 3
- fc2_weight: bfloat16 [2, 3072, 768], P('section', 'tensor', 'dp'), may hold values from -0.109375 to 0.109375
- fc2_bias: bfloat16 [2, 768], P('section', ('dp', 'tensor')), may hold values from -3 to 3
Outputs:
- section_outputs: bfloat16 [2, 2, 4, 2048, 768], P('section', None, 'dp', 'tensor')
- input_grads: bfloat16 [2, 2, 4, 2048, 768], P('section', None, 'dp', 'tensor')
- ln1_gain_grad: float32 [2, 768], P('section', ('dp', 'tensor'))
- ln1_bias_grad: float32 [2, 768], P('section', ('dp', 'tensor'))
- qkv_weight_grad: float32 [2, 768, 2304], P('section', 'dp', 'tensor')
- qkv_bias_grad: float32 [2, 12, 192], P('section', 'tensor', 'dp')
- out_weight_grad: float32 [2, 768, 768], P('section', 'tensor', 'dp')
- out_bias_grad: float32 [2, 768], P('section', ('dp', 'tensor'))
- ln2_gain_grad: float32 [2, 768], P('section', ('dp', 'tensor'))
- ln2_bias_grad: float32 [2, 768], P('section', ('dp', 'tensor'))
- fc1_weight_grad: float32 [2, 768, 3072], P('section', 'dp', 'tensor')
- fc1_bias_grad: float32 [2, 12, 256], P('section', 'tensor', 'dp')
- fc2_weight_grad: float32 [2, 3072, 768], P('section', 'tensor', 'dp')
- fc2_bias_grad: float32 [2, 768], P('section', ('dp', 'tensor'))
The draws below stay inside these ranges and needn't reach their ends.
Inputs may be any that keep to these rules, and one draw needn't show every extreme that they name: `segments`: within a row the document numbers never fall; a document holds 1 to 1024 tokens.
All inputs are finite; a program needn't handle non-finite values.
Results may differ from the reference program's by a relative error of at most 0.018.
Values may be sent and summed in bfloat16 or wider, within the bound.
A program may use at most 256 MiB of HBM per device.

```python
import math
import jax
import jax.numpy as jnp
import numpy as np
from jax import lax

D = 768
HEADS = 12
HEAD_DIM = 64
ROTARY = 16
FF = 3072
SEQ = 2048
MICRO = 2
DOCS = 4
DOC_MAX = 1024
BLOCK = 128
QBLOCK = 512
SECTIONS = 2
ROWS = 4


def draw_live_blocks(key, part):
    count_key, pick_key = jax.random.split(key)
    most_blocks = SEQ // BLOCK
    counts = jax.random.randint(count_key, (MICRO * ROWS,), most_blocks // 2, most_blocks + 1)
    chosen = jax.random.randint(pick_key, (), 0, MICRO * ROWS)
    filled = jnp.where(jnp.arange(MICRO * ROWS) == chosen, most_blocks, counts)
    return filled.reshape(MICRO, ROWS).astype(jnp.int32)


def block_levels(rng, extent, cuts, low, high):
    loudness, own = 1.0, jax.random.fold_in(rng, 6)
    for axis_at, parts in cuts:
        heights = jnp.exp(jax.random.uniform(jax.random.fold_in(own, axis_at), (parts,), jnp.float32, low / len(cuts), high / len(cuts)))
        loudness = loudness * jnp.repeat(heights, extent[axis_at] // parts).reshape([-1 if axis == axis_at else 1 for axis in range(len(extent))])
    return loudness


def profile(count, total, most, skew):
    weights = [(1 << 20) // math.isqrt(grade ** skew) + 1 for grade in range(2, count + 1)]
    spare, given = total - most - (count - 1), [1] * (count - 1)
    while spare > 0:
        movable = [i for i in range(count - 1) if given[i] < most]
        pool, budget = sum([weights[i] for i in movable]), spare
        for i in movable:
            addition = min(most - given[i], max(1, budget * weights[i] // pool), spare)
            given[i] = given[i] + addition
            spare = spare - addition
    return np.array([most] + given)


def uneven_parts(key, number_of, total, most, skew):
    if number_of == 2:
        one = jax.random.randint(key, (), max(1, total - most), min(most, total - 1) + 1)
        return jnp.stack([one, total - one])
    sizes = jnp.asarray(profile(number_of, total, most, skew), jnp.int32)
    pairs = (number_of - 1) // 2
    donor, taker = sizes[1:1 + 2 * pairs:2], sizes[2:2 + 2 * pairs:2]
    room = jnp.minimum(donor - 1, most - taker)
    moved = jax.random.randint(jax.random.fold_in(key, 1), (pairs,), 0, 1 << 20) % (room + 1)
    sizes = sizes.at[1:1 + 2 * pairs:2].set(donor - moved).at[2:2 + 2 * pairs:2].set(taker + moved)
    return sizes[jax.random.permutation(jax.random.fold_in(key, 2), number_of)]


def bell_draw(stream_key, extent, width, bound, cuts=(), kind=jnp.bfloat16):
    entries = width * jax.random.normal(stream_key, extent, jnp.float32)
    if cuts:
        entries = entries * block_levels(stream_key, extent, cuts, -0.22, 0.18)
    return jnp.clip(entries, -bound, bound).astype(kind)


def setup_inputs(seed: int = 0) -> dict:
    keys = jax.random.split(jax.random.key(seed), 17)
    return {
        "inputs": bell_draw(keys[0], (MICRO, ROWS, SEQ, D), 1.0, 6.0, ((1, 4), (2, 4))),
        "cotangent": bell_draw(keys[1], (MICRO, ROWS, SEQ, D), 1.0, 6.0, ((1, 4), (2, 4))),
        "segments": jax.vmap(lambda own: jnp.searchsorted(jnp.cumsum(uneven_parts(own, DOCS, SEQ, DOC_MAX, 1)), jnp.arange(SEQ), side="right"))(jax.random.split(keys[2], MICRO * ROWS)).reshape((MICRO, ROWS, SEQ)).astype(jnp.int32),
        "live_blocks": draw_live_blocks(jax.random.fold_in(keys[16], 71), 0),
        "ln1_gain": jnp.clip(1.0 + 0.15 * jax.random.normal(keys[4], (SECTIONS, D), jnp.float32), 0.25, 1.75).astype(jnp.bfloat16),
        "ln1_bias": bell_draw(keys[5], (SECTIONS, D), 0.5, 3.0, ((0, 2), (1, 16))),
        "qkv_weight": bell_draw(keys[6], (SECTIONS, D, 3 * D), D ** -0.5, 0.21875, ((0, 2), (1, 4), (2, 4))),
        "qkv_bias": bell_draw(keys[7], (SECTIONS, HEADS, 3 * HEAD_DIM), 0.3, 2.0, ((0, 2), (1, 4), (2, 4))),
        "out_weight": bell_draw(keys[8], (SECTIONS, D, D), (D // 16) ** -0.5, 0.875, ((0, 2), (1, 4), (2, 4))),
        "out_bias": bell_draw(keys[9], (SECTIONS, D), 0.5, 3.0, ((0, 2), (1, 16))),
        "ln2_gain": jnp.clip(1.0 + 0.15 * jax.random.normal(keys[10], (SECTIONS, D), jnp.float32), 0.25, 1.75).astype(jnp.bfloat16),
        "ln2_bias": bell_draw(keys[11], (SECTIONS, D), 0.5, 3.0, ((0, 2), (1, 16))),
        "fc1_weight": bell_draw(keys[12], (SECTIONS, D, FF), D ** -0.5, 0.21875, ((0, 2), (1, 4), (2, 4))),
        "fc1_bias": bell_draw(keys[13], (SECTIONS, HEADS, FF // HEADS), 0.5, 3.0, ((0, 2), (1, 4), (2, 4))),
        "fc2_weight": bell_draw(keys[14], (SECTIONS, FF, D), FF ** -0.5, 0.109375, ((0, 2), (1, 4), (2, 4))),
        "fc2_bias": bell_draw(keys[15], (SECTIONS, D), 0.5, 3.0, ((0, 2), (1, 16))),
    }


EPS = 1e-05
NEGATIVE = -1e+30
HIGHEST = lax.Precision.HIGHEST

@jax.custom_vjp
def low(v):
    return lax.optimization_barrier(v.astype(jnp.bfloat16)).astype(jnp.float32)

@jax.custom_vjp
def low_back(v):
    return v

def low_keep(v):
    return (low(v), None)

def low_pass(kept, grad):
    return (grad,)

def back_keep(v):
    return (v, None)

def back_low(kept, grad):
    return (low(grad),)
low.defvjp(low_keep, low_pass)
low_back.defvjp(back_keep, back_low)

def layer_norm(values, gain, bias):
    average = lax.optimization_barrier(jnp.mean(values, axis=-1, keepdims=True))
    centered = values - average
    spread = lax.optimization_barrier(jnp.mean(centered * centered, axis=-1, keepdims=True))
    return centered * lax.rsqrt(spread + EPS) * gain + bias

def positions_of(segment):
    counter = jnp.arange(segment.shape[0], dtype=jnp.int32)
    starts = jnp.concatenate([jnp.ones((1,), dtype=bool), segment[1:] != segment[:-1]])
    doc_start = lax.cummax(jnp.where(starts, counter, 0), axis=0)
    return counter - doc_start

def rotary_tables(segment):
    positions = positions_of(segment).astype(jnp.float32)
    frequency = 10000.0 ** (-(jnp.arange(ROTARY // 2, dtype=jnp.float32) * (2.0 / ROTARY)))
    angles = positions[:, None] * frequency[None, :]
    angles = jnp.concatenate([angles, angles], axis=-1)
    return (jnp.cos(angles)[:, None, :], jnp.sin(angles)[:, None, :])

def rotate(values, cosines, sines):
    half_width = ROTARY // 2
    rotated_part = values[..., :ROTARY]
    swapped = jnp.concatenate([-rotated_part[..., half_width:], rotated_part[..., :half_width]], axis=-1)
    return jnp.concatenate([rotated_part * cosines + swapped * sines, values[..., ROTARY:]], axis=-1)

def allowed_block(segment, live_count, offset, count):
    query_index = offset + jnp.arange(count, dtype=jnp.int32)
    key_index = jnp.arange(segment.shape[0], dtype=jnp.int32)
    query_docs = lax.dynamic_slice_in_dim(segment, offset, count)
    same_doc = query_docs[:, None] == segment[None, :]
    causal = key_index[None, :] <= query_index[:, None]
    present = (key_index < live_count * BLOCK)[None, :] | (key_index[None, :] == query_index[:, None])
    return same_doc & causal & present

def attention(query_rows, key_rows, value_rows, segment, live_count):
    blocks = query_rows.shape[0] // QBLOCK
    starts = jnp.arange(blocks, dtype=jnp.int32) * QBLOCK
    pieces = query_rows.reshape(blocks, QBLOCK, HEADS, HEAD_DIM)

    def one_block(element):
        block_rows, offset = element
        scores = jnp.einsum('qhd,khd->hqk', block_rows, key_rows, precision=HIGHEST) * 0.125
        scores = low_back(scores)
        scores = jnp.where(allowed_block(segment, live_count, offset, QBLOCK)[None], scores, NEGATIVE)
        row_max = lax.optimization_barrier(jnp.max(scores, axis=-1, keepdims=True))
        weights = jnp.exp(scores - row_max)
        probability = weights / lax.optimization_barrier(jnp.sum(weights, axis=-1, keepdims=True))
        return jnp.einsum('hqk,khd->qhd', low(probability), value_rows, precision=HIGHEST)
    attended = lax.map(jax.checkpoint(one_block), (pieces, starts))
    return attended.reshape(query_rows.shape[0], HEADS * HEAD_DIM)

def layer(values, params, segment, live_count):
    gain_first, bias_first, mix_weight, mix_bias, out_matrix, out_shift, gain_second, bias_second, up_matrix, up_bias, down_matrix, down_shift = params
    normed_first = low(layer_norm(values, gain_first, bias_first))
    normed_second = low(layer_norm(values, gain_second, bias_second))
    projected = jnp.dot(normed_first, mix_weight, precision=HIGHEST) + mix_bias.reshape(-1)
    projected = low_back(projected).reshape(values.shape[0], HEADS, 3 * HEAD_DIM)
    cosines, sines = rotary_tables(segment)
    query_rows = low(rotate(projected[..., :HEAD_DIM], cosines, sines))
    key_rows = low(rotate(projected[..., HEAD_DIM:2 * HEAD_DIM], cosines, sines))
    value_rows = low(projected[..., 2 * HEAD_DIM:])
    attended = low_back(low(attention(query_rows, key_rows, value_rows, segment, live_count)))
    hidden = low_back(jnp.dot(normed_second, up_matrix, precision=HIGHEST) + up_bias.reshape(-1))
    active = low(jax.nn.gelu(hidden, approximate=False))
    branch = jnp.dot(attended, out_matrix, precision=HIGHEST) + jnp.dot(active, down_matrix, precision=HIGHEST)
    return values + branch + out_shift + down_shift

def reference(inputs, cotangent, segments, live_blocks, ln1_gain, ln1_bias, qkv_weight, qkv_bias, out_weight, out_bias, ln2_gain, ln2_bias, fc1_weight, fc1_bias, fc2_weight, fc2_bias):
    params = tuple((weight.astype(jnp.float32) for weight in (ln1_gain, ln1_bias, qkv_weight, qkv_bias, out_weight, out_bias, ln2_gain, ln2_bias, fc1_weight, fc1_bias, fc2_weight, fc2_bias)))
    first_rows = inputs.reshape(-1, SEQ, D).astype(jnp.float32)
    tangents = cotangent.reshape(-1, SEQ, D).astype(jnp.float32)
    row_segments = segments.reshape(-1, SEQ)
    row_lives = live_blocks.reshape(-1)

    def both_layers(first_in, boundary_probe, weights, segment, live_count):
        section_first = tuple((weight[0] for weight in weights))
        section_second = tuple((weight[1] for weight in weights))
        middle = low(layer(first_in, section_first, segment, live_count))
        passed = low_back(middle + boundary_probe)
        return (middle, layer(passed, section_second, segment, live_count))

    def one_row(totals, element):
        first_in, tangent, segment, live_count = element
        boundary_probe = jnp.zeros_like(first_in)

        def closed(first_arg, probe_arg, weight_arg):
            return both_layers(first_arg, probe_arg, weight_arg, segment, live_count)
        (middle, last_out), pullback = jax.vjp(closed, first_in, boundary_probe, params)
        d_first, d_probe, d_params = pullback((jnp.zeros_like(middle), tangent))
        totals = tuple((running + adding for running, adding in zip(totals, d_params)))
        return (totals, (middle.astype(jnp.bfloat16), last_out.astype(jnp.bfloat16), d_first.astype(jnp.bfloat16), d_probe.astype(jnp.bfloat16)))
    blank_totals = tuple((jnp.zeros_like(weight) for weight in params))
    totals, (middles, finals, first_grads, probe_grads) = lax.scan(one_row, blank_totals, (first_rows, tangents, row_segments, row_lives))
    whole_shape = inputs.shape
    section_outputs = jnp.stack([middles.reshape(whole_shape), finals.reshape(whole_shape)])
    input_grads = jnp.stack([first_grads.reshape(whole_shape), probe_grads.reshape(whole_shape)])
    return (section_outputs, input_grads, totals[0], totals[1], totals[2], totals[3], totals[4], totals[5], totals[6], totals[7], totals[8], totals[9], totals[10], totals[11])
```

```python
import functools

import jax
import jax.numpy as jnp
from jax import lax
from jax.experimental import pallas as pl
from jax.experimental.pallas import tpu as pltpu
from jax.sharding import PartitionSpec as P

F32 = jnp.float32
BF = jnp.bfloat16
MESH = pl.DeviceIdType.MESH
HD = 64
ROT = 16
LIVE = 128
QB = 256
HW = 256
SUB = 64
EPS = 1e-05
NEG = -1e30
VMEM = pl.BlockSpec(memory_space=pltpu.VMEM)
ANY = pl.BlockSpec(memory_space=pl.ANY)
SMEM = pl.BlockSpec(memory_space=pltpu.SMEM)
DMA = pltpu.SemaphoreType.DMA


def sds(shape, dtype):
    return jax.ShapeDtypeStruct(shape, dtype)


def dg(a, b, ca, cb):
    return lax.dot_general(a, b, (((ca,), (cb,)), ((), ())), preferred_element_type=F32)


def dot(a, b):
    return jnp.dot(a, b, preferred_element_type=F32)


def ds(start, size):
    return pl.ds(pl.multiple_of(start, size), size)


def norm_stats(x):
    mu = jnp.mean(x, axis=-1, keepdims=True)
    xc = x - mu
    var = jnp.mean(xc * xc, axis=-1, keepdims=True)
    return xc, lax.rsqrt(var + EPS)


def head_lanes(width, heads):
    lane = lax.broadcasted_iota(jnp.int32, (1, width), 1)
    return [(lane >= h * HD) & (lane < (h + 1) * HD) for h in range(heads)]


def allow_mask(kc, sq, diag):
    m = kc == sq
    if diag:
        r = lax.broadcasted_iota(jnp.int32, (QB, QB), 0)
        c = lax.broadcasted_iota(jnp.int32, (QB, QB), 1)
        m = (m & (r <= c)) | (r == c)
    return m


def attn_fwd_kernel(heads, b_ref, q_ref, k_ref, v_ref, sr_ref, kc_ref, o_ref, lse_ref, vt, s_scr):
    n = q_ref.shape[0] // QB
    width = q_ref.shape[1]
    hm = head_lanes(width, heads)

    def turn(i, _):
        vt[:, ds(i * QB, QB)] = v_ref[ds(i * QB, QB), :].T
        return 0

    lax.fori_loop(0, n, turn, 0)

    def qloop(i, _):
        qi = ds(i * QB, QB)
        q = q_ref[qi, :]
        qm = [jnp.where(hm[h], q, jnp.zeros_like(q)) for h in range(heads)]
        sq = sr_ref[0:1, qi]
        lo = b_ref[0, i]
        hi = b_ref[1, i]

        def scores(j, slot, ms, diag):
            kj = ds(j * QB, QB)
            k = k_ref[kj, :]
            mask = allow_mask(kc_ref[kj, 0:1], sq, diag)
            out = []
            for h in range(heads):
                s = jnp.where(mask, dg(k, qm[h], 1, 1), NEG)
                s_scr[h, ds(slot * QB, QB), :] = s
                out.append(jnp.maximum(ms[h], jnp.max(s, axis=0, keepdims=True)))
            return tuple(out)

        ms = tuple(jnp.full((1, QB), NEG, F32) for _ in range(heads))
        ms = scores(i, 0, ms, True)
        ms = lax.fori_loop(lo, hi, lambda j, ms: scores(j, j - lo + 1, ms, False), ms)

        def weigh(j, slot, st):
            kj = ds(j * QB, QB)
            out = []
            for h in range(heads):
                total, acc = st[h]
                p = jnp.exp(s_scr[h, ds(slot * QB, QB), :] - ms[h])
                total = total + jnp.sum(p, axis=0, keepdims=True)
                acc = acc + dot(vt[h * HD : (h + 1) * HD, kj], p.astype(BF))
                out.append((total, acc))
            return tuple(out)

        st = tuple((jnp.zeros((1, QB), F32), jnp.zeros((HD, QB), F32)) for _ in range(heads))
        st = weigh(i, 0, st)
        st = lax.fori_loop(lo, hi, lambda j, st: weigh(j, j - lo + 1, st), st)
        ot = [st[h][1] * (1.0 / st[h][0]) for h in range(heads)]
        ot = jnp.concatenate(ot + [jnp.zeros((width - heads * HD, QB), F32)], axis=0)
        o_ref[qi, :] = ot.T.astype(BF)
        lse = [ms[h] + jnp.log(st[h][0]) for h in range(heads)]
        lse_ref[:, qi] = jnp.concatenate(lse + [jnp.zeros((8 - heads, QB), F32)], axis=0)
        return 0

    lax.fori_loop(0, n, qloop, 0)


def attn_fwd(heads, bounds, q, k, v, sr, kc):
    rows, width = q.shape
    return pl.pallas_call(
        functools.partial(attn_fwd_kernel, heads),
        out_shape=(sds((rows, width), BF), sds((8, rows), F32)),
        in_specs=[SMEM] + [VMEM] * 5,
        out_specs=(VMEM, VMEM),
        scratch_shapes=[pltpu.VMEM((width, rows), BF), pltpu.VMEM((heads, rows + QB, QB), F32)],
        compiler_params=pltpu.CompilerParams(vmem_limit_bytes=40 << 20),
        name="attn_fwd",
    )(bounds, q, k, v, sr, kc)


def turn_lanes(x, tab, sign):
    width = x.shape[1]
    c, s1, s2 = [jnp.concatenate([tab[:, a * 128 : (a + 1) * 128]] * (width // 128), axis=1) for a in range(3)]
    moved = pltpu.roll(x, width - ROT // 2, 1) * s1 + pltpu.roll(x, ROT // 2, 1) * s2
    return x * c + moved if sign > 0 else x * c - moved


def attn_bwd_kernel(
    heads, b_ref, q_ref, k_ref, v_ref, o_ref, do_ref, lse_ref, sr_ref, kc_ref, tab_ref, out_ref, kt, dk, dv
):
    rows, width = q_ref.shape
    n = rows // QB
    hm = head_lanes(width, heads)

    def turn(i, _):
        kt[:, ds(i * QB, QB)] = k_ref[ds(i * QB, QB), :].T
        return 0

    lax.fori_loop(0, n, turn, 0)
    dk[...] = jnp.zeros_like(dk)
    dv[...] = jnp.zeros_like(dv)
    rowid = lax.broadcasted_iota(jnp.int32, (8, width), 0)
    lane = lax.broadcasted_iota(jnp.int32, (8, width), 1)
    sel = ((lane >= rowid * HD) & (lane < (rowid + 1) * HD)).astype(F32).astype(BF)

    def qloop(i, _):
        qi = ds(i * QB, QB)
        q = q_ref[qi, :]
        do = do_ref[qi, :]
        z = jnp.zeros_like(q)
        qm = [jnp.where(hm[h], q, z) for h in range(heads)]
        dom = [jnp.where(hm[h], do, z) for h in range(heads)]
        qcat = jnp.concatenate(qm, axis=0)
        docat = jnp.concatenate(dom, axis=0)
        prod = do.astype(F32) * o_ref[qi, :].astype(F32)
        high = prod.astype(BF)
        low = (prod - high.astype(F32)).astype(BF)
        delta = dg(sel, high, 1, 1) + dg(sel, low, 1, 1)
        lse = lse_ref[:, qi]
        sq = sr_ref[0:1, qi]
        lo = b_ref[0, i]
        hi = b_ref[1, i]

        def step(j, dqs, diag):
            kj = ds(j * QB, QB)
            k = k_ref[kj, :]
            v = v_ref[kj, :]
            mask = allow_mask(kc_ref[kj, 0:1], sq, diag)
            ps, dss, out = [], [], []
            for h in range(heads):
                s = dg(k, qm[h], 1, 1)
                dp = dg(v, dom[h], 1, 1)
                p = jnp.where(mask, jnp.exp(jnp.where(mask, s - lse[h : h + 1, :], 0.0)), 0.0)
                score_grad = (p * (dp - delta[h : h + 1, :])).astype(BF)
                ps.append(p.astype(BF))
                dss.append(score_grad)
                out.append(dqs[h] + dot(kt[h * HD : (h + 1) * HD, kj], score_grad))
            dv[kj, :] += dot(jnp.concatenate(ps, axis=1), docat)
            dk[kj, :] += dot(jnp.concatenate(dss, axis=1), qcat)
            return tuple(out)

        dqs = tuple(jnp.zeros((HD, QB), F32) for _ in range(heads))
        dqs = step(i, dqs, True)
        dqs = lax.fori_loop(lo, hi, lambda j, d: step(j, d, False), dqs)
        dq = jnp.concatenate(list(dqs) + [jnp.zeros((width - heads * HD, QB), F32)], axis=0).T * 0.125
        out_ref[qi, 0:width] = turn_lanes(dq, tab_ref[qi, :], -1).astype(BF)
        return 0

    lax.fori_loop(0, n, qloop, 0)

    def finish(i, _):
        ii = ds(i * QB, QB)
        out_ref[ii, width : 2 * width] = turn_lanes(dk[ii, :], tab_ref[ii, :], -1).astype(BF)
        out_ref[ii, 2 * width : 3 * width] = dv[ii, :].astype(BF)
        return 0

    lax.fori_loop(0, n, finish, 0)


def attn_bwd(heads, bounds, q, k, v, o, do, lse, sr, kc, tab):
    rows, width = q.shape
    return pl.pallas_call(
        functools.partial(attn_bwd_kernel, heads),
        out_shape=sds((rows, 3 * width), BF),
        in_specs=[SMEM] + [VMEM] * 9,
        out_specs=VMEM,
        scratch_shapes=[
            pltpu.VMEM((width, rows), BF),
            pltpu.VMEM((rows, width), F32),
            pltpu.VMEM((rows, width), F32),
        ],
        compiler_params=pltpu.CompilerParams(vmem_limit_bytes=50 << 20),
        name="attn_bwd",
    )(bounds, q, k, v, o, do, lse, sr, kc, tab)


def places():
    t = lax.axis_index("tensor")
    x, y = t % 2, t // 2
    return t, 2 * y + (1 - x), 2 * (1 - y) + x, 3 - t


def greet(peers):
    bar = pltpu.get_barrier_semaphore()
    for peer in peers:
        pl.semaphore_signal(bar, inc=1, device_id=peer, device_id_type=MESH)
    pl.semaphore_wait(bar, len(peers))


def push(src, dst, ssem, rsem, peer):
    return pltpu.make_async_remote_copy(
        src_ref=src, dst_ref=dst, send_sem=ssem, recv_sem=rsem, device_id=peer, device_id_type=MESH
    )


def pick(i, values):
    out = values[-1]
    for n in range(len(values) - 2, -1, -1):
        out = jnp.where(i == n, values[n], out)
    return out


class Gather:
    def __init__(self, full, ssem, rsem):
        self.t, self.px, self.py, self.pd = places()
        self.full, self.ssem, self.rsem = full, ssem, rsem
        self.half = full.shape[0] // 8

    def rows(self, c, h):
        return ds((2 * c + h) * self.half, self.half)

    def copy(self, i, c, h, peer):
        ref = self.full.at[self.rows(c, h)]
        return push(ref, ref, self.ssem.at[i], self.rsem.at[i], {"tensor": peer})

    def plan(self):
        t, px, py = self.t, self.px, self.py
        return [
            self.copy(0, t, 0, px),
            self.copy(1, t, 1, py),
            self.copy(2, t, 1, px),
            self.copy(3, t, 0, py),
            self.copy(4, px, 0, py),
            self.copy(5, py, 1, px),
        ]

    def order(self, i):
        t, px, py, pd = self.t, self.px, self.py, self.pd
        return pick(i, [t, t, px, py, px, py, pd, pd]), pick(i, [0, 1, 0, 1, 1, 0, 0, 1])

    def arrive(self, i):
        plan = self.plan()

        @pl.when(i == 2)
        def _():
            plan[0].wait_recv()
            plan[4].start()
            plan[1].wait_recv()
            plan[5].start()

        for step in (4, 5, 6, 7):

            @pl.when(i == step)
            def _(step=step):
                plan[step - 2].wait_recv()

    def finish(self):
        for c in self.plan():
            c.wait_send()

    def run(self, work):
        def body(i, _):
            self.arrive(i)
            c, h = self.order(i)
            work((2 * c + h) * self.half)
            return 0

        lax.fori_loop(0, 8, body, 0)
        self.finish()


class Scatter:
    def __init__(self, part, r1x, r1y, r2x, r2y, ssem, rsem):
        self.t, self.px, self.py, self.pd = places()
        self.part, self.r1x, self.r1y, self.r2x, self.r2y = part, r1x, r1y, r2x, r2y
        self.ssem, self.rsem = ssem, rsem
        self.half = part.shape[0] // 8

    def rows(self, c, h):
        return ds((2 * c + h) * self.half, self.half)

    def copy(self, i, c, h, dst, peer):
        return push(self.part.at[self.rows(c, h)], dst, self.ssem.at[i], self.rsem.at[i], {"tensor": peer})

    def plan(self):
        px, py, pd = self.px, self.py, self.pd
        return [
            self.copy(0, pd, 0, self.r1x.at[1], px),
            self.copy(1, pd, 1, self.r1y.at[1], py),
            self.copy(2, px, 0, self.r1x.at[0], px),
            self.copy(3, py, 1, self.r1y.at[0], py),
            self.copy(4, py, 0, self.r2y, py),
            self.copy(5, px, 1, self.r2x, px),
        ]

    def run(self, work, between=None):
        t, px, py, pd = self.t, self.px, self.py, self.pd
        plan = self.plan()

        def body(i, _):
            c = pick(i, [pd, pd, px, py, py, px, t, t])
            h = pick(i, [0, 1, 0, 1, 0, 1, 0, 1])
            work((2 * c + h) * self.half)
            for step in range(4):

                @pl.when(i == step)
                def _(step=step):
                    plan[step].start()

            return 0

        lax.fori_loop(0, 8, body, 0)
        for first, c, h, buf, second in ((0, py, 0, self.r1x, 4), (1, px, 1, self.r1y, 5)):
            plan[first].wait_recv()

            def add(i, _, c=c, h=h, buf=buf):
                rr = ds((2 * c + h) * self.half + i * SUB, SUB)
                got = buf[1, ds(i * SUB, SUB), :].astype(F32)
                self.part[rr, :] = (self.part[rr, :].astype(F32) + got).astype(BF)
                return 0

            lax.fori_loop(0, self.half // SUB, add, 0)
            plan[second].start()
        if between is not None:
            between()

    def arrive(self, h):
        plan = self.plan()
        if h == 0:
            plan[2].wait_recv()
            plan[4].wait_recv()
        else:
            plan[3].wait_recv()
            plan[5].wait_recv()

    def total(self, h, i):
        near, far = (self.r1x, self.r2y) if h == 0 else (self.r1y, self.r2x)
        rr = ds((2 * self.t + h) * self.half + i * SUB, SUB)
        sub = ds(i * SUB, SUB)
        return self.part[rr, :].astype(F32) + near[0, sub, :].astype(F32) + far[sub, :].astype(F32)

    def finish(self):
        for c in self.plan():
            c.wait_send()


def scatter_scratch(rows, width):
    half = rows // 8
    return [
        pltpu.VMEM((rows, width), BF),
        pltpu.VMEM((2, half, width), BF),
        pltpu.VMEM((2, half, width), BF),
        pltpu.VMEM((half, width), BF),
        pltpu.VMEM((half, width), BF),
        DMA((6,)),
        DMA((6,)),
    ]


def gather_kernel(
    dp, tensor, w_ref, sv_ref, pos_ref, fr_ref, wf_ref, vec_ref, tab_ref, own, wss, wrs, fss, frs, vss, vrs
):
    s, z, t = lax.axis_index("section"), lax.axis_index("dp"), lax.axis_index("tensor")
    rows = w_ref.shape[0]
    mate = {"section": 1 - s}
    ring = [{"dp": (z + d) % dp} for d in range(1, dp)]
    group = [{"tensor": (t + d) % tensor} for d in range(1, tensor)]
    greet([mate] + ring + group)

    def block(layer, zz):
        return wf_ref.at[layer, ds(zz * rows, rows)]

    mine = [
        pltpu.make_async_copy(w_ref, block(s, z), own.at[0]),
        pltpu.make_async_copy(sv_ref, vec_ref.at[s, t, z], own.at[1]),
    ]
    for c in mine:
        c.start()
    nv = dp - 1 + tensor - 1 + 1
    first = [push(sv_ref, vec_ref.at[s, t, z], vss.at[d], vrs.at[d], peer) for d, peer in enumerate(ring)]
    for c in first:
        c.start()
    sends = [push(w_ref, block(s, z), wss.at[d], wrs.at[d], peer) for d, peer in enumerate(ring)]
    for c in sends:
        c.start()
    onward = [push(w_ref, block(s, z), fss.at[0], frs.at[0], mate)]
    onward[0].start()
    ang = fr_ref[:, 0:1] * pos_ref[...].astype(F32)
    cs, sn = jnp.cos(ang), jnp.sin(ang)
    wide = ang.shape[1]
    one, zero = jnp.ones((HD - ROT, wide), F32), jnp.zeros((HD - ROT, wide), F32)
    z8 = jnp.zeros_like(cs)
    pieces = ([cs, cs, one] * 2, [-sn, z8, zero] * 2, [z8, sn, zero] * 2)
    for a, piece in enumerate(pieces):
        tab_ref[:, a * 128 : (a + 1) * 128] = jnp.concatenate(piece, axis=0).T
    for c in mine:
        c.wait()
    for c in first:
        c.wait_recv()
    second = []
    for d, peer in enumerate(group):
        i = dp - 1 + d
        second.append(push(vec_ref.at[s, t], vec_ref.at[s, t], vss.at[i], vrs.at[i], peer))
        second[-1].start()
    for c in second:
        c.wait_recv()
    third = push(vec_ref.at[s], vec_ref.at[s], vss.at[nv - 1], vrs.at[nv - 1], mate)
    third.start()
    for d in range(dp - 1):
        sends[d].wait_recv()
        zz = (z - d - 1 + dp) % dp
        onward.append(push(block(s, zz), block(s, zz), fss.at[d + 1], frs.at[d + 1], mate))
        onward[-1].start()
    third.wait_recv()
    for c in onward:
        c.wait_recv()
    for c in first + sends + second + [third] + onward:
        c.wait_send()


def gather_all(dp, tensor, w, sv, pos, fr):
    rows, cols = w.shape
    seq = pos.shape[1]
    nv = dp - 1 + tensor
    return pl.pallas_call(
        functools.partial(gather_kernel, dp, tensor),
        out_shape=(
            sds((2, rows * dp, cols), BF),
            sds((2, tensor, dp) + sv.shape, F32),
            sds((seq, 3 * 128), F32),
        ),
        in_specs=[VMEM] * 4,
        out_specs=(ANY, VMEM, VMEM),
        scratch_shapes=[
            DMA((2,)),
            DMA((dp - 1,)),
            DMA((dp - 1,)),
            DMA((dp,)),
            DMA((dp,)),
            DMA((nv,)),
            DMA((nv,)),
        ],
        compiler_params=pltpu.CompilerParams(collective_id=1, has_side_effects=True, vmem_limit_bytes=40 << 20),
        name="gather_weights",
    )(w, sv, pos, fr)


QKV, FC1, FC2, OUT = 0, 1, 2, 3


def columns(model, ff):
    return {"qkv": 0, "fc1": 3 * HW, "fc2": 3 * HW + ff, "out": 3 * HW + 2 * ff, "end": 3 * HW + 2 * ff + HW}


def project(r0, half, hf, wqkv, wfc1, vec, tab, n1, n2, q, k, v, g, gp):
    rows = ds(r0, half)

    def norm(i, _):
        rr = ds(r0 + i * SUB, SUB)
        xc, r = norm_stats(hf[rr, :].astype(F32))
        xh = xc * r
        n1[rr, :] = (xh * vec[0:1, :] + vec[1:2, :]).astype(BF)
        n2[rr, :] = (xh * vec[3:4, :] + vec[4:5, :]).astype(BF)
        return 0

    lax.fori_loop(0, half // SUB, norm, 0)
    a = n1[rows, :]
    for part, dst in enumerate((q, k, v)):
        cols = slice(part * HW, (part + 1) * HW)
        y = dot(a, wqkv[:, cols]) + vec[6:7, cols]
        if part < 2:
            y = turn_lanes(y, tab[rows, :], 1)
        if part == 0:
            y = y * 0.125
        dst[rows, :] = y.astype(BF)
    a = n2[rows, :]
    for b in range(wfc1.shape[1] // 256):
        cols = slice(b * 256, (b + 1) * 256)
        y = dot(a, wfc1[:, cols]) + vec[7:8, cols]
        cdf = 0.5 + 0.5 * lax.erf(y * 0.7071067811865476)
        g[rows, cols] = (y * cdf).astype(BF)
        gp[rows, cols] = (cdf + y * jnp.exp(-0.5 * y * y) * 0.3989422804014327).astype(BF)


def branch_out(r0, half, o, g, wout, wfc2, part):
    rows = ds(r0, half)
    for b in range(part.shape[1] // 256):
        cols = slice(b * 256, (b + 1) * 256)
        y = dg(o[rows, :], wout[cols, :], 1, 1) + dg(g[rows, :], wfc2[cols, :], 1, 1)
        part[rows, cols] = y.astype(BF)


def back_head(r0, half, dyf, hf, g, gp, n2, o, wfc1, wfc2, wout, vec, do, e2, da, acc, vg):
    rows = ds(r0, half)
    model, ff = wfc1.shape
    dy = dyf[rows, :]
    for b in range(ff // 256):
        cols = slice(b * 256, (b + 1) * 256)
        y = dot(dy, wfc2[:, cols]) * gp[rows, cols].astype(F32)
        low = y.astype(BF)
        da[:, cols] = low
        vg[7:8, cols] += jnp.sum(low.astype(F32), axis=0, keepdims=True)
    do[rows, :] = dot(dy, wout[...]).astype(BF)
    xc, r = norm_stats(hf[rows, :].astype(F32))
    xh = xc * r
    for b in range(model // 256):
        cols = slice(b * 256, (b + 1) * 256)
        dn = dg(da[...], wfc1[cols, :], 1, 1)
        vg[3:4, cols] += jnp.sum(dn * xh[:, cols], axis=0, keepdims=True)
        vg[4:5, cols] += jnp.sum(dn, axis=0, keepdims=True)
        e2[rows, cols] = (dn * vec[3:4, cols]).astype(BF)
    n2t = n2[rows, :].T
    dyt = dy.T
    for b in range(ff // 256):
        cols = slice(b * 256, (b + 1) * 256)
        acc[:, cols] += dot(n2t, da[:, cols])
        acc[:, ff + b * 256 : ff + (b + 1) * 256] += dot(dyt, g[rows, cols])
    acc[:, 2 * ff :] += dot(dyt, o[rows, :])


def back_tail(r0, half, dmix, hf, e2, wqkv, vec, part, vg):
    rows = ds(r0, half)
    dm = dmix[rows, :]
    vg[6:7, :] += jnp.sum(dm.astype(F32), axis=0, keepdims=True)
    xc, r = norm_stats(hf[rows, :].astype(F32))
    xh = xc * r
    for b in range(part.shape[1] // 256):
        cols = slice(b * 256, (b + 1) * 256)
        dn = dg(dm, wqkv[cols, :], 1, 1)
        vg[0:1, cols] += jnp.sum(dn * xh[:, cols], axis=0, keepdims=True)
        vg[1:2, cols] += jnp.sum(dn, axis=0, keepdims=True)
        part[rows, cols] = (dn * vec[0:1, cols] + e2[rows, cols].astype(F32)).astype(BF)


def qkv_grad(n1, dmix, acc, half):
    acc[...] = jnp.zeros_like(acc)

    def body(i, _):
        rows = ds(i * half, half)
        n1t = n1[rows, :].T
        for b in range(3):
            cols = slice(b * HW, (b + 1) * HW)
            acc[:, cols] += dot(n1t, dmix[rows, cols])
        return 0

    lax.fori_loop(0, n1.shape[0] // half, body, 0)


def store_low(acc, out):
    def body(i, _):
        rr = ds(i * SUB, SUB)
        out[rr, :] = acc[rr, :].astype(BF)
        return 0

    lax.fori_loop(0, acc.shape[0] // SUB, body, 0)


def residual_out(sc, own, off, vec, dst, dst2=None, dst2_off=None, after=None):
    for h in range(2):
        sc.arrive(h)

        def body(i, _, h=h):
            rr = ds(h * sc.half + i * SUB, SUB)
            base = own[ds(off + h * sc.half + i * SUB, SUB), :].astype(F32)
            y = (base + sc.total(h, i) + vec[2:3, :] + vec[5:6, :]).astype(BF)
            dst[rr, :] = y
            if dst2 is not None:
                dst2[ds(dst2_off + h * sc.half + i * SUB, SUB), :] = y
            return 0

        lax.fori_loop(0, sc.half // SUB, body, 0)
        if after is not None:
            after(h)


def grad_out(sc, dy, dy_off, hf, vec, dst, dst2=None, dst2_off=None, after=None):
    base = sc.t * 2 * sc.half
    for h in range(2):
        sc.arrive(h)

        def body(i, _, h=h):
            off = h * sc.half + i * SUB
            xc, r = norm_stats(hf[ds(base + off, SUB), :].astype(F32))
            xh = xc * r
            e = sc.total(h, i)
            m1 = jnp.mean(e, axis=-1, keepdims=True)
            m2 = jnp.mean(e * xh, axis=-1, keepdims=True)
            du = dy[ds(dy_off + off, SUB), :].astype(F32) + r * (e - m1 - xh * m2)
            low = du.astype(BF)
            dst[ds(off, SUB), :] = low
            if dst2 is not None:
                dst2[ds(dst2_off + off, SUB), :] = low
            return 0

        lax.fori_loop(0, sc.half // SUB, body, 0)
        if after is not None:
            after(h)


def start_half(ga, h):
    plan = ga.plan()
    for i in ((0, 3) if h == 0 else (1, 2)):
        plan[i].start()


def column_sum(ref, off, count, vg, row):
    def body(i, acc):
        return acc + jnp.sum(ref[ds(off + i * SUB, SUB), :].astype(F32), axis=0, keepdims=True)

    vg[row : row + 1, :] = lax.fori_loop(0, count // SUB, body, jnp.zeros((1, ref.shape[1]), F32))


def load(pairs, sem):
    copies = [pltpu.make_async_copy(a, b, sem.at[i]) for i, (a, b) in enumerate(pairs)]
    for c in copies:
        c.start()
    return copies


def params(cid, mib=58):
    return pltpu.CompilerParams(collective_id=cid, has_side_effects=True, vmem_limit_bytes=mib << 20)


def neighbours():
    t, px, py, pd = places()
    return [{"tensor": px}, {"tensor": py}]


def in_kernel(col, x_ref, wf, vec, tab, hf, n1, n2, q, k, v, g, gp, wqkv, wfc1, gss, grs, lsem):
    greet(neighbours())
    ga = Gather(hf, gss, grs)
    loads = load(
        [
            (x_ref, hf.at[ds(ga.t * 2 * ga.half, 2 * ga.half)]),
            (wf.at[0, :, col["qkv"] : col["fc1"]], wqkv),
            (wf.at[0, :, col["fc1"] : col["fc2"]], wfc1),
        ],
        lsem,
    )
    loads[0].wait()
    start_half(ga, 0)
    start_half(ga, 1)
    loads[1].wait()
    loads[2].wait()
    ga.run(lambda r0: project(r0, ga.half, hf, wqkv, wfc1, vec, tab, n1, n2, q, k, v, g, gp))


def project_shapes(seq, model, ff):
    return (
        sds((seq, model), BF),
        sds((seq, model), BF),
        sds((seq, model), BF),
        sds((seq, HW), BF),
        sds((seq, HW), BF),
        sds((seq, HW), BF),
        sds((seq, ff), BF),
        sds((seq, ff), BF),
    )


def layer_in(col, ff, x, wf, vec, tab):
    seq, model = tab.shape[0], x.shape[1]
    return pl.pallas_call(
        functools.partial(in_kernel, col),
        out_shape=project_shapes(seq, model, ff),
        in_specs=[VMEM, ANY, VMEM, VMEM],
        out_specs=(VMEM,) * 8,
        scratch_shapes=[pltpu.VMEM((model, 3 * HW), BF), pltpu.VMEM((model, ff), BF), DMA((6,)), DMA((6,)), DMA((3,))],
        compiler_params=params(2),
        name="layer_in",
    )(x, wf, vec, tab)


def mid_kernel(
    col, o, g_in, x_ref, wf, vec0, vec1, tab, h_ref, hf, n1, n2, q, k, v, g, gp,
    wout, wfc2, wqkv, wfc1, part, r1x, r1y, r2x, r2y, sss, srs, gss, grs, lsem,
):
    greet(neighbours())
    loads = load(
        [
            (wf.at[0, :, col["out"] : col["end"]], wout),
            (wf.at[0, :, col["fc2"] : col["out"]], wfc2),
            (wf.at[1, :, col["qkv"] : col["fc1"]], wqkv),
            (wf.at[1, :, col["fc1"] : col["fc2"]], wfc1),
        ],
        lsem,
    )
    loads[0].wait()
    loads[1].wait()
    sc = Scatter(part, r1x, r1y, r2x, r2y, sss, srs)
    ga = Gather(hf, gss, grs)
    sc.run(lambda r0: branch_out(r0, sc.half, o, g_in, wout, wfc2, part))
    residual_out(sc, x_ref, 0, vec0, h_ref, hf, sc.t * 2 * sc.half, lambda h: start_half(ga, h))
    loads[2].wait()
    loads[3].wait()
    ga.run(lambda r0: project(r0, ga.half, hf, wqkv, wfc1, vec1, tab, n1, n2, q, k, v, g, gp))
    sc.finish()


def layer_mid(col, ff, o, g, x, wf, vec0, vec1, tab):
    seq, model = tab.shape[0], x.shape[1]
    return pl.pallas_call(
        functools.partial(mid_kernel, col),
        out_shape=(sds(x.shape, BF),) + project_shapes(seq, model, ff),
        in_specs=[VMEM, VMEM, VMEM, ANY, VMEM, VMEM, VMEM],
        out_specs=(VMEM,) * 9,
        scratch_shapes=[
            pltpu.VMEM((model, HW), BF),
            pltpu.VMEM((model, ff), BF),
            pltpu.VMEM((model, 3 * HW), BF),
            pltpu.VMEM((model, ff), BF),
        ]
        + scatter_scratch(seq, model)
        + [DMA((6,)), DMA((6,)), DMA((4,))],
        compiler_params=params(3),
        name="layer_mid",
    )(o, g, x, wf, vec0, vec1, tab)


def turn_kernel(
    col, o, g, h_ref, hf, cot, wf, vec, n2, gp, y_ref, dyf, do, e2, gr, vg,
    wout, wfc2, wfc1, da, acc, part, r1x, r1y, r2x, r2y, sss, srs, gss, grs, lsem,
):
    greet(neighbours())
    ga = Gather(dyf, gss, grs)
    sc = Scatter(part, r1x, r1y, r2x, r2y, sss, srs)
    loads = load(
        [
            (cot, dyf.at[ds(ga.t * 2 * ga.half, 2 * ga.half)]),
            (wf.at[1, :, col["out"] : col["end"]], wout),
            (wf.at[1, :, col["fc2"] : col["out"]], wfc2),
            (wf.at[1, :, col["fc1"] : col["fc2"]], wfc1),
        ],
        lsem,
    )
    loads[0].wait()
    start_half(ga, 0)
    start_half(ga, 1)
    vg[...] = jnp.zeros_like(vg)
    acc[...] = jnp.zeros_like(acc)
    for c in loads[1:]:
        c.wait()
    sc.run(lambda r0: branch_out(r0, sc.half, o, g, wout, wfc2, part))
    ga.run(lambda r0: back_head(r0, ga.half, dyf, hf, g, gp, n2, o, wfc1, wfc2, wout, vec, do, e2, da, acc, vg))
    column_sum(cot, 0, cot.shape[0], vg, 2)
    store_low(acc, gr)
    residual_out(sc, h_ref, 0, vec, y_ref)
    sc.finish()


def layer_turn(col, ff, o, g, h, hf, cot, wf, vec, n2, gp):
    seq, model = hf.shape
    return pl.pallas_call(
        functools.partial(turn_kernel, col),
        out_shape=(
            sds(h.shape, BF),
            sds((seq, model), BF),
            sds((seq, HW), BF),
            sds((seq, model), BF),
            sds((model, 2 * ff + HW), BF),
            sds((8, model), F32),
        ),
        in_specs=[VMEM] * 5 + [ANY] + [VMEM] * 3,
        out_specs=(VMEM,) * 6,
        scratch_shapes=[
            pltpu.VMEM((model, HW), BF),
            pltpu.VMEM((model, ff), BF),
            pltpu.VMEM((model, ff), BF),
            pltpu.VMEM((seq // 8, ff), BF),
            pltpu.VMEM((model, 2 * ff + HW), F32),
        ]
        + scatter_scratch(seq, model)
        + [DMA((6,)), DMA((6,)), DMA((4,))],
        compiler_params=params(4, 63),
        name="layer_turn",
    )(o, g, h, hf, cot, wf, vec, n2, gp)


def back_kernel(
    col, dmix, e2_in, cot, hf, n1, wf, vec1, vec0, xf, g, gp, n2, o, dh_ref, dhf, gq, vgf, do, e2, gr, vgd,
    wqkv, wout, wfc2, wfc1, da, acc, part, r1x, r1y, r2x, r2y, sss, srs, gss, grs, lsem,
):
    greet(neighbours())
    ga = Gather(dhf, gss, grs)
    sc = Scatter(part, r1x, r1y, r2x, r2y, sss, srs)
    loads = load(
        [
            (wf.at[1, :, col["qkv"] : col["fc1"]], wqkv),
            (wf.at[0, :, col["out"] : col["end"]], wout),
            (wf.at[0, :, col["fc2"] : col["out"]], wfc2),
            (wf.at[0, :, col["fc1"] : col["fc2"]], wfc1),
        ],
        lsem,
    )
    vgf[...] = jnp.zeros_like(vgf)
    vgd[...] = jnp.zeros_like(vgd)
    loads[0].wait()

    def between():
        small = acc.at[:, 0 : 3 * HW]
        qkv_grad(n1, dmix, small, sc.half)
        store_low(small, gq)
        acc[...] = jnp.zeros_like(acc)

    sc.run(lambda r0: back_tail(r0, sc.half, dmix, hf, e2_in, wqkv, vec1, part, vgf), between)
    grad_out(sc, cot, 0, hf, vec1, dh_ref, dhf, sc.t * 2 * sc.half, lambda h: start_half(ga, h))
    for c in loads[1:]:
        c.wait()
    ga.run(lambda r0: back_head(r0, ga.half, dhf, xf, g, gp, n2, o, wfc1, wfc2, wout, vec0, do, e2, da, acc, vgd))
    column_sum(dh_ref, 0, dh_ref.shape[0], vgd, 2)
    store_low(acc, gr)
    sc.finish()


def layer_back(col, ff, dmix, e2, cot, hf, n1, wf, vec1, vec0, xf, g, gp, n2, o):
    seq, model = hf.shape
    return pl.pallas_call(
        functools.partial(back_kernel, col),
        out_shape=(
            sds(cot.shape, BF),
            sds((seq, model), BF),
            sds((model, 3 * HW), BF),
            sds((8, model), F32),
            sds((seq, HW), BF),
            sds((seq, model), BF),
            sds((model, 2 * ff + HW), BF),
            sds((8, model), F32),
        ),
        in_specs=[VMEM] * 5 + [ANY] + [VMEM] * 7,
        out_specs=(VMEM,) * 8,
        scratch_shapes=[
            pltpu.VMEM((model, 3 * HW), BF),
            pltpu.VMEM((model, HW), BF),
            pltpu.VMEM((model, ff), BF),
            pltpu.VMEM((model, ff), BF),
            pltpu.VMEM((seq // 8, ff), BF),
            pltpu.VMEM((model, 2 * ff + HW), F32),
        ]
        + scatter_scratch(seq, model)
        + [DMA((6,)), DMA((6,)), DMA((4,))],
        compiler_params=params(5, 63),
        name="layer_back",
    )(dmix, e2, cot, hf, n1, wf, vec1, vec0, xf, g, gp, n2, o)


def last_kernel(
    col, dmix, e2_in, dh, xf, n1, wf, vec0, dx_ref, gq, vgf,
    wqkv, acc, part, r1x, r1y, r2x, r2y, sss, srs, lsem,
):
    greet(neighbours())
    sc = Scatter(part, r1x, r1y, r2x, r2y, sss, srs)
    loads = load([(wf.at[0, :, col["qkv"] : col["fc1"]], wqkv)], lsem)
    vgf[...] = jnp.zeros_like(vgf)
    loads[0].wait()

    def between():
        qkv_grad(n1, dmix, acc, sc.half)
        store_low(acc, gq)

    sc.run(lambda r0: back_tail(r0, sc.half, dmix, xf, e2_in, wqkv, vec0, part, vgf), between)
    grad_out(sc, dh, 0, xf, vec0, dx_ref)
    sc.finish()


def layer_last(col, dmix, e2, dh, xf, n1, wf, vec0):
    seq, model = xf.shape
    return pl.pallas_call(
        functools.partial(last_kernel, col),
        out_shape=(sds(dh.shape, BF), sds((model, 3 * HW), BF), sds((8, model), F32)),
        in_specs=[VMEM] * 5 + [ANY] + [VMEM],
        out_specs=(VMEM,) * 3,
        scratch_shapes=[pltpu.VMEM((model, 3 * HW), BF), pltpu.VMEM((model, 3 * HW), F32)]
        + scatter_scratch(seq, model)
        + [DMA((1,))],
        compiler_params=params(6),
        name="layer_last",
    )(dmix, e2, dh, xf, n1, wf, vec0)


def reduce_kernel(
    dp, tensor, gq0, gr0, gq1, gr1, vf0, vd0, vf1, vd1, out, vout,
    rq, rr, sb, rb, va, vr, vb, gss, grs, pss, prs, vss, vrs,
):
    s, z, t = lax.axis_index("section"), lax.axis_index("dp"), lax.axis_index("tensor")
    mate = {"section": 1 - s}
    ring = [{"dp": (z + d) % dp} for d in range(1, dp)]
    group = [{"tensor": (t + d) % tensor} for d in range(1, tensor)]
    greet([mate] + ring + group)
    rows = out.shape[0]
    nq = gq0.shape[1]

    def swap(q, r):
        return [push(q, rq, gss.at[0], grs.at[0], mate), push(r, rr, gss.at[1], grs.at[1], mate)]

    @pl.when(s == 0)
    def _():
        for c in swap(gq1, gr1):
            c.start()

    @pl.when(s == 1)
    def _():
        for c in swap(gq0, gr0):
            c.start()

    va[0, 0:8, :] = vf0[...] + vd0[...]
    va[0, 8:16, :] = vf1[...] + vd1[...]
    for c in swap(gq0, gr0):
        c.wait_recv()
    vsend = [push(va.at[0], vr.at[0], vss.at[0], vrs.at[0], mate)]
    vsend[0].start()
    sends = [push(sb.at[d], rb.at[d], pss.at[d], prs.at[d], peer) for d, peer in enumerate(ring)]

    def own_sum(zz, write):
        def body(i, _):
            src = ds(zz * rows + i * 16, 16)
            mine = lax.select(s == 0, gq0[src, :].astype(F32), gq1[src, :].astype(F32))
            write(i, 0, nq, mine + rq[src, :].astype(F32))
            mine = lax.select(s == 0, gr0[src, :].astype(F32), gr1[src, :].astype(F32))
            write(i, nq, out.shape[1], mine + rr[src, :].astype(F32))
            return 0

        lax.fori_loop(0, rows // 16, body, 0)

    for d in range(dp - 1):

        def write(i, a, b, value, d=d):
            sb[d, ds(i * 16, 16), a:b] = value.astype(BF)

        own_sum((z + d + 1) % dp, write)
        sends[d].start()
        if d == 0:
            vsend[0].wait_recv()
            va[1] = va[0] + vr[0]
    first = [push(va.at[1], vr.at[1 + d], vss.at[1 + d], vrs.at[1 + d], peer) for d, peer in enumerate(ring)]
    for c in first:
        c.start()

    def write_own(i, a, b, value):
        out[ds(i * 16, 16), a:b] = value

    own_sum(z, write_own)
    total = va[1]
    for d, c in enumerate(first):
        c.wait_recv()
        total = total + vr[1 + d]
    va[2] = total
    for d in range(dp - 1):
        sends[d].wait_recv()

        def add(i, _, d=d):
            rr_ = ds(i * 16, 16)
            out[rr_, :] += rb[d, rr_, :].astype(F32)
            return 0

        lax.fori_loop(0, rows // 16, add, 0)
        if d == 0:
            second = []
            for e, peer in enumerate(group):
                i = dp + e
                second.append(push(va.at[2], vr.at[i], vss.at[i], vrs.at[i], peer))
                second[-1].start()
    extra = jnp.zeros_like(total)
    for e, c in enumerate(second):
        c.wait_recv()
        extra = extra + vr[dp + e]
    row = lax.broadcasted_iota(jnp.int32, total.shape, 0)
    vout[...] = total + jnp.where(row % 8 < 6, extra, 0.0)
    for c in swap(gq0, gr0) + vsend + first + second + sends:
        c.wait_send()


def reduce_all(dp, tensor, gq0, gr0, gq1, gr1, vf0, vd0, vf1, vd1):
    model, nq = gq0.shape
    cols = nq + gr0.shape[1]
    rows = model // dp
    nv = dp + tensor - 1
    return pl.pallas_call(
        functools.partial(reduce_kernel, dp, tensor),
        out_shape=(sds((rows, cols), F32), sds((16, model), F32)),
        in_specs=[VMEM] * 8,
        out_specs=(VMEM, VMEM),
        scratch_shapes=[
            pltpu.VMEM(gq0.shape, BF),
            pltpu.VMEM(gr0.shape, BF),
            pltpu.VMEM((dp - 1, rows, cols), BF),
            pltpu.VMEM((dp - 1, rows, cols), BF),
            pltpu.VMEM((3, 16, model), F32),
            pltpu.VMEM((nv, 16, model), F32),
            pltpu.VMEM((8, 128), F32),
            DMA((2,)),
            DMA((2,)),
            DMA((dp - 1,)),
            DMA((dp - 1,)),
            DMA((nv,)),
            DMA((nv,)),
        ],
        compiler_params=params(7),
        name="reduce_grads",
    )(gq0, gr0, gq1, gr1, vf0, vd0, vf1, vd1)


def attention_plan(seg, live):
    seq = seg.shape[0]
    counter = jnp.arange(seq, dtype=jnp.int32)
    before = [jnp.sum((seg == v).astype(jnp.int32)) for v in range(3)]
    start = sum(jnp.where(seg > v, before[v], 0) for v in range(3))
    kc = jnp.where(counter < live * LIVE, seg, -1)
    lo = start[::QB] // QB
    hi = jnp.minimum(jnp.arange(seq // QB, dtype=jnp.int32), (live * LIVE + QB - 1) // QB)
    bounds = jnp.stack([jnp.minimum(lo, hi), hi]).astype(jnp.int32)
    return bounds, (counter - start)[None, :], seg[None, :], kc[:, None]


def by_part(w):
    rows = w.shape[0]
    heads = w.shape[1] // (3 * HD)
    w = w.reshape(rows, heads, 3, HD).transpose(0, 2, 1, 3).reshape(rows, 3, heads * HD)
    return jnp.pad(w, ((0, 0), (0, 0), (0, HW - heads * HD))).reshape(rows, 3 * HW)


def by_head(w, heads):
    rows = w.shape[0]
    w = w.reshape(rows, 3, HW)[:, :, : heads * HD].reshape(rows, 3, heads, HD)
    return w.transpose(0, 2, 1, 3).reshape(rows, heads * 3 * HD)


def shards(
    dp, tensor, inputs, cotangent, segments, live_blocks, ln1_gain, ln1_bias, qkv_weight, qkv_bias,
    out_weight, out_bias, ln2_gain, ln2_bias, fc1_weight, fc1_bias, fc2_weight, fc2_bias,
):
    s, z, t = lax.axis_index("section"), lax.axis_index("dp"), lax.axis_index("tensor")
    model = inputs.shape[-1]
    ff = fc1_weight.shape[2]
    heads = qkv_bias.shape[1]
    col = columns(model, ff)

    def mine(a):
        return lax.dynamic_index_in_dim(a, s, 0, keepdims=False)[0]

    x, cot, seg, live = mine(inputs), mine(cotangent), mine(segments), mine(live_blocks)
    bounds, pos, sr, kc = attention_plan(seg, live)
    wout = jnp.pad(out_weight[0].T, ((0, 0), (0, HW - heads * HD)))
    w = jnp.concatenate([by_part(qkv_weight[0]), fc1_weight[0], fc2_weight[0].T, wout], axis=1)
    small = jnp.stack([ln1_gain[0], ln1_bias[0], out_bias[0], ln2_gain[0], ln2_bias[0], fc2_bias[0]])
    own = small.shape[1]

    def lanes(a):
        return jnp.pad(a.astype(F32), ((0, 0), (0, 128 - a.shape[1])))

    sv = jnp.concatenate([lanes(small), lanes(qkv_bias[0]), lanes(fc1_bias[0])], axis=0)
    sv = jnp.pad(sv, ((0, -sv.shape[0] % 8), (0, 0)))
    fr = 10000.0 ** (-(jnp.arange(ROT // 2, dtype=F32) * (2.0 / ROT)))
    fr = jnp.broadcast_to(fr[:, None], (ROT // 2, 128))
    wf, vecs, tab = gather_all(dp, tensor, w, sv, pos, fr)
    wide = vecs[..., :6, :own].transpose(0, 3, 2, 1, 4).reshape(2, 6, model)
    here = lax.dynamic_index_in_dim(vecs, t, 1, keepdims=False)
    qw, fw = qkv_bias.shape[2], fc1_bias.shape[2]
    qb = here[:, :, 6 : 6 + heads, :qw].transpose(0, 2, 1, 3).reshape(2, heads * 3 * HD)
    fb = here[:, :, 6 + heads : 6 + 2 * heads, :fw].transpose(0, 2, 1, 3).reshape(2, 1, ff)
    vec = jnp.concatenate([wide, by_part(qb)[:, None], fb], axis=1)
    v0, v1 = vec[0], vec[1]

    xf, n1a, n2a, qa, ka, va, ga, gpa = layer_in(col, ff, x, wf, v0, tab)
    oa, lsea = attn_fwd(heads, bounds, qa, ka, va, sr, kc)
    h, hf, n1b, n2b, qb_, kb, vb, gb, gpb = layer_mid(col, ff, oa, ga, x, wf, v0, v1, tab)
    ob, lseb = attn_fwd(heads, bounds, qb_, kb, vb, sr, kc)
    y, dyf, dob, e2b, grb, vdb = layer_turn(col, ff, ob, gb, h, hf, cot, wf, v1, n2b, gpb)
    dmb = attn_bwd(heads, bounds, qb_, kb, vb, ob, dob, lseb, sr, kc, tab)
    dh, dhf, gqb, vfb, doa, e2a, gra, vda = layer_back(
        col, ff, dmb, e2b, cot, hf, n1b, wf, v1, v0, xf, ga, gpa, n2a, oa
    )
    dma = attn_bwd(heads, bounds, qa, ka, va, oa, doa, lsea, sr, kc, tab)
    dx, gqa, vfa = layer_last(col, dma, e2a, dh, xf, n1a, wf, v0)
    gw, gv = reduce_all(dp, tensor, gqa, gra, gqb, grb, vfa, vda, vfb, vdb)

    first = s == 0

    def swapped(a0, a1):
        got = lax.ppermute(jnp.where(first, a1, a0), "section", [(0, 1), (1, 0)])
        keep = jnp.where(first, a0, a1)
        return jnp.stack([jnp.where(first, keep, got), jnp.where(first, got, keep)])[None, :, None]

    section_outputs = swapped(h, y)
    input_grads = swapped(dx, dh)
    gv = lax.dynamic_index_in_dim(gv.reshape(2, 8, model), s, 0, keepdims=False)
    short = lax.dynamic_slice_in_dim(gv[:6], (z * tensor + t) * own, own, 1)
    gqb_ = by_head(gv[6:7], heads).reshape(heads, 3 * HD)
    gqb_ = lax.dynamic_slice_in_dim(gqb_, z * qw, qw, 1)[None]
    gfb = lax.dynamic_slice_in_dim(gv[7].reshape(heads, ff // heads), z * fw, fw, 1)[None]
    gqkv = by_head(gw[:, : col["fc1"]], heads)[None]
    gfc1 = gw[:, col["fc1"] : col["fc2"]][None]
    gfc2 = gw[:, col["fc2"] : col["out"]].T[None]
    gout = gw[:, col["out"] : col["out"] + heads * HD].T[None]
    return (
        section_outputs,
        input_grads,
        short[0:1],
        short[1:2],
        gqkv,
        gqb_,
        gout,
        short[2:3],
        short[3:4],
        short[4:5],
        gfc1,
        gfb,
        gfc2,
        short[2:3],
    )


def solution(mesh):
    both = ("dp", "tensor")
    in_specs = (
        P(None, "dp", "tensor", None),
        P(None, "dp", "tensor", None),
        P(None, "dp", None),
        P(None, "dp"),
        P("section", both),
        P("section", both),
        P("section", "dp", "tensor"),
        P("section", "tensor", "dp"),
        P("section", "tensor", "dp"),
        P("section", both),
        P("section", both),
        P("section", both),
        P("section", "dp", "tensor"),
        P("section", "tensor", "dp"),
        P("section", "tensor", "dp"),
        P("section", both),
    )
    out_specs = (
        P("section", None, "dp", "tensor", None),
        P("section", None, "dp", "tensor", None),
        P("section", both),
        P("section", both),
        P("section", "dp", "tensor"),
        P("section", "tensor", "dp"),
        P("section", "tensor", "dp"),
        P("section", both),
        P("section", both),
        P("section", both),
        P("section", "dp", "tensor"),
        P("section", "tensor", "dp"),
        P("section", "tensor", "dp"),
        P("section", both),
    )
    body = functools.partial(shards, mesh.shape["dp"], mesh.shape["tensor"])
    return jax.shard_map(body, mesh=mesh, in_specs=in_specs, out_specs=out_specs, check_vma=False)
```

```python
import functools

import jax
import jax.numpy as jnp
from jax import lax
from jax.experimental import pallas as pl
from jax.experimental.pallas import tpu as pltpu
from jax.sharding import PartitionSpec as P

F32 = jnp.float32
BF = jnp.bfloat16
MESH = pl.DeviceIdType.MESH
HD = 64
ROT = 16
LIVE = 128
QB = 256
HW = 256
SUB = 64
EPS = 1e-05
NEG = -1e30
VMEM = pl.BlockSpec(memory_space=pltpu.VMEM)
ANY = pl.BlockSpec(memory_space=pl.ANY)
SMEM = pl.BlockSpec(memory_space=pltpu.SMEM)
DMA = pltpu.SemaphoreType.DMA


def sds(shape, dtype):
    return jax.ShapeDtypeStruct(shape, dtype)


def dg(a, b, ca, cb):
    return lax.dot_general(a, b, (((ca,), (cb,)), ((), ())), preferred_element_type=F32)


def dot(a, b):
    return jnp.dot(a, b, preferred_element_type=F32)


def ds(start, size):
    return pl.ds(pl.multiple_of(start, size), size)


def norm_stats(x):
    mu = jnp.mean(x, axis=-1, keepdims=True)
    xc = x - mu
    var = jnp.mean(xc * xc, axis=-1, keepdims=True)
    return xc, lax.rsqrt(var + EPS)


def head_lanes(width, heads):
    lane = lax.broadcasted_iota(jnp.int32, (1, width), 1)
    return [(lane >= h * HD) & (lane < (h + 1) * HD) for h in range(heads)]


def allow_mask(kc, sq, diag):
    m = kc == sq
    if diag:
        r = lax.broadcasted_iota(jnp.int32, (QB, QB), 0)
        c = lax.broadcasted_iota(jnp.int32, (QB, QB), 1)
        m = (m & (r <= c)) | (r == c)
    return m


def attn_fwd_kernel(heads, b_ref, q_ref, k_ref, v_ref, sr_ref, kc_ref, o_ref, lse_ref, vt, s_scr):
    n = q_ref.shape[0] // QB
    width = q_ref.shape[1]
    hm = head_lanes(width, heads)

    def turn(i, _):
        vt[:, ds(i * QB, QB)] = v_ref[ds(i * QB, QB), :].T
        return 0

    lax.fori_loop(0, n, turn, 0)

    def qloop(i, _):
        qi = ds(i * QB, QB)
        q = q_ref[qi, :]
        qm = [jnp.where(hm[h], q, jnp.zeros_like(q)) for h in range(heads)]
        sq = sr_ref[0:1, qi]
        lo = b_ref[0, i]
        hi = b_ref[1, i]

        def scores(j, slot, ms, diag):
            kj = ds(j * QB, QB)
            k = k_ref[kj, :]
            mask = allow_mask(kc_ref[kj, 0:1], sq, diag)
            out = []
            for h in range(heads):
                s = jnp.where(mask, dg(k, qm[h], 1, 1), NEG)
                s_scr[h, ds(slot * QB, QB), :] = s
                out.append(jnp.maximum(ms[h], jnp.max(s, axis=0, keepdims=True)))
            return tuple(out)

        ms = tuple(jnp.full((1, QB), NEG, F32) for _ in range(heads))
        ms = scores(i, 0, ms, True)
        ms = lax.fori_loop(lo, hi, lambda j, ms: scores(j, j - lo + 1, ms, False), ms)

        def weigh(j, slot, st):
            kj = ds(j * QB, QB)
            out = []
            for h in range(heads):
                total, acc = st[h]
                p = jnp.exp(s_scr[h, ds(slot * QB, QB), :] - ms[h])
                total = total + jnp.sum(p, axis=0, keepdims=True)
                acc = acc + dot(vt[h * HD : (h + 1) * HD, kj], p.astype(BF))
                out.append((total, acc))
            return tuple(out)

        st = tuple((jnp.zeros((1, QB), F32), jnp.zeros((HD, QB), F32)) for _ in range(heads))
        st = weigh(i, 0, st)
        st = lax.fori_loop(lo, hi, lambda j, st: weigh(j, j - lo + 1, st), st)
        ot = [st[h][1] * (1.0 / st[h][0]) for h in range(heads)]
        ot = jnp.concatenate(ot + [jnp.zeros((width - heads * HD, QB), F32)], axis=0)
        o_ref[qi, :] = ot.T.astype(BF)
        lse = [ms[h] + jnp.log(st[h][0]) for h in range(heads)]
        lse_ref[:, qi] = jnp.concatenate(lse + [jnp.zeros((8 - heads, QB), F32)], axis=0)
        return 0

    lax.fori_loop(0, n, qloop, 0)


def attn_fwd(heads, bounds, q, k, v, sr, kc):
    rows, width = q.shape
    return pl.pallas_call(
        functools.partial(attn_fwd_kernel, heads),
        out_shape=(sds((rows, width), BF), sds((8, rows), F32)),
        in_specs=[SMEM] + [VMEM] * 5,
        out_specs=(VMEM, VMEM),
        scratch_shapes=[pltpu.VMEM((width, rows), BF), pltpu.VMEM((heads, rows + QB, QB), F32)],
        compiler_params=pltpu.CompilerParams(vmem_limit_bytes=40 << 20),
        cost_estimate=cost(15),
        name="attn_fwd",
    )(bounds, q, k, v, sr, kc)


def turn_lanes(x, tab, sign):
    width = x.shape[1]
    c, sn = [jnp.concatenate([tab[:, a * 128 : (a + 1) * 128]] * (width // 128), axis=1) for a in range(2)]
    lane = lax.broadcasted_iota(jnp.int32, (1, width), 1) % HD
    moved = jnp.where(lane < ROT // 2, pltpu.roll(x, width - ROT // 2, 1), pltpu.roll(x, ROT // 2, 1)) * sn
    return x * c + moved if sign > 0 else x * c - moved


def attn_bwd_kernel(
    heads, b_ref, q_ref, k_ref, v_ref, o_ref, do_ref, lse_ref, sr_ref, kc_ref, tab_ref, out_ref, kt, dk, dv
):
    rows, width = q_ref.shape
    n = rows // QB
    hm = head_lanes(width, heads)

    def turn(i, _):
        kt[:, ds(i * QB, QB)] = k_ref[ds(i * QB, QB), :].T
        return 0

    lax.fori_loop(0, n, turn, 0)
    dk[...] = jnp.zeros_like(dk)
    dv[...] = jnp.zeros_like(dv)
    rowid = lax.broadcasted_iota(jnp.int32, (8, width), 0)
    lane = lax.broadcasted_iota(jnp.int32, (8, width), 1)
    sel = ((lane >= rowid * HD) & (lane < (rowid + 1) * HD)).astype(F32).astype(BF)

    def qloop(i, _):
        qi = ds(i * QB, QB)
        q = q_ref[qi, :]
        do = do_ref[qi, :]
        z = jnp.zeros_like(q)
        qm = [jnp.where(hm[h], q, z) for h in range(heads)]
        dom = [jnp.where(hm[h], do, z) for h in range(heads)]
        qcat = jnp.concatenate(qm, axis=0)
        docat = jnp.concatenate(dom, axis=0)
        prod = do.astype(F32) * o_ref[qi, :].astype(F32)
        high = prod.astype(BF)
        low = (prod - high.astype(F32)).astype(BF)
        delta = dg(sel, high, 1, 1) + dg(sel, low, 1, 1)
        lse = lse_ref[:, qi]
        sq = sr_ref[0:1, qi]
        lo = b_ref[0, i]
        hi = b_ref[1, i]

        def step(j, dqs, diag):
            kj = ds(j * QB, QB)
            k = k_ref[kj, :]
            v = v_ref[kj, :]
            mask = allow_mask(kc_ref[kj, 0:1], sq, diag)
            ps, dss, out = [], [], []
            for h in range(heads):
                s = dg(k, qm[h], 1, 1)
                dp = dg(v, dom[h], 1, 1)
                p = jnp.where(mask, jnp.exp(jnp.where(mask, s - lse[h : h + 1, :], 0.0)), 0.0)
                score_grad = (p * (dp - delta[h : h + 1, :])).astype(BF)
                ps.append(p.astype(BF))
                dss.append(score_grad)
                out.append(dqs[h] + dot(kt[h * HD : (h + 1) * HD, kj], score_grad))
            dv[kj, :] += dot(jnp.concatenate(ps, axis=1), docat)
            dk[kj, :] += dot(jnp.concatenate(dss, axis=1), qcat)
            return tuple(out)

        dqs = tuple(jnp.zeros((HD, QB), F32) for _ in range(heads))
        dqs = step(i, dqs, True)
        dqs = lax.fori_loop(lo, hi, lambda j, d: step(j, d, False), dqs)
        dq = jnp.concatenate(list(dqs) + [jnp.zeros((width - heads * HD, QB), F32)], axis=0).T * 0.125
        out_ref[qi, 0:width] = turn_lanes(dq, tab_ref[qi, :], -1).astype(BF)
        return 0

    lax.fori_loop(0, n, qloop, 0)

    def finish(i, _):
        ii = ds(i * QB, QB)
        out_ref[ii, width : 2 * width] = turn_lanes(dk[ii, :], tab_ref[ii, :], -1).astype(BF)
        out_ref[ii, 2 * width : 3 * width] = dv[ii, :].astype(BF)
        return 0

    lax.fori_loop(0, n, finish, 0)


def attn_bwd(heads, bounds, q, k, v, o, do, lse, sr, kc, tab):
    rows, width = q.shape
    return pl.pallas_call(
        functools.partial(attn_bwd_kernel, heads),
        out_shape=sds((rows, 3 * width), BF),
        in_specs=[SMEM] + [VMEM] * 9,
        out_specs=VMEM,
        scratch_shapes=[
            pltpu.VMEM((width, rows), BF),
            pltpu.VMEM((rows, width), F32),
            pltpu.VMEM((rows, width), F32),
        ],
        compiler_params=pltpu.CompilerParams(vmem_limit_bytes=50 << 20),
        cost_estimate=cost(35),
        name="attn_bwd",
    )(bounds, q, k, v, o, do, lse, sr, kc, tab)


def places():
    t = lax.axis_index("tensor")
    x, y = t % 2, t // 2
    return t, 2 * y + (1 - x), 2 * (1 - y) + x, 3 - t


def greet(peers):
    bar = pltpu.get_barrier_semaphore()
    for peer in peers:
        pl.semaphore_signal(bar, inc=1, device_id=peer, device_id_type=MESH)
    pl.semaphore_wait(bar, len(peers))


def push(src, dst, ssem, rsem, peer):
    return pltpu.make_async_remote_copy(
        src_ref=src, dst_ref=dst, send_sem=ssem, recv_sem=rsem, device_id=peer, device_id_type=MESH
    )


def pick(i, values):
    out = values[-1]
    for n in range(len(values) - 2, -1, -1):
        out = jnp.where(i == n, values[n], out)
    return out


class Gather:
    def __init__(self, full, ssem, rsem):
        self.t, self.px, self.py, self.pd = places()
        self.full, self.ssem, self.rsem = full, ssem, rsem
        self.half = full.shape[0] // 8

    def rows(self, c, h):
        return ds((2 * c + h) * self.half, self.half)

    def copy(self, i, c, h, peer):
        ref = self.full.at[self.rows(c, h)]
        return push(ref, ref, self.ssem.at[i], self.rsem.at[i], {"tensor": peer})

    def plan(self, i):
        t, px, py = self.t, self.px, self.py
        c, h, peer = [(t, 0, px), (t, 1, py), (t, 1, px), (t, 0, py), (px, 0, py), (py, 1, px)][i]
        return self.copy(i, c, h, peer)

    def order(self, i):
        t, px, py, pd = self.t, self.px, self.py, self.pd
        return pick(i, [t, t, px, py, px, py, pd, pd]), pick(i, [0, 1, 0, 1, 1, 0, 0, 1])

    def arrive(self, i):
        @pl.when(i == 2)
        def _():
            self.plan(0).wait_recv()
            self.plan(4).start()
            self.plan(1).wait_recv()
            self.plan(5).start()

        for step in (4, 5, 6, 7):

            @pl.when(i == step)
            def _(step=step):
                self.plan(step - 2).wait_recv()

    def finish(self):
        for i in range(6):
            self.plan(i).wait_send()

    def run(self, work):
        def body(i, _):
            self.arrive(i)
            c, h = self.order(i)
            work((2 * c + h) * self.half, i)
            return 0

        lax.fori_loop(0, 8, body, 0)
        self.finish()


class Scatter:
    def __init__(self, part, r1x, r1y, r2x, r2y, ssem, rsem):
        self.t, self.px, self.py, self.pd = places()
        self.part, self.r1x, self.r1y, self.r2x, self.r2y = part, r1x, r1y, r2x, r2y
        self.ssem, self.rsem = ssem, rsem
        self.half = part.shape[0] // 8

    def rows(self, c, h):
        return ds((2 * c + h) * self.half, self.half)

    def copy(self, i, c, h, dst, peer):
        return push(self.part.at[self.rows(c, h)], dst, self.ssem.at[i], self.rsem.at[i], {"tensor": peer})

    def plan(self, i):
        px, py, pd = self.px, self.py, self.pd
        c, h, dst, peer = [
            (pd, 0, self.r1x.at[1], px),
            (pd, 1, self.r1y.at[1], py),
            (px, 0, self.r1x.at[0], px),
            (py, 1, self.r1y.at[0], py),
            (py, 0, self.r2y, py),
            (px, 1, self.r2x, px),
        ][i]
        return self.copy(i, c, h, dst, peer)

    def run(self, work, early=None):
        t, px, py, pd = self.t, self.px, self.py, self.pd

        def body(i, _):
            c = pick(i, [pd, pd, px, py, py, px, t, t])
            h = pick(i, [0, 1, 0, 1, 0, 1, 0, 1])
            work((2 * c + h) * self.half)
            for step in range(4):

                @pl.when(i == step)
                def _(step=step):
                    self.plan(step).start()

            return 0

        lax.fori_loop(0, 8, body, 0)
        if early is not None:
            early()
        for first, c, h, buf, second in ((0, py, 0, self.r1x, 4), (1, px, 1, self.r1y, 5)):
            self.plan(first).wait_recv()

            def add(i, _, c=c, h=h, buf=buf):
                rr = ds((2 * c + h) * self.half + i * SUB, SUB)
                got = buf[1, ds(i * SUB, SUB), :].astype(F32)
                self.part[rr, :] = (self.part[rr, :].astype(F32) + got).astype(BF)
                return 0

            lax.fori_loop(0, self.half // SUB, add, 0)
            self.plan(second).start()

    def arrive(self, h):
        for i in (2, 4) if h == 0 else (3, 5):
            self.plan(i).wait_recv()

    def total(self, h, i):
        near, far = (self.r1x, self.r2y) if h == 0 else (self.r1y, self.r2x)
        rr = ds((2 * self.t + h) * self.half + i * SUB, SUB)
        sub = ds(i * SUB, SUB)
        return self.part[rr, :].astype(F32) + near[0, sub, :].astype(F32) + far[sub, :].astype(F32)

    def finish(self):
        for i in range(6):
            self.plan(i).wait_send()


def scatter_scratch(rows, width):
    half = rows // 8
    return [
        pltpu.VMEM((rows, width), BF),
        pltpu.VMEM((2, half, width), BF),
        pltpu.VMEM((2, half, width), BF),
        pltpu.VMEM((half, width), BF),
        pltpu.VMEM((half, width), BF),
        DMA((6,)),
        DMA((6,)),
    ]


class Mesh:
    def __init__(self, dp, tensor):
        self.dp, self.tensor = dp, tensor
        self.s, self.z, self.t = lax.axis_index("section"), lax.axis_index("dp"), lax.axis_index("tensor")
        self.mate = {"section": 1 - self.s}
        self.ring = [{"dp": (self.z + d) % dp} for d in range(1, dp)]
        self.group = [{"tensor": (self.t + d) % tensor} for d in range(1, tensor)]


class WeightGather:
    def __init__(self, me, layer, shard, full, groups, sems):
        self.me, self.layer, self.shard, self.full, self.groups = me, layer, shard, full, groups
        self.own, self.wss, self.wrs, self.fss, self.frs = sems
        self.rows = shard.shape[0]

    def block(self, zz, g):
        a, b = self.groups[g]
        return self.full.at[ds(zz * self.rows, self.rows), a:b]

    def mine(self, g):
        a, b = self.groups[g]
        return self.shard.at[:, a:b]

    def local(self, g):
        return pltpu.make_async_copy(self.mine(g), self.block(self.me.z, g), self.own.at[g])

    def out(self, g, d):
        return push(self.mine(g), self.block(self.me.z, g), self.wss.at[g, d], self.wrs.at[g, d], self.me.ring[d])

    def hand(self, g, d):
        zz = (self.me.z + self.me.dp - d) % self.me.dp
        src = self.mine(g) if d == 0 else self.block(zz, g)
        return push(src, self.block(zz, g), self.fss.at[g, d], self.frs.at[g, d], self.me.mate)

    def send(self):
        @pl.when(self.me.s == self.layer)
        def _():
            for g in range(len(self.groups)):
                for d in range(self.me.dp - 1):
                    self.out(g, d).start()
                self.hand(g, 0).start()
                self.local(g).start()

    def wait(self, g):
        @pl.when(self.me.s == self.layer)
        def _():
            for d in range(self.me.dp - 1):
                self.out(g, d).wait_recv()
                self.hand(g, d + 1).start()
            self.local(g).wait()

        @pl.when(self.me.s != self.layer)
        def _():
            for d in range(self.me.dp):
                self.hand(g, d).wait_recv()

    def finish(self):
        @pl.when(self.me.s == self.layer)
        def _():
            for g in range(len(self.groups)):
                for d in range(self.me.dp - 1):
                    self.out(g, d).wait_send()
                for d in range(self.me.dp):
                    self.hand(g, d).wait_send()

    @staticmethod
    def scratch(dp, n):
        return [DMA((n,)), DMA((n, dp - 1)), DMA((n, dp - 1)), DMA((n, dp)), DMA((n, dp))]


class GradReduce:
    def __init__(self, me, layer, grad, got, sb, own, hand_sems, rb=None, ring_sems=None):
        self.me, self.layer, self.grad, self.got, self.sb, self.own = me, layer, grad, got, sb, own
        self.hss, self.hrs = hand_sems
        self.rb, self.ring_sems = rb, ring_sems
        self.rows = own.shape[0]

    def hand(self, src=None):
        return push(self.grad if src is None else src, self.got, self.hss, self.hrs, self.me.mate)

    def send(self, src=None):
        @pl.when(self.me.s != self.layer)
        def _():
            self.hand(src).start()

    def out(self, d):
        pss, prs = self.ring_sems
        return push(self.sb.at[d], self.rb.at[d], pss.at[d], prs.at[d], self.me.ring[d])

    def blocks(self, zz, write):
        def body(i, _):
            rr = ds(zz * self.rows + i * 16, 16)
            write(ds(i * 16, 16), self.grad[rr, :].astype(F32) + self.got[rr, :].astype(F32))
            return 0

        lax.fori_loop(0, self.rows // 16, body, 0)

    def reduce(self):
        @pl.when(self.me.s == self.layer)
        def _():
            self.hand().wait_recv()
            for d in range(self.me.dp - 1):

                def write(rr, value, d=d):
                    self.sb[d, rr, :] = value.astype(BF)

                self.blocks((self.me.z + d + 1) % self.me.dp, write)
                if self.rb is not None:
                    self.out(d).start()

            def write(rr, value):
                self.own[rr, :] = value

            self.blocks(self.me.z, write)

    def collect(self):
        @pl.when(self.me.s == self.layer)
        def _():
            for d in range(self.me.dp - 1):
                self.out(d).wait_recv()

                def add(i, _, d=d):
                    rr = ds(i * 16, 16)
                    self.own[rr, :] += self.rb[d, rr, :].astype(F32)
                    return 0

                lax.fori_loop(0, self.rows // 16, add, 0)
            for d in range(self.me.dp - 1):
                self.out(d).wait_send()

    def finish(self, src=None):
        @pl.when(self.me.s != self.layer)
        def _():
            self.hand(src).wait_send()


class VectorGather:
    def __init__(self, me, sv, buf, ss, rs, own):
        self.me, self.sv, self.buf, self.ss, self.rs, self.own = me, sv, buf, ss, rs, own

    def local(self):
        me = self.me
        return pltpu.make_async_copy(self.sv, self.buf.at[me.s, me.t, me.z], self.own)

    def stage(self, n):
        me = self.me
        if n == 0:
            dst = self.buf.at[me.s, me.t, me.z]
            return [push(self.sv, dst, self.ss.at[d], self.rs.at[d], peer) for d, peer in enumerate(me.ring)]
        base = me.dp - 1
        if n == 1:
            ref = self.buf.at[me.s, me.t]
            return [
                push(ref, ref, self.ss.at[base + d], self.rs.at[base + d], peer) for d, peer in enumerate(me.group)
            ]
        i = base + me.tensor - 1
        ref = self.buf.at[me.s]
        return [push(ref, ref, self.ss.at[i], self.rs.at[i], me.mate)]

    def send(self, n):
        if n == 0:
            self.local().start()
        for c in self.stage(n):
            c.start()

    def wait(self, n):
        if n == 0:
            self.local().wait()
        for c in self.stage(n):
            c.wait_recv()

    def finish(self):
        for n in range(3):
            for c in self.stage(n):
                c.wait_send()

    def build(self, vecs, heads, own, qw, fw):
        me, buf = self.me, self.buf
        for layer in range(2):
            wide = [buf[layer, tt, zz, 0:8, :][:, 0:own] for zz in range(me.dp) for tt in range(me.tensor)]
            vecs[layer, 0:8, :] = jnp.concatenate(wide, axis=1)
            here = [buf[layer, me.t, zz] for zz in range(me.dp)]
            by = [jnp.concatenate([p[6 + h : 7 + h, 0:qw] for p in here], axis=1) for h in range(heads)]
            qb = []
            for part in range(3):
                qb += [b[:, part * HD : (part + 1) * HD] for b in by] + [jnp.zeros((1, HW - heads * HD), F32)]
            vecs[layer, 6:7, :] = jnp.concatenate(qb, axis=1)
            fb = [p[6 + heads + h : 7 + heads + h, 0:fw] for h in range(heads) for p in here]
            vecs[layer, 7:8, :] = jnp.concatenate(fb, axis=1)


class VectorReduce:
    def __init__(self, me, va, vr, ss, rs):
        self.me, self.va, self.vr, self.ss, self.rs = me, va, vr, ss, rs

    def stage(self, n):
        me, va, vr, ss, rs = self.me, self.va, self.vr, self.ss, self.rs
        peers, base = [([me.mate], 0), (me.ring, 1), (me.group, me.dp)][n]
        return [push(va.at[n], vr.at[base + d], ss.at[base + d], rs.at[base + d], p) for d, p in enumerate(peers)]

    def send(self, n):
        for c in self.stage(n):
            c.start()

    def add(self, n, out):
        base = [0, 1, self.me.dp][n]
        total = jnp.zeros(self.va.shape[1:], F32)
        for d, c in enumerate(self.stage(n)):
            c.wait_recv()
            total = total + self.vr[base + d]
        if n == 2:
            row = lax.broadcasted_iota(jnp.int32, total.shape, 0)
            total = jnp.where(row % 8 < 6, total, 0.0)
        out[...] = self.va[n] + total

    def finish(self):
        for n in range(3):
            for c in self.stage(n):
                c.wait_send()


def rotary_table(pos_ref, fr_ref, tab):
    ang = fr_ref[:, 0:1] * pos_ref[...].astype(F32)
    cs, sn = jnp.cos(ang), jnp.sin(ang)
    one = jnp.ones((HD - ROT, ang.shape[1]), F32)
    tab[:, 0:128] = jnp.concatenate([cs, cs, one] * 2, axis=0).T
    tab[:, 128:256] = jnp.concatenate([-sn, sn, jnp.zeros_like(one)] * 2, axis=0).T


QKV, FC1, FC2, OUT = 0, 1, 2, 3


def columns(model, ff):
    return {"qkv": 0, "fc1": 3 * HW, "fc2": 3 * HW + ff, "out": 3 * HW + 2 * ff, "end": 3 * HW + 2 * ff + HW}


def project_qkv(r0, half, hf, wqkv, vec, tab, n1, n2, q, k, v):
    rows = ds(r0, half)

    def norm(i, _):
        rr = ds(r0 + i * SUB, SUB)
        xc, r = norm_stats(hf[rr, :].astype(F32))
        xh = xc * r
        n1[rr, :] = (xh * vec[0:1, :] + vec[1:2, :]).astype(BF)
        n2[rr, :] = (xh * vec[3:4, :] + vec[4:5, :]).astype(BF)
        return 0

    lax.fori_loop(0, half // SUB, norm, 0)
    a = n1[rows, :]
    for part, dst in enumerate((q, k, v)):
        cols = slice(part * HW, (part + 1) * HW)
        y = dot(a, wqkv[:, cols]) + vec[6:7, cols]
        if part < 2:
            y = turn_lanes(y, tab[rows, :], 1)
        if part == 0:
            y = y * 0.125
        dst[rows, :] = y.astype(BF)


def project_fc1(r0, half, wfc1, vec, n2, g, gp):
    rows = ds(r0, half)
    a = n2[rows, :]
    for b in range(wfc1.shape[1] // 256):
        cols = slice(b * 256, (b + 1) * 256)
        y = dot(a, wfc1[:, cols]) + vec[7:8, cols]
        cdf = 0.5 + 0.5 * lax.erf(y * 0.7071067811865476)
        g[rows, cols] = (y * cdf).astype(BF)
        gp[rows, cols] = (cdf + y * jnp.exp(-0.5 * y * y) * 0.3989422804014327).astype(BF)


def branch_out(r0, half, o, g, wout, wfc2, part):
    rows = ds(r0, half)
    for b in range(part.shape[1] // 256):
        cols = slice(b * 256, (b + 1) * 256)
        y = dg(o[rows, :], wout[cols, :], 1, 1) + dg(g[rows, :], wfc2[cols, :], 1, 1)
        part[rows, cols] = y.astype(BF)


def back_head(r0, half, dyf, hf, g, gp, n2, o, wfc1, wfc2, wout, vec, do, e2, da, acc, vg):
    rows = ds(r0, half)
    model, ff = wfc1.shape
    dy = dyf[rows, :]
    for b in range(ff // 256):
        cols = slice(b * 256, (b + 1) * 256)
        y = dot(dy, wfc2[:, cols]) * gp[rows, cols].astype(F32)
        low = y.astype(BF)
        da[:, cols] = low
        vg[7:8, cols] += jnp.sum(low.astype(F32), axis=0, keepdims=True)
    do[rows, :] = dot(dy, wout[...]).astype(BF)
    xc, r = norm_stats(hf[rows, :].astype(F32))
    xh = xc * r
    for b in range(model // 256):
        cols = slice(b * 256, (b + 1) * 256)
        dn = dg(da[...], wfc1[cols, :], 1, 1)
        vg[3:4, cols] += jnp.sum(dn * xh[:, cols], axis=0, keepdims=True)
        vg[4:5, cols] += jnp.sum(dn, axis=0, keepdims=True)
        e2[rows, cols] = (dn * vec[3:4, cols]).astype(BF)
    n2t = n2[rows, :].T
    dyt = dy.T
    for b in range(ff // 256):
        cols = slice(b * 256, (b + 1) * 256)
        acc[:, cols] += dot(n2t, da[:, cols])
        acc[:, ff + b * 256 : ff + (b + 1) * 256] += dot(dyt, g[rows, cols])
    acc[:, 2 * ff :] += dot(dyt, o[rows, :])


def back_tail(r0, half, dmix, hf, e2, wqkv, vec, part, vg):
    rows = ds(r0, half)
    dm = dmix[rows, :]
    vg[6:7, :] += jnp.sum(dm.astype(F32), axis=0, keepdims=True)
    xc, r = norm_stats(hf[rows, :].astype(F32))
    xh = xc * r
    for b in range(part.shape[1] // 256):
        cols = slice(b * 256, (b + 1) * 256)
        dn = dg(dm, wqkv[cols, :], 1, 1)
        vg[0:1, cols] += jnp.sum(dn * xh[:, cols], axis=0, keepdims=True)
        vg[1:2, cols] += jnp.sum(dn, axis=0, keepdims=True)
        part[rows, cols] = (dn * vec[0:1, cols] + e2[rows, cols].astype(F32)).astype(BF)


def qkv_grad(n1, dmix, acc, half):
    acc[...] = jnp.zeros_like(acc)

    def body(i, _):
        rows = ds(i * half, half)
        n1t = n1[rows, :].T
        for b in range(3):
            cols = slice(b * HW, (b + 1) * HW)
            acc[:, cols] += dot(n1t, dmix[rows, cols])
        return 0

    lax.fori_loop(0, n1.shape[0] // half, body, 0)


def store_low(acc, out):
    def body(i, _):
        rr = ds(i * SUB, SUB)
        out[rr, :] = acc[rr, :].astype(BF)
        return 0

    lax.fori_loop(0, acc.shape[0] // SUB, body, 0)


def residual_out(sc, own, off, vec, dst, dst2=None, dst2_off=None, after=None):
    for h in range(2):
        sc.arrive(h)

        def body(i, _, h=h):
            rr = ds(h * sc.half + i * SUB, SUB)
            base = own[ds(off + h * sc.half + i * SUB, SUB), :].astype(F32)
            y = (base + sc.total(h, i) + vec[2:3, :] + vec[5:6, :]).astype(BF)
            dst[rr, :] = y
            if dst2 is not None:
                dst2[ds(dst2_off + h * sc.half + i * SUB, SUB), :] = y
            return 0

        lax.fori_loop(0, sc.half // SUB, body, 0)
        if after is not None:
            after(h)


def grad_out(sc, dy, dy_off, hf, vec, dst, dst2=None, dst2_off=None, after=None):
    base = sc.t * 2 * sc.half
    for h in range(2):
        sc.arrive(h)

        def body(i, _, h=h):
            off = h * sc.half + i * SUB
            xc, r = norm_stats(hf[ds(base + off, SUB), :].astype(F32))
            xh = xc * r
            e = sc.total(h, i)
            m1 = jnp.mean(e, axis=-1, keepdims=True)
            m2 = jnp.mean(e * xh, axis=-1, keepdims=True)
            du = dy[ds(dy_off + off, SUB), :].astype(F32) + r * (e - m1 - xh * m2)
            low = du.astype(BF)
            dst[ds(off, SUB), :] = low
            if dst2 is not None:
                dst2[ds(dst2_off + off, SUB), :] = low
            return 0

        lax.fori_loop(0, sc.half // SUB, body, 0)
        if after is not None:
            after(h)


def start_half(ga, h):
    for i in (0, 3) if h == 0 else (1, 2):
        ga.plan(i).start()


def column_sum(ref, off, count, vg, row):
    def body(i, acc):
        return acc + jnp.sum(ref[ds(off + i * SUB, SUB), :].astype(F32), axis=0, keepdims=True)

    vg[row : row + 1, :] = lax.fori_loop(0, count // SUB, body, jnp.zeros((1, ref.shape[1]), F32))


def load(pairs, sem):
    copies = [pltpu.make_async_copy(a, b, sem.at[i]) for i, (a, b) in enumerate(pairs)]
    for c in copies:
        c.start()
    return copies


def params(cid, mib=58):
    return pltpu.CompilerParams(collective_id=cid, has_side_effects=True, vmem_limit_bytes=mib << 20)


def cost(us):
    return pl.CostEstimate(flops=int(us * 8e8), bytes_accessed=0, transcendentals=0)


def neighbours():
    t, px, py, pd = places()
    return [{"tensor": px}, {"tensor": py}]


class Stores:
    def __init__(self, pairs, half, sem):
        self.pairs, self.half, self.sem = pairs, half, sem

    def copy(self, n, r0, i):
        src, dst = self.pairs[n]
        rows = ds(r0, self.half)
        return pltpu.make_async_copy(src.at[rows], dst.at[rows], self.sem.at[n, i])

    def start(self, which, r0, i):
        for n in which:
            self.copy(n, r0, i).start()

    def finish(self):
        def body(i, _):
            for n in range(len(self.pairs)):
                self.copy(n, i * self.half, i).wait()
            return 0

        lax.fori_loop(0, 8, body, 0)


def in_kernel(
    cfg, x_ref, w_ref, sv_ref, pos_ref, fr_ref, hf_o, n1_o, n2_o, g_o, gp_o, tab_o, w_o, vecs, q, k, v,
    hf, n1, n2, g, gp, tab, wfull, vb, gss, grs, lsem, ssem, vss, vrs, *wsems,
):
    col, dp, tensor = cfg["col"], cfg["dp"], cfg["tensor"]
    me = Mesh(dp, tensor)
    greet([me.mate] + me.ring + me.group)
    ga = Gather(hf, gss, grs)
    wg = WeightGather(me, 0, w_ref, wfull, cfg["groups"], wsems)
    vg = VectorGather(me, sv_ref, vb, vss, vrs, lsem.at[1])
    st = Stores([(hf, hf_o), (n1, n1_o), (n2, n2_o), (g, g_o), (gp, gp_o)], ga.half, ssem)
    mine = pltpu.make_async_copy(x_ref, hf.at[ds(ga.t * 2 * ga.half, 2 * ga.half)], lsem.at[0])
    mine.start()
    vg.send(0)
    wg.send()
    mine.wait()
    start_half(ga, 0)
    start_half(ga, 1)
    vg.wait(0)
    vg.send(1)
    rotary_table(pos_ref, fr_ref, tab)
    vg.wait(1)
    vg.send(2)
    tab_out = pltpu.make_async_copy(tab, tab_o, lsem.at[2])
    tab_out.start()
    vg.wait(2)
    vg.build(vecs, cfg["heads"], cfg["own"], cfg["qw"], cfg["fw"])
    vec = vecs.at[0]
    wg.wait(0)

    def fc1(i):
        c, h = ga.order(i)
        r0 = (2 * c + h) * ga.half
        project_fc1(r0, ga.half, wfull.at[:, col["fc1"] : col["fc2"]], vec, n2, g, gp)
        st.start((3, 4), r0, i)

    def work(r0, i):
        project_qkv(r0, ga.half, hf, wfull.at[:, 0 : col["fc1"]], vec, tab, n1, n2, q, k, v)
        st.start((0, 1, 2), r0, i)

        @pl.when(i == 4)
        def _():
            wg.wait(1)

        @pl.when(i >= 4)
        def _():
            fc1(i - 4)

    ga.run(work)

    def late(i, _):
        fc1(i)
        return 0

    lax.fori_loop(4, 8, late, 0)
    wg.wait(2)
    w_out = pltpu.make_async_copy(wfull, w_o, lsem.at[3])
    w_out.start()
    st.finish()
    tab_out.wait()
    wg.finish()
    vg.finish()
    w_out.wait()


def layer_in(cfg, x, w, sv, pos, fr):
    seq, model, ff = pos.shape[1], x.shape[1], cfg["ff"]
    dp, tensor = cfg["dp"], cfg["tensor"]
    rows = sds((seq, model), BF)
    heads = sds((seq, HW), BF)
    nv = dp - 1 + tensor
    wide = pltpu.VMEM((seq, model), BF)
    return pl.pallas_call(
        functools.partial(in_kernel, cfg),
        out_shape=(rows, rows, rows, sds((seq, ff), BF), sds((seq, ff), BF), sds((seq, 256), F32),
                   sds((model, w.shape[1]), BF), sds((2, 8, model), F32), heads, heads, heads),
        in_specs=[VMEM] * 5,
        out_specs=(ANY,) * 7 + (VMEM,) * 4,
        scratch_shapes=[
            wide, wide, wide, pltpu.VMEM((seq, ff), BF), pltpu.VMEM((seq, ff), BF), pltpu.VMEM((seq, 256), F32),
            pltpu.VMEM((model, w.shape[1]), BF), pltpu.VMEM((2, tensor, dp) + sv.shape, F32),
            DMA((6,)), DMA((6,)), DMA((4,)), DMA((5, 8)), DMA((nv,)), DMA((nv,)),
        ]
        + WeightGather.scratch(dp, 3),
        compiler_params=params(2),
        cost_estimate=cost(38),
        name="layer_in",
    )(x, w, sv, pos, fr)


def mid_kernel(
    cfg, o, g_in, x_ref, w_ref, w0, vecs, tab_in, h_ref, hf_o, n1_o, n2_o, g_o, gp_o, w_o, q, k, v,
    wout, wfc2, hf, n1, n2, g, gp, tab, wfull, part, r1x, r1y, r2x, r2y, sss, srs, gss, grs, lsem, ssem, *wsems,
):
    col = cfg["col"]
    me = Mesh(cfg["dp"], cfg["tensor"])
    loads = load(
        [
            (w0.at[:, col["out"] : col["end"]], wout),
            (w0.at[:, col["fc2"] : col["out"]], wfc2),
            (g_in, g),
            (tab_in, tab),
        ],
        lsem,
    )
    greet([me.mate] + me.ring + neighbours())
    wg = WeightGather(me, 1, w_ref, wfull, cfg["groups"], wsems)
    wg.send()
    for c in loads:
        c.wait()
    sc = Scatter(part, r1x, r1y, r2x, r2y, sss, srs)
    ga = Gather(hf, gss, grs)
    st = Stores([(hf, hf_o), (n1, n1_o), (n2, n2_o), (g, g_o), (gp, gp_o)], ga.half, ssem)
    sc.run(lambda r0: branch_out(r0, sc.half, o, g, wout, wfc2, part))
    wg.wait(0)
    residual_out(sc, x_ref, 0, vecs.at[0], h_ref, hf, sc.t * 2 * sc.half, lambda h: start_half(ga, h))
    wg.wait(1)
    vec = vecs.at[1]

    def work(r0, i):
        project_qkv(r0, ga.half, hf, wfull.at[:, 0 : col["fc1"]], vec, tab, n1, n2, q, k, v)
        project_fc1(r0, ga.half, wfull.at[:, col["fc1"] : col["fc2"]], vec, n2, g, gp)
        st.start(range(5), r0, i)

    ga.run(work)
    wg.wait(2)
    w_out = pltpu.make_async_copy(wfull, w_o, lsem.at[0])
    w_out.start()
    sc.finish()
    wg.finish()
    st.finish()
    w_out.wait()


def layer_mid(cfg, o, g, x, w, w0, vecs, tab):
    seq, model, ff = tab.shape[0], x.shape[1], cfg["ff"]
    rows = sds((seq, model), BF)
    heads = sds((seq, HW), BF)
    wide = pltpu.VMEM((seq, model), BF)
    return pl.pallas_call(
        functools.partial(mid_kernel, cfg),
        out_shape=(sds(x.shape, BF), rows, rows, rows, sds((seq, ff), BF), sds((seq, ff), BF), sds(w0.shape, BF),
                   heads, heads, heads),
        in_specs=[VMEM, ANY, VMEM, VMEM, ANY, VMEM, ANY],
        out_specs=(VMEM,) + (ANY,) * 6 + (VMEM,) * 3,
        scratch_shapes=[
            pltpu.VMEM((model, HW), BF), pltpu.VMEM((model, ff), BF),
            wide, wide, wide, pltpu.VMEM((seq, ff), BF), pltpu.VMEM((seq, ff), BF), pltpu.VMEM((seq, 256), F32),
            pltpu.VMEM(w0.shape, BF),
        ]
        + scatter_scratch(seq, model)
        + [DMA((6,)), DMA((6,)), DMA((4,)), DMA((5, 8))]
        + WeightGather.scratch(cfg["dp"], 3),
        compiler_params=params(3),
        cost_estimate=cost(65),
        name="layer_mid",
    )(o, g, x, w, w0, vecs, tab)


def turn_kernel(
    cfg, o, g_in, h_ref, hf_in, cot, cx, cy, cd0, cd1, w1, vecs, n2_in, gp_in, y_ref, do, e2_o, gr, vg,
    g, hf, dyf, n2, gp, e2, wout, wfc2, wfc1, da, acc, part, r1x, r1y, r2x, r2y, sss, srs, lsem, ssem,
):
    col = cfg["col"]
    t, px, py, pd = places()
    sc = Scatter(part, r1x, r1y, r2x, r2y, sss, srs)
    half = sc.half

    def rows(c, h, n):
        return dyf.at[ds((2 * c + h) * half, n * half)]

    loads = load(
        [
            (w1.at[:, col["out"] : col["end"]], wout),
            (w1.at[:, col["fc2"] : col["out"]], wfc2),
            (g_in, g),
            (w1.at[:, col["fc1"] : col["fc2"]], wfc1),
            (cot, rows(t, 0, 2)),
            (cx, rows(px, 0, 2)),
            (cy, rows(py, 0, 2)),
            (cd0, rows(pd, 0, 1)),
            (cd1, rows(pd, 1, 1)),
            (gp_in, gp),
            (hf_in, hf),
            (n2_in, n2),
        ],
        lsem,
    )
    greet(neighbours())
    for c in loads[:3]:
        c.wait()
    vec = vecs.at[1]
    st = Stores([(e2, e2_o)], half, ssem)

    def early():
        vg[...] = jnp.zeros_like(vg)
        acc[...] = jnp.zeros_like(acc)
        for c in loads[3:]:
            c.wait()

        def body(i, _):
            r0 = i * half
            back_head(r0, half, dyf, hf, g, gp, n2, o, wfc1, wfc2, wout, vec, do, e2, da, acc, vg)
            st.start((0,), r0, i)
            return 0

        lax.fori_loop(0, 4, body, 0)

    def rest():
        def body(i, _):
            r0 = i * half
            back_head(r0, half, dyf, hf, g, gp, n2, o, wfc1, wfc2, wout, vec, do, e2, da, acc, vg)
            st.start((0,), r0, i)
            return 0

        lax.fori_loop(4, 8, body, 0)
        column_sum(cot_rows, 0, 2 * half, vg, 2)
        store_low(acc, gr)

    cot_rows = dyf.at[ds(2 * t * half, 2 * half)]
    sc.run(lambda r0: branch_out(r0, half, o, g, wout, wfc2, part), early)
    rest()
    residual_out(sc, h_ref, 0, vec, y_ref)
    sc.finish()
    st.finish()


def layer_turn(cfg, o, g, h, hf, cots, w1, vecs, n2, gp):
    seq, model = hf.shape
    ff = cfg["ff"]
    wide, hidden = pltpu.VMEM((seq, model), BF), pltpu.VMEM((seq, ff), BF)
    return pl.pallas_call(
        functools.partial(turn_kernel, cfg),
        out_shape=(
            sds(h.shape, BF),
            sds((seq, HW), BF),
            sds((seq, model), BF),
            sds((model, 2 * ff + HW), BF),
            sds((8, model), F32),
        ),
        in_specs=[VMEM, ANY, VMEM, ANY] + [ANY] * 5 + [ANY, VMEM, ANY, ANY],
        out_specs=(VMEM, VMEM, ANY, VMEM, VMEM),
        scratch_shapes=[
            hidden, wide, wide, wide, hidden, wide,
            pltpu.VMEM((model, HW), BF), pltpu.VMEM((model, ff), BF), pltpu.VMEM((model, ff), BF),
            pltpu.VMEM((seq // 8, ff), BF), pltpu.VMEM((model, 2 * ff + HW), F32),
        ]
        + scatter_scratch(seq, model)
        + [DMA((12,)), DMA((1, 8))],
        compiler_params=params(4, 63),
        cost_estimate=cost(40),
        name="layer_turn",
    )(o, g, h, hf, *cots, w1, vecs, n2, gp)


def back_kernel(
    cfg, dmix, e2_in, cot, hf_in, n1_in, w1, w0, vecs, xf_in, g_in, gp_in, n2_in, o, gr1,
    dh_ref, e2_o, do, vgf, vgd, out1, sba, owna, sbb, ownb,
    a, b, e2, g, gp, wqkv, wout, wfc2, wfc1, dhf, da, acc, gq, gr, got, gotq, sb, rb,
    part, r1x, r1y, r2x, r2y, sss, srs, gss, grs, lsem, ssem, hss, hrs, pss, prs,
):
    col = cfg["col"]
    me = Mesh(cfg["dp"], cfg["tensor"])
    loads = load(
        [
            (w1.at[:, col["qkv"] : col["fc1"]], wqkv),
            (hf_in, a),
            (e2_in, e2),
            (n1_in, b),
            (gr1, gr),
            (w0.at[:, col["out"] : col["end"]], wout),
            (w0.at[:, col["fc2"] : col["out"]], wfc2),
            (w0.at[:, col["fc1"] : col["fc2"]], wfc1),
            (g_in, g),
            (gp_in, gp),
        ],
        lsem,
    )
    greet([me.mate] + me.ring + neighbours())
    ga = Gather(dhf, gss, grs)
    sc = Scatter(part, r1x, r1y, r2x, r2y, sss, srs)
    red1 = GradReduce(me, 1, gr, got, sb, out1, (hss.at[0], hrs.at[0]), rb, (pss, prs))
    redq = GradReduce(me, 1, gq, gotq, sbb, ownb, (hss.at[1], hrs.at[1]))
    red0 = GradReduce(me, 0, gr, got, sba, owna, (hss.at[2], hrs.at[2]))
    st = Stores([(e2, e2_o)], ga.half, ssem)
    red1.send(gr1)
    vgf[...] = jnp.zeros_like(vgf)
    vgd[...] = jnp.zeros_like(vgd)
    for c in loads[:3]:
        c.wait()

    def early():
        loads[3].wait()
        small = acc.at[:, 0 : 3 * HW]
        qkv_grad(b, dmix, small, sc.half)
        store_low(small, gq)
        redq.send()
        loads[4].wait()
        red1.reduce()

    sc.run(lambda r0: back_tail(r0, sc.half, dmix, a, e2, wqkv, vecs.at[1], part, vgf), early)
    acc[...] = jnp.zeros_like(acc)
    again = pltpu.make_async_copy(n2_in, b, lsem.at[10])
    again.start()
    grad_out(sc, cot, 0, a, vecs.at[1], dh_ref, dhf, sc.t * 2 * sc.half, lambda h: start_half(ga, h))
    other = pltpu.make_async_copy(xf_in, a, lsem.at[11])
    other.start()
    for c in loads[5:]:
        c.wait()
    redq.reduce()
    again.wait()
    other.wait()

    def work(r0, i):
        back_head(r0, ga.half, dhf, a, g, gp, b, o, wfc1, wfc2, wout, vecs.at[0], do, e2, da, acc, vgd)
        st.start((0,), r0, i)

    ga.run(work)
    red1.collect()
    red1.finish(gr1)
    store_low(acc, gr)
    red0.send()
    column_sum(dh_ref, 0, dh_ref.shape[0], vgd, 2)
    red0.reduce()
    sc.finish()
    st.finish()
    redq.finish()
    red0.finish()


def layer_back(cfg, dmix, e2, cot, hf, n1, w1, w0, vecs, xf, g, gp, n2, o, gr1):
    seq, model = hf.shape
    ff, dp = cfg["ff"], cfg["dp"]
    rows, nr, nq = model // dp, 2 * ff + HW, 3 * HW
    wide, hidden = pltpu.VMEM((seq, model), BF), pltpu.VMEM((seq, ff), BF)
    return pl.pallas_call(
        functools.partial(back_kernel, cfg),
        out_shape=(
            sds(cot.shape, BF),
            sds((seq, model), BF),
            sds((seq, HW), BF),
            sds((8, model), F32),
            sds((8, model), F32),
            sds((rows, nr), F32),
            sds((dp - 1, rows, nr), BF),
            sds((rows, nr), F32),
            sds((dp - 1, rows, nq), BF),
            sds((rows, nq), F32),
        ),
        in_specs=[VMEM, ANY, VMEM, ANY, ANY, ANY, ANY, VMEM, ANY, ANY, ANY, ANY, VMEM, ANY],
        out_specs=(VMEM, ANY) + (VMEM,) * 8,
        scratch_shapes=[
            wide, wide, wide, hidden, hidden,
            pltpu.VMEM((model, nq), BF), pltpu.VMEM((model, HW), BF), pltpu.VMEM((model, ff), BF),
            pltpu.VMEM((model, ff), BF), wide, pltpu.VMEM((seq // 8, ff), BF), pltpu.VMEM((model, nr), F32),
            pltpu.VMEM((model, nq), BF), pltpu.VMEM((model, nr), BF), pltpu.VMEM((model, nr), BF),
            pltpu.VMEM((model, nq), BF), pltpu.VMEM((dp - 1, rows, nr), BF), pltpu.VMEM((dp - 1, rows, nr), BF),
        ]
        + scatter_scratch(seq, model)
        + [DMA((6,)), DMA((6,)), DMA((12,)), DMA((1, 8)), DMA((3,)), DMA((3,)), DMA((dp - 1,)), DMA((dp - 1,))],
        compiler_params=pltpu.CompilerParams(collective_id=5, has_side_effects=True, vmem_limit_bytes=67043328),
        cost_estimate=cost(65),
        name="layer_back",
    )(dmix, e2, cot, hf, n1, w1, w0, vecs, xf, g, gp, n2, o, gr1)


def last_kernel(
    cfg, dmix, e2_in, dh, xf_in, n1_in, w0, vecs, vf1, vd1, vd0, dx_ref, gqo, vout,
    xf, n1, e2, wqkv, acc, gq, got, sb, rb, vgf, va, vr,
    part, r1x, r1y, r2x, r2y, sss, srs, lsem, hss, hrs, pss, prs, vss, vrs,
):
    col = cfg["col"]
    me = Mesh(cfg["dp"], cfg["tensor"])
    loads = load([(w0.at[:, col["qkv"] : col["fc1"]], wqkv), (xf_in, xf), (e2_in, e2), (n1_in, n1)], lsem)
    greet([me.mate] + me.ring + me.group)
    sc = Scatter(part, r1x, r1y, r2x, r2y, sss, srs)
    red = GradReduce(me, 0, gq, got, sb, gqo, (hss.at[0], hrs.at[0]), rb, (pss, prs))
    vr_ = VectorReduce(me, va, vr, vss, vrs)
    vgf[...] = jnp.zeros_like(vgf)
    for c in loads[:3]:
        c.wait()

    def early():
        va[0, 0:8, :] = vgf[...] + vd0[...]
        va[0, 8:16, :] = vf1[...] + vd1[...]
        loads[3].wait()
        qkv_grad(n1, dmix, acc, sc.half)
        store_low(acc, gq)
        red.send()
        vr_.send(0)
        red.reduce()
        vr_.add(0, va.at[1])

    sc.run(lambda r0: back_tail(r0, sc.half, dmix, xf, e2, wqkv, vecs.at[0], part, vgf), early)
    vr_.send(1)
    red.finish()
    vr_.add(1, va.at[2])
    vr_.send(2)
    grad_out(sc, dh, 0, xf, vecs.at[0], dx_ref)
    red.collect()
    vr_.add(2, vout)
    vr_.finish()
    sc.finish()


def layer_last(cfg, dmix, e2, dh, xf, n1, w0, vecs, vf1, vd1, vd0):
    seq, model = xf.shape
    dp, tensor = cfg["dp"], cfg["tensor"]
    rows, nq = model // dp, 3 * HW
    nv = dp + tensor - 1
    wide = pltpu.VMEM((seq, model), BF)
    return pl.pallas_call(
        functools.partial(last_kernel, cfg),
        out_shape=(sds(dh.shape, BF), sds((rows, nq), F32), sds((16, model), F32)),
        in_specs=[VMEM, ANY, VMEM, ANY, ANY, ANY] + [VMEM] * 4,
        out_specs=(VMEM,) * 3,
        scratch_shapes=[
            wide, wide, wide, pltpu.VMEM((model, nq), BF), pltpu.VMEM((model, nq), F32),
            pltpu.VMEM((model, nq), BF), pltpu.VMEM((model, nq), BF),
            pltpu.VMEM((dp - 1, rows, nq), BF), pltpu.VMEM((dp - 1, rows, nq), BF),
            pltpu.VMEM((8, model), F32), pltpu.VMEM((3, 16, model), F32), pltpu.VMEM((nv, 16, model), F32),
        ]
        + scatter_scratch(seq, model)
        + [DMA((4,)), DMA((1,)), DMA((1,)), DMA((dp - 1,)), DMA((dp - 1,)), DMA((nv,)), DMA((nv,))],
        compiler_params=params(6),
        cost_estimate=cost(35),
        name="layer_last",
    )(dmix, e2, dh, xf, n1, w0, vecs, vf1, vd1, vd0)


def attention_plan(seg, live):
    seq = seg.shape[0]
    counter = jnp.arange(seq, dtype=jnp.int32)
    before = [jnp.sum((seg == v).astype(jnp.int32)) for v in range(3)]
    start = sum(jnp.where(seg > v, before[v], 0) for v in range(3))
    kc = jnp.where(counter < live * LIVE, seg, -1)
    lo = start[::QB] // QB
    hi = jnp.minimum(jnp.arange(seq // QB, dtype=jnp.int32), (live * LIVE + QB - 1) // QB)
    bounds = jnp.stack([jnp.minimum(lo, hi), hi]).astype(jnp.int32)
    return bounds, (counter - start)[None, :], seg[None, :], kc[:, None]


def by_part(w):
    rows = w.shape[0]
    heads = w.shape[1] // (3 * HD)
    w = w.reshape(rows, heads, 3, HD).transpose(0, 2, 1, 3).reshape(rows, 3, heads * HD)
    return jnp.pad(w, ((0, 0), (0, 0), (0, HW - heads * HD))).reshape(rows, 3 * HW)


def by_head(w, heads):
    rows = w.shape[0]
    w = w.reshape(rows, 3, HW)[:, :, : heads * HD].reshape(rows, 3, heads, HD)
    return w.transpose(0, 2, 1, 3).reshape(rows, heads * 3 * HD)


def shards(
    dp, tensor, inputs, cotangent, segments, live_blocks, ln1_gain, ln1_bias, qkv_weight, qkv_bias,
    out_weight, out_bias, ln2_gain, ln2_bias, fc1_weight, fc1_bias, fc2_weight, fc2_bias,
):
    s, z, t = lax.axis_index("section"), lax.axis_index("dp"), lax.axis_index("tensor")
    model = inputs.shape[-1]
    ff = fc1_weight.shape[2]
    heads = qkv_bias.shape[1]
    col = columns(model, ff)

    def mine(a):
        return lax.dynamic_index_in_dim(a, s, 0, keepdims=False)[0]

    x, cot, seg, live = mine(inputs), mine(cotangent), mine(segments), mine(live_blocks)
    bounds, pos, sr, kc = attention_plan(seg, live)
    wout = jnp.pad(out_weight[0].T, ((0, 0), (0, HW - heads * HD)))
    w = jnp.concatenate([by_part(qkv_weight[0]), fc1_weight[0], fc2_weight[0].T, wout], axis=1)
    small = jnp.stack([ln1_gain[0], ln1_bias[0], out_bias[0], ln2_gain[0], ln2_bias[0], fc2_bias[0]])
    own = small.shape[1]

    def lanes(a):
        return jnp.pad(a.astype(F32), ((0, 0), (0, 128 - a.shape[1])))

    sv = jnp.concatenate([lanes(small), lanes(qkv_bias[0]), lanes(fc1_bias[0])], axis=0)
    sv = jnp.pad(sv, ((0, -sv.shape[0] % 8), (0, 0)))
    fr = 10000.0 ** (-(jnp.arange(ROT // 2, dtype=F32) * (2.0 / ROT)))
    fr = jnp.broadcast_to(fr[:, None], (ROT // 2, 128))
    cfg = {
        "col": col, "ff": ff, "heads": heads, "dp": dp, "tensor": tensor, "own": own,
        "qw": qkv_bias.shape[2], "fw": fc1_bias.shape[2],
        "groups": [(0, col["fc1"]), (col["fc1"], col["fc2"]), (col["fc2"], col["end"])],
    }
    t_pairs = [[(i, i + 1 - 2 * (i % 2)) for i in range(tensor)], [(i, (i + 2) % tensor) for i in range(tensor)]]

    xf, n1a, n2a, ga, gpa, tab, w0, vecs, qa, ka, va = layer_in(cfg, x, w, sv, pos, fr)
    half = cot.shape[0] // 2
    cot_, _ = lax.optimization_barrier((cot, qa))
    cx = lax.ppermute(cot_, "tensor", t_pairs[0])
    cy = lax.ppermute(cot_, "tensor", t_pairs[1])
    oa, lsea = attn_fwd(heads, bounds, qa, ka, va, sr, kc)
    h, hf, n1b, n2b, gb, gpb, w1, qb, kb, vb = layer_mid(cfg, oa, ga, x, w, w0, vecs, tab)
    cx_, cy_, _ = lax.optimization_barrier((cx, cy, qb))
    cd0 = lax.ppermute(cx_[:half], "tensor", t_pairs[1])
    cd1 = lax.ppermute(cy_[half:], "tensor", t_pairs[0])
    ob, lseb = attn_fwd(heads, bounds, qb, kb, vb, sr, kc)
    y, dob, e2b, grb, vdb = layer_turn(cfg, ob, gb, h, hf, (cot, cx, cy, cd0, cd1), w1, vecs, n2b, gpb)
    dmb = attn_bwd(heads, bounds, qb, kb, vb, ob, dob, lseb, sr, kc, tab)
    dh, e2a, doa, vfb, vda, gr1, sba, owna, sbb, ownb = layer_back(
        cfg, dmb, e2b, cot, hf, n1b, w1, w0, vecs, xf, ga, gpa, n2a, oa, grb
    )

    def over_dp(blocks, section):
        def pairs(d):
            return [(section * dp + i, section * dp + (i + d) % dp) for i in range(dp)]

        return [lax.ppermute(blocks[d - 1], ("section", "dp"), pairs(d)) for d in range(1, dp)]

    got_r = over_dp(sba, 0)
    got_q = over_dp(sbb, 1)
    dma = attn_bwd(heads, bounds, qa, ka, va, oa, doa, lsea, sr, kc, tab)
    dx, gq0, gv = layer_last(cfg, dma, e2a, dh, xf, n1a, w0, vecs, vfb, vdb, vda)
    first = s == 0
    gr = jnp.where(first, owna + sum(a.astype(F32) for a in got_r), gr1)
    gq = jnp.where(first, gq0, ownb + sum(a.astype(F32) for a in got_q))

    def swapped(a0, a1):
        got = lax.ppermute(jnp.where(first, a1, a0), "section", [(0, 1), (1, 0)])
        keep = jnp.where(first, a0, a1)
        return jnp.stack([jnp.where(first, keep, got), jnp.where(first, got, keep)])[None, :, None]

    section_outputs = swapped(h, y)
    input_grads = swapped(dx, dh)
    gv = lax.dynamic_index_in_dim(gv.reshape(2, 8, model), s, 0, keepdims=False)
    short = lax.dynamic_slice_in_dim(gv[:6], (z * tensor + t) * own, own, 1)
    gqb_ = by_head(gv[6:7], heads).reshape(heads, 3 * HD)
    gqb_ = lax.dynamic_slice_in_dim(gqb_, z * cfg["qw"], cfg["qw"], 1)[None]
    gfb = lax.dynamic_slice_in_dim(gv[7].reshape(heads, ff // heads), z * cfg["fw"], cfg["fw"], 1)[None]
    gqkv = by_head(gq, heads)[None]
    gfc1 = gr[:, :ff][None]
    gfc2 = gr[:, ff : 2 * ff].T[None]
    gout = gr[:, 2 * ff : 2 * ff + heads * HD].T[None]
    return (
        section_outputs,
        input_grads,
        short[0:1],
        short[1:2],
        gqkv,
        gqb_,
        gout,
        short[2:3],
        short[3:4],
        short[4:5],
        gfc1,
        gfb,
        gfc2,
        short[2:3],
    )


def solution(mesh):
    both = ("dp", "tensor")
    in_specs = (
        P(None, "dp", "tensor", None),
        P(None, "dp", "tensor", None),
        P(None, "dp", None),
        P(None, "dp"),
        P("section", both),
        P("section", both),
        P("section", "dp", "tensor"),
        P("section", "tensor", "dp"),
        P("section", "tensor", "dp"),
        P("section", both),
        P("section", both),
        P("section", both),
        P("section", "dp", "tensor"),
        P("section", "tensor", "dp"),
        P("section", "tensor", "dp"),
        P("section", both),
    )
    out_specs = (
        P("section", None, "dp", "tensor", None),
        P("section", None, "dp", "tensor", None),
        P("section", both),
        P("section", both),
        P("section", "dp", "tensor"),
        P("section", "tensor", "dp"),
        P("section", "tensor", "dp"),
        P("section", both),
        P("section", both),
        P("section", both),
        P("section", "dp", "tensor"),
        P("section", "tensor", "dp"),
        P("section", "tensor", "dp"),
        P("section", both),
    )
    body = functools.partial(shards, mesh.shape["dp"], mesh.shape["tensor"])
    return jax.shard_map(body, mesh=mesh, in_specs=in_specs, out_specs=out_specs, check_vma=False)
```

```python
import functools

import jax
import jax.numpy as jnp
import numpy as np
from jax import lax
from jax.experimental import pallas as pl
from jax.experimental.pallas import tpu as pltpu
from jax.sharding import PartitionSpec as P

F32 = jnp.float32
BF = jnp.bfloat16
MESH = pl.DeviceIdType.MESH
HD = 64
ROT = 16
LIVE = 128
DOCS = 4
DOC_MAX = 1024
QB = 256
HW = 256
SUB = 256
EPS = 1e-05
NEG = -1e30
VMEM = pl.BlockSpec(memory_space=pltpu.VMEM)
ANY = pl.BlockSpec(memory_space=pltpu.HBM)
SMEM = pl.BlockSpec(memory_space=pltpu.SMEM)
DMA = pltpu.SemaphoreType.DMA


def sds(shape, dtype):
    return jax.ShapeDtypeStruct(shape, dtype)


def dg(a, b, ca, cb):
    return lax.dot_general(a, b, (((ca,), (cb,)), ((), ())), preferred_element_type=F32)


def dot(a, b):
    return jnp.dot(a, b, preferred_element_type=F32)


def ds(start, size):
    return pl.ds(pl.multiple_of(start, size), size)


def norm_stats(x):
    mu = jnp.mean(x, axis=-1, keepdims=True)
    xc = x - mu
    var = jnp.mean(xc * xc, axis=-1, keepdims=True)
    return xc, lax.rsqrt(var + EPS)


def head_lanes(width, heads):
    lane = lax.broadcasted_iota(jnp.int32, (1, width), 1)
    return [(lane >= h * HD) & (lane < (h + 1) * HD) for h in range(heads)]


def allow_mask(kc, sq, diag):
    m = kc == sq
    if diag:
        r = lax.broadcasted_iota(jnp.int32, (QB, QB), 0)
        c = lax.broadcasted_iota(jnp.int32, (QB, QB), 1)
        m = (m & (r <= c)) | (r == c)
    return m


def block_bounds(seg, live, i, n):
    s = lax.axis_index("tensor") // 2
    doc = seg[s, 0, i * QB]

    def body(j, count):
        return count + jnp.where((j < i) & (seg[s, 0, (j + 1) * QB - 1] == doc), 1, 0)

    hi = jnp.minimum(i, (live[s, 0] * LIVE + QB - 1) // QB)
    return jnp.minimum(i - lax.fori_loop(0, n, body, 0), hi), hi


def turn_blocks(src, dst):
    def turn(i, _):
        dst[:, ds(i * QB, QB)] = src[ds(i * QB, QB), :].T
        return 0

    lax.fori_loop(0, src.shape[0] // QB, turn, 0)


def attn_fwd_block(i, lo, hi, heads, q_ref, k_ref, vt, sr_ref, kc_ref, s_scr, o_ref, lse_ref):
    width = q_ref.shape[1]
    qi = ds(i * QB, QB)
    q = q_ref[qi, :]
    qm = [jnp.where(m, q, jnp.zeros_like(q)) for m in head_lanes(width, heads)]
    sq = sr_ref[0:1, qi]

    def scores(j, slot, ms, diag):
        kj = ds(j * QB, QB)
        k = k_ref[kj, :]
        mask = allow_mask(kc_ref[kj, 0:1], sq, diag)
        out = []
        for h in range(heads):
            s = jnp.where(mask, dg(k, qm[h], 1, 1), NEG)
            s_scr[h, ds(slot * QB, QB), :] = s
            out.append(jnp.maximum(ms[h], jnp.max(s, axis=0, keepdims=True)))
        return tuple(out)

    ms = tuple(jnp.full((1, QB), NEG, F32) for _ in range(heads))
    ms = scores(i, 0, ms, True)
    ms = lax.fori_loop(lo, hi, lambda j, ms: scores(j, j - lo + 1, ms, False), ms)

    def weigh(j, slot, st):
        kj = ds(j * QB, QB)
        out = []
        for h in range(heads):
            total, acc = st[h]
            p = jnp.exp(s_scr[h, ds(slot * QB, QB), :] - ms[h])
            total = total + jnp.sum(p, axis=0, keepdims=True)
            acc = acc + dot(vt[h * HD : (h + 1) * HD, kj], p.astype(BF))
            out.append((total, acc))
        return tuple(out)

    st = tuple((jnp.zeros((1, QB), F32), jnp.zeros((HD, QB), F32)) for _ in range(heads))
    st = weigh(i, 0, st)
    st = lax.fori_loop(lo, hi, lambda j, st: weigh(j, j - lo + 1, st), st)
    ot = [st[h][1] * (1.0 / st[h][0]) for h in range(heads)]
    ot = jnp.concatenate(ot + [jnp.zeros((width - heads * HD, QB), F32)], axis=0)
    o_ref[qi, :] = ot.T.astype(BF)
    lse = [ms[h] + jnp.log(st[h][0]) for h in range(heads)]
    lse_ref[:, qi] = jnp.concatenate(lse + [jnp.zeros((8 - heads, QB), F32)], axis=0)


def attn_fwd_kernel(heads, seg, live, q_in, k_in, v_in, sr_ref, kc_ref, o_out, lse_ref, q, k, v, o, vt, s_scr, lsem, osem):
    n = q.shape[0] // QB
    loads = load([(v_in, v), (q_in, q), (k_in, k)], lsem)
    loads[0].wait()
    turn_blocks(v, vt)
    loads[1].wait()
    loads[2].wait()

    def out(i):
        rows = ds(i * QB, QB)
        return pltpu.make_async_copy(o.at[rows], o_out.at[rows], osem.at[i])

    def qloop(i, _):
        lo, hi = block_bounds(seg, live, i, n)
        attn_fwd_block(i, lo, hi, heads, q, k, vt, sr_ref, kc_ref, s_scr, o, lse_ref)
        out(i).start()
        return 0

    lax.fori_loop(0, n, qloop, 0)

    def drain(i, _):
        out(i).wait()
        return 0

    lax.fori_loop(0, n, drain, 0)


def attn_fwd(heads, seg, live, q, k, v, sr, kc):
    rows, width = q.shape
    buf = pltpu.VMEM((rows, width), BF)
    return pl.pallas_call(
        functools.partial(attn_fwd_kernel, heads),
        out_shape=(sds((rows, width), BF), sds((8, rows), F32)),
        in_specs=[SMEM, SMEM, ANY, ANY, ANY, VMEM, VMEM],
        out_specs=(ANY, VMEM),
        scratch_shapes=[buf, buf, buf, buf, pltpu.VMEM((width, rows), BF), pltpu.VMEM((heads, rows + QB, QB), F32),
                        DMA((3,)), DMA((rows // QB,))],
        compiler_params=pltpu.CompilerParams(vmem_limit_bytes=67043328),
        cost_estimate=cost(12),
        name="attn_fwd",
    )(seg, live, q, k, v, sr, kc)


def turn_lanes(x, tab, sign):
    width = x.shape[1]
    c, sn = [jnp.concatenate([tab[:, a * 128 : (a + 1) * 128]] * (width // 128), axis=1) for a in range(2)]
    lane = lax.broadcasted_iota(jnp.int32, (1, width), 1) % HD
    moved = jnp.where(lane < ROT // 2, pltpu.roll(x, width - ROT // 2, 1), pltpu.roll(x, ROT // 2, 1)) * sn
    return x * c + moved if sign > 0 else x * c - moved


def attn_bwd_block(i, lo, hi, heads, q_ref, k_ref, v_ref, o_ref, do_ref, kt, lse_ref, sr_ref, kc_ref, tab, dk, dv, out):
    width = q_ref.shape[1]
    hm = head_lanes(width, heads)
    rowid = lax.broadcasted_iota(jnp.int32, (8, width), 0)
    lane = lax.broadcasted_iota(jnp.int32, (8, width), 1)
    sel = ((lane >= rowid * HD) & (lane < (rowid + 1) * HD)).astype(F32).astype(BF)
    qi = ds(i * QB, QB)
    q = q_ref[qi, :]
    do = do_ref[qi, :]
    z = jnp.zeros_like(q)
    qm = [jnp.where(hm[h], q, z) for h in range(heads)]
    dom = [jnp.where(hm[h], do, z) for h in range(heads)]
    qcat = jnp.concatenate(qm, axis=0)
    docat = jnp.concatenate(dom, axis=0)
    prod = do.astype(F32) * o_ref[qi, :].astype(F32)
    high = prod.astype(BF)
    low = (prod - high.astype(F32)).astype(BF)
    delta = dg(sel, high, 1, 1) + dg(sel, low, 1, 1)
    lse = lse_ref[:, qi]
    sq = sr_ref[0:1, qi]

    def step(j, dqs, diag):
        kj = ds(j * QB, QB)
        k = k_ref[kj, :]
        v = v_ref[kj, :]
        mask = allow_mask(kc_ref[kj, 0:1], sq, diag)
        ps, dss, res = [], [], []
        for h in range(heads):
            s = dg(k, qm[h], 1, 1)
            dp = dg(v, dom[h], 1, 1)
            p = jnp.exp(jnp.where(mask, s - lse[h : h + 1, :], NEG))
            score_grad = (p * (dp - delta[h : h + 1, :])).astype(BF)
            ps.append(p.astype(BF))
            dss.append(score_grad)
            res.append(dqs[h] + dot(kt[h * HD : (h + 1) * HD, kj], score_grad))
        dv[kj, :] += dot(jnp.concatenate(ps, axis=1), docat)
        dk[kj, :] += dot(jnp.concatenate(dss, axis=1), qcat)
        return tuple(res)

    dqs = tuple(jnp.zeros((HD, QB), F32) for _ in range(heads))
    dqs = step(i, dqs, True)
    dqs = lax.fori_loop(lo, hi, lambda j, d: step(j, d, False), dqs)
    dq = jnp.concatenate(list(dqs) + [jnp.zeros((width - heads * HD, QB), F32)], axis=0).T * 0.125
    out[qi, 0:width] = turn_lanes(dq, tab[qi, :], -1).astype(BF)


def attn_bwd_kernel(
    heads, seg, live, q_in, k_in, v_in, o_in, do_in, lse_ref, sr_ref, kc_ref, tab_in, out_ref,
    q, k, v, o, do, tab, out, kt, dk, dv, lsem, osem,
):
    rows, width = q.shape
    n = rows // QB
    loads = load([(k_in, k), (q_in, q), (v_in, v), (do_in, do), (o_in, o), (tab_in, tab)], lsem)
    dk[...] = jnp.zeros_like(dk)
    dv[...] = jnp.zeros_like(dv)
    loads[0].wait()
    turn_blocks(k, kt)
    for c in loads[1:]:
        c.wait()

    def qloop(i, _):
        lo, hi = block_bounds(seg, live, i, n)
        attn_bwd_block(i, lo, hi, heads, q, k, v, o, do, kt, lse_ref, sr_ref, kc_ref, tab, dk, dv, out)
        return 0

    lax.fori_loop(0, n, qloop, 0)

    def leave(i):
        rr = ds(i * QB, QB)
        return pltpu.make_async_copy(out.at[rr], out_ref.at[rr], osem.at[i])

    def finish(i, _):
        ii = ds(i * QB, QB)
        out[ii, width : 2 * width] = turn_lanes(dk[ii, :], tab[ii, :], -1).astype(BF)
        out[ii, 2 * width : 3 * width] = dv[ii, :].astype(BF)
        leave(i).start()
        return 0

    lax.fori_loop(0, n, finish, 0)

    def drain(i, _):
        leave(i).wait()
        return 0

    lax.fori_loop(0, n, drain, 0)


def attn_bwd(heads, seg, live, q, k, v, o, do, lse, sr, kc, tab):
    rows, width = q.shape
    buf = pltpu.VMEM((rows, width), BF)
    return pl.pallas_call(
        functools.partial(attn_bwd_kernel, heads),
        out_shape=sds((rows, 3 * width), BF),
        in_specs=[SMEM, SMEM] + [ANY] * 5 + [VMEM] * 3 + [ANY],
        out_specs=ANY,
        scratch_shapes=[buf, buf, buf, buf, buf, pltpu.VMEM(tab.shape, F32), pltpu.VMEM((rows, 3 * width), BF),
                        pltpu.VMEM((width, rows), BF), pltpu.VMEM((rows, width), F32), pltpu.VMEM((rows, width), F32),
                        DMA((6,)), DMA((rows // QB,))],
        compiler_params=pltpu.CompilerParams(vmem_limit_bytes=67043328),
        cost_estimate=cost(26),
        name="attn_bwd",
    )(seg, live, q, k, v, o, do, lse, sr, kc, tab)


class Mesh:
    def __init__(self, dp, tensor):
        self.dp, self.tensor = dp, tensor
        self.s, self.z, self.t = lax.axis_index("section"), lax.axis_index("dp"), lax.axis_index("tensor")
        self.x, self.y = self.t % 2, self.t // 2
        self.px, self.py = 2 * self.y + (1 - self.x), 2 * (1 - self.y) + self.x
        self.mate = {"section": 1 - self.s}
        self.beside = {"tensor": self.px}
        self.beside_mate = {"tensor": self.px, "section": 1 - self.s}
        self.across = {"tensor": self.py}
        self.across_mate = {"tensor": self.py, "section": 1 - self.s}
        self.ring = [{"dp": (self.z + d) % dp} for d in range(1, dp)]
        self.group = [{"tensor": (self.t + d) % tensor} for d in range(1, tensor)]
        self.quarter = 2 * self.s + self.x

    def across_core(self, core):
        return {"tensor": self.py, "section": core}


def greet(peers):
    bar = pltpu.get_barrier_semaphore()
    for peer in peers:
        pl.semaphore_signal(bar, inc=1, device_id=peer, device_id_type=MESH)
    pl.semaphore_wait(bar, len(peers))


def push(src, dst, ssem, rsem, peer):
    return pltpu.make_async_remote_copy(
        src_ref=src, dst_ref=dst, send_sem=ssem, recv_sem=rsem, device_id=peer, device_id_type=MESH
    )


def pick(i, values):
    out = values[-1]
    for n in range(len(values) - 2, -1, -1):
        out = jnp.where(i == n, values[n], out)
    return out


class Tokens:
    def __init__(self, me, seq):
        self.me, self.half = me, seq // 8

    def start_of(self, a, b, h):
        return (4 * a + 2 * b + h) * self.half

    def rows(self, a, b, h):
        return ds(self.start_of(a, b, h), self.half)

    def own(self, a):
        return self.start_of(a, self.me.x, self.me.s)


class Gather(Tokens):
    def __init__(self, me, full, ssem, rsem, first=0):
        super().__init__(me, full.shape[0])
        self.full, self.ssem, self.rsem, self.first = full, ssem, rsem, first

    def side(self, n):
        return self.first if n == 0 else 1 - self.first

    def plan(self, i):
        me, a = self.me, self.side(i % 2)
        ref = self.full.at[self.rows(a, (1 - me.x) if i >= 4 else me.x, me.s)]
        return push(ref, ref, self.ssem.at[i], self.rsem.at[i], me.beside if i in (2, 3) else me.mate)

    def start(self, n):
        self.plan(n).start()
        self.plan(2 + n).start()

    def order(self, i):
        me = self.me
        a = pick(i, [self.side(n) for n in (0, 1, 0, 1, 0, 0, 1, 1)])
        b = jnp.where(i < 4, me.x, 1 - me.x)
        h = pick(i, [me.s, me.s, 1 - me.s, 1 - me.s, me.s, 1 - me.s, me.s, 1 - me.s])
        return self.start_of(a, b, h)

    def step(self, i):
        if i in (2, 3):
            self.plan(i - 2).wait_recv()
        if i in (4, 6):
            n = i // 2 - 2
            self.plan(2 + n).wait_recv()
            self.plan(4 + n).start()
        if i in (5, 7):
            self.plan(4 + i // 2 - 2).wait_recv()

    def arrive(self, i):
        for n in range(2, 8):

            @pl.when(i == n)
            def _(n=n):
                self.step(n)

    def finish(self):
        for i in range(6):
            self.plan(i).wait_send()

    def run(self, work):
        def body(i, _):
            self.arrive(i)
            work(self.order(i), i)
            return 0

        lax.fori_loop(0, 8, body, 0)
        self.finish()


class Scatter(Tokens):
    def __init__(self, me, part, mr, xr, ssem, rsem, first=0):
        super().__init__(me, part.shape[0])
        self.part, self.mr, self.xr, self.ssem, self.rsem, self.first = part, mr, xr, ssem, rsem, first

    def side(self, n):
        return self.first if n == 0 else 1 - self.first

    def plan(self, i):
        me = self.me
        if i < 4:
            b = (1 - me.x) if i < 2 else me.x
            src, dst, peer = self.rows(self.side(i % 2), b, 1 - me.s), self.mr.at[i], me.mate
        else:
            src, dst, peer = self.rows(self.side(i - 4), 1 - me.x, me.s), self.xr.at[i - 4], me.beside
        return push(self.part.at[src], dst, self.ssem.at[i], self.rsem.at[i], peer)

    def run(self, work, early=None):
        me = self.me

        def body(i, _):
            k = i // 2
            b = jnp.where(k < 2, 1 - me.x, me.x)
            h = jnp.where(i % 2 == 0, 1 - me.s, me.s)
            work(self.start_of(jnp.where(k % 2 == 0, self.side(0), self.side(1)), b, h), i)
            for n in range(4):

                @pl.when(i == 2 * n)
                def _(n=n):
                    self.plan(n).start()

            for n in range(2):

                @pl.when(i == 2 * n + 1)
                def _(n=n):
                    self.plan(n).wait_recv()
                    base = self.start_of(self.side(n), 1 - me.x, me.s)

                    def add(j, _):
                        rr = ds(base + j * SUB, SUB)
                        got = self.mr[n, ds(j * SUB, SUB), :].astype(F32)
                        self.part[rr, :] = (self.part[rr, :].astype(F32) + got).astype(BF)
                        return 0

                    lax.fori_loop(0, self.half // SUB, add, 0)
                    self.plan(4 + n).start()

            return 0

        lax.fori_loop(0, 8, body, 0)
        if early is not None:
            early()

    def arrive(self, n):
        self.plan(2 + n).wait_recv()
        self.plan(4 + n).wait_recv()

    def total(self, n, i):
        rr = ds(self.own(self.side(n)) + i * SUB, SUB)
        sub = ds(i * SUB, SUB)
        return self.part[rr, :].astype(F32) + self.mr[2 + n, sub, :].astype(F32) + self.xr[n, sub, :].astype(F32)

    def finish(self):
        for i in range(6):
            self.plan(i).wait_send()


def scatter_scratch(rows, width):
    half = rows // 8
    return [
        pltpu.VMEM((rows, width), BF),
        pltpu.VMEM((4, half, width), BF),
        pltpu.VMEM((2, half, width), BF),
        DMA((6,)),
        DMA((6,)),
    ]


class WeightGather:
    def __init__(self, me, layer, shard, full, gat, groups, sems):
        self.me, self.layer, self.shard, self.full, self.gat, self.groups = me, layer, shard, full, gat, groups
        self.own, self.wss, self.wrs, self.fss, self.frs, self.yss, self.yrs = sems
        self.rows = shard.shape[0]
        self.collects = me.s == layer
        self.keeps = me.y == layer

    def block(self, ref, zz, g):
        a, b = self.groups[g]
        return ref.at[ds(zz * self.rows, self.rows), a:b]

    def mine(self, g):
        a, b = self.groups[g]
        return self.shard.at[:, a:b]

    def local(self, g):
        return pltpu.make_async_copy(self.mine(g), self.block(self.full, self.me.z, g), self.own.at[g])

    def out(self, g, d, ref):
        dst = self.block(ref, self.me.z, g)
        return push(self.mine(g), dst, self.wss.at[g, d], self.wrs.at[g, d], self.me.ring[d])

    def hand(self, g, d, ref, across):
        zz = (self.me.z + self.me.dp - d) % self.me.dp
        src = self.mine(g) if d == 0 else self.block(ref, zz, g)
        ss, rs = (self.yss, self.yrs) if across else (self.fss, self.frs)
        peer = self.me.across_core(self.me.y) if across else self.me.mate
        return push(src, self.block(self.full, zz, g), ss.at[g, d], rs.at[g, d], peer)

    def both(self, do):
        @pl.when(self.collects & self.keeps)
        def _():
            do(self.full, True)

        @pl.when(self.collects & jnp.logical_not(self.keeps))
        def _():
            do(self.gat, False)

    def send_ring(self):
        def do(ref, keeps):
            for g in range(len(self.groups)):
                for d in range(self.me.dp - 1):
                    self.out(g, d, ref).start()

        self.both(do)

    def send_own(self, g):
        def do(ref, keeps):
            self.hand(g, 0, ref, True).start()
            if keeps:
                self.local(g).start()
            else:
                self.hand(g, 0, ref, False).start()

        self.both(do)

    def forward(self, g, blocks=None):
        def do(ref, keeps):
            for d in range(self.me.dp - 1) if blocks is None else blocks:
                self.out(g, d, ref).wait_recv()
                self.hand(g, d + 1, ref, True).start()
                if not keeps:
                    self.hand(g, d + 1, ref, False).start()

        self.both(do)

    def ready(self, g):
        me = self.me

        @pl.when(self.collects & self.keeps)
        def _():
            self.local(g).wait()

        @pl.when(me.s != me.y)
        def _():
            for d in range(me.dp):
                self.hand(g, d, self.full, True).wait_recv()

        @pl.when((me.s == me.y) & jnp.logical_not(self.collects))
        def _():
            for d in range(me.dp):
                self.hand(g, d, self.full, False).wait_recv()

    def finish(self):
        def do(ref, keeps):
            for g in range(len(self.groups)):
                for d in range(self.me.dp - 1):
                    self.out(g, d, ref).wait_send()
                for d in range(self.me.dp):
                    self.hand(g, d, ref, True).wait_send()
                    if not keeps:
                        self.hand(g, d, ref, False).wait_send()

        self.both(do)

    @staticmethod
    def scratch(dp, n):
        return [DMA((n,)), DMA((n, dp - 1)), DMA((n, dp - 1))] + [DMA((n, dp))] * 4


class GradReduce:
    def __init__(self, me, layer, src, mine, got, across, sb, rb, own, sems):
        self.me, self.layer, self.src, self.mine, self.got, self.across = me, layer, src, mine, got, across
        self.sb, self.rb, self.own = sb, rb, own
        self.hss, self.hrs, self.yss, self.yrs, self.pss, self.prs = sems
        self.rows = own.shape[0]
        self.sums = me.s == layer
        self.holds = me.y == layer

    @staticmethod
    def scratch(dp):
        return [DMA((1,)), DMA((1,)), DMA((dp,)), DMA((dp,)), DMA((dp - 1,)), DMA((dp - 1,))]

    def hand(self):
        return push(self.src, self.got, self.hss.at[0], self.hrs.at[0], self.me.mate)

    def zz(self, d):
        return (self.me.z + d + 1) % self.me.dp

    def over(self, d):
        rr = ds(self.zz(d) * self.rows, self.rows)
        peer = self.me.across_core(self.layer)
        return push(self.src.at[rr], self.across.at[rr], self.yss.at[d], self.yrs.at[d], peer)

    def out(self, d):
        return push(self.sb.at[d], self.rb.at[d], self.pss.at[d], self.prs.at[d], self.me.ring[d])

    def send(self):
        me = self.me

        @pl.when(me.s != me.y)
        def _():
            for d in range(me.dp):
                self.over(d).start()

        @pl.when((me.s == me.y) & jnp.logical_not(self.sums))
        def _():
            self.hand().start()

    def step(self, d):
        me = self.me

        @pl.when(self.sums)
        def _():
            if d == 0:

                @pl.when(jnp.logical_not(self.holds))
                def _():
                    self.hand().wait_recv()

            self.over(d).wait_recv()
            last = d == me.dp - 1

            def add(ref):
                def body(i, _):
                    rr = ds(self.zz(d) * self.rows + i * 16, 16)
                    value = ref[rr, :].astype(F32) + self.across[rr, :].astype(F32)
                    if last:
                        self.own[ds(i * 16, 16), :] = value
                    else:
                        self.sb[d, ds(i * 16, 16), :] = value.astype(BF)
                    return 0

                lax.fori_loop(0, self.rows // 16, body, 0)

            if self.mine is self.got:
                add(self.mine)
            else:

                @pl.when(self.holds)
                def _():
                    add(self.mine)

                @pl.when(jnp.logical_not(self.holds))
                def _():
                    add(self.got)

            if not last:
                self.out(d).start()

    def collect(self):
        me = self.me

        @pl.when(self.sums)
        def _():
            for d in range(me.dp - 1):
                self.out(d).wait_recv()

                def add(i, _, d=d):
                    rr = ds(i * 16, 16)
                    self.own[rr, :] += self.rb[d, rr, :].astype(F32)
                    return 0

                lax.fori_loop(0, self.rows // 16, add, 0)
            for d in range(me.dp - 1):
                self.out(d).wait_send()

    def finish(self):
        me = self.me

        @pl.when(me.s != me.y)
        def _():
            for d in range(me.dp):
                self.over(d).wait_send()

        @pl.when((me.s == me.y) & jnp.logical_not(self.sums))
        def _():
            self.hand().wait_send()


class VectorGather:
    def __init__(self, me, sv, buf, ss, rs, own):
        self.me, self.sv, self.buf, self.ss, self.rs, self.own = me, sv, buf, ss, rs, own

    def local(self):
        me = self.me
        return pltpu.make_async_copy(self.sv, self.buf.at[me.s, me.t, me.z], self.own)

    def stage(self, n):
        me = self.me
        if n == 0:
            dst = self.buf.at[me.s, me.t, me.z]
            return [push(self.sv, dst, self.ss.at[d], self.rs.at[d], peer) for d, peer in enumerate(me.ring)]
        base = me.dp - 1
        if n == 1:
            ref = self.buf.at[me.s, me.t]
            return [
                push(ref, ref, self.ss.at[base + d], self.rs.at[base + d], peer) for d, peer in enumerate(me.group)
            ]
        i = base + me.tensor - 1
        ref = self.buf.at[me.s]
        return [push(ref, ref, self.ss.at[i], self.rs.at[i], me.mate)]

    def send(self, n):
        if n == 0:
            self.local().start()
        for c in self.stage(n):
            c.start()

    def wait(self, n):
        if n == 0:
            self.local().wait()
        for c in self.stage(n):
            c.wait_recv()

    def finish(self):
        for n in range(3):
            for c in self.stage(n):
                c.wait_send()

    def build(self, vecs, heads, own, qw, fw):
        me, buf = self.me, self.buf
        for layer in range(2):
            wide = [buf[layer, tt, zz, 0:8, :][:, 0:own] for zz in range(me.dp) for tt in range(me.tensor)]
            vecs[layer, 0:8, :] = jnp.concatenate(wide, axis=1)
            here = [buf[layer, me.quarter, zz] for zz in range(me.dp)]
            by = [jnp.concatenate([p[6 + h : 7 + h, 0:qw] for p in here], axis=1) for h in range(heads)]
            qb = []
            for part in range(3):
                qb += [b[:, part * HD : (part + 1) * HD] for b in by] + [jnp.zeros((1, HW - heads * HD), F32)]
            vecs[layer, 6:7, :] = jnp.concatenate(qb, axis=1)
            fb = [p[6 + heads + h : 7 + heads + h, 0:fw] for h in range(heads) for p in here]
            vecs[layer, 7:8, :] = jnp.concatenate(fb, axis=1)


class VectorReduce:
    def __init__(self, me, va, vr, ss, rs):
        self.me, self.va, self.vr, self.ss, self.rs = me, va, vr, ss, rs

    def stage(self, n):
        me, va, vr, ss, rs = self.me, self.va, self.vr, self.ss, self.rs
        peers, base = [([me.across], 0), (me.ring, 1), ([me.mate, me.beside, me.beside_mate], me.dp)][n]
        return [push(va.at[n], vr.at[base + d], ss.at[base + d], rs.at[base + d], p) for d, p in enumerate(peers)]

    def send(self, n):
        for c in self.stage(n):
            c.start()

    def add(self, n, out):
        base = [0, 1, self.me.dp][n]
        for c in self.stage(n):
            c.wait_recv()
        if n < 2:
            total = self.va[n]
            for d in range(len(self.stage(n))):
                total = total + self.vr[base + d]
            out[...] = total
            return
        mine, mate = self.va[2], self.vr[base]
        row = lax.broadcasted_iota(jnp.int32, mine.shape, 0)
        quarter = jnp.where(self.me.s == self.me.y, mine, mate)
        out[...] = jnp.where(row % 8 < 6, mine + mate + self.vr[base + 1] + self.vr[base + 2], quarter)

    def finish(self):
        for n in range(3):
            for c in self.stage(n):
                c.wait_send()


def document_tables(seg, live, fr_ref, tab, srow, kcol):
    seq = seg.shape[1]
    count = lax.broadcasted_iota(jnp.int32, seg.shape, 1)
    start = jnp.zeros_like(seg)
    for doc in range(DOCS - 1):
        before = jnp.sum(jnp.where(seg == doc, 1.0, 0.0), axis=1, keepdims=True).astype(jnp.int32)
        start = start + jnp.where(seg > doc, before, 0)
    ang = fr_ref[:, 0:1] * (count - start).astype(F32)
    cs, sn = jnp.cos(ang), jnp.sin(ang)
    one = jnp.ones((HD - ROT, seq), F32)
    tab[:, 0:128] = jnp.concatenate([cs, cs, one] * 2, axis=0).T
    tab[:, 128:256] = jnp.concatenate([-sn, sn, jnp.zeros_like(one)] * 2, axis=0).T
    srow[...] = jnp.broadcast_to(seg, srow.shape)
    keys = jnp.where(count < live * LIVE, seg, -1).astype(F32)
    for b in range(seq // QB):
        part = jnp.broadcast_to(keys[:, b * QB : (b + 1) * QB], (128, QB))
        kcol[b * QB : (b + 1) * QB, :] = part.T.astype(jnp.int32)


QKV, FC1, FC2, OUT = 0, 1, 2, 3


def columns(model, ff):
    return {"qkv": 0, "fc1": 3 * HW, "fc2": 3 * HW + ff, "out": 3 * HW + 2 * ff, "end": 3 * HW + 2 * ff + HW}


def project_norm(r0, half, hf, vec, n1, n2):
    rows = ds(r0, half)
    xc, r = norm_stats(hf[rows, :].astype(F32))
    xh = xc * r
    n1[rows, :] = (xh * vec[0:1, :] + vec[1:2, :]).astype(BF)
    n2[rows, :] = (xh * vec[3:4, :] + vec[4:5, :]).astype(BF)


def project_qkv(r0, half, wqkv, vec, tab, n1, q, k, v):
    rows = ds(r0, half)
    a = n1[rows, :]
    for part, dst in enumerate((q, k, v)):
        cols = slice(part * HW, (part + 1) * HW)
        y = dot(a, wqkv[:, cols]) + vec[6:7, cols]
        if part < 2:
            y = turn_lanes(y, tab[rows, :], 1)
        if part == 0:
            y = y * 0.125
        dst[rows, :] = y.astype(BF)


def project_fc1(r0, half, wfc1, vec, n2, g, gp):
    rows = ds(r0, half)
    a = n2[rows, :]
    for b in range(wfc1.shape[1] // 256):
        cols = slice(b * 256, (b + 1) * 256)
        y = dot(a, wfc1[:, cols]) + vec[7:8, cols]
        cdf = 0.5 + 0.5 * lax.erf(y * 0.7071067811865476)
        g[rows, cols] = (y * cdf).astype(BF)
        gp[rows, cols] = (cdf + y * jnp.exp(-0.5 * y * y) * 0.3989422804014327).astype(BF)


def branch_out(r0, half, o, g, wout, wfc2, part):
    rows = ds(r0, half)
    for b in range(part.shape[1] // 256):
        cols = slice(b * 256, (b + 1) * 256)
        y = dg(o[rows, :], wout[cols, :], 1, 1) + dg(g[rows, :], wfc2[cols, :], 1, 1)
        part[rows, cols] = y.astype(BF)


def back_head(r0, half, dyf, hf, g, gp, n2, o, wfc1, wfc2, wout, vec, do, e2, da, acc, vg):
    rows = ds(r0, half)
    model, ff = wfc1.shape
    dy = dyf[rows, :]
    for b in range(ff // 256):
        cols = slice(b * 256, (b + 1) * 256)
        y = dot(dy, wfc2[:, cols]) * gp[rows, cols].astype(F32)
        low = y.astype(BF)
        da[:, cols] = low
        vg[7:8, cols] += jnp.sum(low.astype(F32), axis=0, keepdims=True)
    do[rows, :] = dot(dy, wout[...]).astype(BF)
    xc, r = norm_stats(hf[rows, :].astype(F32))
    xh = xc * r
    for b in range(model // 256):
        cols = slice(b * 256, (b + 1) * 256)
        dn = dg(da[...], wfc1[cols, :], 1, 1)
        vg[3:4, cols] += jnp.sum(dn * xh[:, cols], axis=0, keepdims=True)
        vg[4:5, cols] += jnp.sum(dn, axis=0, keepdims=True)
        e2[rows, cols] = (dn * vec[3:4, cols]).astype(BF)
    n2t = n2[rows, :].T
    dyt = dy.T
    for b in range(ff // 256):
        cols = slice(b * 256, (b + 1) * 256)
        acc[:, cols] += dot(n2t, da[:, cols])
        acc[:, ff + b * 256 : ff + (b + 1) * 256] += dot(dyt, g[rows, cols])
    acc[:, 2 * ff :] += dot(dyt, o[rows, :])


def back_tail(r0, half, dmix, hf, e2, wqkv, vec, part, vg):
    rows = ds(r0, half)
    dm = dmix[rows, :]
    vg[6:7, :] += jnp.sum(dm.astype(F32), axis=0, keepdims=True)
    xc, r = norm_stats(hf[rows, :].astype(F32))
    xh = xc * r
    for b in range(part.shape[1] // 256):
        cols = slice(b * 256, (b + 1) * 256)
        dn = dg(dm, wqkv[cols, :], 1, 1)
        vg[0:1, cols] += jnp.sum(dn * xh[:, cols], axis=0, keepdims=True)
        vg[1:2, cols] += jnp.sum(dn, axis=0, keepdims=True)
        part[rows, cols] = (dn * vec[0:1, cols] + e2[rows, cols].astype(F32)).astype(BF)


def qkv_grad(n1, dmix, acc, half):
    acc[...] = jnp.zeros_like(acc)

    def body(i, _):
        rows = ds(i * half, half)
        n1t = n1[rows, :].T
        for b in range(3):
            cols = slice(b * HW, (b + 1) * HW)
            acc[:, cols] += dot(n1t, dmix[rows, cols])
        return 0

    lax.fori_loop(0, n1.shape[0] // half, body, 0)


def store_low(acc, out):
    def body(i, _):
        rr = ds(i * SUB, SUB)
        out[rr, :] = acc[rr, :].astype(BF)
        return 0

    lax.fori_loop(0, acc.shape[0] // SUB, body, 0)


def residual_out(sc, own, vec, write, after=None):
    for a in range(2):
        sc.arrive(a)

        def body(i, _, a=a):
            base = own[ds(sc.own(sc.side(a)) + i * SUB, SUB), :].astype(F32)
            write(a, i, (base + sc.total(a, i) + vec[2:3, :] + vec[5:6, :]).astype(BF))
            return 0

        lax.fori_loop(0, sc.half // SUB, body, 0)
        if after is not None:
            after(a)


def grad_out(sc, dy, hf, vec, write, after=None):
    for a in range(2):
        sc.arrive(a)

        def body(i, _, a=a):
            rr = ds(sc.own(sc.side(a)) + i * SUB, SUB)
            xc, r = norm_stats(hf[rr, :].astype(F32))
            xh = xc * r
            e = sc.total(a, i)
            m1 = jnp.mean(e, axis=-1, keepdims=True)
            m2 = jnp.mean(e * xh, axis=-1, keepdims=True)
            write(a, i, (dy(a, i).astype(F32) + r * (e - m1 - xh * m2)).astype(BF))
            return 0

        lax.fori_loop(0, sc.half // SUB, body, 0)
        if after is not None:
            after(a)


def column_sum(tok, ref, vg, row):
    total = jnp.zeros((1, ref.shape[1]), F32)
    for a in range(2):

        def body(i, acc, a=a):
            return acc + jnp.sum(ref[ds(tok.own(a) + i * SUB, SUB), :].astype(F32), axis=0, keepdims=True)

        total = lax.fori_loop(0, tok.half // SUB, body, total)
    vg[row : row + 1, :] = total


def load(pairs, sem):
    copies = [pltpu.make_async_copy(a, b, sem.at[i]) for i, (a, b) in enumerate(pairs)]
    for c in copies:
        c.start()
    return copies


def params(cid):
    return pltpu.CompilerParams(collective_id=cid, has_side_effects=True, vmem_limit_bytes=67043328)


def cost(us):
    return pl.CostEstimate(flops=int(us * 8e8), bytes_accessed=0, transcendentals=0)


class Stores:
    def __init__(self, pairs, half, sem):
        self.pairs, self.half, self.sem = pairs, half, sem

    def copy(self, n, r0, i):
        src, dst = self.pairs[n]
        rows = ds(r0, self.half)
        return pltpu.make_async_copy(src.at[rows], dst.at[rows], self.sem.at[n, i])

    def start(self, which, r0, i):
        for n in which:
            self.copy(n, r0, i).start()

    def finish(self):
        def body(i, _):
            for n in range(len(self.pairs)):
                self.copy(n, i * self.half, i).wait()
            return 0

        lax.fori_loop(0, 8, body, 0)


def in_kernel(
    cfg, in_ref, cot_ref, seg_ref, live, w_ref, sv_ref, fr_ref,
    hf_o, n1_o, n2_o, g_o, gp_o, tab_o, w_o, q_o, k_o, v_o, cf_o, vecs, srow, kcol,
    hf, n1, n2, g, gp, tab, q, k, v, wfull, gat, vb, cot, gss, grs, css, crs, yss, yrs, lsem, ssem, vss, vrs, *wsems,
):
    col, dp, tensor = cfg["col"], cfg["dp"], cfg["tensor"]
    me = Mesh(dp, tensor)
    ga = Gather(me, hf, gss, grs, me.y)
    gc = Gather(me, cf_o, css, crs, me.y)
    half = ga.half
    part = ds(me.s * half, half)
    first = pltpu.make_async_copy(in_ref.at[me.y, 0, part], hf.at[ds(ga.own(me.y), half)], lsem.at[0])
    first.start()
    up = pltpu.make_async_copy(cot_ref.at[me.y, 0, part], cot, lsem.at[4])
    up.start()
    greet([me.mate, me.across_mate] + me.ring + me.group)
    over = [
        push(ref.at[1 - me.y, 0, part], full.at[ds(ga.own(me.y), half)], yss.at[n], yrs.at[n], me.across)
        for n, (ref, full) in enumerate(((in_ref, hf), (cot_ref, cf_o)))
    ]
    wg = WeightGather(me, 0, w_ref, wfull, gat, cfg["groups"], wsems)
    vg = VectorGather(me, sv_ref, vb, vss, vrs, lsem.at[1])
    st = Stores([(hf, hf_o), (n1, n1_o), (n2, n2_o), (g, g_o), (gp, gp_o), (q, q_o), (k, k_o), (v, v_o)], half, ssem)
    vg.send(0)
    wg.send_ring()
    first.wait()
    document_tables(seg_ref[me.y], live[me.y, 0], fr_ref, tab, srow, kcol)
    vg.wait(0)
    vg.send(1)
    ga.start(0)
    over[0].start()
    wg.send_own(0)
    tab_out = pltpu.make_async_copy(tab, tab_o, lsem.at[2])
    tab_out.start()
    vg.wait(1)
    vg.send(2)
    up.wait()
    cot_out = pltpu.make_async_copy(cot, cf_o.at[ds(gc.own(me.y), half)], lsem.at[5])
    cot_out.start()
    vg.wait(2)
    vg.build(vecs, cfg["heads"], cfg["own"], cfg["qw"], cfg["fw"])
    vec = vecs.at[0]

    def norm(r0, i):
        project_norm(r0, half, hf, vec, n1, n2)
        st.start((0, 1, 2), r0, i)

        @pl.when(i == 0)
        def _():
            over[0].wait_recv()
            ga.start(1)

        @pl.when(i == 1)
        def _():
            wg.forward(0)
            wg.send_own(1)
            wg.send_own(2)

    ga.run(norm)
    cot_out.wait()
    gc.start(0)
    wg.ready(0)

    def qkv(i, _):
        r0 = ga.order(i)
        project_qkv(r0, half, wfull.at[:, 0 : col["fc1"]], vec, tab, n1, q, k, v)
        st.start((5, 6, 7), r0, i)
        return 0

    lax.fori_loop(0, 8, qkv, 0)
    wg.forward(1)
    over[1].start()
    wg.ready(1)

    def fc1(i, _):
        r0 = ga.order(i)
        project_fc1(r0, half, wfull.at[:, col["fc1"] : col["fc2"]], vec, n2, g, gp)
        st.start((3, 4), r0, i)

        @pl.when(i == 6)
        def _():
            wg.forward(2)

        return 0

    lax.fori_loop(0, 8, fc1, 0)
    gc.step(2)
    gc.step(4)
    over[1].wait_recv()
    gc.start(1)
    st.finish()
    tab_out.wait()
    wg.ready(2)
    w_out = pltpu.make_async_copy(wfull, w_o, lsem.at[3])
    w_out.start()
    for n in (3, 5, 6, 7):
        gc.step(n)
    wg.finish()
    vg.finish()
    gc.finish()
    for c in over:
        c.wait_send()
    w_out.wait()


def layer_in(cfg, inputs, cotangent, segments, live, w, sv, fr):
    seq, model, ff = segments.shape[2], inputs.shape[3], cfg["ff"]
    dp, tensor = cfg["dp"], cfg["tensor"]
    rows, hidden = sds((seq, model), BF), sds((seq, ff), BF)
    heads = sds((seq, HW), BF)
    nv = dp - 1 + tensor
    wide, wide_h, wide_q = pltpu.VMEM((seq, model), BF), pltpu.VMEM((seq, ff), BF), pltpu.VMEM((seq, HW), BF)
    weights = pltpu.VMEM((model, w.shape[1]), BF)
    return pl.pallas_call(
        functools.partial(in_kernel, cfg),
        out_shape=(rows, rows, rows, hidden, hidden, sds((seq, 256), F32), sds((model, w.shape[1]), BF),
                   heads, heads, heads, rows,
                   sds((2, 8, model), F32), sds((8, seq), jnp.int32), sds((seq, 128), jnp.int32)),
        in_specs=[ANY, ANY, VMEM, SMEM, VMEM, VMEM, VMEM],
        out_specs=(ANY,) * 11 + (VMEM,) * 3,
        scratch_shapes=[
            wide, wide, wide, wide_h, wide_h, pltpu.VMEM((seq, 256), F32), wide_q, wide_q, wide_q,
            weights, weights, pltpu.VMEM((2, tensor, dp) + sv.shape, F32),
            pltpu.VMEM((seq // 8, model), BF),
            DMA((6,)), DMA((6,)), DMA((6,)), DMA((6,)), DMA((2,)), DMA((2,)), DMA((6,)), DMA((8, 8)),
            DMA((nv,)), DMA((nv,)),
        ]
        + WeightGather.scratch(dp, 3),
        compiler_params=params(2),
        cost_estimate=cost(45),
        name="layer_in",
    )(inputs, cotangent, segments, live, w, sv, fr)


def mid_kernel(
    cfg, q_in, k_in, v_in, srow, kcol, g_in, x_in, w_ref, w0, vecs, tab_in,
    o_o, lse, hf_o, n1_o, n2_o, g_o, gp_o, w_o, q_o, k_o, v_o,
    wout, wfc2, hf, n1, n2, g, gp, tab, wfull, gat, q, k, v, o, vt, s_scr,
    part, mr, xr, sss, srs, gss, grs, lsem, ssem, osem, *wsems,
):
    col, heads = cfg["col"], cfg["heads"]
    me = Mesh(cfg["dp"], cfg["tensor"])
    sc = Scatter(me, part, mr, xr, sss, srs)
    ga = Gather(me, hf, gss, grs)
    half = sc.half
    loads = load(
        [
            (v_in, v),
            (q_in, q),
            (k_in, k),
            (w0.at[:, col["out"] : col["end"]], wout),
            (w0.at[:, col["fc2"] : col["out"]], wfc2),
            (g_in, g),
            (tab_in, tab),
        ]
        + [(x_in.at[ds(sc.own(a), half)], hf.at[ds(sc.own(a), half)]) for a in range(2)],
        lsem,
    )
    greet([me.mate, me.beside, me.across, me.across_mate] + me.ring)
    wg = WeightGather(me, 1, w_ref, wfull, gat, cfg["groups"], wsems)
    wg.send_ring()
    for n in range(3):
        wg.send_own(n)
    loads[0].wait()
    turn_blocks(v, vt)
    for c in loads[1:]:
        c.wait()
    st = Stores([(hf, hf_o), (n1, n1_o), (n2, n2_o), (g, g_o), (gp, gp_o), (q, q_o), (k, k_o), (v, v_o)], half, ssem)
    st_o = Stores([(o, o_o)], half, osem)

    def out(r0, i):
        b = r0 // QB
        attn_fwd_block(b, jnp.maximum(b - DOC_MAX // QB, 0), b, heads, q, k, vt, srow, kcol, s_scr, o, lse)
        st_o.start((0,), r0, i)
        branch_out(r0, half, o, g, wout, wfc2, part)

        @pl.when(i == 6)
        def _():
            wg.forward(0)

    sc.run(out)

    def write(a, i, value):
        hf[ds(sc.own(a) + i * SUB, SUB), :] = value

    residual_out(sc, hf, vecs.at[0], write, ga.start)
    wg.forward(1)
    vec = vecs.at[1]

    def fc1(i):
        r0 = ga.order(i)
        project_fc1(r0, half, wfull.at[:, col["fc1"] : col["fc2"]], vec, n2, g, gp)
        st.start((3, 4), r0, i)

    def work(r0, i):
        project_norm(r0, half, hf, vec, n1, n2)

        @pl.when(i == 0)
        def _():
            wg.ready(0)

        project_qkv(r0, half, wfull.at[:, 0 : col["fc1"]], vec, tab, n1, q, k, v)
        st.start((0, 1, 2, 5, 6, 7), r0, i)

        @pl.when(i == 4)
        def _():
            wg.ready(1)

        @pl.when(i >= 4)
        def _():
            fc1(i - 4)

        @pl.when(i == 5)
        def _():
            wg.forward(2)

    ga.run(work)

    def late(i, _):
        fc1(i)
        return 0

    lax.fori_loop(4, 8, late, 0)
    st.finish()
    wg.ready(2)
    w_out = pltpu.make_async_copy(wfull, w_o, lsem.at[0])
    w_out.start()
    sc.finish()
    wg.finish()
    st_o.finish()
    w_out.wait()


def layer_mid(cfg, q, k, v, srow, kcol, g, xf, w, w0, vecs, tab):
    seq, model, ff = tab.shape[0], xf.shape[1], cfg["ff"]
    rows, hidden, heads = sds((seq, model), BF), sds((seq, ff), BF), sds((seq, HW), BF)
    wide, wide_h, wide_q = pltpu.VMEM((seq, model), BF), pltpu.VMEM((seq, ff), BF), pltpu.VMEM((seq, HW), BF)
    return pl.pallas_call(
        functools.partial(mid_kernel, cfg),
        out_shape=(heads, sds((8, seq), F32), rows, rows, rows, hidden, hidden, sds(w0.shape, BF), heads, heads, heads),
        in_specs=[ANY, ANY, ANY, VMEM, VMEM, ANY, ANY, VMEM, ANY, VMEM, ANY],
        out_specs=(ANY, VMEM) + (ANY,) * 9,
        scratch_shapes=[
            pltpu.VMEM((model, HW), BF), pltpu.VMEM((model, ff), BF),
            wide, wide, wide, wide_h, wide_h, pltpu.VMEM((seq, 256), F32),
            pltpu.VMEM(w0.shape, BF), pltpu.VMEM(w0.shape, BF),
            wide_q, wide_q, wide_q, wide_q, pltpu.VMEM((HW, seq), BF),
            pltpu.VMEM((cfg["heads"], DOC_MAX + QB, QB), F32),
        ]
        + scatter_scratch(seq, model)
        + [DMA((6,)), DMA((6,)), DMA((9,)), DMA((8, 8)), DMA((1, 8))]
        + WeightGather.scratch(cfg["dp"], 3),
        compiler_params=params(3),
        cost_estimate=cost(70),
        name="layer_mid",
    )(q, k, v, srow, kcol, g, xf, w, w0, vecs, tab)


def turn_kernel(
    cfg, o_in, g_in, hf_in, cf, w1, vecs, n2_in, gp_in, y_o, do_o, e2_o, gr_o, vg,
    o, g, hf, dyf, n2, gp, e2, do, y, gr, wout, wfc2, wfc1, da, acc,
    part, mr, xr, sss, srs, lsem, ssem,
):
    col = cfg["col"]
    me = Mesh(cfg["dp"], cfg["tensor"])
    sc = Scatter(me, part, mr, xr, sss, srs)
    half = sc.half
    loads = load(
        [
            (w1.at[:, col["out"] : col["end"]], wout),
            (w1.at[:, col["fc2"] : col["out"]], wfc2),
            (o_in, o),
            (g_in, g),
            (w1.at[:, col["fc1"] : col["fc2"]], wfc1),
            (cf, dyf),
            (gp_in, gp),
            (hf_in, hf),
            (n2_in, n2),
        ],
        lsem,
    )
    greet([me.mate, me.beside])
    for c in loads[:4]:
        c.wait()
    vec = vecs.at[1]
    st = Stores([(e2, e2_o), (do, do_o)], half, ssem)

    def early():
        vg[...] = jnp.zeros_like(vg)
        acc[...] = jnp.zeros_like(acc)
        for c in loads[4:]:
            c.wait()

        def head(i, _):
            r0 = i * half
            back_head(r0, half, dyf, hf, g, gp, n2, o, wfc1, wfc2, wout, vec, do, e2, da, acc, vg)
            st.start((0, 1), r0, i)
            return 0

        lax.fori_loop(0, 8, head, 0)

    sc.run(lambda r0, i: branch_out(r0, half, o, g, wout, wfc2, part), early)
    column_sum(sc, dyf, vg, 2)
    store_low(acc, gr)
    gr_out = pltpu.make_async_copy(gr, gr_o, lsem.at[0])
    gr_out.start()

    def write(a, i, value):
        y[a, ds(i * SUB, SUB), :] = value

    residual_out(sc, hf, vec, write)
    y_out = pltpu.make_async_copy(y, y_o, lsem.at[1])
    y_out.start()
    sc.finish()
    st.finish()
    gr_out.wait()
    y_out.wait()


def layer_turn(cfg, o, g, hf, cf, w1, vecs, n2, gp):
    seq, model = hf.shape
    ff = cfg["ff"]
    wide, hidden, heads = pltpu.VMEM((seq, model), BF), pltpu.VMEM((seq, ff), BF), pltpu.VMEM((seq, HW), BF)
    owned = (2, seq // 8, model)
    return pl.pallas_call(
        functools.partial(turn_kernel, cfg),
        out_shape=(
            sds(owned, BF),
            sds((seq, HW), BF),
            sds((seq, model), BF),
            sds((model, 2 * ff + HW), BF),
            sds((8, model), F32),
        ),
        in_specs=[ANY] * 5 + [VMEM, ANY, ANY],
        out_specs=(ANY,) * 4 + (VMEM,),
        scratch_shapes=[
            heads, hidden, wide, wide, wide, hidden, wide, heads, pltpu.VMEM(owned, BF),
            pltpu.VMEM((model, 2 * ff + HW), BF),
            pltpu.VMEM((model, HW), BF), pltpu.VMEM((model, ff), BF), pltpu.VMEM((model, ff), BF),
            pltpu.VMEM((seq // 8, ff), BF), pltpu.VMEM((model, 2 * ff + HW), F32),
        ]
        + scatter_scratch(seq, model)
        + [DMA((9,)), DMA((2, 8))],
        compiler_params=params(4),
        cost_estimate=cost(40),
        name="layer_turn",
    )(o, g, hf, cf, w1, vecs, n2, gp)


def back_kernel(
    cfg, dm_in, e2_in, cf, hf_in, n1_in, w1, w0, vecs, xf_in, g_in, gp_in, n2_in, o_in, gr1,
    dh_o, e2_o, do_o, vgf, vgd, out1_o, outq_o, gr_o,
    dmix, o, do, a, b, e2, g, gp, wqkv, wout, wfc2, wfc1, dhf, da, acc, gq, gr, got, gotq, acrq,
    sb, rb, sbq, rbq, out1, outq, part, mr, xr, sss, srs, gss, grs, lsem, ssem, *rsems,
):
    col, dp = cfg["col"], cfg["dp"]
    me = Mesh(dp, cfg["tensor"])
    ga = Gather(me, dhf, gss, grs)
    sc = Scatter(me, part, mr, xr, sss, srs)
    half = sc.half
    own = [ds(sc.own(n), half) for n in range(2)]
    loads = load(
        [
            (w1.at[:, col["qkv"] : col["fc1"]], wqkv),
            (dm_in, dmix),
            (hf_in, a),
            (e2_in, e2),
            (n1_in, b),
            (w0.at[:, col["out"] : col["end"]], wout),
            (w0.at[:, col["fc2"] : col["out"]], wfc2),
            (w0.at[:, col["fc1"] : col["fc2"]], wfc1),
            (g_in, g),
            (gp_in, gp),
            (o_in, o),
        ]
        + [(cf.at[rr], dhf.at[rr]) for rr in own],
        lsem,
    )
    gr_load = pltpu.make_async_copy(gr1, gr, lsem.at[13])
    holds = (me.s == 1) & (me.y == 1)

    @pl.when(holds)
    def _():
        gr_load.start()

    greet([me.mate, me.beside, me.across, me.across_mate] + me.ring)
    red1 = GradReduce(me, 1, gr1, gr, gr, got, sb, rb, out1, rsems[:6])
    redq = GradReduce(me, 1, gq, gq, gotq, acrq, sbq, rbq, outq, rsems[6:])
    st = Stores([(e2, e2_o), (do, do_o), (dhf, dh_o)], half, ssem)
    red1.send()
    vgf[...] = jnp.zeros_like(vgf)
    vgd[...] = jnp.zeros_like(vgd)
    for c in loads[:4]:
        c.wait()

    def early():
        loads[4].wait()
        small = acc.at[:, 0 : 3 * HW]
        qkv_grad(b, dmix, small, half)
        store_low(small, gq)
        redq.send()

        @pl.when(holds)
        def _():
            gr_load.wait()

        red1.step(0)

    sc.run(lambda r0, i: back_tail(r0, half, dmix, a, e2, wqkv, vecs.at[1], part, vgf), early)
    acc[...] = jnp.zeros_like(acc)
    again = pltpu.make_async_copy(n2_in, b, lsem.at[14])
    again.start()
    for c in loads[5:]:
        c.wait()
    for d in range(1, dp // 2):
        red1.step(d)

    def write(n, i, value):
        dhf[ds(sc.own(n) + i * SUB, SUB), :] = value

    grad_out(sc, lambda n, i: dhf[ds(sc.own(n) + i * SUB, SUB), :], a, vecs.at[1], write, ga.start)
    other = pltpu.make_async_copy(xf_in, a, lsem.at[15])
    other.start()
    again.wait()
    other.wait()

    def work(r0, i):
        back_head(r0, half, dhf, a, g, gp, b, o, wfc1, wfc2, wout, vecs.at[0], do, e2, da, acc, vgd)
        st.start((0, 1, 2), r0, i)

        @pl.when(i == 1)
        def _():
            for d in range(dp // 2, dp - 1):
                red1.step(d)

        @pl.when(i == 3)
        def _():
            red1.step(dp - 1)

        @pl.when(i == 5)
        def _():
            redq.step(0)

    ga.run(work)
    for d in range(1, dp):
        redq.step(d)
    store_low(acc, gr)
    gr_out = pltpu.make_async_copy(gr, gr_o, lsem.at[0])
    gr_out.start()
    column_sum(sc, dhf, vgd, 2)
    red1.collect()
    redq.collect()
    outs = [pltpu.make_async_copy(out1, out1_o, lsem.at[1]), pltpu.make_async_copy(outq, outq_o, lsem.at[2])]
    for c in outs:
        c.start()
    red1.finish()
    redq.finish()
    sc.finish()
    st.finish()
    gr_out.wait()
    for c in outs:
        c.wait()


def layer_back(cfg, dmix, e2, cf, hf, n1, w1, w0, vecs, xf, g, gp, n2, o, gr1):
    seq, model = hf.shape
    ff, dp = cfg["ff"], cfg["dp"]
    rows, nr, nq = model // dp, 2 * ff + HW, 3 * HW
    wide, hidden, heads = pltpu.VMEM((seq, model), BF), pltpu.VMEM((seq, ff), BF), pltpu.VMEM((seq, HW), BF)
    return pl.pallas_call(
        functools.partial(back_kernel, cfg),
        out_shape=(
            sds((seq, model), BF),
            sds((seq, model), BF),
            sds((seq, HW), BF),
            sds((8, model), F32),
            sds((8, model), F32),
            sds((rows, nr), F32),
            sds((rows, nq), F32),
            sds((model, nr), BF),
        ),
        in_specs=[ANY] * 7 + [VMEM] + [ANY] * 6,
        out_specs=(ANY, ANY, ANY, VMEM, VMEM, ANY, ANY, ANY),
        scratch_shapes=[
            pltpu.VMEM((seq, nq), BF), heads, heads, wide, wide, wide, hidden, hidden,
            pltpu.VMEM((model, nq), BF), pltpu.VMEM((model, HW), BF), pltpu.VMEM((model, ff), BF),
            pltpu.VMEM((model, ff), BF), wide, pltpu.VMEM((seq // 8, ff), BF), pltpu.VMEM((model, nr), F32),
            pltpu.VMEM((model, nq), BF), pltpu.VMEM((model, nr), BF), pltpu.VMEM((model, nr), BF),
            pltpu.VMEM((model, nq), BF), pltpu.VMEM((model, nq), BF),
            pltpu.VMEM((dp - 1, rows, nr), BF), pltpu.VMEM((dp - 1, rows, nr), BF),
            pltpu.VMEM((dp - 1, rows, nq), BF), pltpu.VMEM((dp - 1, rows, nq), BF),
            pltpu.VMEM((rows, nr), F32), pltpu.VMEM((rows, nq), F32),
        ]
        + scatter_scratch(seq, model)
        + [DMA((6,)), DMA((6,)), DMA((16,)), DMA((3, 8))]
        + GradReduce.scratch(dp) * 2,
        compiler_params=params(5),
        cost_estimate=cost(70),
        name="layer_back",
    )(dmix, e2, cf, hf, n1, w1, w0, vecs, xf, g, gp, n2, o, gr1)


def last_kernel(
    cfg, q_in, k_in, v_in, o_in, do_in, lse, srow, kcol, tab_in, e2_in, dh_in, xf_in, n1_in, w0, vecs, vf1, vd1, vd0,
    gr0, out1, outq, hf_in, y_in, so, ig, fq_o, fr_o, vec_o,
    q, k, v, o, do, tab, kt, dk, dv, dmix, dh, dx, xf, n1, e2, wqkv, gq, gotq, acrq, sbq, rbq, gr, got, sb, rb, fq, fr,
    vgf, va, vr, vout, part, mr, xr, sss, srs, lsem, vss, vrs, oss, ors, *rsems,
):
    col, heads, dp = cfg["col"], cfg["heads"], cfg["dp"]
    me = Mesh(dp, cfg["tensor"])
    sc = Scatter(me, part, mr, xr, sss, srs, 1 - me.y)
    half = sc.half
    seq = xf.shape[0]
    width = q.shape[1]
    own = [ds(sc.own(n), half) for n in range(2)]
    loads = load(
        [
            (k_in, k),
            (q_in, q),
            (v_in, v),
            (do_in, do),
            (o_in, o),
            (tab_in, tab),
            (w0.at[:, col["qkv"] : col["fc1"]], wqkv),
            (xf_in, xf),
            (e2_in, e2),
            (n1_in, n1),
        ]
        + [(dh_in.at[rr], dh.at[n]) for n, rr in enumerate(own)],
        lsem,
    )
    gr_load = pltpu.make_async_copy(gr0, gr, lsem.at[12])
    holds = (me.s == 0) & (me.y == 0)

    @pl.when(holds)
    def _():
        gr_load.start()

    greet([me.mate, me.beside, me.beside_mate, me.across, me.across_mate] + me.ring)
    redr = GradReduce(me, 0, gr0, gr, gr, got, sb, rb, fr, rsems[:6])
    redq = GradReduce(me, 0, gq, gq, gotq, acrq, sbq, rbq, fq, rsems[6:])
    vr_ = VectorReduce(me, va, vr, vss, vrs)
    redr.send()

    def at(dst, h):
        return dst.at[0, me.y, 0, pl.ds(h * half, half)]

    def full_out(src, dst, i):
        chunk = 2 * half
        mine, theirs = ds(me.t * chunk, chunk), ds(me.py * chunk, chunk)
        return [
            pltpu.make_async_copy(src.at[mine], dst.at[0, me.y, 0], lsem.at[13]),
            push(src.at[theirs], dst.at[0, me.y, 0], oss.at[i], ors.at[i], me.across),
        ]

    def owned_out(src, dst, core, i):
        here, far = src.at[me.y], src.at[1 - me.y]
        place = dst.at[0, me.y, 0, ds(me.s * half, half)]
        across = push(far, place, oss.at[i], ors.at[i + me.s], me.across_core(core))
        local = pltpu.make_async_copy(here, place, lsem.at[14])
        mate = push(here, place, oss.at[i + 2], ors.at[i + 2], me.mate)
        return across, local, mate

    def whole(n):
        return full_out(hf_in, so, 0) if n == 0 else full_out(dh_in, ig, 0)

    for n in range(2):

        @pl.when(me.s == n)
        def _(n=n):
            for c in whole(n):
                c.start()

    def start_here(src, dst, core, i):
        across, local, mate = owned_out(src, dst, core, i)

        @pl.when(me.s == core)
        def _():
            local.start()

        @pl.when(me.s != core)
        def _():
            mate.start()

    def wait_owned(src, dst, core, i):
        across, local, mate = owned_out(src, dst, core, i)
        across.wait_send()

        @pl.when(me.s == core)
        def _():
            local.wait()
            mate.wait_recv()
            for n in range(2):
                push(src.at[0], at(dst, n), oss.at[i], ors.at[i + n], me.across_core(core)).wait_recv()

        @pl.when(me.s != core)
        def _():
            mate.wait_send()

    owned_out(y_in, so, 1, 1)[0].start()
    start_here(y_in, so, 1, 1)
    old = [pltpu.make_async_copy(out1, fr, lsem.at[15]), pltpu.make_async_copy(outq, fq, lsem.at[16])]

    @pl.when(me.s == 1)
    def _():
        for c in old:
            c.start()

    vgf[...] = jnp.zeros_like(vgf)
    dk[...] = jnp.zeros_like(dk)
    dv[...] = jnp.zeros_like(dv)
    loads[0].wait()
    turn_blocks(k, kt)
    for c in loads[1:6]:
        c.wait()

    @pl.when(holds)
    def _():
        gr_load.wait()

    n_blocks = seq // QB

    def qloop(i, _):
        lo = jnp.maximum(i - DOC_MAX // QB, 0)
        attn_bwd_block(i, lo, i, heads, q, k, v, o, do, kt, lse, srow, kcol, tab, dk, dv, dmix)
        for at_block, steps in (
            (n_blocks // 2 - 1, range(0, 1)),
            (n_blocks // 2, range(1, dp // 2)),
            (n_blocks // 2 + 1, range(dp // 2, dp - 1)),
            (n_blocks - 2, range(dp - 1, dp)),
        ):

            @pl.when(i == at_block)
            def _(steps=steps):
                for d in steps:
                    redr.step(d)

        return 0

    lax.fori_loop(0, n_blocks, qloop, 0)

    def close(i, _):
        ii = ds(i * QB, QB)
        dmix[ii, width : 2 * width] = turn_lanes(dk[ii, :], tab[ii, :], -1).astype(BF)
        dmix[ii, 2 * width : 3 * width] = dv[ii, :].astype(BF)
        return 0

    lax.fori_loop(0, n_blocks, close, 0)
    for c in loads[6:]:
        c.wait()

    def early():
        va[0, 0:8, :] = vgf[...] + vd0[...]
        va[0, 8:16, :] = vf1[...] + vd1[...]
        vr_.send(0)
        nf = gq.shape[0]
        accs = [dk.at[0:nf], dk.at[nf : 2 * nf], dv.at[0:nf]]
        for acc in accs:
            acc[...] = jnp.zeros_like(acc)

        def body(i, _):
            rows = ds(i * half, half)
            n1t = n1[rows, :].T
            for p, acc in enumerate(accs):
                acc[...] += dot(n1t, dmix[rows, p * HW : (p + 1) * HW])
            return 0

        lax.fori_loop(0, 8, body, 0)
        for p, acc in enumerate(accs):
            gq[:, p * HW : (p + 1) * HW] = acc[...].astype(BF)
        vr_.add(0, va.at[1])
        vr_.send(1)
        redq.send()
        vr_.add(1, va.at[2])
        vr_.send(2)
        redq.step(0)

    sc.run(lambda r0, i: back_tail(r0, half, dmix, xf, e2, wqkv, vecs.at[0], part, vgf), early)
    for d in range(1, dp - 1):
        redq.step(d)

    def write(n, i, value):
        dx[sc.side(n), ds(i * SUB, SUB), :] = value

    def leave(n):
        if n == 0:
            owned_out(dx, ig, 0, 4)[0].start()
        else:
            start_here(dx, ig, 0, 4)

    grad_out(sc, lambda n, i: dh[sc.side(n), ds(i * SUB, SUB), :], xf, vecs.at[0], write, leave)
    redq.step(dp - 1)
    vr_.add(2, vout)
    vec_o[...] = jnp.where(me.s == 0, vout[0:8, :], vout[8:16, :])
    redr.collect()
    redq.collect()

    @pl.when(me.s == 1)
    def _():
        for c in old:
            c.wait()

    ends = [pltpu.make_async_copy(fr, fr_o, lsem.at[0]), pltpu.make_async_copy(fq, fq_o, lsem.at[1])]
    for c in ends:
        c.start()
    redr.finish()
    redq.finish()
    vr_.finish()
    sc.finish()
    for n in range(2):

        @pl.when(me.s == n)
        def _(n=n):
            for c in whole(n):
                c.wait()

    wait_owned(y_in, so, 1, 1)
    wait_owned(dx, ig, 0, 4)
    for c in ends:
        c.wait()


def layer_last(cfg, q, k, v, o, do, lse, sr, kc, tab, e2, dh, xf, n1, w0, vecs, vf1, vd1, vd0, gr0, out1, outq, hf, y):
    seq, model = xf.shape
    dp, tensor, ff = cfg["dp"], cfg["tensor"], cfg["ff"]
    rows, nr, nq = model // dp, 2 * ff + HW, 3 * HW
    nv = dp + tensor - 1
    wide, owned, heads = pltpu.VMEM((seq, model), BF), pltpu.VMEM((2, seq // 8, model), BF), pltpu.VMEM((seq, HW), BF)
    both = sds((1, 2, 1, seq // 4, model), BF)
    return pl.pallas_call(
        functools.partial(last_kernel, cfg),
        out_shape=(both, both, sds((rows, nq), F32), sds((rows, nr), F32), sds((8, model), F32)),
        in_specs=[ANY] * 5 + [VMEM] * 3 + [ANY] * 6 + [VMEM] * 4 + [ANY] * 5,
        out_specs=(ANY, ANY, ANY, ANY, VMEM),
        scratch_shapes=[
            heads, heads, heads, heads, heads, pltpu.VMEM(tab.shape, F32), pltpu.VMEM((HW, seq), BF),
            pltpu.VMEM((seq, HW), F32), pltpu.VMEM((seq, HW), F32), pltpu.VMEM((seq, nq), BF), owned, owned,
            wide, wide, wide, pltpu.VMEM((model, nq), BF),
            pltpu.VMEM((model, nq), BF), pltpu.VMEM((model, nq), BF), pltpu.VMEM((model, nq), BF),
            pltpu.VMEM((dp - 1, rows, nq), BF), pltpu.VMEM((dp - 1, rows, nq), BF),
            pltpu.VMEM((model, nr), BF), pltpu.VMEM((model, nr), BF),
            pltpu.VMEM((dp - 1, rows, nr), BF), pltpu.VMEM((dp - 1, rows, nr), BF),
            pltpu.VMEM((rows, nq), F32), pltpu.VMEM((rows, nr), F32),
            pltpu.VMEM((8, model), F32), pltpu.VMEM((3, 16, model), F32), pltpu.VMEM((nv, 16, model), F32),
            pltpu.VMEM((16, model), F32),
        ]
        + scatter_scratch(seq, model)
        + [DMA((17,)), DMA((nv,)), DMA((nv,)), DMA((7,)), DMA((7,))]
        + GradReduce.scratch(dp) * 2,
        compiler_params=params(6),
        cost_estimate=cost(80),
        name="layer_last",
    )(q, k, v, o, do, lse, sr, kc, tab, e2, dh, xf, n1, w0, vecs, vf1, vd1, vd0, gr0, out1, outq, hf, y)


def finish_kernel(
    cfg, so_in, ig_in, fq_in, fr_in, vec, so, ig, bg1, bb1, gqkv, bqkv, gout, bdy, bdy2, bg2, bb2, gfc1, bfc1, gfc2,
    a, b, fq, fr, lsem, osem,
):
    heads, ff, own, qw, fw = cfg["heads"], cfg["ff"], cfg["own"], cfg["qw"], cfg["fw"]
    me = Mesh(cfg["dp"], cfg["tensor"])
    loads = load([(fr_in, fr), (fq_in, fq), (so_in, a), (ig_in, b)], lsem)
    model = vec.shape[1]
    short = pltpu.roll(vec[...], (model - (me.z * me.tensor + me.t) * own) % model, 1)
    for row, ref in ((0, bg1), (1, bb1), (2, bdy), (2, bdy2), (3, bg2), (4, bb2)):
        ref[...] = short[row : row + 1, 0:own]
    for h in range(heads):
        parts = [vec[6:7, p * HW + h * HD : p * HW + (h + 1) * HD] for p in range(3)]
        one = jnp.concatenate(parts + [jnp.zeros((1, HW - 3 * HD), F32)], axis=1)
        one = jnp.broadcast_to(one, (8, HW))
        bqkv[h] = pltpu.roll(one, (HW - me.z * qw) % HW, 1)[0:1, 0:qw]
        wide = ff // heads
        one = jnp.broadcast_to(vec[7:8, h * wide : (h + 1) * wide], (8, wide))
        bfc1[h] = pltpu.roll(one, (wide - me.z * fw) % wide, 1)[0:1, 0:fw]
    loads[0].wait()
    gfc1[0] = fr[:, 0:ff]
    gfc2[...] = fr[:, ff : 2 * ff]
    gout[0] = fr[:, 2 * ff : 2 * ff + HW].T[0 : heads * HD, :]
    loads[2].wait()
    loads[3].wait()
    outs = [pltpu.make_async_copy(a, so, osem.at[0]), pltpu.make_async_copy(b, ig, osem.at[1])]
    for c in outs:
        c.start()
    loads[1].wait()
    pieces = [fq[:, p * HW + h * HD : p * HW + (h + 1) * HD] for h in range(heads) for p in range(3)]
    gqkv[0] = jnp.concatenate(pieces, axis=1)
    for c in outs:
        c.wait()


def finish(cfg, so, ig, fq, fr, vec):
    heads, ff, rows = cfg["heads"], cfg["ff"], fq.shape[0]
    line = sds((1, cfg["own"]), F32)
    return pl.pallas_call(
        functools.partial(finish_kernel, cfg),
        out_shape=(sds(so.shape, BF), sds(ig.shape, BF), line, line, sds((1, rows, heads * 3 * HD), F32),
                   sds((heads, 1, cfg["qw"]), F32), sds((1, heads * HD, rows), F32), line, line, line, line,
                   sds((1, rows, ff), F32), sds((heads, 1, cfg["fw"]), F32), sds((rows, ff), F32)),
        in_specs=[ANY] * 4 + [VMEM],
        out_specs=(ANY, ANY) + (VMEM,) * 12,
        scratch_shapes=[
            pltpu.VMEM(so.shape, BF), pltpu.VMEM(ig.shape, BF), pltpu.VMEM(fq.shape, F32), pltpu.VMEM(fr.shape, F32),
            DMA((4,)), DMA((2,)),
        ],
        compiler_params=pltpu.CompilerParams(vmem_limit_bytes=67043328),
        cost_estimate=cost(5),
        name="finish",
    )(so, ig, fq, fr, vec)


def by_part(w):
    rows = w.shape[0]
    heads = w.shape[1] // (3 * HD)
    w = w.reshape(rows, heads, 3, HD).transpose(0, 2, 1, 3).reshape(rows, 3, heads * HD)
    return jnp.pad(w, ((0, 0), (0, 0), (0, HW - heads * HD))).reshape(rows, 3 * HW)


def shards(
    dp, tensor, inputs, cotangent, segments, live_blocks, ln1_gain, ln1_bias, qkv_weight, qkv_bias,
    out_weight, out_bias, ln2_gain, ln2_bias, fc1_weight, fc1_bias, fc2_weight, fc2_bias,
):
    model = inputs.shape[-1]
    ff = fc1_weight.shape[2]
    heads = qkv_bias.shape[1]
    col = columns(model, ff)
    wout = jnp.pad(out_weight[0].T, ((0, 0), (0, HW - heads * HD)))
    w = jnp.concatenate([by_part(qkv_weight[0]), fc1_weight[0], fc2_weight[0].T, wout], axis=1)
    small = jnp.stack([ln1_gain[0], ln1_bias[0], out_bias[0], ln2_gain[0], ln2_bias[0], fc2_bias[0]])

    def lanes(a):
        return jnp.pad(a.astype(F32), ((0, 0), (0, 128 - a.shape[1])))

    sv = jnp.concatenate([lanes(small), lanes(qkv_bias[0]), lanes(fc1_bias[0])], axis=0)
    sv = jnp.pad(sv, ((0, -sv.shape[0] % 8), (0, 0)))
    fr = np.float32(10000.0) ** (-(np.arange(ROT // 2, dtype=np.float32) * np.float32(2.0 / ROT)))
    fr = jnp.asarray(np.broadcast_to(fr[:, None], (ROT // 2, 128)).astype(np.float32))
    cfg = {
        "col": col, "ff": ff, "heads": heads, "dp": dp, "tensor": tensor, "own": small.shape[1],
        "qw": qkv_bias.shape[2], "fw": fc1_bias.shape[2],
        "groups": [(0, col["fc1"]), (col["fc1"], col["fc2"]), (col["fc2"], col["end"])],
    }

    xf, n1a, n2a, ga, gpa, tab, w0, qa, ka, va, cf, vecs, sr, kc = layer_in(
        cfg, inputs, cotangent, segments, live_blocks, w, sv, fr
    )
    oa, lsea, hf, n1b, n2b, gb, gpb, w1, qb, kb, vb = layer_mid(cfg, qa, ka, va, sr, kc, ga, xf, w, w0, vecs, tab)
    ob, lseb = attn_fwd(heads, segments, live_blocks, qb, kb, vb, sr, kc)
    y, dob, e2b, grb, vdb = layer_turn(cfg, ob, gb, hf, cf, w1, vecs, n2b, gpb)
    dmb = attn_bwd(heads, segments, live_blocks, qb, kb, vb, ob, dob, lseb, sr, kc, tab)
    dhf, e2a, doa, vfb, vda, out1, outq, gra = layer_back(
        cfg, dmb, e2b, cf, hf, n1b, w1, w0, vecs, xf, ga, gpa, n2a, oa, grb
    )
    last_part = finish(
        cfg,
        *layer_last(
            cfg, qa, ka, va, oa, doa, lsea, sr, kc, tab, e2a, dhf, xf, n1a, w0, vecs, vfb, vdb, vda, gra, out1, outq, hf, y
        ),
    )
    so, ig, bg1, bb1, gqkv, bqkv, gout, bdy, bdy2, bg2, bb2, gfc1, bfc1, gfc2 = last_part
    bqkv, bfc1, gfc2 = bqkv.transpose(1, 0, 2), bfc1.transpose(1, 0, 2), gfc2.T[None]
    return (so, ig, bg1, bb1, gqkv, bqkv, gout, bdy, bg2, bb2, gfc1, bfc1, gfc2, bdy2)


def solution(mesh):
    both = ("dp", "tensor")
    in_specs = (
        P(None, "dp", "tensor", None),
        P(None, "dp", "tensor", None),
        P(None, "dp", None),
        P(None, "dp"),
        P("section", both),
        P("section", both),
        P("section", "dp", "tensor"),
        P("section", "tensor", "dp"),
        P("section", "tensor", "dp"),
        P("section", both),
        P("section", both),
        P("section", both),
        P("section", "dp", "tensor"),
        P("section", "tensor", "dp"),
        P("section", "tensor", "dp"),
        P("section", both),
    )
    out_specs = (
        P("section", None, "dp", "tensor", None),
        P("section", None, "dp", "tensor", None),
        P("section", both),
        P("section", both),
        P("section", "dp", "tensor"),
        P("section", "tensor", "dp"),
        P("section", "tensor", "dp"),
        P("section", both),
        P("section", both),
        P("section", both),
        P("section", "dp", "tensor"),
        P("section", "tensor", "dp"),
        P("section", "tensor", "dp"),
        P("section", both),
    )
    body = functools.partial(shards, mesh.shape["dp"], mesh.shape["tensor"])
    return jax.shard_map(body, mesh=mesh, in_specs=in_specs, out_specs=out_specs, check_vma=False)
```

```python
import functools

import jax
import jax.numpy as jnp
import numpy as np
from jax import lax
from jax.experimental import pallas as pl
from jax.experimental.pallas import tpu as pltpu
from jax.sharding import PartitionSpec as P

F32 = jnp.float32
BF = jnp.bfloat16
MESH = pl.DeviceIdType.MESH
HD = 64
ROT = 16
LIVE = 128
DOCS = 4
DOC_MAX = 1024
QB = 256
HW = 256
SUB = 256
EPS = 1e-05
NEG = -1e30
VMEM = pl.BlockSpec(memory_space=pltpu.VMEM)
ANY = pl.BlockSpec(memory_space=pltpu.HBM)
SMEM = pl.BlockSpec(memory_space=pltpu.SMEM)
DMA = pltpu.SemaphoreType.DMA


def sds(shape, dtype):
    return jax.ShapeDtypeStruct(shape, dtype)


def dg(a, b, ca, cb):
    return lax.dot_general(a, b, (((ca,), (cb,)), ((), ())), preferred_element_type=F32)


def dot(a, b):
    return jnp.dot(a, b, preferred_element_type=F32)


def ds(start, size):
    return pl.ds(pl.multiple_of(start, size), size)


def norm_stats(x):
    mu = jnp.mean(x, axis=-1, keepdims=True)
    xc = x - mu
    var = jnp.mean(xc * xc, axis=-1, keepdims=True)
    return xc, lax.rsqrt(var + EPS)


def head_lanes(width, heads):
    lane = lax.broadcasted_iota(jnp.int32, (1, width), 1)
    return [(lane >= h * HD) & (lane < (h + 1) * HD) for h in range(heads)]


def allow_mask(kc, sq, diag):
    m = kc == sq
    if diag:
        r = lax.broadcasted_iota(jnp.int32, (QB, QB), 0)
        c = lax.broadcasted_iota(jnp.int32, (QB, QB), 1)
        m = (m & (r <= c)) | (r == c)
    return m


def block_bounds(seg, live, i, n):
    s = lax.axis_index("tensor") // 2
    doc = seg[s, 0, i * QB]

    def body(j, count):
        return count + jnp.where((j < i) & (seg[s, 0, (j + 1) * QB - 1] == doc), 1, 0)

    hi = jnp.minimum(i, (live[0, s] * LIVE + QB - 1) // QB)
    return jnp.minimum(i - lax.fori_loop(0, n, body, 0), hi), hi


def turn_blocks(src, dst):
    def turn(i, _):
        dst[:, ds(i * QB, QB)] = src[ds(i * QB, QB), :].T
        return 0

    lax.fori_loop(0, src.shape[0] // QB, turn, 0)


def attn_fwd_block(i, lo, hi, heads, q_ref, k_ref, vt, sr_ref, kc_ref, s_scr, o_ref, lse_ref):
    width = q_ref.shape[1]
    qi = ds(i * QB, QB)
    q = q_ref[qi, :]
    qm = [jnp.where(m, q, jnp.zeros_like(q)) for m in head_lanes(width, heads)]
    sq = sr_ref[0:1, qi]

    def scores(j, slot, ms, diag):
        kj = ds(j * QB, QB)
        k = k_ref[kj, :]
        mask = allow_mask(kc_ref[kj, 0:1], sq, diag)
        out = []
        for h in range(heads):
            s = jnp.where(mask, dg(k, qm[h], 1, 1), NEG)
            s_scr[h, ds(slot * QB, QB), :] = s
            out.append(jnp.maximum(ms[h], jnp.max(s, axis=0, keepdims=True)))
        return tuple(out)

    ms = tuple(jnp.full((1, QB), NEG, F32) for _ in range(heads))
    ms = scores(i, 0, ms, True)
    ms = lax.fori_loop(lo, hi, lambda j, ms: scores(j, j - lo + 1, ms, False), ms)

    def weigh(j, slot, st):
        kj = ds(j * QB, QB)
        out = []
        for h in range(heads):
            total, acc = st[h]
            p = jnp.exp(s_scr[h, ds(slot * QB, QB), :] - ms[h])
            total = total + jnp.sum(p, axis=0, keepdims=True)
            acc = acc + dot(vt[h * HD : (h + 1) * HD, kj], p.astype(BF))
            out.append((total, acc))
        return tuple(out)

    st = tuple((jnp.zeros((1, QB), F32), jnp.zeros((HD, QB), F32)) for _ in range(heads))
    st = weigh(i, 0, st)
    st = lax.fori_loop(lo, hi, lambda j, st: weigh(j, j - lo + 1, st), st)
    ot = [st[h][1] * (1.0 / st[h][0]) for h in range(heads)]
    ot = jnp.concatenate(ot + [jnp.zeros((width - heads * HD, QB), F32)], axis=0)
    o_ref[qi, :] = ot.T.astype(BF)
    lse = [ms[h] + jnp.log(st[h][0]) for h in range(heads)]
    lse_ref[:, qi] = jnp.concatenate(lse + [jnp.zeros((8 - heads, QB), F32)], axis=0)


def attn_fwd_kernel(heads, seg, live, q_in, k_in, v_in, sr_ref, kc_ref, o_out, lse_ref, q, k, v, o, vt, s_scr, lsem, osem):
    n = q.shape[0] // QB
    loads = load([(v_in, v), (q_in, q), (k_in, k)], lsem)
    loads[0].wait()
    turn_blocks(v, vt)
    loads[1].wait()
    loads[2].wait()

    def out(i):
        rows = ds(i * QB, QB)
        return pltpu.make_async_copy(o.at[rows], o_out.at[rows], osem.at[i])

    def qloop(i, _):
        lo, hi = block_bounds(seg, live, i, n)
        attn_fwd_block(i, lo, hi, heads, q, k, vt, sr_ref, kc_ref, s_scr, o, lse_ref)
        out(i).start()
        return 0

    lax.fori_loop(0, n, qloop, 0)

    def drain(i, _):
        out(i).wait()
        return 0

    lax.fori_loop(0, n, drain, 0)


def attn_fwd(heads, seg, live, q, k, v, sr, kc):
    rows, width = q.shape
    buf = pltpu.VMEM((rows, width), BF)
    return pl.pallas_call(
        functools.partial(attn_fwd_kernel, heads),
        out_shape=(sds((rows, width), BF), sds((8, rows), F32)),
        in_specs=[SMEM, SMEM, ANY, ANY, ANY, VMEM, VMEM],
        out_specs=(ANY, VMEM),
        scratch_shapes=[buf, buf, buf, buf, pltpu.VMEM((width, rows), BF), pltpu.VMEM((heads, rows + QB, QB), F32),
                        DMA((3,)), DMA((rows // QB,))],
        compiler_params=pltpu.CompilerParams(vmem_limit_bytes=67043328),
        cost_estimate=cost(12),
        name="attn_fwd",
    )(seg, live, q, k, v, sr, kc)


def turn_lanes(x, tab, sign):
    width = x.shape[1]
    c, sn = [jnp.concatenate([tab[:, a * 128 : (a + 1) * 128]] * (width // 128), axis=1) for a in range(2)]
    lane = lax.broadcasted_iota(jnp.int32, (1, width), 1) % HD
    moved = jnp.where(lane < ROT // 2, pltpu.roll(x, width - ROT // 2, 1), pltpu.roll(x, ROT // 2, 1)) * sn
    return x * c + moved if sign > 0 else x * c - moved


def attn_bwd_block(i, lo, hi, heads, q_ref, k_ref, v_ref, o_ref, do_ref, kt, lse_ref, sr_ref, kc_ref, tab, dk, dv, out):
    width = q_ref.shape[1]
    hm = head_lanes(width, heads)
    rowid = lax.broadcasted_iota(jnp.int32, (8, width), 0)
    lane = lax.broadcasted_iota(jnp.int32, (8, width), 1)
    sel = ((lane >= rowid * HD) & (lane < (rowid + 1) * HD)).astype(F32).astype(BF)
    qi = ds(i * QB, QB)
    q = q_ref[qi, :]
    do = do_ref[qi, :]
    z = jnp.zeros_like(q)
    qm = [jnp.where(hm[h], q, z) for h in range(heads)]
    dom = [jnp.where(hm[h], do, z) for h in range(heads)]
    qcat = jnp.concatenate(qm, axis=0)
    docat = jnp.concatenate(dom, axis=0)
    prod = do.astype(F32) * o_ref[qi, :].astype(F32)
    high = prod.astype(BF)
    low = (prod - high.astype(F32)).astype(BF)
    delta = dg(sel, high, 1, 1) + dg(sel, low, 1, 1)
    lse = lse_ref[:, qi]
    sq = sr_ref[0:1, qi]

    def step(j, dqs, diag):
        kj = ds(j * QB, QB)
        k = k_ref[kj, :]
        v = v_ref[kj, :]
        mask = allow_mask(kc_ref[kj, 0:1], sq, diag)
        ps, dss, res = [], [], []
        for h in range(heads):
            s = dg(k, qm[h], 1, 1)
            dp = dg(v, dom[h], 1, 1)
            p = jnp.exp(jnp.where(mask, s - lse[h : h + 1, :], NEG))
            score_grad = (p * (dp - delta[h : h + 1, :])).astype(BF)
            ps.append(p.astype(BF))
            dss.append(score_grad)
            res.append(dqs[h] + dot(kt[h * HD : (h + 1) * HD, kj], score_grad))
        dv[kj, :] += dot(jnp.concatenate(ps, axis=1), docat)
        dk[kj, :] += dot(jnp.concatenate(dss, axis=1), qcat)
        return tuple(res)

    dqs = tuple(jnp.zeros((HD, QB), F32) for _ in range(heads))
    dqs = step(i, dqs, True)
    dqs = lax.fori_loop(lo, hi, lambda j, d: step(j, d, False), dqs)
    dq = jnp.concatenate(list(dqs) + [jnp.zeros((width - heads * HD, QB), F32)], axis=0).T * 0.125
    out[qi, 0:width] = turn_lanes(dq, tab[qi, :], -1).astype(BF)


def attn_bwd_kernel(
    heads, seg, live, q_in, k_in, v_in, o_in, do_in, lse_ref, sr_ref, kc_ref, tab_in, out_ref,
    q, k, v, o, do, tab, out, kt, dk, dv, lsem, osem,
):
    rows, width = q.shape
    n = rows // QB
    loads = load([(k_in, k), (q_in, q), (v_in, v), (do_in, do), (o_in, o), (tab_in, tab)], lsem)
    dk[...] = jnp.zeros_like(dk)
    dv[...] = jnp.zeros_like(dv)
    loads[0].wait()
    turn_blocks(k, kt)
    for c in loads[1:]:
        c.wait()

    def qloop(i, _):
        lo, hi = block_bounds(seg, live, i, n)
        attn_bwd_block(i, lo, hi, heads, q, k, v, o, do, kt, lse_ref, sr_ref, kc_ref, tab, dk, dv, out)
        return 0

    lax.fori_loop(0, n, qloop, 0)

    def leave(i):
        rr = ds(i * QB, QB)
        return pltpu.make_async_copy(out.at[rr], out_ref.at[rr], osem.at[i])

    def finish(i, _):
        ii = ds(i * QB, QB)
        out[ii, width : 2 * width] = turn_lanes(dk[ii, :], tab[ii, :], -1).astype(BF)
        out[ii, 2 * width : 3 * width] = dv[ii, :].astype(BF)
        leave(i).start()
        return 0

    lax.fori_loop(0, n, finish, 0)

    def drain(i, _):
        leave(i).wait()
        return 0

    lax.fori_loop(0, n, drain, 0)


def attn_bwd(heads, seg, live, q, k, v, o, do, lse, sr, kc, tab):
    rows, width = q.shape
    buf = pltpu.VMEM((rows, width), BF)
    return pl.pallas_call(
        functools.partial(attn_bwd_kernel, heads),
        out_shape=sds((rows, 3 * width), BF),
        in_specs=[SMEM, SMEM] + [ANY] * 5 + [VMEM] * 3 + [ANY],
        out_specs=ANY,
        scratch_shapes=[buf, buf, buf, buf, buf, pltpu.VMEM(tab.shape, F32), pltpu.VMEM((rows, 3 * width), BF),
                        pltpu.VMEM((width, rows), BF), pltpu.VMEM((rows, width), F32), pltpu.VMEM((rows, width), F32),
                        DMA((6,)), DMA((rows // QB,))],
        compiler_params=pltpu.CompilerParams(vmem_limit_bytes=67043328),
        cost_estimate=cost(26),
        name="attn_bwd",
    )(seg, live, q, k, v, o, do, lse, sr, kc, tab)


class Mesh:
    def __init__(self, dp, tensor):
        self.dp, self.tensor = dp, tensor
        self.s, self.z, self.t = lax.axis_index("section"), lax.axis_index("dp"), lax.axis_index("tensor")
        self.x, self.y = self.t % 2, self.t // 2
        self.px, self.py = 2 * self.y + (1 - self.x), 2 * (1 - self.y) + self.x
        self.mate = {"section": 1 - self.s}
        self.beside = {"tensor": self.px}
        self.beside_mate = {"tensor": self.px, "section": 1 - self.s}
        self.across = {"tensor": self.py}
        self.across_mate = {"tensor": self.py, "section": 1 - self.s}
        self.ring = [{"dp": (self.z + d) % dp} for d in range(1, dp)]
        self.group = [{"tensor": (self.t + d) % tensor} for d in range(1, tensor)]
        self.quarter = 2 * self.s + self.x

    def across_core(self, core):
        return {"tensor": self.py, "section": core}


def greet(peers):
    bar = pltpu.get_barrier_semaphore()
    for peer in peers:
        pl.semaphore_signal(bar, inc=1, device_id=peer, device_id_type=MESH)
    pl.semaphore_wait(bar, len(peers))


def push(src, dst, ssem, rsem, peer):
    return pltpu.make_async_remote_copy(
        src_ref=src, dst_ref=dst, send_sem=ssem, recv_sem=rsem, device_id=peer, device_id_type=MESH
    )


def pick(i, values):
    out = values[-1]
    for n in range(len(values) - 2, -1, -1):
        out = jnp.where(i == n, values[n], out)
    return out


class Tokens:
    def __init__(self, me, seq):
        self.me, self.half = me, seq // 8

    def start_of(self, a, b, h):
        return (4 * a + 2 * b + h) * self.half

    def rows(self, a, b, h):
        return ds(self.start_of(a, b, h), self.half)

    def own(self, a):
        return self.start_of(a, self.me.x, self.me.s)


class Gather(Tokens):
    def __init__(self, me, full, ssem, rsem, first=0):
        super().__init__(me, full.shape[0])
        self.full, self.ssem, self.rsem, self.first = full, ssem, rsem, first

    def side(self, n):
        return self.first if n == 0 else 1 - self.first

    def plan(self, i):
        me, a = self.me, self.side(i % 2)
        ref = self.full.at[self.rows(a, (1 - me.x) if i >= 4 else me.x, me.s)]
        return push(ref, ref, self.ssem.at[i], self.rsem.at[i], me.beside if i in (2, 3) else me.mate)

    def start(self, n):
        self.plan(n).start()
        self.plan(2 + n).start()

    def order(self, i):
        me = self.me
        a = pick(i, [self.side(n) for n in (0, 1, 0, 1, 0, 0, 1, 1)])
        b = jnp.where(i < 4, me.x, 1 - me.x)
        h = pick(i, [me.s, me.s, 1 - me.s, 1 - me.s, me.s, 1 - me.s, me.s, 1 - me.s])
        return self.start_of(a, b, h)

    def step(self, i):
        if i in (2, 3):
            self.plan(i - 2).wait_recv()
        if i in (4, 6):
            n = i // 2 - 2
            self.plan(2 + n).wait_recv()
            self.plan(4 + n).start()
        if i in (5, 7):
            self.plan(4 + i // 2 - 2).wait_recv()

    def arrive(self, i):
        for n in range(2, 8):

            @pl.when(i == n)
            def _(n=n):
                self.step(n)

    def finish(self):
        for i in range(6):
            self.plan(i).wait_send()

    def run(self, work):
        def body(i, _):
            self.arrive(i)
            work(self.order(i), i)
            return 0

        lax.fori_loop(0, 8, body, 0)
        self.finish()


class Scatter(Tokens):
    def __init__(self, me, part, mr, xr, ssem, rsem, first=0):
        super().__init__(me, part.shape[0])
        self.part, self.mr, self.xr, self.ssem, self.rsem, self.first = part, mr, xr, ssem, rsem, first

    def side(self, n):
        return self.first if n == 0 else 1 - self.first

    def plan(self, i):
        me = self.me
        if i < 4:
            b = (1 - me.x) if i < 2 else me.x
            src, dst, peer = self.rows(self.side(i % 2), b, 1 - me.s), self.mr.at[i], me.mate
        else:
            src, dst, peer = self.rows(self.side(i - 4), 1 - me.x, me.s), self.xr.at[i - 4], me.beside
        return push(self.part.at[src], dst, self.ssem.at[i], self.rsem.at[i], peer)

    def run(self, work, early=None):
        me = self.me

        def body(i, _):
            k = i // 2
            b = jnp.where(k < 2, 1 - me.x, me.x)
            h = jnp.where(i % 2 == 0, 1 - me.s, me.s)
            work(self.start_of(jnp.where(k % 2 == 0, self.side(0), self.side(1)), b, h), i)
            for n in range(4):

                @pl.when(i == 2 * n)
                def _(n=n):
                    self.plan(n).start()

            for n in range(2):

                @pl.when(i == 2 * n + 1)
                def _(n=n):
                    self.plan(n).wait_recv()
                    base = self.start_of(self.side(n), 1 - me.x, me.s)

                    def add(j, _):
                        rr = ds(base + j * SUB, SUB)
                        got = self.mr[n, ds(j * SUB, SUB), :].astype(F32)
                        self.part[rr, :] = (self.part[rr, :].astype(F32) + got).astype(BF)
                        return 0

                    lax.fori_loop(0, self.half // SUB, add, 0)
                    self.plan(4 + n).start()

            return 0

        lax.fori_loop(0, 8, body, 0)
        if early is not None:
            early()

    def arrive(self, n):
        self.plan(2 + n).wait_recv()
        self.plan(4 + n).wait_recv()

    def total(self, n, i):
        rr = ds(self.own(self.side(n)) + i * SUB, SUB)
        sub = ds(i * SUB, SUB)
        return self.part[rr, :].astype(F32) + self.mr[2 + n, sub, :].astype(F32) + self.xr[n, sub, :].astype(F32)

    def finish(self):
        for i in range(6):
            self.plan(i).wait_send()


def scatter_scratch(rows, width):
    half = rows // 8
    return [
        pltpu.VMEM((rows, width), BF),
        pltpu.VMEM((4, half, width), BF),
        pltpu.VMEM((2, half, width), BF),
        DMA((6,)),
        DMA((6,)),
    ]


class WeightGather:
    def __init__(self, me, layer, shard, full, gat, groups, sems):
        self.me, self.layer, self.shard, self.full, self.gat, self.groups = me, layer, shard, full, gat, groups
        self.own, self.wss, self.wrs, self.fss, self.frs, self.yss, self.yrs = sems
        self.rows = shard.shape[0]
        self.collects = me.s == layer
        self.keeps = me.y == layer

    def block(self, ref, zz, g):
        a, b = self.groups[g]
        return ref.at[ds(zz * self.rows, self.rows), a:b]

    def mine(self, g):
        a, b = self.groups[g]
        return self.shard.at[:, a:b]

    def local(self, g):
        return pltpu.make_async_copy(self.mine(g), self.block(self.full, self.me.z, g), self.own.at[g])

    def out(self, g, d, ref):
        dst = self.block(ref, self.me.z, g)
        return push(self.mine(g), dst, self.wss.at[g, d], self.wrs.at[g, d], self.me.ring[d])

    def hand(self, g, d, ref, across):
        zz = (self.me.z + self.me.dp - d) % self.me.dp
        src = self.mine(g) if d == 0 else self.block(ref, zz, g)
        ss, rs = (self.yss, self.yrs) if across else (self.fss, self.frs)
        peer = self.me.across_core(self.me.y) if across else self.me.mate
        return push(src, self.block(self.full, zz, g), ss.at[g, d], rs.at[g, d], peer)

    def both(self, do):
        @pl.when(self.collects & self.keeps)
        def _():
            do(self.full, True)

        @pl.when(self.collects & jnp.logical_not(self.keeps))
        def _():
            do(self.gat, False)

    def send_ring(self):
        def do(ref, keeps):
            for g in range(len(self.groups)):
                for d in range(self.me.dp - 1):
                    self.out(g, d, ref).start()

        self.both(do)

    def send_own(self, g):
        def do(ref, keeps):
            self.hand(g, 0, ref, True).start()
            if keeps:
                self.local(g).start()
            else:
                self.hand(g, 0, ref, False).start()

        self.both(do)

    def forward(self, g, blocks=None):
        def do(ref, keeps):
            for d in range(self.me.dp - 1) if blocks is None else blocks:
                self.out(g, d, ref).wait_recv()
                self.hand(g, d + 1, ref, True).start()
                if not keeps:
                    self.hand(g, d + 1, ref, False).start()

        self.both(do)

    def ready(self, g):
        me = self.me

        @pl.when(self.collects & self.keeps)
        def _():
            self.local(g).wait()

        @pl.when(me.s != me.y)
        def _():
            for d in range(me.dp):
                self.hand(g, d, self.full, True).wait_recv()

        @pl.when((me.s == me.y) & jnp.logical_not(self.collects))
        def _():
            for d in range(me.dp):
                self.hand(g, d, self.full, False).wait_recv()

    def finish(self):
        def do(ref, keeps):
            for g in range(len(self.groups)):
                for d in range(self.me.dp - 1):
                    self.out(g, d, ref).wait_send()
                for d in range(self.me.dp):
                    self.hand(g, d, ref, True).wait_send()
                    if not keeps:
                        self.hand(g, d, ref, False).wait_send()

        self.both(do)

    @staticmethod
    def scratch(dp, n):
        return [DMA((n,)), DMA((n, dp - 1)), DMA((n, dp - 1))] + [DMA((n, dp))] * 4


class GradReduce:
    def __init__(self, me, layer, src, mine, got, across, sb, rb, own, sems):
        self.me, self.layer, self.src, self.mine, self.got, self.across = me, layer, src, mine, got, across
        self.sb, self.rb, self.own = sb, rb, own
        self.hss, self.hrs, self.yss, self.yrs, self.pss, self.prs = sems
        self.rows = own.shape[0]
        self.some = 96 if self.rows % 96 == 0 else 48
        self.sums = me.s == layer
        self.holds = me.y == layer

    @staticmethod
    def scratch(dp):
        return [DMA((1,)), DMA((1,)), DMA((dp,)), DMA((dp,)), DMA((dp - 1,)), DMA((dp - 1,))]

    def hand(self):
        return push(self.src, self.got, self.hss.at[0], self.hrs.at[0], self.me.mate)

    def zz(self, d):
        return (self.me.z + d + 1) % self.me.dp

    def over(self, d):
        rr = ds(self.zz(d) * self.rows, self.rows)
        peer = self.me.across_core(self.layer)
        return push(self.src.at[rr], self.across.at[rr], self.yss.at[d], self.yrs.at[d], peer)

    def out(self, d):
        return push(self.sb.at[d], self.rb.at[d], self.pss.at[d], self.prs.at[d], self.me.ring[d])

    def send(self):
        me = self.me

        @pl.when(me.s != me.y)
        def _():
            for d in range(me.dp):
                self.over(d).start()

        @pl.when((me.s == me.y) & jnp.logical_not(self.sums))
        def _():
            self.hand().start()

    def step(self, d):
        me = self.me

        @pl.when(self.sums)
        def _():
            if d == 0:

                @pl.when(jnp.logical_not(self.holds))
                def _():
                    self.hand().wait_recv()

            self.over(d).wait_recv()
            last = d == me.dp - 1
            step = self.some

            def add(ref):
                def body(i, _):
                    rr = ds(self.zz(d) * self.rows + i * step, step)
                    value = ref[rr, :].astype(F32) + self.across[rr, :].astype(F32)
                    if last:
                        self.own[ds(i * step, step), :] = value
                    else:
                        self.sb[d, ds(i * step, step), :] = value.astype(BF)
                    return 0

                lax.fori_loop(0, self.rows // step, body, 0)

            if self.mine is self.got:
                add(self.mine)
            else:

                @pl.when(self.holds)
                def _():
                    add(self.mine)

                @pl.when(jnp.logical_not(self.holds))
                def _():
                    add(self.got)

            if not last:
                self.out(d).start()

    def collect(self):
        me = self.me

        @pl.when(self.sums)
        def _():
            for d in range(me.dp - 1):
                self.out(d).wait_recv()

                def add(i, _, d=d):
                    rr = ds(i * self.some, self.some)
                    self.own[rr, :] += self.rb[d, rr, :].astype(F32)
                    return 0

                lax.fori_loop(0, self.rows // self.some, add, 0)
            for d in range(me.dp - 1):
                self.out(d).wait_send()

    def finish(self):
        me = self.me

        @pl.when(me.s != me.y)
        def _():
            for d in range(me.dp):
                self.over(d).wait_send()

        @pl.when((me.s == me.y) & jnp.logical_not(self.sums))
        def _():
            self.hand().wait_send()


class VectorGather:
    def __init__(self, me, sv, buf, ss, rs, own):
        self.me, self.sv, self.buf, self.ss, self.rs, self.own = me, sv, buf, ss, rs, own

    def local(self):
        me = self.me
        return pltpu.make_async_copy(self.sv, self.buf.at[me.s, me.t, me.z], self.own)

    def stage(self, n):
        me = self.me
        if n == 0:
            dst = self.buf.at[me.s, me.t, me.z]
            return [push(self.sv, dst, self.ss.at[d], self.rs.at[d], peer) for d, peer in enumerate(me.ring)]
        base = me.dp - 1
        if n == 1:
            ref = self.buf.at[me.s, me.t]
            return [
                push(ref, ref, self.ss.at[base + d], self.rs.at[base + d], peer) for d, peer in enumerate(me.group)
            ]
        i = base + me.tensor - 1
        ref = self.buf.at[me.s]
        return [push(ref, ref, self.ss.at[i], self.rs.at[i], me.mate)]

    def send(self, n):
        if n == 0:
            self.local().start()
        for c in self.stage(n):
            c.start()

    def wait(self, n):
        if n == 0:
            self.local().wait()
        for c in self.stage(n):
            c.wait_recv()

    def finish(self):
        for n in range(3):
            for c in self.stage(n):
                c.wait_send()

    def build(self, vecs, heads, own, qw, fw):
        me, buf = self.me, self.buf
        for layer in range(2):
            wide = [buf[layer, tt, zz, 0:8, :][:, 0:own] for zz in range(me.dp) for tt in range(me.tensor)]
            vecs[layer, 0:8, :] = jnp.concatenate(wide, axis=1)
            here = [buf[layer, me.quarter, zz] for zz in range(me.dp)]
            by = [jnp.concatenate([p[6 + h : 7 + h, 0:qw] for p in here], axis=1) for h in range(heads)]
            qb = []
            for part in range(3):
                qb += [b[:, part * HD : (part + 1) * HD] for b in by] + [jnp.zeros((1, HW - heads * HD), F32)]
            vecs[layer, 6:7, :] = jnp.concatenate(qb, axis=1)
            fb = [p[6 + heads + h : 7 + heads + h, 0:fw] for h in range(heads) for p in here]
            vecs[layer, 7:8, :] = jnp.concatenate(fb, axis=1)


class VectorReduce:
    def __init__(self, me, va, vr, ss, rs):
        self.me, self.va, self.vr, self.ss, self.rs = me, va, vr, ss, rs

    def stage(self, n):
        me, va, vr, ss, rs = self.me, self.va, self.vr, self.ss, self.rs
        peers, base = [([me.across], 0), (me.ring, 1), ([me.mate, me.beside, me.beside_mate], me.dp)][n]
        return [push(va.at[n], vr.at[base + d], ss.at[base + d], rs.at[base + d], p) for d, p in enumerate(peers)]

    def send(self, n):
        for c in self.stage(n):
            c.start()

    def add(self, n, out):
        base = [0, 1, self.me.dp][n]
        for c in self.stage(n):
            c.wait_recv()
        if n < 2:
            total = self.va[n]
            for d in range(len(self.stage(n))):
                total = total + self.vr[base + d]
            out[...] = total
            return
        mine, mate = self.va[2], self.vr[base]
        row = lax.broadcasted_iota(jnp.int32, mine.shape, 0)
        quarter = jnp.where(self.me.s == self.me.y, mine, mate)
        out[...] = jnp.where(row % 8 < 6, mine + mate + self.vr[base + 1] + self.vr[base + 2], quarter)

    def finish(self):
        for n in range(3):
            for c in self.stage(n):
                c.wait_send()


def document_tables(seg, live, fr_ref, tab, srow, kcol):
    seq = seg.shape[1]
    count = lax.broadcasted_iota(jnp.int32, seg.shape, 1)
    start = jnp.zeros_like(seg)
    for doc in range(DOCS - 1):
        before = jnp.sum(jnp.where(seg == doc, 1.0, 0.0), axis=1, keepdims=True).astype(jnp.int32)
        start = start + jnp.where(seg > doc, before, 0)
    ang = fr_ref[:, 0:1] * (count - start).astype(F32)
    cs, sn = jnp.cos(ang), jnp.sin(ang)
    one = jnp.ones((HD - ROT, seq), F32)
    tab[:, 0:128] = jnp.concatenate([cs, cs, one] * 2, axis=0).T
    tab[:, 128:256] = jnp.concatenate([-sn, sn, jnp.zeros_like(one)] * 2, axis=0).T
    srow[...] = jnp.broadcast_to(seg, srow.shape)
    keys = jnp.where(count < live * LIVE, seg, -1).astype(F32)
    for b in range(seq // QB):
        part = jnp.broadcast_to(keys[:, b * QB : (b + 1) * QB], (128, QB))
        kcol[b * QB : (b + 1) * QB, :] = part.T.astype(jnp.int32)


QKV, FC1, FC2, OUT = 0, 1, 2, 3


def columns(model, ff):
    return {"qkv": 0, "fc1": 3 * HW, "fc2": 3 * HW + ff, "out": 3 * HW + 2 * ff, "end": 3 * HW + 2 * ff + HW}


def project_norm(r0, half, hf, vec, n1, n2):
    rows = ds(r0, half)
    xc, r = norm_stats(hf[rows, :].astype(F32))
    xh = xc * r
    n1[rows, :] = (xh * vec[0:1, :] + vec[1:2, :]).astype(BF)
    n2[rows, :] = (xh * vec[3:4, :] + vec[4:5, :]).astype(BF)


def project_qkv(r0, half, wqkv, vec, tab, n1, q, k, v):
    rows = ds(r0, half)
    a = n1[rows, :]
    for part, dst in enumerate((q, k, v)):
        cols = slice(part * HW, (part + 1) * HW)
        y = dot(a, wqkv[:, cols]) + vec[6:7, cols]
        if part < 2:
            y = turn_lanes(y, tab[rows, :], 1)
        if part == 0:
            y = y * 0.125
        dst[rows, :] = y.astype(BF)


def project_fc1(r0, half, wfc1, vec, n2, g, gp):
    rows = ds(r0, half)
    a = n2[rows, :]
    for b in range(wfc1.shape[1] // 256):
        cols = slice(b * 256, (b + 1) * 256)
        y = dot(a, wfc1[:, cols]) + vec[7:8, cols]
        cdf = 0.5 + 0.5 * lax.erf(y * 0.7071067811865476)
        g[rows, cols] = (y * cdf).astype(BF)
        gp[rows, cols] = (cdf + y * jnp.exp(-0.5 * y * y) * 0.3989422804014327).astype(BF)


def branch_out(r0, half, o, g, wout, wfc2, part):
    rows = ds(r0, half)
    for b in range(part.shape[1] // 256):
        cols = slice(b * 256, (b + 1) * 256)
        y = dg(o[rows, :], wout[cols, :], 1, 1) + dg(g[rows, :], wfc2[cols, :], 1, 1)
        part[rows, cols] = y.astype(BF)


def back_head(r0, half, dyf, hf, g, gp, n2, o, wfc1, wfc2, wout, vec, do, e2, da, acc, vg):
    rows = ds(r0, half)
    model, ff = wfc1.shape
    dy = dyf[rows, :]
    for b in range(ff // 256):
        cols = slice(b * 256, (b + 1) * 256)
        y = dot(dy, wfc2[:, cols]) * gp[rows, cols].astype(F32)
        low = y.astype(BF)
        da[:, cols] = low
        vg[7:8, cols] += jnp.sum(low.astype(F32), axis=0, keepdims=True)
    do[rows, :] = dot(dy, wout[...]).astype(BF)
    xc, r = norm_stats(hf[rows, :].astype(F32))
    xh = xc * r
    for b in range(model // 256):
        cols = slice(b * 256, (b + 1) * 256)
        dn = dg(da[...], wfc1[cols, :], 1, 1)
        vg[3:4, cols] += jnp.sum(dn * xh[:, cols], axis=0, keepdims=True)
        vg[4:5, cols] += jnp.sum(dn, axis=0, keepdims=True)
        e2[rows, cols] = (dn * vec[3:4, cols]).astype(BF)
    n2t = n2[rows, :].T
    dyt = dy.T
    for b in range(ff // 256):
        cols = slice(b * 256, (b + 1) * 256)
        acc[:, cols] += dot(n2t, da[:, cols])
        acc[:, ff + b * 256 : ff + (b + 1) * 256] += dot(dyt, g[rows, cols])
    acc[:, 2 * ff :] += dot(dyt, o[rows, :])


def back_tail(r0, half, dmix, hf, e2, wqkv, vec, part, vg):
    rows = ds(r0, half)
    dm = dmix[rows, :]
    vg[6:7, :] += jnp.sum(dm.astype(F32), axis=0, keepdims=True)
    xc, r = norm_stats(hf[rows, :].astype(F32))
    xh = xc * r
    for b in range(part.shape[1] // 256):
        cols = slice(b * 256, (b + 1) * 256)
        dn = dg(dm, wqkv[cols, :], 1, 1)
        vg[0:1, cols] += jnp.sum(dn * xh[:, cols], axis=0, keepdims=True)
        vg[1:2, cols] += jnp.sum(dn, axis=0, keepdims=True)
        part[rows, cols] = (dn * vec[0:1, cols] + e2[rows, cols].astype(F32)).astype(BF)


def qkv_grad(n1, dmix, acc, half):
    acc[...] = jnp.zeros_like(acc)

    def body(i, _):
        rows = ds(i * half, half)
        n1t = n1[rows, :].T
        for b in range(3):
            cols = slice(b * HW, (b + 1) * HW)
            acc[:, cols] += dot(n1t, dmix[rows, cols])
        return 0

    lax.fori_loop(0, n1.shape[0] // half, body, 0)


def store_low(acc, out):
    def body(i, _):
        rr = ds(i * SUB, SUB)
        out[rr, :] = acc[rr, :].astype(BF)
        return 0

    lax.fori_loop(0, acc.shape[0] // SUB, body, 0)


def residual_out(sc, own, vec, write, after=None):
    for a in range(2):
        sc.arrive(a)

        def body(i, _, a=a):
            base = own[ds(sc.own(sc.side(a)) + i * SUB, SUB), :].astype(F32)
            write(a, i, (base + sc.total(a, i) + vec[2:3, :] + vec[5:6, :]).astype(BF))
            return 0

        lax.fori_loop(0, sc.half // SUB, body, 0)
        if after is not None:
            after(a)


def grad_out(sc, dy, hf, vec, write, after=None):
    for a in range(2):
        sc.arrive(a)

        def body(i, _, a=a):
            rr = ds(sc.own(sc.side(a)) + i * SUB, SUB)
            xc, r = norm_stats(hf[rr, :].astype(F32))
            xh = xc * r
            e = sc.total(a, i)
            m1 = jnp.mean(e, axis=-1, keepdims=True)
            m2 = jnp.mean(e * xh, axis=-1, keepdims=True)
            write(a, i, (dy(a, i).astype(F32) + r * (e - m1 - xh * m2)).astype(BF))
            return 0

        lax.fori_loop(0, sc.half // SUB, body, 0)
        if after is not None:
            after(a)


def column_sum(tok, ref, vg, row):
    total = jnp.zeros((1, ref.shape[1]), F32)
    for a in range(2):

        def body(i, acc, a=a):
            return acc + jnp.sum(ref[ds(tok.own(a) + i * SUB, SUB), :].astype(F32), axis=0, keepdims=True)

        total = lax.fori_loop(0, tok.half // SUB, body, total)
    vg[row : row + 1, :] = total


def load(pairs, sem):
    copies = [pltpu.make_async_copy(a, b, sem.at[i]) for i, (a, b) in enumerate(pairs)]
    for c in copies:
        c.start()
    return copies


def params(cid):
    return pltpu.CompilerParams(collective_id=cid, has_side_effects=True, vmem_limit_bytes=67043328)


def cost(us):
    return pl.CostEstimate(flops=int(us * 8e8), bytes_accessed=0, transcendentals=0)


class Stores:
    def __init__(self, pairs, half, sem):
        self.pairs, self.half, self.sem = pairs, half, sem

    def copy(self, n, r0, i):
        src, dst = self.pairs[n]
        rows = ds(r0, self.half)
        return pltpu.make_async_copy(src.at[rows], dst.at[rows], self.sem.at[n, i])

    def start(self, which, r0, i):
        for n in which:
            self.copy(n, r0, i).start()

    def finish(self):
        def body(i, _):
            for n in range(len(self.pairs)):
                self.copy(n, i * self.half, i).wait()
            return 0

        lax.fori_loop(0, 8, body, 0)


def in_kernel(
    cfg, in_ref, cot_ref, seg_ref, live, w_ref, sv_ref, fr_ref,
    hf_o, n1_o, n2_o, g_o, gp_o, tab_o, w_o, q_o, k_o, v_o, cf_o, vecs, srow, kcol,
    hf, n1, n2, g, gp, tab, q, k, v, wfull, gat, vb, cot, gss, grs, css, crs, yss, yrs, lsem, ssem, vss, vrs, *wsems,
):
    col, dp, tensor = cfg["col"], cfg["dp"], cfg["tensor"]
    me = Mesh(dp, tensor)
    ga = Gather(me, hf, gss, grs, me.y)
    gc = Gather(me, cf_o, css, crs, me.y)
    half = ga.half
    part = ds(me.s * half, half)
    first = pltpu.make_async_copy(in_ref.at[me.y, 0, part], hf.at[ds(ga.own(me.y), half)], lsem.at[0])
    first.start()
    up = pltpu.make_async_copy(cot_ref.at[me.y, 0, part], cot, lsem.at[4])
    up.start()
    greet([me.mate, me.across_mate] + me.ring + me.group)
    over = [
        push(ref.at[1 - me.y, 0, part], full.at[ds(ga.own(me.y), half)], yss.at[n], yrs.at[n], me.across)
        for n, (ref, full) in enumerate(((in_ref, hf), (cot_ref, cf_o)))
    ]
    wg = WeightGather(me, 0, w_ref, wfull, gat, cfg["groups"], wsems)
    vg = VectorGather(me, sv_ref, vb, vss, vrs, lsem.at[1])
    st = Stores([(hf, hf_o), (n1, n1_o), (n2, n2_o), (g, g_o), (gp, gp_o), (q, q_o), (k, k_o), (v, v_o)], half, ssem)
    vg.send(0)
    wg.send_ring()
    first.wait()
    document_tables(seg_ref[me.y], live[0, me.y], fr_ref, tab, srow, kcol)
    vg.wait(0)
    vg.send(1)
    ga.start(0)
    over[0].start()
    wg.send_own(0)
    tab_out = pltpu.make_async_copy(tab, tab_o, lsem.at[2])
    tab_out.start()
    vg.wait(1)
    vg.send(2)
    up.wait()
    cot_out = pltpu.make_async_copy(cot, cf_o.at[ds(gc.own(me.y), half)], lsem.at[5])
    cot_out.start()
    vg.wait(2)
    vg.build(vecs, cfg["heads"], cfg["own"], cfg["qw"], cfg["fw"])
    vec = vecs.at[0]

    def norm(r0, i):
        project_norm(r0, half, hf, vec, n1, n2)
        st.start((0, 1, 2), r0, i)

        @pl.when(i == 0)
        def _():
            over[0].wait_recv()
            ga.start(1)

        @pl.when(i == 1)
        def _():
            wg.forward(0)
            wg.send_own(1)
            wg.send_own(2)

    ga.run(norm)
    cot_out.wait()
    gc.start(0)
    wg.ready(0)

    def qkv(i, _):
        r0 = ga.order(i)
        project_qkv(r0, half, wfull.at[:, 0 : col["fc1"]], vec, tab, n1, q, k, v)
        st.start((5, 6, 7), r0, i)
        return 0

    lax.fori_loop(0, 8, qkv, 0)
    wg.forward(1)
    over[1].start()
    wg.ready(1)

    def fc1(i, _):
        r0 = ga.order(i)
        project_fc1(r0, half, wfull.at[:, col["fc1"] : col["fc2"]], vec, n2, g, gp)
        st.start((3, 4), r0, i)

        @pl.when(i == 6)
        def _():
            wg.forward(2)

        return 0

    lax.fori_loop(0, 8, fc1, 0)
    gc.step(2)
    gc.step(4)
    over[1].wait_recv()
    gc.start(1)
    st.finish()
    tab_out.wait()
    wg.ready(2)
    w_out = pltpu.make_async_copy(wfull, w_o, lsem.at[3])
    w_out.start()
    for n in (3, 5, 6, 7):
        gc.step(n)
    wg.finish()
    vg.finish()
    gc.finish()
    for c in over:
        c.wait_send()
    w_out.wait()


def layer_in(cfg, inputs, cotangent, segments, live, w, sv, fr):
    seq, model, ff = segments.shape[2], inputs.shape[3], cfg["ff"]
    dp, tensor = cfg["dp"], cfg["tensor"]
    rows, hidden = sds((seq, model), BF), sds((seq, ff), BF)
    heads = sds((seq, HW), BF)
    nv = dp - 1 + tensor
    wide, wide_h, wide_q = pltpu.VMEM((seq, model), BF), pltpu.VMEM((seq, ff), BF), pltpu.VMEM((seq, HW), BF)
    weights = pltpu.VMEM((model, w.shape[1]), BF)
    return pl.pallas_call(
        functools.partial(in_kernel, cfg),
        out_shape=(rows, rows, rows, hidden, hidden, sds((seq, 256), F32), sds((model, w.shape[1]), BF),
                   heads, heads, heads, rows,
                   sds((2, 8, model), F32), sds((8, seq), jnp.int32), sds((seq, 128), jnp.int32)),
        in_specs=[ANY, ANY, VMEM, SMEM, VMEM, VMEM, VMEM],
        out_specs=(ANY,) * 11 + (VMEM,) * 3,
        scratch_shapes=[
            wide, wide, wide, wide_h, wide_h, pltpu.VMEM((seq, 256), F32), wide_q, wide_q, wide_q,
            weights, weights, pltpu.VMEM((2, tensor, dp) + sv.shape, F32),
            pltpu.VMEM((seq // 8, model), BF),
            DMA((6,)), DMA((6,)), DMA((6,)), DMA((6,)), DMA((2,)), DMA((2,)), DMA((6,)), DMA((8, 8)),
            DMA((nv,)), DMA((nv,)),
        ]
        + WeightGather.scratch(dp, 3),
        compiler_params=params(2),
        cost_estimate=cost(45),
        name="layer_in",
    )(inputs, cotangent, segments, live, w, sv, fr)


def mid_kernel(
    cfg, q_in, k_in, v_in, srow, kcol, g_in, x_in, w_ref, w0, vecs, tab_in,
    o_o, lse, hf_o, n1_o, n2_o, g_o, gp_o, w_o, q_o, k_o, v_o,
    wout, wfc2, hf, n1, n2, g, gp, tab, wfull, gat, q, k, v, o, vt, s_scr,
    part, mr, xr, sss, srs, gss, grs, lsem, ssem, osem, *wsems,
):
    col, heads = cfg["col"], cfg["heads"]
    me = Mesh(cfg["dp"], cfg["tensor"])
    sc = Scatter(me, part, mr, xr, sss, srs)
    ga = Gather(me, hf, gss, grs)
    half = sc.half
    loads = load(
        [
            (v_in, v),
            (q_in, q),
            (k_in, k),
            (w0.at[:, col["out"] : col["end"]], wout),
            (w0.at[:, col["fc2"] : col["out"]], wfc2),
            (g_in, g),
            (tab_in, tab),
        ]
        + [(x_in.at[ds(sc.own(a), half)], hf.at[ds(sc.own(a), half)]) for a in range(2)],
        lsem,
    )
    greet([me.mate, me.beside, me.across, me.across_mate] + me.ring)
    wg = WeightGather(me, 1, w_ref, wfull, gat, cfg["groups"], wsems)
    wg.send_ring()
    for n in range(3):
        wg.send_own(n)
    loads[0].wait()
    turn_blocks(v, vt)
    for c in loads[1:]:
        c.wait()
    st = Stores([(hf, hf_o), (n1, n1_o), (n2, n2_o), (g, g_o), (gp, gp_o), (q, q_o), (k, k_o), (v, v_o)], half, ssem)
    st_o = Stores([(o, o_o)], half, osem)

    def out(r0, i):
        b = r0 // QB
        attn_fwd_block(b, jnp.maximum(b - DOC_MAX // QB, 0), b, heads, q, k, vt, srow, kcol, s_scr, o, lse)
        st_o.start((0,), r0, i)
        branch_out(r0, half, o, g, wout, wfc2, part)

        @pl.when(i == 6)
        def _():
            wg.forward(0)

    sc.run(out)

    def write(a, i, value):
        hf[ds(sc.own(a) + i * SUB, SUB), :] = value

    residual_out(sc, hf, vecs.at[0], write, ga.start)
    wg.forward(1)
    vec = vecs.at[1]

    def fc1(i):
        r0 = ga.order(i)
        project_fc1(r0, half, wfull.at[:, col["fc1"] : col["fc2"]], vec, n2, g, gp)
        st.start((3, 4), r0, i)

    def work(r0, i):
        project_norm(r0, half, hf, vec, n1, n2)

        @pl.when(i == 0)
        def _():
            wg.ready(0)

        project_qkv(r0, half, wfull.at[:, 0 : col["fc1"]], vec, tab, n1, q, k, v)
        st.start((0, 1, 2, 5, 6, 7), r0, i)

        @pl.when(i == 4)
        def _():
            wg.ready(1)

        @pl.when(i >= 4)
        def _():
            fc1(i - 4)

        @pl.when(i == 5)
        def _():
            wg.forward(2)

    ga.run(work)

    def late(i, _):
        fc1(i)
        return 0

    lax.fori_loop(4, 8, late, 0)
    st.finish()
    wg.ready(2)
    w_out = pltpu.make_async_copy(wfull, w_o, lsem.at[0])
    w_out.start()
    sc.finish()
    wg.finish()
    st_o.finish()
    w_out.wait()


def layer_mid(cfg, q, k, v, srow, kcol, g, xf, w, w0, vecs, tab):
    seq, model, ff = tab.shape[0], xf.shape[1], cfg["ff"]
    rows, hidden, heads = sds((seq, model), BF), sds((seq, ff), BF), sds((seq, HW), BF)
    wide, wide_h, wide_q = pltpu.VMEM((seq, model), BF), pltpu.VMEM((seq, ff), BF), pltpu.VMEM((seq, HW), BF)
    return pl.pallas_call(
        functools.partial(mid_kernel, cfg),
        out_shape=(heads, sds((8, seq), F32), rows, rows, rows, hidden, hidden, sds(w0.shape, BF), heads, heads, heads),
        in_specs=[ANY, ANY, ANY, VMEM, VMEM, ANY, ANY, VMEM, ANY, VMEM, ANY],
        out_specs=(ANY, VMEM) + (ANY,) * 9,
        scratch_shapes=[
            pltpu.VMEM((model, HW), BF), pltpu.VMEM((model, ff), BF),
            wide, wide, wide, wide_h, wide_h, pltpu.VMEM((seq, 256), F32),
            pltpu.VMEM(w0.shape, BF), pltpu.VMEM(w0.shape, BF),
            wide_q, wide_q, wide_q, wide_q, pltpu.VMEM((HW, seq), BF),
            pltpu.VMEM((cfg["heads"], DOC_MAX + QB, QB), F32),
        ]
        + scatter_scratch(seq, model)
        + [DMA((6,)), DMA((6,)), DMA((9,)), DMA((8, 8)), DMA((1, 8))]
        + WeightGather.scratch(cfg["dp"], 3),
        compiler_params=params(3),
        cost_estimate=cost(70),
        name="layer_mid",
    )(q, k, v, srow, kcol, g, xf, w, w0, vecs, tab)


def turn_kernel(
    cfg, o_in, g_in, hf_in, cf, w1, vecs, n2_in, gp_in, y_o, do_o, e2_o, gr_o, vg,
    o, g, hf, dyf, n2, gp, e2, do, y, gr, wout, wfc2, wfc1, da, acc,
    part, mr, xr, sss, srs, lsem, ssem,
):
    col = cfg["col"]
    me = Mesh(cfg["dp"], cfg["tensor"])
    sc = Scatter(me, part, mr, xr, sss, srs)
    half = sc.half
    loads = load(
        [
            (w1.at[:, col["out"] : col["end"]], wout),
            (w1.at[:, col["fc2"] : col["out"]], wfc2),
            (o_in, o),
            (g_in, g),
            (w1.at[:, col["fc1"] : col["fc2"]], wfc1),
            (cf, dyf),
            (gp_in, gp),
            (hf_in, hf),
            (n2_in, n2),
        ],
        lsem,
    )
    greet([me.mate, me.beside])
    for c in loads[:4]:
        c.wait()
    vec = vecs.at[1]
    st = Stores([(e2, e2_o), (do, do_o)], half, ssem)

    def early():
        vg[...] = jnp.zeros_like(vg)
        acc[...] = jnp.zeros_like(acc)
        for c in loads[4:]:
            c.wait()

        def head(i, _):
            r0 = i * half
            back_head(r0, half, dyf, hf, g, gp, n2, o, wfc1, wfc2, wout, vec, do, e2, da, acc, vg)
            st.start((0, 1), r0, i)
            return 0

        lax.fori_loop(0, 8, head, 0)

    sc.run(lambda r0, i: branch_out(r0, half, o, g, wout, wfc2, part), early)
    column_sum(sc, dyf, vg, 2)
    store_low(acc, gr)
    gr_out = pltpu.make_async_copy(gr, gr_o, lsem.at[0])
    gr_out.start()

    def write(a, i, value):
        y[a, ds(i * SUB, SUB), :] = value

    residual_out(sc, hf, vec, write)
    y_out = pltpu.make_async_copy(y, y_o, lsem.at[1])
    y_out.start()
    sc.finish()
    st.finish()
    gr_out.wait()
    y_out.wait()


def layer_turn(cfg, o, g, hf, cf, w1, vecs, n2, gp):
    seq, model = hf.shape
    ff = cfg["ff"]
    wide, hidden, heads = pltpu.VMEM((seq, model), BF), pltpu.VMEM((seq, ff), BF), pltpu.VMEM((seq, HW), BF)
    owned = (2, seq // 8, model)
    return pl.pallas_call(
        functools.partial(turn_kernel, cfg),
        out_shape=(
            sds(owned, BF),
            sds((seq, HW), BF),
            sds((seq, model), BF),
            sds((model, 2 * ff + HW), BF),
            sds((8, model), F32),
        ),
        in_specs=[ANY] * 5 + [VMEM, ANY, ANY],
        out_specs=(ANY,) * 4 + (VMEM,),
        scratch_shapes=[
            heads, hidden, wide, wide, wide, hidden, wide, heads, pltpu.VMEM(owned, BF),
            pltpu.VMEM((model, 2 * ff + HW), BF),
            pltpu.VMEM((model, HW), BF), pltpu.VMEM((model, ff), BF), pltpu.VMEM((model, ff), BF),
            pltpu.VMEM((seq // 8, ff), BF), pltpu.VMEM((model, 2 * ff + HW), F32),
        ]
        + scatter_scratch(seq, model)
        + [DMA((9,)), DMA((2, 8))],
        compiler_params=params(4),
        cost_estimate=cost(40),
        name="layer_turn",
    )(o, g, hf, cf, w1, vecs, n2, gp)


def back_kernel(
    cfg, dm_in, e2_in, cf, hf_in, n1_in, w1, w0, vecs, xf_in, g_in, gp_in, n2_in, o_in, gr1,
    dh_o, e2_o, do_o, vgf, vgd, out1_o, outq_o, gr_o,
    dmix, o, do, a, b, e2, g, gp, wqkv, wout, wfc2, wfc1, dhf, da, acc, gq, gr, got, gotq, acrq,
    sb, rb, sbq, rbq, out1, outq, part, mr, xr, sss, srs, gss, grs, lsem, ssem, *rsems,
):
    col, dp = cfg["col"], cfg["dp"]
    me = Mesh(dp, cfg["tensor"])
    ga = Gather(me, dhf, gss, grs)
    sc = Scatter(me, part, mr, xr, sss, srs)
    half = sc.half
    own = [ds(sc.own(n), half) for n in range(2)]
    loads = load(
        [
            (w1.at[:, col["qkv"] : col["fc1"]], wqkv),
            (dm_in, dmix),
            (hf_in, a),
            (e2_in, e2),
            (n1_in, b),
            (w0.at[:, col["out"] : col["end"]], wout),
            (w0.at[:, col["fc2"] : col["out"]], wfc2),
            (w0.at[:, col["fc1"] : col["fc2"]], wfc1),
            (g_in, g),
            (gp_in, gp),
            (o_in, o),
        ]
        + [(cf.at[rr], dhf.at[rr]) for rr in own],
        lsem,
    )
    gr_load = pltpu.make_async_copy(gr1, gr, lsem.at[13])
    holds = (me.s == 1) & (me.y == 1)

    @pl.when(holds)
    def _():
        gr_load.start()

    greet([me.mate, me.beside, me.across, me.across_mate] + me.ring)
    red1 = GradReduce(me, 1, gr1, gr, gr, got, sb, rb, out1, rsems[:6])
    redq = GradReduce(me, 1, gq, gq, gotq, acrq, sbq, rbq, outq, rsems[6:])
    st = Stores([(e2, e2_o), (do, do_o), (dhf, dh_o)], half, ssem)
    red1.send()
    vgf[...] = jnp.zeros_like(vgf)
    vgd[...] = jnp.zeros_like(vgd)
    for c in loads[:4]:
        c.wait()

    def early():
        loads[4].wait()
        small = acc.at[:, 0 : 3 * HW]
        qkv_grad(b, dmix, small, half)
        store_low(small, gq)
        redq.send()

        @pl.when(holds)
        def _():
            gr_load.wait()

        red1.step(0)

    sc.run(lambda r0, i: back_tail(r0, half, dmix, a, e2, wqkv, vecs.at[1], part, vgf), early)
    acc[...] = jnp.zeros_like(acc)
    again = pltpu.make_async_copy(n2_in, b, lsem.at[14])
    again.start()
    for c in loads[5:]:
        c.wait()
    for d in range(1, dp // 2):
        red1.step(d)

    def write(n, i, value):
        dhf[ds(sc.own(n) + i * SUB, SUB), :] = value

    grad_out(sc, lambda n, i: dhf[ds(sc.own(n) + i * SUB, SUB), :], a, vecs.at[1], write, ga.start)
    other = pltpu.make_async_copy(xf_in, a, lsem.at[15])
    other.start()
    again.wait()
    other.wait()

    def work(r0, i):
        back_head(r0, half, dhf, a, g, gp, b, o, wfc1, wfc2, wout, vecs.at[0], do, e2, da, acc, vgd)
        st.start((0, 1, 2), r0, i)

        @pl.when(i == 1)
        def _():
            for d in range(dp // 2, dp - 1):
                red1.step(d)

        @pl.when(i == 3)
        def _():
            red1.step(dp - 1)

        @pl.when(i == 5)
        def _():
            redq.step(0)

    ga.run(work)
    for d in range(1, dp):
        redq.step(d)
    store_low(acc, gr)
    gr_out = pltpu.make_async_copy(gr, gr_o, lsem.at[0])
    gr_out.start()
    column_sum(sc, dhf, vgd, 2)
    red1.collect()
    redq.collect()
    outs = [pltpu.make_async_copy(out1, out1_o, lsem.at[1]), pltpu.make_async_copy(outq, outq_o, lsem.at[2])]
    for c in outs:
        c.start()
    red1.finish()
    redq.finish()
    sc.finish()
    st.finish()
    gr_out.wait()
    for c in outs:
        c.wait()


def layer_back(cfg, dmix, e2, cf, hf, n1, w1, w0, vecs, xf, g, gp, n2, o, gr1):
    seq, model = hf.shape
    ff, dp = cfg["ff"], cfg["dp"]
    rows, nr, nq = model // dp, 2 * ff + HW, 3 * HW
    wide, hidden, heads = pltpu.VMEM((seq, model), BF), pltpu.VMEM((seq, ff), BF), pltpu.VMEM((seq, HW), BF)
    return pl.pallas_call(
        functools.partial(back_kernel, cfg),
        out_shape=(
            sds((seq, model), BF),
            sds((seq, model), BF),
            sds((seq, HW), BF),
            sds((8, model), F32),
            sds((8, model), F32),
            sds((rows, nr), F32),
            sds((rows, nq), F32),
            sds((model, nr), BF),
        ),
        in_specs=[ANY] * 7 + [VMEM] + [ANY] * 6,
        out_specs=(ANY, ANY, ANY, VMEM, VMEM, ANY, ANY, ANY),
        scratch_shapes=[
            pltpu.VMEM((seq, nq), BF), heads, heads, wide, wide, wide, hidden, hidden,
            pltpu.VMEM((model, nq), BF), pltpu.VMEM((model, HW), BF), pltpu.VMEM((model, ff), BF),
            pltpu.VMEM((model, ff), BF), wide, pltpu.VMEM((seq // 8, ff), BF), pltpu.VMEM((model, nr), F32),
            pltpu.VMEM((model, nq), BF), pltpu.VMEM((model, nr), BF), pltpu.VMEM((model, nr), BF),
            pltpu.VMEM((model, nq), BF), pltpu.VMEM((model, nq), BF),
            pltpu.VMEM((dp - 1, rows, nr), BF), pltpu.VMEM((dp - 1, rows, nr), BF),
            pltpu.VMEM((dp - 1, rows, nq), BF), pltpu.VMEM((dp - 1, rows, nq), BF),
            pltpu.VMEM((rows, nr), F32), pltpu.VMEM((rows, nq), F32),
        ]
        + scatter_scratch(seq, model)
        + [DMA((6,)), DMA((6,)), DMA((16,)), DMA((3, 8))]
        + GradReduce.scratch(dp) * 2,
        compiler_params=params(5),
        cost_estimate=cost(70),
        name="layer_back",
    )(dmix, e2, cf, hf, n1, w1, w0, vecs, xf, g, gp, n2, o, gr1)


def last_kernel(
    cfg, q_in, k_in, v_in, o_in, do_in, lse, srow, kcol, tab_in, e2_in, dh_in, xf_in, n1_in, w0, vecs, vf1, vd1, vd0,
    gr0, out1, outq, hf_in, y_in, so, ig, fq_o, fr_o, vec_o,
    q, k, v, o, do, tab, kt, dk, dv, dmix, dh, dx, xf, n1, e2, wqkv, gq, gotq, acrq, sbq, rbq, gr, got, sb, rb, fq, fr,
    vgf, va, vr, vout, part, mr, xr, sss, srs, lsem, vss, vrs, oss, ors, *rsems,
):
    col, heads, dp = cfg["col"], cfg["heads"], cfg["dp"]
    me = Mesh(dp, cfg["tensor"])
    sc = Scatter(me, part, mr, xr, sss, srs, 1 - me.y)
    half = sc.half
    seq = xf.shape[0]
    width = q.shape[1]
    own = [ds(sc.own(n), half) for n in range(2)]
    loads = load(
        [
            (k_in, k),
            (q_in, q),
            (v_in, v),
            (do_in, do),
            (o_in, o),
            (tab_in, tab),
            (w0.at[:, col["qkv"] : col["fc1"]], wqkv),
            (xf_in, xf),
            (e2_in, e2),
            (n1_in, n1),
        ]
        + [(dh_in.at[rr], dh.at[n]) for n, rr in enumerate(own)],
        lsem,
    )
    gr_load = pltpu.make_async_copy(gr0, gr, lsem.at[12])
    holds = (me.s == 0) & (me.y == 0)

    @pl.when(holds)
    def _():
        gr_load.start()

    greet([me.mate, me.beside, me.beside_mate, me.across, me.across_mate] + me.ring)
    redr = GradReduce(me, 0, gr0, gr, gr, got, sb, rb, fr, rsems[:6])
    redq = GradReduce(me, 0, gq, gq, gotq, acrq, sbq, rbq, fq, rsems[6:])
    vr_ = VectorReduce(me, va, vr, vss, vrs)
    redr.send()

    def at(dst, h):
        return dst.at[0, me.y, 0, pl.ds(h * half, half)]

    def full_out(src, dst, i):
        chunk = 2 * half
        mine, theirs = ds(me.t * chunk, chunk), ds(me.py * chunk, chunk)
        return [
            pltpu.make_async_copy(src.at[mine], dst.at[0, me.y, 0], lsem.at[13]),
            push(src.at[theirs], dst.at[0, me.y, 0], oss.at[i], ors.at[i], me.across),
        ]

    def owned_out(src, dst, core, i):
        here, far = src.at[me.y], src.at[1 - me.y]
        place = dst.at[0, me.y, 0, ds(me.s * half, half)]
        across = push(far, place, oss.at[i], ors.at[i + me.s], me.across_core(core))
        local = pltpu.make_async_copy(here, place, lsem.at[14])
        mate = push(here, place, oss.at[i + 2], ors.at[i + 2], me.mate)
        return across, local, mate

    def whole(n):
        return full_out(hf_in, so, 0) if n == 0 else full_out(dh_in, ig, 0)

    for n in range(2):

        @pl.when(me.s == n)
        def _(n=n):
            for c in whole(n):
                c.start()

    def start_here(src, dst, core, i):
        across, local, mate = owned_out(src, dst, core, i)

        @pl.when(me.s == core)
        def _():
            local.start()

        @pl.when(me.s != core)
        def _():
            mate.start()

    def wait_owned(src, dst, core, i):
        across, local, mate = owned_out(src, dst, core, i)
        across.wait_send()

        @pl.when(me.s == core)
        def _():
            local.wait()
            mate.wait_recv()
            for n in range(2):
                push(src.at[0], at(dst, n), oss.at[i], ors.at[i + n], me.across_core(core)).wait_recv()

        @pl.when(me.s != core)
        def _():
            mate.wait_send()

    owned_out(y_in, so, 1, 1)[0].start()
    start_here(y_in, so, 1, 1)
    old = [pltpu.make_async_copy(out1, fr, lsem.at[15]), pltpu.make_async_copy(outq, fq, lsem.at[16])]

    @pl.when(me.s == 1)
    def _():
        for c in old:
            c.start()

    vgf[...] = jnp.zeros_like(vgf)
    dk[...] = jnp.zeros_like(dk)
    dv[...] = jnp.zeros_like(dv)
    loads[0].wait()
    turn_blocks(k, kt)
    for c in loads[1:6]:
        c.wait()

    @pl.when(holds)
    def _():
        gr_load.wait()

    n_blocks = seq // QB

    def qloop(i, _):
        lo = jnp.maximum(i - DOC_MAX // QB, 0)
        attn_bwd_block(i, lo, i, heads, q, k, v, o, do, kt, lse, srow, kcol, tab, dk, dv, dmix)
        for at_block, steps in (
            (n_blocks // 2 - 1, range(0, 1)),
            (n_blocks // 2, range(1, dp // 2)),
            (n_blocks // 2 + 1, range(dp // 2, dp - 1)),
            (n_blocks - 2, range(dp - 1, dp)),
        ):

            @pl.when(i == at_block)
            def _(steps=steps):
                for d in steps:
                    redr.step(d)

        return 0

    lax.fori_loop(0, n_blocks, qloop, 0)

    def close(i, _):
        ii = ds(i * QB, QB)
        dmix[ii, width : 2 * width] = turn_lanes(dk[ii, :], tab[ii, :], -1).astype(BF)
        dmix[ii, 2 * width : 3 * width] = dv[ii, :].astype(BF)
        return 0

    lax.fori_loop(0, n_blocks, close, 0)
    for c in loads[6:]:
        c.wait()

    def early():
        va[0, 0:8, :] = vgf[...] + vd0[...]
        va[0, 8:16, :] = vf1[...] + vd1[...]
        vr_.send(0)
        nf = gq.shape[0]
        accs = [dk.at[0:nf], dk.at[nf : 2 * nf], dv.at[0:nf]]
        for acc in accs:
            acc[...] = jnp.zeros_like(acc)

        def body(i, _):
            rows = ds(i * half, half)
            n1t = n1[rows, :].T
            for p, acc in enumerate(accs):
                acc[...] += dot(n1t, dmix[rows, p * HW : (p + 1) * HW])
            return 0

        lax.fori_loop(0, 8, body, 0)
        for p, acc in enumerate(accs):
            gq[:, p * HW : (p + 1) * HW] = acc[...].astype(BF)
        vr_.add(0, va.at[1])
        vr_.send(1)
        redq.send()
        vr_.add(1, va.at[2])
        vr_.send(2)
        redq.step(0)

    sc.run(lambda r0, i: back_tail(r0, half, dmix, xf, e2, wqkv, vecs.at[0], part, vgf), early)
    for d in range(1, dp - 1):
        redq.step(d)

    def write(n, i, value):
        dx[sc.side(n), ds(i * SUB, SUB), :] = value

    def leave(n):
        if n == 0:
            owned_out(dx, ig, 0, 4)[0].start()
        else:
            start_here(dx, ig, 0, 4)

    grad_out(sc, lambda n, i: dh[sc.side(n), ds(i * SUB, SUB), :], xf, vecs.at[0], write, leave)
    redq.step(dp - 1)
    vr_.add(2, vout)
    vec_o[...] = jnp.where(me.s == 0, vout[0:8, :], vout[8:16, :])
    redr.collect()
    redq.collect()

    @pl.when(me.s == 1)
    def _():
        for c in old:
            c.wait()

    ends = [pltpu.make_async_copy(fr, fr_o, lsem.at[0]), pltpu.make_async_copy(fq, fq_o, lsem.at[1])]
    for c in ends:
        c.start()
    redr.finish()
    redq.finish()
    vr_.finish()
    sc.finish()
    for n in range(2):

        @pl.when(me.s == n)
        def _(n=n):
            for c in whole(n):
                c.wait()

    wait_owned(y_in, so, 1, 1)
    wait_owned(dx, ig, 0, 4)
    for c in ends:
        c.wait()


def layer_last(cfg, q, k, v, o, do, lse, sr, kc, tab, e2, dh, xf, n1, w0, vecs, vf1, vd1, vd0, gr0, out1, outq, hf, y):
    seq, model = xf.shape
    dp, tensor, ff = cfg["dp"], cfg["tensor"], cfg["ff"]
    rows, nr, nq = model // dp, 2 * ff + HW, 3 * HW
    nv = dp + tensor - 1
    wide, owned, heads = pltpu.VMEM((seq, model), BF), pltpu.VMEM((2, seq // 8, model), BF), pltpu.VMEM((seq, HW), BF)
    both = sds((1, 2, 1, seq // 4, model), BF)
    return pl.pallas_call(
        functools.partial(last_kernel, cfg),
        out_shape=(both, both, sds((rows, nq), F32), sds((rows, nr), F32), sds((8, model), F32)),
        in_specs=[ANY] * 5 + [VMEM] * 3 + [ANY] * 6 + [VMEM] * 4 + [ANY] * 5,
        out_specs=(ANY, ANY, ANY, ANY, VMEM),
        scratch_shapes=[
            heads, heads, heads, heads, heads, pltpu.VMEM(tab.shape, F32), pltpu.VMEM((HW, seq), BF),
            pltpu.VMEM((seq, HW), F32), pltpu.VMEM((seq, HW), F32), pltpu.VMEM((seq, nq), BF), owned, owned,
            wide, wide, wide, pltpu.VMEM((model, nq), BF),
            pltpu.VMEM((model, nq), BF), pltpu.VMEM((model, nq), BF), pltpu.VMEM((model, nq), BF),
            pltpu.VMEM((dp - 1, rows, nq), BF), pltpu.VMEM((dp - 1, rows, nq), BF),
            pltpu.VMEM((model, nr), BF), pltpu.VMEM((model, nr), BF),
            pltpu.VMEM((dp - 1, rows, nr), BF), pltpu.VMEM((dp - 1, rows, nr), BF),
            pltpu.VMEM((rows, nq), F32), pltpu.VMEM((rows, nr), F32),
            pltpu.VMEM((8, model), F32), pltpu.VMEM((3, 16, model), F32), pltpu.VMEM((nv, 16, model), F32),
            pltpu.VMEM((16, model), F32),
        ]
        + scatter_scratch(seq, model)
        + [DMA((17,)), DMA((nv,)), DMA((nv,)), DMA((7,)), DMA((7,))]
        + GradReduce.scratch(dp) * 2,
        compiler_params=params(6),
        cost_estimate=cost(80),
        name="layer_last",
    )(q, k, v, o, do, lse, sr, kc, tab, e2, dh, xf, n1, w0, vecs, vf1, vd1, vd0, gr0, out1, outq, hf, y)


def finish_kernel(
    cfg, so_in, ig_in, fq_in, fr_in, vec, so, ig, bg1, bb1, gqkv, bqkv, gout, bdy, bdy2, bg2, bb2, gfc1, bfc1, gfc2,
    a, b, fq, fr, lsem, osem,
):
    heads, ff, own, qw, fw = cfg["heads"], cfg["ff"], cfg["own"], cfg["qw"], cfg["fw"]
    me = Mesh(cfg["dp"], cfg["tensor"])
    loads = load([(fr_in, fr), (fq_in, fq), (so_in, a), (ig_in, b)], lsem)
    model = vec.shape[1]
    short = pltpu.roll(vec[...], (model - (me.z * me.tensor + me.t) * own) % model, 1)
    for row, ref in ((0, bg1), (1, bb1), (2, bdy), (2, bdy2), (3, bg2), (4, bb2)):
        ref[...] = short[row : row + 1, 0:own]
    for h in range(heads):
        parts = [vec[6:7, p * HW + h * HD : p * HW + (h + 1) * HD] for p in range(3)]
        one = jnp.concatenate(parts + [jnp.zeros((1, HW - 3 * HD), F32)], axis=1)
        one = jnp.broadcast_to(one, (8, HW))
        bqkv[h] = pltpu.roll(one, (HW - me.z * qw) % HW, 1)[0:1, 0:qw]
        wide = ff // heads
        one = jnp.broadcast_to(vec[7:8, h * wide : (h + 1) * wide], (8, wide))
        bfc1[h] = pltpu.roll(one, (wide - me.z * fw) % wide, 1)[0:1, 0:fw]
    loads[0].wait()
    gfc1[0] = fr[:, 0:ff]
    gfc2[...] = fr[:, ff : 2 * ff]
    gout[0] = fr[:, 2 * ff : 2 * ff + HW].T[0 : heads * HD, :]
    loads[2].wait()
    loads[3].wait()
    outs = [pltpu.make_async_copy(a, so, osem.at[0]), pltpu.make_async_copy(b, ig, osem.at[1])]
    for c in outs:
        c.start()
    loads[1].wait()
    pieces = [fq[:, p * HW + h * HD : p * HW + (h + 1) * HD] for h in range(heads) for p in range(3)]
    gqkv[0] = jnp.concatenate(pieces, axis=1)
    for c in outs:
        c.wait()


def finish(cfg, so, ig, fq, fr, vec):
    heads, ff, rows = cfg["heads"], cfg["ff"], fq.shape[0]
    line = sds((1, cfg["own"]), F32)
    return pl.pallas_call(
        functools.partial(finish_kernel, cfg),
        out_shape=(sds(so.shape, BF), sds(ig.shape, BF), line, line, sds((1, rows, heads * 3 * HD), F32),
                   sds((heads, 1, cfg["qw"]), F32), sds((1, heads * HD, rows), F32), line, line, line, line,
                   sds((1, rows, ff), F32), sds((heads, 1, cfg["fw"]), F32), sds((rows, ff), F32)),
        in_specs=[ANY] * 4 + [VMEM],
        out_specs=(ANY, ANY) + (VMEM,) * 12,
        scratch_shapes=[
            pltpu.VMEM(so.shape, BF), pltpu.VMEM(ig.shape, BF), pltpu.VMEM(fq.shape, F32), pltpu.VMEM(fr.shape, F32),
            DMA((4,)), DMA((2,)),
        ],
        compiler_params=pltpu.CompilerParams(vmem_limit_bytes=67043328),
        cost_estimate=cost(5),
        name="finish",
    )(so, ig, fq, fr, vec)


def by_part(w):
    rows = w.shape[0]
    heads = w.shape[1] // (3 * HD)
    w = w.reshape(rows, heads, 3, HD).transpose(0, 2, 1, 3).reshape(rows, 3, heads * HD)
    return jnp.pad(w, ((0, 0), (0, 0), (0, HW - heads * HD))).reshape(rows, 3 * HW)


def shards(
    dp, tensor, inputs, cotangent, segments, live_blocks, ln1_gain, ln1_bias, qkv_weight, qkv_bias,
    out_weight, out_bias, ln2_gain, ln2_bias, fc1_weight, fc1_bias, fc2_weight, fc2_bias,
):
    live_blocks = live_blocks.T
    model = inputs.shape[-1]
    ff = fc1_weight.shape[2]
    heads = qkv_bias.shape[1]
    col = columns(model, ff)
    wout = jnp.pad(out_weight[0].T, ((0, 0), (0, HW - heads * HD)))
    w = jnp.concatenate([by_part(qkv_weight[0]), fc1_weight[0], fc2_weight[0].T, wout], axis=1)
    small = jnp.stack([ln1_gain[0], ln1_bias[0], out_bias[0], ln2_gain[0], ln2_bias[0], fc2_bias[0]])

    def lanes(a):
        return jnp.pad(a.astype(F32), ((0, 0), (0, 128 - a.shape[1])))

    sv = jnp.concatenate([lanes(small), lanes(qkv_bias[0]), lanes(fc1_bias[0])], axis=0)
    sv = jnp.pad(sv, ((0, -sv.shape[0] % 8), (0, 0)))
    fr = np.float32(10000.0) ** (-(np.arange(ROT // 2, dtype=np.float32) * np.float32(2.0 / ROT)))
    fr = jnp.asarray(np.broadcast_to(fr[:, None], (ROT // 2, 128)).astype(np.float32))
    cfg = {
        "col": col, "ff": ff, "heads": heads, "dp": dp, "tensor": tensor, "own": small.shape[1],
        "qw": qkv_bias.shape[2], "fw": fc1_bias.shape[2],
        "groups": [(0, col["fc1"]), (col["fc1"], col["fc2"]), (col["fc2"], col["end"])],
    }

    xf, n1a, n2a, ga, gpa, tab, w0, qa, ka, va, cf, vecs, sr, kc = layer_in(
        cfg, inputs, cotangent, segments, live_blocks, w, sv, fr
    )
    oa, lsea, hf, n1b, n2b, gb, gpb, w1, qb, kb, vb = layer_mid(cfg, qa, ka, va, sr, kc, ga, xf, w, w0, vecs, tab)
    ob, lseb = attn_fwd(heads, segments, live_blocks, qb, kb, vb, sr, kc)
    y, dob, e2b, grb, vdb = layer_turn(cfg, ob, gb, hf, cf, w1, vecs, n2b, gpb)
    dmb = attn_bwd(heads, segments, live_blocks, qb, kb, vb, ob, dob, lseb, sr, kc, tab)
    dhf, e2a, doa, vfb, vda, out1, outq, gra = layer_back(
        cfg, dmb, e2b, cf, hf, n1b, w1, w0, vecs, xf, ga, gpa, n2a, oa, grb
    )
    last_part = finish(
        cfg,
        *layer_last(
            cfg, qa, ka, va, oa, doa, lsea, sr, kc, tab, e2a, dhf, xf, n1a, w0, vecs, vfb, vdb, vda, gra, out1, outq, hf, y
        ),
    )
    so, ig, bg1, bb1, gqkv, bqkv, gout, bdy, bdy2, bg2, bb2, gfc1, bfc1, gfc2 = last_part
    bqkv, bfc1, gfc2 = bqkv.transpose(1, 0, 2), bfc1.transpose(1, 0, 2), gfc2.T[None]
    return (so, ig, bg1, bb1, gqkv, bqkv, gout, bdy, bg2, bb2, gfc1, bfc1, gfc2, bdy2)


def solution(mesh):
    both = ("dp", "tensor")
    in_specs = (
        P(None, "dp", "tensor", None),
        P(None, "dp", "tensor", None),
        P(None, "dp", None),
        P(None, "dp"),
        P("section", both),
        P("section", both),
        P("section", "dp", "tensor"),
        P("section", "tensor", "dp"),
        P("section", "tensor", "dp"),
        P("section", both),
        P("section", both),
        P("section", both),
        P("section", "dp", "tensor"),
        P("section", "tensor", "dp"),
        P("section", "tensor", "dp"),
        P("section", both),
    )
    out_specs = (
        P("section", None, "dp", "tensor", None),
        P("section", None, "dp", "tensor", None),
        P("section", both),
        P("section", both),
        P("section", "dp", "tensor"),
        P("section", "tensor", "dp"),
        P("section", "tensor", "dp"),
        P("section", both),
        P("section", both),
        P("section", both),
        P("section", "dp", "tensor"),
        P("section", "tensor", "dp"),
        P("section", "tensor", "dp"),
        P("section", both),
    )
    body = functools.partial(shards, mesh.shape["dp"], mesh.shape["tensor"])
    return jax.shard_map(body, mesh=mesh, in_specs=in_specs, out_specs=out_specs, check_vma=False)
```

```python
import functools

import jax
import jax.numpy as jnp
import numpy as np
from jax import lax
from jax.experimental import pallas as pl
from jax.experimental.pallas import tpu as pltpu
from jax.sharding import PartitionSpec as P

F32 = jnp.float32
BF = jnp.bfloat16
MESH = pl.DeviceIdType.MESH
HD = 64
ROT = 16
LIVE = 128
DOCS = 4
DOC_MAX = 1024
QB = 256
HW = 256
SUB = 256
EPS = 1e-05
NEG = -1e30
VMEM = pl.BlockSpec(memory_space=pltpu.VMEM)
ANY = pl.BlockSpec(memory_space=pltpu.HBM)
SMEM = pl.BlockSpec(memory_space=pltpu.SMEM)
DMA = pltpu.SemaphoreType.DMA


def sds(shape, dtype):
    return jax.ShapeDtypeStruct(shape, dtype)


def dg(a, b, ca, cb):
    return lax.dot_general(a, b, (((ca,), (cb,)), ((), ())), preferred_element_type=F32)


def dot(a, b):
    return jnp.dot(a, b, preferred_element_type=F32)


def ds(start, size):
    return pl.ds(pl.multiple_of(start, size), size)


def norm_stats(x):
    mu = jnp.mean(x, axis=-1, keepdims=True)
    xc = x - mu
    var = jnp.mean(xc * xc, axis=-1, keepdims=True)
    return xc, lax.rsqrt(var + EPS)


def head_lanes(width, heads):
    lane = lax.broadcasted_iota(jnp.int32, (1, width), 1)
    return [(lane >= h * HD) & (lane < (h + 1) * HD) for h in range(heads)]


def allow_mask(kc, sq, diag):
    m = kc == sq
    if diag:
        r = lax.broadcasted_iota(jnp.int32, (QB, QB), 0)
        c = lax.broadcasted_iota(jnp.int32, (QB, QB), 1)
        m = (m & (r <= c)) | (r == c)
    return m


def block_bounds(seg, live, i, n):
    s = lax.axis_index("tensor") // 2
    doc = seg[s, 0, i * QB]

    def body(j, count):
        return count + jnp.where((j < i) & (seg[s, 0, (j + 1) * QB - 1] == doc), 1, 0)

    hi = jnp.minimum(i, (live[0, s] * LIVE + QB - 1) // QB)
    return jnp.minimum(i - lax.fori_loop(0, n, body, 0), hi), hi


def turn_blocks(src, dst):
    def turn(i, _):
        dst[:, ds(i * QB, QB)] = src[ds(i * QB, QB), :].T
        return 0

    lax.fori_loop(0, src.shape[0] // QB, turn, 0)


def attn_fwd_block(i, lo, hi, heads, q_ref, k_ref, vt, sr_ref, kc_ref, s_scr, o_ref, lse_ref):
    width = q_ref.shape[1]
    qi = ds(i * QB, QB)
    q = q_ref[qi, :]
    qm = [jnp.where(m, q, jnp.zeros_like(q)) for m in head_lanes(width, heads)]
    sq = sr_ref[0:1, qi]

    def scores(j, slot, ms, diag):
        kj = ds(j * QB, QB)
        k = k_ref[kj, :]
        mask = allow_mask(kc_ref[kj, 0:1], sq, diag)
        out = []
        for h in range(heads):
            s = jnp.where(mask, dg(k, qm[h], 1, 1), NEG)
            s_scr[h, ds(slot * QB, QB), :] = s
            out.append(jnp.maximum(ms[h], jnp.max(s, axis=0, keepdims=True)))
        return tuple(out)

    ms = tuple(jnp.full((1, QB), NEG, F32) for _ in range(heads))
    ms = scores(i, 0, ms, True)
    ms = lax.fori_loop(lo, hi, lambda j, ms: scores(j, j - lo + 1, ms, False), ms)

    def weigh(j, slot, st):
        kj = ds(j * QB, QB)
        out = []
        for h in range(heads):
            total, acc = st[h]
            p = jnp.exp(s_scr[h, ds(slot * QB, QB), :] - ms[h])
            total = total + jnp.sum(p, axis=0, keepdims=True)
            acc = acc + dot(vt[h * HD : (h + 1) * HD, kj], p.astype(BF))
            out.append((total, acc))
        return tuple(out)

    st = tuple((jnp.zeros((1, QB), F32), jnp.zeros((HD, QB), F32)) for _ in range(heads))
    st = weigh(i, 0, st)
    st = lax.fori_loop(lo, hi, lambda j, st: weigh(j, j - lo + 1, st), st)
    ot = [st[h][1] * (1.0 / st[h][0]) for h in range(heads)]
    ot = jnp.concatenate(ot + [jnp.zeros((width - heads * HD, QB), F32)], axis=0)
    o_ref[qi, :] = ot.T.astype(BF)
    lse = [ms[h] + jnp.log(st[h][0]) for h in range(heads)]
    lse_ref[:, qi] = jnp.concatenate(lse + [jnp.zeros((8 - heads, QB), F32)], axis=0)


def attn_fwd_kernel(heads, seg, live, q_in, k_in, v_in, sr_ref, kc_ref, o_out, lse_ref, q, k, v, o, vt, s_scr, lsem, osem):
    n = q.shape[0] // QB
    loads = load([(v_in, v), (q_in, q), (k_in, k)], lsem)
    loads[0].wait()
    turn_blocks(v, vt)
    loads[1].wait()
    loads[2].wait()

    def out(i):
        rows = ds(i * QB, QB)
        return pltpu.make_async_copy(o.at[rows], o_out.at[rows], osem.at[i])

    def qloop(i, _):
        lo, hi = block_bounds(seg, live, i, n)
        attn_fwd_block(i, lo, hi, heads, q, k, vt, sr_ref, kc_ref, s_scr, o, lse_ref)
        out(i).start()
        return 0

    lax.fori_loop(0, n, qloop, 0)

    def drain(i, _):
        out(i).wait()
        return 0

    lax.fori_loop(0, n, drain, 0)


def attn_fwd(heads, seg, live, q, k, v, sr, kc):
    rows, width = q.shape
    buf = pltpu.VMEM((rows, width), BF)
    return pl.pallas_call(
        functools.partial(attn_fwd_kernel, heads),
        out_shape=(sds((rows, width), BF), sds((8, rows), F32)),
        in_specs=[SMEM, SMEM, ANY, ANY, ANY, VMEM, VMEM],
        out_specs=(ANY, VMEM),
        scratch_shapes=[buf, buf, buf, buf, pltpu.VMEM((width, rows), BF), pltpu.VMEM((heads, rows + QB, QB), F32),
                        DMA((3,)), DMA((rows // QB,))],
        compiler_params=pltpu.CompilerParams(vmem_limit_bytes=67043328),
        cost_estimate=cost(12),
        name="attn_fwd",
    )(seg, live, q, k, v, sr, kc)


def turn_lanes(x, tab, sign):
    width = x.shape[1]
    c, sn = [jnp.concatenate([tab[:, a * 128 : (a + 1) * 128]] * (width // 128), axis=1) for a in range(2)]
    lane = lax.broadcasted_iota(jnp.int32, (1, width), 1) % HD
    moved = jnp.where(lane < ROT // 2, pltpu.roll(x, width - ROT // 2, 1), pltpu.roll(x, ROT // 2, 1)) * sn
    return x * c + moved if sign > 0 else x * c - moved


def attn_bwd_block(i, lo, hi, heads, q_ref, k_ref, v_ref, o_ref, do_ref, kt, lse_ref, sr_ref, kc_ref, tab, dk, dv, out):
    width = q_ref.shape[1]
    hm = head_lanes(width, heads)
    rowid = lax.broadcasted_iota(jnp.int32, (8, width), 0)
    lane = lax.broadcasted_iota(jnp.int32, (8, width), 1)
    sel = ((lane >= rowid * HD) & (lane < (rowid + 1) * HD)).astype(F32).astype(BF)
    qi = ds(i * QB, QB)
    q = q_ref[qi, :]
    do = do_ref[qi, :]
    z = jnp.zeros_like(q)
    qm = [jnp.where(hm[h], q, z) for h in range(heads)]
    dom = [jnp.where(hm[h], do, z) for h in range(heads)]
    qcat = jnp.concatenate(qm, axis=0)
    docat = jnp.concatenate(dom, axis=0)
    prod = do.astype(F32) * o_ref[qi, :].astype(F32)
    high = prod.astype(BF)
    low = (prod - high.astype(F32)).astype(BF)
    delta = dg(sel, high, 1, 1) + dg(sel, low, 1, 1)
    lse = lse_ref[:, qi]
    sq = sr_ref[0:1, qi]

    def step(j, dqs, diag):
        kj = ds(j * QB, QB)
        k = k_ref[kj, :]
        v = v_ref[kj, :]
        mask = allow_mask(kc_ref[kj, 0:1], sq, diag)
        ps, dss, res = [], [], []
        for h in range(heads):
            s = dg(k, qm[h], 1, 1)
            dp = dg(v, dom[h], 1, 1)
            p = jnp.exp(jnp.where(mask, s - lse[h : h + 1, :], NEG))
            score_grad = (p * (dp - delta[h : h + 1, :])).astype(BF)
            ps.append(p.astype(BF))
            dss.append(score_grad)
            res.append(dqs[h] + dot(kt[h * HD : (h + 1) * HD, kj], score_grad))
        dv[kj, :] += dot(jnp.concatenate(ps, axis=1), docat)
        dk[kj, :] += dot(jnp.concatenate(dss, axis=1), qcat)
        return tuple(res)

    dqs = tuple(jnp.zeros((HD, QB), F32) for _ in range(heads))
    dqs = step(i, dqs, True)
    dqs = lax.fori_loop(lo, hi, lambda j, d: step(j, d, False), dqs)
    dq = jnp.concatenate(list(dqs) + [jnp.zeros((width - heads * HD, QB), F32)], axis=0).T * 0.125
    out[qi, 0:width] = turn_lanes(dq, tab[qi, :], -1).astype(BF)


def attn_bwd_kernel(
    heads, seg, live, q_in, k_in, v_in, o_in, do_in, lse_ref, sr_ref, kc_ref, tab_in, out_ref,
    q, k, v, o, do, tab, out, kt, dk, dv, lsem, osem,
):
    rows, width = q.shape
    n = rows // QB
    loads = load([(k_in, k), (q_in, q), (v_in, v), (do_in, do), (o_in, o), (tab_in, tab)], lsem)
    dk[...] = jnp.zeros_like(dk)
    dv[...] = jnp.zeros_like(dv)
    loads[0].wait()
    turn_blocks(k, kt)
    for c in loads[1:]:
        c.wait()

    def qloop(i, _):
        lo, hi = block_bounds(seg, live, i, n)
        attn_bwd_block(i, lo, hi, heads, q, k, v, o, do, kt, lse_ref, sr_ref, kc_ref, tab, dk, dv, out)
        return 0

    lax.fori_loop(0, n, qloop, 0)

    def leave(i):
        rr = ds(i * QB, QB)
        return pltpu.make_async_copy(out.at[rr], out_ref.at[rr], osem.at[i])

    def finish(i, _):
        ii = ds(i * QB, QB)
        out[ii, width : 2 * width] = turn_lanes(dk[ii, :], tab[ii, :], -1).astype(BF)
        out[ii, 2 * width : 3 * width] = dv[ii, :].astype(BF)
        leave(i).start()
        return 0

    lax.fori_loop(0, n, finish, 0)

    def drain(i, _):
        leave(i).wait()
        return 0

    lax.fori_loop(0, n, drain, 0)


def attn_bwd(heads, seg, live, q, k, v, o, do, lse, sr, kc, tab):
    rows, width = q.shape
    buf = pltpu.VMEM((rows, width), BF)
    return pl.pallas_call(
        functools.partial(attn_bwd_kernel, heads),
        out_shape=sds((rows, 3 * width), BF),
        in_specs=[SMEM, SMEM] + [ANY] * 5 + [VMEM] * 3 + [ANY],
        out_specs=ANY,
        scratch_shapes=[buf, buf, buf, buf, buf, pltpu.VMEM(tab.shape, F32), pltpu.VMEM((rows, 3 * width), BF),
                        pltpu.VMEM((width, rows), BF), pltpu.VMEM((rows, width), F32), pltpu.VMEM((rows, width), F32),
                        DMA((6,)), DMA((rows // QB,))],
        compiler_params=pltpu.CompilerParams(vmem_limit_bytes=67043328),
        cost_estimate=cost(26),
        name="attn_bwd",
    )(seg, live, q, k, v, o, do, lse, sr, kc, tab)


class Mesh:
    def __init__(self, dp, tensor):
        self.dp, self.tensor = dp, tensor
        self.s, self.z, self.t = lax.axis_index("section"), lax.axis_index("dp"), lax.axis_index("tensor")
        self.x, self.y = self.t % 2, self.t // 2
        self.px, self.py = 2 * self.y + (1 - self.x), 2 * (1 - self.y) + self.x
        self.mate = {"section": 1 - self.s}
        self.beside = {"tensor": self.px}
        self.beside_mate = {"tensor": self.px, "section": 1 - self.s}
        self.across = {"tensor": self.py}
        self.across_mate = {"tensor": self.py, "section": 1 - self.s}
        self.ring = [{"dp": (self.z + d) % dp} for d in range(1, dp)]
        self.group = [{"tensor": (self.t + d) % tensor} for d in range(1, tensor)]
        self.quarter = 2 * self.s + self.x

    def across_core(self, core):
        return {"tensor": self.py, "section": core}


def greet(peers):
    bar = pltpu.get_barrier_semaphore()
    for peer in peers:
        pl.semaphore_signal(bar, inc=1, device_id=peer, device_id_type=MESH)
    pl.semaphore_wait(bar, len(peers))


def push(src, dst, ssem, rsem, peer):
    return pltpu.make_async_remote_copy(
        src_ref=src, dst_ref=dst, send_sem=ssem, recv_sem=rsem, device_id=peer, device_id_type=MESH
    )


def pick(i, values):
    out = values[-1]
    for n in range(len(values) - 2, -1, -1):
        out = jnp.where(i == n, values[n], out)
    return out


class Tokens:
    def __init__(self, me, seq):
        self.me, self.half = me, seq // 8

    def start_of(self, a, b, h):
        return (4 * a + 2 * b + h) * self.half

    def rows(self, a, b, h):
        return ds(self.start_of(a, b, h), self.half)

    def own(self, a):
        return self.start_of(a, self.me.x, self.me.s)


class Gather(Tokens):
    def __init__(self, me, full, ssem, rsem, first=0):
        super().__init__(me, full.shape[0])
        self.full, self.ssem, self.rsem, self.first = full, ssem, rsem, first

    def side(self, n):
        return self.first if n == 0 else 1 - self.first

    def plan(self, i):
        me, a = self.me, self.side(i % 2)
        ref = self.full.at[self.rows(a, (1 - me.x) if i >= 4 else me.x, me.s)]
        return push(ref, ref, self.ssem.at[i], self.rsem.at[i], me.beside if i in (2, 3) else me.mate)

    def start(self, n):
        self.plan(n).start()
        self.plan(2 + n).start()

    def order(self, i):
        me = self.me
        a = pick(i, [self.side(n) for n in (0, 1, 0, 1, 0, 0, 1, 1)])
        b = jnp.where(i < 4, me.x, 1 - me.x)
        h = pick(i, [me.s, me.s, 1 - me.s, 1 - me.s, me.s, 1 - me.s, me.s, 1 - me.s])
        return self.start_of(a, b, h)

    def step(self, i):
        if i in (2, 3):
            self.plan(i - 2).wait_recv()
        if i in (4, 6):
            n = i // 2 - 2
            self.plan(2 + n).wait_recv()
            self.plan(4 + n).start()
        if i in (5, 7):
            self.plan(4 + i // 2 - 2).wait_recv()

    def arrive(self, i):
        for n in range(2, 8):

            @pl.when(i == n)
            def _(n=n):
                self.step(n)

    def finish(self):
        for i in range(6):
            self.plan(i).wait_send()

    def run(self, work):
        def body(i, _):
            self.arrive(i)
            work(self.order(i), i)
            return 0

        lax.fori_loop(0, 8, body, 0)
        self.finish()


class Scatter(Tokens):
    def __init__(self, me, part, mr, xr, ssem, rsem, first=0):
        super().__init__(me, part.shape[0])
        self.part, self.mr, self.xr, self.ssem, self.rsem, self.first = part, mr, xr, ssem, rsem, first

    def side(self, n):
        return self.first if n == 0 else 1 - self.first

    def plan(self, i):
        me = self.me
        if i < 4:
            b = (1 - me.x) if i < 2 else me.x
            src, dst, peer = self.rows(self.side(i % 2), b, 1 - me.s), self.mr.at[i], me.mate
        else:
            src, dst, peer = self.rows(self.side(i - 4), 1 - me.x, me.s), self.xr.at[i - 4], me.beside
        return push(self.part.at[src], dst, self.ssem.at[i], self.rsem.at[i], peer)

    def run(self, work, early=None):
        me = self.me

        def body(i, _):
            k = i // 2
            b = jnp.where(k < 2, 1 - me.x, me.x)
            h = jnp.where(i % 2 == 0, 1 - me.s, me.s)
            work(self.start_of(jnp.where(k % 2 == 0, self.side(0), self.side(1)), b, h), i)
            for n in range(4):

                @pl.when(i == 2 * n)
                def _(n=n):
                    self.plan(n).start()

            for n in range(2):

                @pl.when(i == 2 * n + 1)
                def _(n=n):
                    self.plan(n).wait_recv()
                    base = self.start_of(self.side(n), 1 - me.x, me.s)

                    def add(j, _):
                        rr = ds(base + j * SUB, SUB)
                        got = self.mr[n, ds(j * SUB, SUB), :].astype(F32)
                        self.part[rr, :] = (self.part[rr, :].astype(F32) + got).astype(BF)
                        return 0

                    lax.fori_loop(0, self.half // SUB, add, 0)
                    self.plan(4 + n).start()

            return 0

        lax.fori_loop(0, 8, body, 0)
        if early is not None:
            early()

    def arrive(self, n):
        self.plan(2 + n).wait_recv()
        self.plan(4 + n).wait_recv()

    def total(self, n, i):
        rr = ds(self.own(self.side(n)) + i * SUB, SUB)
        sub = ds(i * SUB, SUB)
        return self.part[rr, :].astype(F32) + self.mr[2 + n, sub, :].astype(F32) + self.xr[n, sub, :].astype(F32)

    def finish(self):
        for i in range(6):
            self.plan(i).wait_send()


def scatter_scratch(rows, width):
    half = rows // 8
    return [
        pltpu.VMEM((rows, width), BF),
        pltpu.VMEM((4, half, width), BF),
        pltpu.VMEM((2, half, width), BF),
        DMA((6,)),
        DMA((6,)),
    ]


class WeightGather:
    def __init__(self, me, layer, shard, full, gat, groups, sems):
        self.me, self.layer, self.shard, self.full, self.gat, self.groups = me, layer, shard, full, gat, groups
        self.own, self.wss, self.wrs, self.fss, self.frs, self.yss, self.yrs = sems
        self.rows = shard.shape[0]
        self.collects = me.s == layer
        self.keeps = me.y == layer

    def block(self, ref, zz, g):
        a, b = self.groups[g]
        return ref.at[ds(zz * self.rows, self.rows), a:b]

    def mine(self, g):
        a, b = self.groups[g]
        return self.shard.at[:, a:b]

    def local(self, g):
        return pltpu.make_async_copy(self.mine(g), self.block(self.full, self.me.z, g), self.own.at[g])

    def out(self, g, d, ref):
        dst = self.block(ref, self.me.z, g)
        return push(self.mine(g), dst, self.wss.at[g, d], self.wrs.at[g, d], self.me.ring[d])

    def hand(self, g, d, ref, across):
        zz = (self.me.z + self.me.dp - d) % self.me.dp
        src = self.mine(g) if d == 0 else self.block(ref, zz, g)
        ss, rs = (self.yss, self.yrs) if across else (self.fss, self.frs)
        peer = self.me.across_core(self.me.y) if across else self.me.mate
        return push(src, self.block(self.full, zz, g), ss.at[g, d], rs.at[g, d], peer)

    def both(self, do):
        @pl.when(self.collects & self.keeps)
        def _():
            do(self.full, True)

        @pl.when(self.collects & jnp.logical_not(self.keeps))
        def _():
            do(self.gat, False)

    def send_ring(self):
        def do(ref, keeps):
            for g in range(len(self.groups)):
                for d in range(self.me.dp - 1):
                    self.out(g, d, ref).start()

        self.both(do)

    def send_own(self, g):
        def do(ref, keeps):
            self.hand(g, 0, ref, True).start()
            if keeps:
                self.local(g).start()
            else:
                self.hand(g, 0, ref, False).start()

        self.both(do)

    def forward(self, g, blocks=None):
        def do(ref, keeps):
            for d in range(self.me.dp - 1) if blocks is None else blocks:
                self.out(g, d, ref).wait_recv()
                self.hand(g, d + 1, ref, True).start()
                if not keeps:
                    self.hand(g, d + 1, ref, False).start()

        self.both(do)

    def ready(self, g):
        me = self.me

        @pl.when(self.collects & self.keeps)
        def _():
            self.local(g).wait()

        @pl.when(me.s != me.y)
        def _():
            for d in range(me.dp):
                self.hand(g, d, self.full, True).wait_recv()

        @pl.when((me.s == me.y) & jnp.logical_not(self.collects))
        def _():
            for d in range(me.dp):
                self.hand(g, d, self.full, False).wait_recv()

    def finish(self):
        def do(ref, keeps):
            for g in range(len(self.groups)):
                for d in range(self.me.dp - 1):
                    self.out(g, d, ref).wait_send()
                for d in range(self.me.dp):
                    self.hand(g, d, ref, True).wait_send()
                    if not keeps:
                        self.hand(g, d, ref, False).wait_send()

        self.both(do)

    @staticmethod
    def scratch(dp, n):
        return [DMA((n,)), DMA((n, dp - 1)), DMA((n, dp - 1))] + [DMA((n, dp))] * 4


class GradReduce:
    def __init__(self, me, layer, src, mine, got, across, sb, rb, own, sems):
        self.me, self.layer, self.src, self.mine, self.got, self.across = me, layer, src, mine, got, across
        self.sb, self.rb, self.own = sb, rb, own
        self.hss, self.hrs, self.yss, self.yrs, self.pss, self.prs = sems
        self.rows = own.shape[0]
        self.some = 96 if self.rows % 96 == 0 else 48
        self.sums = me.s == layer
        self.holds = me.y == layer

    @staticmethod
    def scratch(dp):
        return [DMA((1,)), DMA((1,)), DMA((dp,)), DMA((dp,)), DMA((dp - 1,)), DMA((dp - 1,))]

    def hand(self):
        return push(self.src, self.got, self.hss.at[0], self.hrs.at[0], self.me.mate)

    def zz(self, d):
        return (self.me.z + d + 1) % self.me.dp

    def over(self, d):
        rr = ds(self.zz(d) * self.rows, self.rows)
        peer = self.me.across_core(self.layer)
        return push(self.src.at[rr], self.across.at[rr], self.yss.at[d], self.yrs.at[d], peer)

    def out(self, d):
        return push(self.sb.at[d], self.rb.at[d], self.pss.at[d], self.prs.at[d], self.me.ring[d])

    def send(self):
        me = self.me

        @pl.when(me.s != me.y)
        def _():
            for d in range(me.dp):
                self.over(d).start()

        @pl.when((me.s == me.y) & jnp.logical_not(self.sums))
        def _():
            self.hand().start()

    def step(self, d):
        me = self.me

        @pl.when(self.sums)
        def _():
            if d == 0:

                @pl.when(jnp.logical_not(self.holds))
                def _():
                    self.hand().wait_recv()

            self.over(d).wait_recv()
            last = d == me.dp - 1
            step = self.some

            def add(ref):
                def body(i, _):
                    rr = ds(self.zz(d) * self.rows + i * step, step)
                    value = ref[rr, :].astype(F32) + self.across[rr, :].astype(F32)
                    if last:
                        self.own[ds(i * step, step), :] = value
                    else:
                        self.sb[d, ds(i * step, step), :] = value.astype(BF)
                    return 0

                lax.fori_loop(0, self.rows // step, body, 0)

            if self.mine is self.got:
                add(self.mine)
            else:

                @pl.when(self.holds)
                def _():
                    add(self.mine)

                @pl.when(jnp.logical_not(self.holds))
                def _():
                    add(self.got)

            if not last:
                self.out(d).start()

    def collect(self):
        me = self.me

        @pl.when(self.sums)
        def _():
            for d in range(me.dp - 1):
                self.out(d).wait_recv()

                def add(i, _, d=d):
                    rr = ds(i * self.some, self.some)
                    self.own[rr, :] += self.rb[d, rr, :].astype(F32)
                    return 0

                lax.fori_loop(0, self.rows // self.some, add, 0)
            for d in range(me.dp - 1):
                self.out(d).wait_send()

    def finish(self):
        me = self.me

        @pl.when(me.s != me.y)
        def _():
            for d in range(me.dp):
                self.over(d).wait_send()

        @pl.when((me.s == me.y) & jnp.logical_not(self.sums))
        def _():
            self.hand().wait_send()


class VectorGather:
    def __init__(self, me, sv, buf, ss, rs, own):
        self.me, self.sv, self.buf, self.ss, self.rs, self.own = me, sv, buf, ss, rs, own

    def local(self):
        me = self.me
        return pltpu.make_async_copy(self.sv, self.buf.at[me.s, me.t, me.z], self.own)

    def stage(self, n):
        me = self.me
        if n == 0:
            dst = self.buf.at[me.s, me.t, me.z]
            return [push(self.sv, dst, self.ss.at[d], self.rs.at[d], peer) for d, peer in enumerate(me.ring)]
        base = me.dp - 1
        if n == 1:
            ref = self.buf.at[me.s, me.t]
            return [
                push(ref, ref, self.ss.at[base + d], self.rs.at[base + d], peer) for d, peer in enumerate(me.group)
            ]
        i = base + me.tensor - 1
        ref = self.buf.at[me.s]
        return [push(ref, ref, self.ss.at[i], self.rs.at[i], me.mate)]

    def send(self, n):
        if n == 0:
            self.local().start()
        for c in self.stage(n):
            c.start()

    def wait(self, n):
        if n == 0:
            self.local().wait()
        for c in self.stage(n):
            c.wait_recv()

    def finish(self):
        for n in range(3):
            for c in self.stage(n):
                c.wait_send()

    def build(self, vecs, heads, own, qw, fw):
        me, buf = self.me, self.buf
        for layer in range(2):
            wide = [buf[layer, tt, zz, 0:8, :][:, 0:own] for zz in range(me.dp) for tt in range(me.tensor)]
            vecs[layer, 0:8, :] = jnp.concatenate(wide, axis=1)
            here = [buf[layer, me.quarter, zz] for zz in range(me.dp)]
            by = [jnp.concatenate([p[6 + h : 7 + h, 0:qw] for p in here], axis=1) for h in range(heads)]
            qb = []
            for part in range(3):
                qb += [b[:, part * HD : (part + 1) * HD] for b in by] + [jnp.zeros((1, HW - heads * HD), F32)]
            vecs[layer, 6:7, :] = jnp.concatenate(qb, axis=1)
            fb = [p[6 + heads + h : 7 + heads + h, 0:fw] for h in range(heads) for p in here]
            vecs[layer, 7:8, :] = jnp.concatenate(fb, axis=1)


class VectorReduce:
    def __init__(self, me, va, vr, ss, rs):
        self.me, self.va, self.vr, self.ss, self.rs = me, va, vr, ss, rs

    def stage(self, n):
        me, va, vr, ss, rs = self.me, self.va, self.vr, self.ss, self.rs
        peers, base = [([me.across], 0), (me.ring, 1), ([me.mate, me.beside, me.beside_mate], me.dp)][n]
        return [push(va.at[n], vr.at[base + d], ss.at[base + d], rs.at[base + d], p) for d, p in enumerate(peers)]

    def send(self, n):
        for c in self.stage(n):
            c.start()

    def add(self, n, out):
        base = [0, 1, self.me.dp][n]
        for c in self.stage(n):
            c.wait_recv()
        if n < 2:
            total = self.va[n]
            for d in range(len(self.stage(n))):
                total = total + self.vr[base + d]
            out[...] = total
            return
        mine, mate = self.va[2], self.vr[base]
        row = lax.broadcasted_iota(jnp.int32, mine.shape, 0)
        quarter = jnp.where(self.me.s == self.me.y, mine, mate)
        out[...] = jnp.where(row % 8 < 6, mine + mate + self.vr[base + 1] + self.vr[base + 2], quarter)

    def finish(self):
        for n in range(3):
            for c in self.stage(n):
                c.wait_send()


def document_tables(seg, live, fr_ref, tab, srow, kcol):
    seq = seg.shape[1]
    count = lax.broadcasted_iota(jnp.int32, seg.shape, 1)
    start = jnp.zeros_like(seg)
    for doc in range(DOCS - 1):
        before = jnp.sum(jnp.where(seg == doc, 1.0, 0.0), axis=1, keepdims=True).astype(jnp.int32)
        start = start + jnp.where(seg > doc, before, 0)
    ang = fr_ref[:, 0:1] * (count - start).astype(F32)
    cs, sn = jnp.cos(ang), jnp.sin(ang)
    one = jnp.ones((HD - ROT, seq), F32)
    tab[:, 0:128] = jnp.concatenate([cs, cs, one] * 2, axis=0).T
    tab[:, 128:256] = jnp.concatenate([-sn, sn, jnp.zeros_like(one)] * 2, axis=0).T
    srow[...] = jnp.broadcast_to(seg, srow.shape)
    keys = jnp.where(count < live * LIVE, seg, -1).astype(F32)
    for b in range(seq // QB):
        part = jnp.broadcast_to(keys[:, b * QB : (b + 1) * QB], (128, QB))
        kcol[b * QB : (b + 1) * QB, :] = part.T.astype(jnp.int32)


QKV, FC1, FC2, OUT = 0, 1, 2, 3


def columns(model, ff):
    return {"qkv": 0, "fc1": 3 * HW, "fc2": 3 * HW + ff, "out": 3 * HW + 2 * ff, "end": 3 * HW + 2 * ff + HW}


def project_norm(r0, half, hf, vec, n1, n2):
    rows = ds(r0, half)
    xc, r = norm_stats(hf[rows, :].astype(F32))
    xh = xc * r
    n1[rows, :] = (xh * vec[0:1, :] + vec[1:2, :]).astype(BF)
    n2[rows, :] = (xh * vec[3:4, :] + vec[4:5, :]).astype(BF)


def project_qkv(r0, half, wqkv, vec, tab, n1, q, k, v):
    rows = ds(r0, half)
    a = n1[rows, :]
    for part, dst in enumerate((q, k, v)):
        cols = slice(part * HW, (part + 1) * HW)
        y = dot(a, wqkv[:, cols]) + vec[6:7, cols]
        if part < 2:
            y = turn_lanes(y, tab[rows, :], 1)
        if part == 0:
            y = y * 0.125
        dst[rows, :] = y.astype(BF)


def project_fc1(r0, half, wfc1, vec, n2, g, gp):
    rows = ds(r0, half)
    a = n2[rows, :]
    for b in range(wfc1.shape[1] // 256):
        cols = slice(b * 256, (b + 1) * 256)
        y = dot(a, wfc1[:, cols]) + vec[7:8, cols]
        cdf = 0.5 + 0.5 * lax.erf(y * 0.7071067811865476)
        g[rows, cols] = (y * cdf).astype(BF)
        gp[rows, cols] = (cdf + y * jnp.exp(-0.5 * y * y) * 0.3989422804014327).astype(BF)


def branch_out(r0, half, o, g, wout, wfc2, part):
    rows = ds(r0, half)
    for b in range(part.shape[1] // 256):
        cols = slice(b * 256, (b + 1) * 256)
        y = dg(o[rows, :], wout[cols, :], 1, 1) + dg(g[rows, :], wfc2[cols, :], 1, 1)
        part[rows, cols] = y.astype(BF)


def back_head(r0, half, dyf, hf, g, gp, n2, o, wfc1, wfc2, wout, vec, do, e2, da, acc, vg):
    rows = ds(r0, half)
    model, ff = wfc1.shape
    dy = dyf[rows, :]
    for b in range(ff // 256):
        cols = slice(b * 256, (b + 1) * 256)
        y = dot(dy, wfc2[:, cols]) * gp[rows, cols].astype(F32)
        low = y.astype(BF)
        da[:, cols] = low
        vg[7:8, cols] += jnp.sum(low.astype(F32), axis=0, keepdims=True)
    do[rows, :] = dot(dy, wout[...]).astype(BF)
    xc, r = norm_stats(hf[rows, :].astype(F32))
    xh = xc * r
    for b in range(model // 256):
        cols = slice(b * 256, (b + 1) * 256)
        dn = dg(da[...], wfc1[cols, :], 1, 1)
        vg[3:4, cols] += jnp.sum(dn * xh[:, cols], axis=0, keepdims=True)
        vg[4:5, cols] += jnp.sum(dn, axis=0, keepdims=True)
        e2[rows, cols] = (dn * vec[3:4, cols]).astype(BF)
    n2t = n2[rows, :].T
    dyt = dy.T
    for b in range(ff // 256):
        cols = slice(b * 256, (b + 1) * 256)
        acc[:, cols] += dot(n2t, da[:, cols])
        acc[:, ff + b * 256 : ff + (b + 1) * 256] += dot(dyt, g[rows, cols])
    acc[:, 2 * ff :] += dot(dyt, o[rows, :])


def back_tail(r0, half, dmix, hf, e2, wqkv, vec, part, vg):
    rows = ds(r0, half)
    dm = dmix[rows, :]
    vg[6:7, :] += jnp.sum(dm.astype(F32), axis=0, keepdims=True)
    xc, r = norm_stats(hf[rows, :].astype(F32))
    xh = xc * r
    for b in range(part.shape[1] // 256):
        cols = slice(b * 256, (b + 1) * 256)
        dn = dg(dm, wqkv[cols, :], 1, 1)
        vg[0:1, cols] += jnp.sum(dn * xh[:, cols], axis=0, keepdims=True)
        vg[1:2, cols] += jnp.sum(dn, axis=0, keepdims=True)
        part[rows, cols] = (dn * vec[0:1, cols] + e2[rows, cols].astype(F32)).astype(BF)


def qkv_grad(n1, dmix, acc, half):
    acc[...] = jnp.zeros_like(acc)

    def body(i, _):
        rows = ds(i * half, half)
        n1t = n1[rows, :].T
        for b in range(3):
            cols = slice(b * HW, (b + 1) * HW)
            acc[:, cols] += dot(n1t, dmix[rows, cols])
        return 0

    lax.fori_loop(0, n1.shape[0] // half, body, 0)


def store_low(acc, out):
    def body(i, _):
        rr = ds(i * SUB, SUB)
        out[rr, :] = acc[rr, :].astype(BF)
        return 0

    lax.fori_loop(0, acc.shape[0] // SUB, body, 0)


def residual_out(sc, own, vec, write, after=None):
    for a in range(2):
        sc.arrive(a)

        def body(i, _, a=a):
            base = own[ds(sc.own(sc.side(a)) + i * SUB, SUB), :].astype(F32)
            write(a, i, (base + sc.total(a, i) + vec[2:3, :] + vec[5:6, :]).astype(BF))
            return 0

        lax.fori_loop(0, sc.half // SUB, body, 0)
        if after is not None:
            after(a)


def grad_out(sc, dy, hf, vec, write, after=None):
    for a in range(2):
        sc.arrive(a)

        def body(i, _, a=a):
            rr = ds(sc.own(sc.side(a)) + i * SUB, SUB)
            xc, r = norm_stats(hf[rr, :].astype(F32))
            xh = xc * r
            e = sc.total(a, i)
            m1 = jnp.mean(e, axis=-1, keepdims=True)
            m2 = jnp.mean(e * xh, axis=-1, keepdims=True)
            write(a, i, (dy(a, i).astype(F32) + r * (e - m1 - xh * m2)).astype(BF))
            return 0

        lax.fori_loop(0, sc.half // SUB, body, 0)
        if after is not None:
            after(a)


def column_sum(tok, ref, vg, row):
    total = jnp.zeros((1, ref.shape[1]), F32)
    for a in range(2):

        def body(i, acc, a=a):
            return acc + jnp.sum(ref[ds(tok.own(a) + i * SUB, SUB), :].astype(F32), axis=0, keepdims=True)

        total = lax.fori_loop(0, tok.half // SUB, body, total)
    vg[row : row + 1, :] = total


def load(pairs, sem):
    copies = [pltpu.make_async_copy(a, b, sem.at[i]) for i, (a, b) in enumerate(pairs)]
    for c in copies:
        c.start()
    return copies


def params(cid):
    return pltpu.CompilerParams(collective_id=cid, has_side_effects=True, vmem_limit_bytes=67043328)


def cost(us):
    return pl.CostEstimate(flops=int(us * 8e8), bytes_accessed=0, transcendentals=0)


class OwnedOut:
    def __init__(self, me, src, dst, core, ss, rs, local):
        self.me, self.src, self.dst, self.core, self.ss, self.rs, self.local = me, src, dst, core, ss, rs, local

    def place(self):
        return self.dst.at[self.me.y, self.me.s]

    def far(self):
        me = self.me
        return push(self.src.at[1 - me.y], self.place(), self.ss.at[0], self.rs.at[me.s], me.across_core(self.core))

    def mate(self):
        return push(self.src.at[self.me.y], self.place(), self.ss.at[1], self.rs.at[2], self.me.mate)

    def here(self):
        return pltpu.make_async_copy(self.src.at[self.me.y], self.place(), self.local)

    def start_here(self):
        @pl.when(self.me.s == self.core)
        def _():
            self.here().start()

        @pl.when(self.me.s != self.core)
        def _():
            self.mate().start()

    def wait(self):
        me = self.me
        self.far().wait_send()

        @pl.when(me.s == self.core)
        def _():
            self.here().wait()
            self.mate().wait_recv()
            for n in range(2):
                place = self.dst.at[1 - me.y, n]
                push(self.src.at[0], place, self.ss.at[0], self.rs.at[n], me.across_core(self.core)).wait_recv()

        @pl.when(me.s != self.core)
        def _():
            self.mate().wait_send()


class Stores:
    def __init__(self, pairs, half, sem):
        self.pairs, self.half, self.sem = pairs, half, sem

    def copy(self, n, r0, i):
        src, dst = self.pairs[n]
        rows = ds(r0, self.half)
        return pltpu.make_async_copy(src.at[rows], dst.at[rows], self.sem.at[n, i])

    def start(self, which, r0, i):
        for n in which:
            self.copy(n, r0, i).start()

    def finish(self):
        def body(i, _):
            for n in range(len(self.pairs)):
                self.copy(n, i * self.half, i).wait()
            return 0

        lax.fori_loop(0, 8, body, 0)


def in_kernel(
    cfg, in_ref, cot_ref, seg_ref, live, w_ref, sv_ref, fr_ref,
    hf_o, n1_o, n2_o, g_o, gp_o, tab_o, w_o, q_o, k_o, v_o, cf_o, vecs, srow, kcol,
    hf, n1, n2, g, gp, tab, q, k, v, wfull, gat, vb, cot, gss, grs, css, crs, yss, yrs, lsem, ssem, vss, vrs, *wsems,
):
    col, dp, tensor = cfg["col"], cfg["dp"], cfg["tensor"]
    me = Mesh(dp, tensor)
    ga = Gather(me, hf, gss, grs, me.y)
    gc = Gather(me, cf_o, css, crs, me.y)
    half = ga.half
    part = ds(me.s * half, half)
    first = pltpu.make_async_copy(in_ref.at[me.y, 0, part], hf.at[ds(ga.own(me.y), half)], lsem.at[0])
    first.start()
    up = pltpu.make_async_copy(cot_ref.at[me.y, 0, part], cot, lsem.at[4])
    up.start()
    greet([me.mate, me.across_mate] + me.ring + me.group)
    over = push(in_ref.at[1 - me.y, 0, part], hf.at[ds(ga.own(me.y), half)], yss.at[0], yrs.at[0], me.across)
    wg = WeightGather(me, 0, w_ref, wfull, gat, cfg["groups"], wsems)
    vg = VectorGather(me, sv_ref, vb, vss, vrs, lsem.at[1])
    st = Stores([(hf, hf_o), (n1, n1_o), (n2, n2_o), (g, g_o), (gp, gp_o), (q, q_o), (k, k_o), (v, v_o)], half, ssem)
    vg.send(0)
    wg.send_ring()
    first.wait()
    document_tables(seg_ref[me.y], live[0, me.y], fr_ref, tab, srow, kcol)
    vg.wait(0)
    vg.send(1)
    ga.start(0)
    over.start()
    wg.send_own(0)
    tab_out = pltpu.make_async_copy(tab, tab_o, lsem.at[2])
    tab_out.start()
    vg.wait(1)
    vg.send(2)
    up.wait()
    cot_out = pltpu.make_async_copy(cot, cf_o.at[ds(gc.own(me.y), half)], lsem.at[5])
    cot_out.start()
    vg.wait(2)
    vg.build(vecs, cfg["heads"], cfg["own"], cfg["qw"], cfg["fw"])
    vec = vecs.at[0]

    def norm(r0, i):
        project_norm(r0, half, hf, vec, n1, n2)
        st.start((0, 1, 2), r0, i)

        @pl.when(i == 0)
        def _():
            over.wait_recv()
            ga.start(1)

        @pl.when(i == 1)
        def _():
            wg.forward(0)
            wg.send_own(1)

    ga.run(norm)
    cot_out.wait()
    gc.plan(0).start()
    gc.plan(2).start()
    wg.ready(0)

    def qkv(i, _):
        r0 = ga.order(i)
        project_qkv(r0, half, wfull.at[:, 0 : col["fc1"]], vec, tab, n1, q, k, v)
        st.start((5, 6, 7), r0, i)
        return 0

    lax.fori_loop(0, 8, qkv, 0)
    wg.forward(1)
    wg.send_own(2)
    wg.send_own(3)
    wg.ready(1)
    wg.forward(2)

    def fc1(i, _):
        r0 = ga.order(i)
        project_fc1(r0, half, wfull.at[:, col["fc1"] : col["fc2"]], vec, n2, g, gp)
        st.start((3, 4), r0, i)

        @pl.when(i == 5)
        def _():
            wg.forward(3)

        return 0

    lax.fori_loop(0, 8, fc1, 0)
    gc.step(2)
    gc.step(4)
    gc.step(5)
    st.finish()
    tab_out.wait()
    wg.ready(2)
    wg.ready(3)
    w_out = pltpu.make_async_copy(wfull, w_o, lsem.at[3])
    w_out.start()
    wg.finish()
    vg.finish()
    for n in (0, 2, 4):
        gc.plan(n).wait_send()
    over.wait_send()
    w_out.wait()


def layer_in(cfg, inputs, cotangent, segments, live, w, sv, fr):
    seq, model, ff = segments.shape[2], inputs.shape[3], cfg["ff"]
    dp, tensor = cfg["dp"], cfg["tensor"]
    rows, hidden = sds((seq, model), BF), sds((seq, ff), BF)
    heads = sds((seq, HW), BF)
    nv = dp - 1 + tensor
    wide, wide_h, wide_q = pltpu.VMEM((seq, model), BF), pltpu.VMEM((seq, ff), BF), pltpu.VMEM((seq, HW), BF)
    weights = pltpu.VMEM((model, w.shape[1]), BF)
    return pl.pallas_call(
        functools.partial(in_kernel, cfg),
        out_shape=(rows, rows, rows, hidden, hidden, sds((seq, 256), F32), sds((model, w.shape[1]), BF),
                   heads, heads, heads, rows,
                   sds((2, 8, model), F32), sds((8, seq), jnp.int32), sds((seq, 128), jnp.int32)),
        in_specs=[ANY, ANY, VMEM, SMEM, VMEM, VMEM, VMEM],
        out_specs=(ANY,) * 11 + (VMEM,) * 3,
        scratch_shapes=[
            wide, wide, wide, wide_h, wide_h, pltpu.VMEM((seq, 256), F32), wide_q, wide_q, wide_q,
            weights, weights, pltpu.VMEM((2, tensor, dp) + sv.shape, F32),
            pltpu.VMEM((seq // 8, model), BF),
            DMA((6,)), DMA((6,)), DMA((6,)), DMA((6,)), DMA((1,)), DMA((1,)), DMA((6,)), DMA((8, 8)),
            DMA((nv,)), DMA((nv,)),
        ]
        + WeightGather.scratch(dp, 4),
        compiler_params=params(2),
        cost_estimate=cost(45),
        name="layer_in",
    )(inputs, cotangent, segments, live, w, sv, fr)


def mid_kernel(
    cfg, q_in, k_in, v_in, srow, kcol, g_in, x_in, w_ref, w0, vecs, tab_in,
    o_o, lse, hf_o, n1_o, n2_o, g_o, gp_o, w_o, q_o, k_o, v_o,
    wout, wfc2, hf, n1, n2, g, gp, tab, wfull, gat, q, k, v, o, vt, s_scr,
    part, mr, xr, sss, srs, gss, grs, lsem, ssem, osem, *wsems,
):
    col, heads = cfg["col"], cfg["heads"]
    me = Mesh(cfg["dp"], cfg["tensor"])
    sc = Scatter(me, part, mr, xr, sss, srs)
    ga = Gather(me, hf, gss, grs)
    half = sc.half
    loads = load(
        [
            (v_in, v),
            (q_in, q),
            (k_in, k),
            (w0.at[:, col["out"] : col["end"]], wout),
            (w0.at[:, col["fc2"] : col["out"]], wfc2),
            (g_in, g),
            (tab_in, tab),
        ]
        + [(x_in.at[ds(sc.own(a), half)], hf.at[ds(sc.own(a), half)]) for a in range(2)],
        lsem,
    )
    greet([me.mate, me.beside, me.across, me.across_mate] + me.ring)
    wg = WeightGather(me, 1, w_ref, wfull, gat, cfg["groups"], wsems)
    wg.send_ring()
    for n in range(4):
        wg.send_own(n)
    loads[0].wait()
    turn_blocks(v, vt)
    for c in loads[1:]:
        c.wait()
    st = Stores([(hf, hf_o), (n1, n1_o), (n2, n2_o), (g, g_o), (gp, gp_o), (q, q_o), (k, k_o), (v, v_o)], half, ssem)
    st_o = Stores([(o, o_o)], half, osem)

    def out(r0, i):
        b = r0 // QB
        attn_fwd_block(b, jnp.maximum(b - DOC_MAX // QB, 0), b, heads, q, k, vt, srow, kcol, s_scr, o, lse)
        st_o.start((0,), r0, i)
        branch_out(r0, half, o, g, wout, wfc2, part)

        @pl.when(i == 6)
        def _():
            wg.forward(0)

    sc.run(out)

    def write(a, i, value):
        hf[ds(sc.own(a) + i * SUB, SUB), :] = value

    residual_out(sc, hf, vecs.at[0], write, ga.start)
    wg.forward(1)
    vec = vecs.at[1]

    def fc1(i):
        r0 = ga.order(i)
        project_fc1(r0, half, wfull.at[:, col["fc1"] : col["fc2"]], vec, n2, g, gp)
        st.start((3, 4), r0, i)

    def work(r0, i):
        project_norm(r0, half, hf, vec, n1, n2)

        @pl.when(i == 0)
        def _():
            wg.ready(0)

        project_qkv(r0, half, wfull.at[:, 0 : col["fc1"]], vec, tab, n1, q, k, v)
        st.start((0, 1, 2, 5, 6, 7), r0, i)

        @pl.when(i == 4)
        def _():
            wg.ready(1)

        @pl.when(i >= 4)
        def _():
            fc1(i - 4)

        @pl.when(i == 5)
        def _():
            wg.forward(2)

        @pl.when(i == 7)
        def _():
            wg.forward(3)

    ga.run(work)

    def late(i, _):
        fc1(i)
        return 0

    lax.fori_loop(4, 8, late, 0)
    st.finish()
    wg.ready(2)
    wg.ready(3)
    w_out = pltpu.make_async_copy(wfull, w_o, lsem.at[0])
    w_out.start()
    sc.finish()
    wg.finish()
    st_o.finish()
    w_out.wait()


def layer_mid(cfg, q, k, v, srow, kcol, g, xf, w, w0, vecs, tab):
    seq, model, ff = tab.shape[0], xf.shape[1], cfg["ff"]
    rows, hidden, heads = sds((seq, model), BF), sds((seq, ff), BF), sds((seq, HW), BF)
    wide, wide_h, wide_q = pltpu.VMEM((seq, model), BF), pltpu.VMEM((seq, ff), BF), pltpu.VMEM((seq, HW), BF)
    return pl.pallas_call(
        functools.partial(mid_kernel, cfg),
        out_shape=(heads, sds((8, seq), F32), rows, rows, rows, hidden, hidden, sds(w0.shape, BF), heads, heads, heads),
        in_specs=[ANY, ANY, ANY, VMEM, VMEM, ANY, ANY, VMEM, ANY, VMEM, ANY],
        out_specs=(ANY, VMEM) + (ANY,) * 9,
        scratch_shapes=[
            pltpu.VMEM((model, HW), BF), pltpu.VMEM((model, ff), BF),
            wide, wide, wide, wide_h, wide_h, pltpu.VMEM((seq, 256), F32),
            pltpu.VMEM(w0.shape, BF), pltpu.VMEM(w0.shape, BF),
            wide_q, wide_q, wide_q, wide_q, pltpu.VMEM((HW, seq), BF),
            pltpu.VMEM((cfg["heads"], DOC_MAX + QB, QB), F32),
        ]
        + scatter_scratch(seq, model)
        + [DMA((6,)), DMA((6,)), DMA((9,)), DMA((8, 8)), DMA((1, 8))]
        + WeightGather.scratch(cfg["dp"], 4),
        compiler_params=params(3),
        cost_estimate=cost(70),
        name="layer_mid",
    )(q, k, v, srow, kcol, g, xf, w, w0, vecs, tab)


def turn_kernel(
    cfg, o_in, g_in, hf_in, cf, cot_ref, w1, vecs, n2_in, gp_in, y_o, do_o, e2_o, gr_o, hx, cy, vg,
    o, g, hf, dyf, n2, gp, e2, do, y, gr, wout, wfc2, wfc1, da, acc,
    part, mr, xr, sss, srs, gss, grs, yss, yrs, lsem, ssem,
):
    col = cfg["col"]
    me = Mesh(cfg["dp"], cfg["tensor"])
    sc = Scatter(me, part, mr, xr, sss, srs)
    half = sc.half
    gt = Gather(me, dyf, gss, grs, me.y)
    near = ds(4 * me.y * half, 4 * half)
    loads = load(
        [
            (w1.at[:, col["out"] : col["end"]], wout),
            (w1.at[:, col["fc2"] : col["out"]], wfc2),
            (o_in, o),
            (g_in, g),
            (w1.at[:, col["fc1"] : col["fc2"]], wfc1),
            (cf.at[near], dyf.at[near]),
            (gp_in, gp),
            (hf_in, hf),
            (n2_in, n2),
        ],
        lsem,
    )
    greet([me.mate, me.beside, me.across])
    over = push(
        cot_ref.at[1 - me.y, 0, ds(me.s * half, half)], dyf.at[ds(gt.own(me.y), half)], yss.at[0], yrs.at[0], me.across
    )
    over.start()
    cy_out = pltpu.make_async_copy(dyf.at[ds(gt.own(1 - me.y), half)], cy, lsem.at[2])
    h_over = push(hf_in.at[ds(me.py * 2 * half, 2 * half)], hx, yss.at[1], yrs.at[1], me.across)

    @pl.when(me.s == 0)
    def _():
        h_over.start()

    for c in loads[:4]:
        c.wait()
    vec = vecs.at[1]
    st = Stores([(e2, e2_o), (do, do_o)], half, ssem)

    def early():
        vg[...] = jnp.zeros_like(vg)
        acc[...] = jnp.zeros_like(acc)
        for c in loads[4:]:
            c.wait()
        over.wait_recv()
        gt.start(1)
        cy_out.start()

        def head(i, _):
            for n, step in ((5, 3), (6, 6), (7, 7)):

                @pl.when(i == n)
                def _(step=step):
                    gt.step(step)

            far_b = jnp.where(i < 6, me.x, 1 - me.x)
            far_h = jnp.where(i % 2 == 0, me.s, 1 - me.s)
            r0 = jnp.where(i < 4, (4 * me.y + i) * half, gt.start_of(1 - me.y, far_b, far_h))
            back_head(r0, half, dyf, hf, g, gp, n2, o, wfc1, wfc2, wout, vec, do, e2, da, acc, vg)
            st.start((0, 1), r0, i)
            return 0

        lax.fori_loop(0, 8, head, 0)

    sc.run(lambda r0, i: branch_out(r0, half, o, g, wout, wfc2, part), early)
    column_sum(sc, dyf, vg, 2)
    store_low(acc, gr)
    gr_out = pltpu.make_async_copy(gr, gr_o, lsem.at[0])
    gr_out.start()

    def write(a, i, value):
        y[a, ds(i * SUB, SUB), :] = value

    residual_out(sc, hf, vec, write)
    y_out = pltpu.make_async_copy(y, y_o, lsem.at[1])
    y_out.start()
    sc.finish()
    st.finish()
    cy_out.wait()
    over.wait_send()
    for n in (1, 3, 5):
        gt.plan(n).wait_send()

    @pl.when(me.s == 0)
    def _():
        h_over.wait()

    gr_out.wait()
    y_out.wait()


def layer_turn(cfg, o, g, hf, cf, cotangent, w1, vecs, n2, gp):
    seq, model = hf.shape
    ff = cfg["ff"]
    wide, hidden, heads = pltpu.VMEM((seq, model), BF), pltpu.VMEM((seq, ff), BF), pltpu.VMEM((seq, HW), BF)
    owned = (2, seq // 8, model)
    return pl.pallas_call(
        functools.partial(turn_kernel, cfg),
        out_shape=(
            sds(owned, BF),
            sds((seq, HW), BF),
            sds((seq, model), BF),
            sds((model, 2 * ff + HW), BF),
            sds((seq // 4, model), BF),
            sds((seq // 8, model), BF),
            sds((8, model), F32),
        ),
        in_specs=[ANY] * 6 + [VMEM, ANY, ANY],
        out_specs=(ANY,) * 6 + (VMEM,),
        scratch_shapes=[
            heads, hidden, wide, wide, wide, hidden, wide, heads, pltpu.VMEM(owned, BF),
            pltpu.VMEM((model, 2 * ff + HW), BF),
            pltpu.VMEM((model, HW), BF), pltpu.VMEM((model, ff), BF), pltpu.VMEM((model, ff), BF),
            pltpu.VMEM((seq // 8, ff), BF), pltpu.VMEM((model, 2 * ff + HW), F32),
        ]
        + scatter_scratch(seq, model)
        + [DMA((6,)), DMA((6,)), DMA((2,)), DMA((2,)), DMA((9,)), DMA((2, 8))],
        compiler_params=params(4),
        cost_estimate=cost(40),
        name="layer_turn",
    )(o, g, hf, cf, cotangent, w1, vecs, n2, gp)


def back_kernel(
    cfg, dm_in, e2_in, cf, cy, hf_in, n1_in, w1, w0, vecs, xf_in, g_in, gp_in, n2_in, o_in, gr1, y_in,
    dh_o, e2_o, do_o, vgf, vgd, out1_o, outq_o, gr_o, yx,
    dmix, o, do, a, b, e2, g, gp, wqkv, wout, wfc2, wfc1, dhf, da, acc, gq, gr, got, gotq, acrq,
    sb, rb, sbq, rbq, out1, outq, part, mr, xr, sss, srs, gss, grs, lsem, ssem, oss, ors, osem, *rsems,
):
    col, dp = cfg["col"], cfg["dp"]
    me = Mesh(dp, cfg["tensor"])
    ga = Gather(me, dhf, gss, grs)
    sc = Scatter(me, part, mr, xr, sss, srs)
    half = sc.half
    loads = load(
        [
            (w1.at[:, col["qkv"] : col["fc1"]], wqkv),
            (dm_in, dmix),
            (hf_in, a),
            (e2_in, e2),
            (n1_in, b),
            (w0.at[:, col["out"] : col["end"]], wout),
            (w0.at[:, col["fc2"] : col["out"]], wfc2),
            (w0.at[:, col["fc1"] : col["fc2"]], wfc1),
            (g_in, g),
            (gp_in, gp),
            (o_in, o),
        ]
        + [(cf.at[ds(sc.own(me.y), half)], dhf.at[ds(sc.own(me.y), half)]), (cy, dhf.at[ds(sc.own(1 - me.y), half)])],
        lsem,
    )
    gr_load = pltpu.make_async_copy(gr1, gr, lsem.at[13])
    holds = (me.s == 1) & (me.y == 1)

    @pl.when(holds)
    def _():
        gr_load.start()

    greet([me.mate, me.beside, me.across, me.across_mate] + me.ring)
    red1 = GradReduce(me, 1, gr1, gr, gr, got, sb, rb, out1, rsems[:6])
    redq = GradReduce(me, 1, gq, gq, gotq, acrq, sbq, rbq, outq, rsems[6:])
    st = Stores([(e2, e2_o), (do, do_o), (dhf, dh_o)], half, ssem)
    ys = OwnedOut(me, y_in, yx, 1, oss, ors, osem.at[0])
    red1.send()
    vgf[...] = jnp.zeros_like(vgf)
    vgd[...] = jnp.zeros_like(vgd)
    for c in loads[:4]:
        c.wait()

    def early():
        loads[4].wait()
        small = acc.at[:, 0 : 3 * HW]
        qkv_grad(b, dmix, small, half)
        store_low(small, gq)
        redq.send()
        ys.far().start()
        ys.start_here()

        @pl.when(holds)
        def _():
            gr_load.wait()

        red1.step(0)

    sc.run(lambda r0, i: back_tail(r0, half, dmix, a, e2, wqkv, vecs.at[1], part, vgf), early)
    acc[...] = jnp.zeros_like(acc)
    again = pltpu.make_async_copy(n2_in, b, lsem.at[14])
    again.start()
    for c in loads[5:]:
        c.wait()
    for d in range(1, dp // 2):
        red1.step(d)

    def write(n, i, value):
        dhf[ds(sc.own(n) + i * SUB, SUB), :] = value

    grad_out(sc, lambda n, i: dhf[ds(sc.own(n) + i * SUB, SUB), :], a, vecs.at[1], write, ga.start)
    other = pltpu.make_async_copy(xf_in, a, lsem.at[15])
    other.start()
    again.wait()
    other.wait()

    def work(r0, i):
        back_head(r0, half, dhf, a, g, gp, b, o, wfc1, wfc2, wout, vecs.at[0], do, e2, da, acc, vgd)
        st.start((0, 1, 2), r0, i)

        @pl.when(i == 1)
        def _():
            for d in range(dp // 2, dp - 1):
                red1.step(d)

        @pl.when(i == 3)
        def _():
            red1.step(dp - 1)

        @pl.when(i == 5)
        def _():
            redq.step(0)

    ga.run(work)
    for d in range(1, dp):
        redq.step(d)
    store_low(acc, gr)
    gr_out = pltpu.make_async_copy(gr, gr_o, lsem.at[0])
    gr_out.start()
    column_sum(sc, dhf, vgd, 2)
    red1.collect()
    redq.collect()
    outs = [pltpu.make_async_copy(out1, out1_o, lsem.at[1]), pltpu.make_async_copy(outq, outq_o, lsem.at[2])]
    for c in outs:
        c.start()
    red1.finish()
    redq.finish()
    sc.finish()
    st.finish()
    gr_out.wait()
    ys.wait()
    for c in outs:
        c.wait()


def layer_back(cfg, dmix, e2, cf, cy, hf, n1, w1, w0, vecs, xf, g, gp, n2, o, gr1, y):
    seq, model = hf.shape
    ff, dp = cfg["ff"], cfg["dp"]
    rows, nr, nq = model // dp, 2 * ff + HW, 3 * HW
    wide, hidden, heads = pltpu.VMEM((seq, model), BF), pltpu.VMEM((seq, ff), BF), pltpu.VMEM((seq, HW), BF)
    return pl.pallas_call(
        functools.partial(back_kernel, cfg),
        out_shape=(
            sds((seq, model), BF),
            sds((seq, model), BF),
            sds((seq, HW), BF),
            sds((8, model), F32),
            sds((8, model), F32),
            sds((rows, nr), F32),
            sds((rows, nq), F32),
            sds((model, nr), BF),
            sds((2,) + y.shape, BF),
        ),
        in_specs=[ANY] * 8 + [VMEM] + [ANY] * 7,
        out_specs=(ANY, ANY, ANY, VMEM, VMEM, ANY, ANY, ANY, ANY),
        scratch_shapes=[
            pltpu.VMEM((seq, nq), BF), heads, heads, wide, wide, wide, hidden, hidden,
            pltpu.VMEM((model, nq), BF), pltpu.VMEM((model, HW), BF), pltpu.VMEM((model, ff), BF),
            pltpu.VMEM((model, ff), BF), wide, pltpu.VMEM((seq // 8, ff), BF), pltpu.VMEM((model, nr), F32),
            pltpu.VMEM((model, nq), BF), pltpu.VMEM((model, nr), BF), pltpu.VMEM((model, nr), BF),
            pltpu.VMEM((model, nq), BF), pltpu.VMEM((model, nq), BF),
            pltpu.VMEM((dp - 1, rows, nr), BF), pltpu.VMEM((dp - 1, rows, nr), BF),
            pltpu.VMEM((dp - 1, rows, nq), BF), pltpu.VMEM((dp - 1, rows, nq), BF),
            pltpu.VMEM((rows, nr), F32), pltpu.VMEM((rows, nq), F32),
        ]
        + scatter_scratch(seq, model)
        + [DMA((6,)), DMA((6,)), DMA((16,)), DMA((3, 8)), DMA((2,)), DMA((3,)), DMA((1,))]
        + GradReduce.scratch(dp) * 2,
        compiler_params=params(5),
        cost_estimate=cost(70),
        name="layer_back",
    )(dmix, e2, cf, cy, hf, n1, w1, w0, vecs, xf, g, gp, n2, o, gr1, y)


def last_kernel(
    cfg, q_in, k_in, v_in, o_in, do_in, lse, srow, kcol, tab_in, e2_in, dh_in, xf_in, n1_in, w0, vecs, vf1, vd1, vd0,
    gr0, out1, outq, dhx, dxx, fq_o, fr_o, vec_o,
    q, k, v, o, do, tab, kt, dk, dv, dmix, dh, dx, xf, n1, e2, wqkv, gq, gotq, acrq, sbq, rbq, gr, got, sb, rb, fq, fr,
    vgf, va, vr, vout, part, mr, xr, sss, srs, lsem, vss, vrs, oss, ors, *rsems,
):
    col, heads, dp = cfg["col"], cfg["heads"], cfg["dp"]
    me = Mesh(dp, cfg["tensor"])
    sc = Scatter(me, part, mr, xr, sss, srs, 1 - me.y)
    half = sc.half
    seq = xf.shape[0]
    width = q.shape[1]
    own = [ds(sc.own(n), half) for n in range(2)]
    loads = load(
        [
            (k_in, k),
            (q_in, q),
            (v_in, v),
            (do_in, do),
            (o_in, o),
            (tab_in, tab),
            (w0.at[:, col["qkv"] : col["fc1"]], wqkv),
            (xf_in, xf),
            (e2_in, e2),
            (n1_in, n1),
        ]
        + [(dh_in.at[rr], dh.at[n]) for n, rr in enumerate(own)],
        lsem,
    )
    gr_load = pltpu.make_async_copy(gr0, gr, lsem.at[12])
    holds = (me.s == 0) & (me.y == 0)

    @pl.when(holds)
    def _():
        gr_load.start()

    greet([me.mate, me.beside, me.beside_mate, me.across, me.across_mate] + me.ring)
    redr = GradReduce(me, 0, gr0, gr, gr, got, sb, rb, fr, rsems[:6])
    redq = GradReduce(me, 0, gq, gq, gotq, acrq, sbq, rbq, fq, rsems[6:])
    vr_ = VectorReduce(me, va, vr, vss, vrs)
    redr.send()

    dh_over = push(dh_in.at[ds(me.py * 2 * half, 2 * half)], dhx, oss.at[2], ors.at[3], me.across)

    @pl.when(me.s == 1)
    def _():
        dh_over.start()

    xs = OwnedOut(me, dx, dxx, 0, oss, ors, lsem.at[14])
    old = [pltpu.make_async_copy(out1, fr, lsem.at[15]), pltpu.make_async_copy(outq, fq, lsem.at[16])]

    @pl.when(me.s == 1)
    def _():
        for c in old:
            c.start()

    vgf[...] = jnp.zeros_like(vgf)
    dk[...] = jnp.zeros_like(dk)
    dv[...] = jnp.zeros_like(dv)
    loads[0].wait()
    turn_blocks(k, kt)
    for c in loads[1:6]:
        c.wait()

    @pl.when(holds)
    def _():
        gr_load.wait()

    n_blocks = seq // QB

    def qloop(i, _):
        lo = jnp.maximum(i - DOC_MAX // QB, 0)
        attn_bwd_block(i, lo, i, heads, q, k, v, o, do, kt, lse, srow, kcol, tab, dk, dv, dmix)
        for at_block, steps in (
            (n_blocks // 2 - 1, range(0, 1)),
            (n_blocks // 2, range(1, dp // 2)),
            (n_blocks // 2 + 1, range(dp // 2, dp - 1)),
            (n_blocks - 2, range(dp - 1, dp)),
        ):

            @pl.when(i == at_block)
            def _(steps=steps):
                for d in steps:
                    redr.step(d)

        return 0

    lax.fori_loop(0, n_blocks, qloop, 0)

    def close(i, _):
        ii = ds(i * QB, QB)
        dmix[ii, width : 2 * width] = turn_lanes(dk[ii, :], tab[ii, :], -1).astype(BF)
        dmix[ii, 2 * width : 3 * width] = dv[ii, :].astype(BF)
        return 0

    lax.fori_loop(0, n_blocks, close, 0)
    for c in loads[6:]:
        c.wait()

    nf = gq.shape[0]
    accs = [dk.at[0:nf], dk.at[nf : 2 * nf], dv.at[0:nf]]
    for acc in accs:
        acc[...] = jnp.zeros_like(acc)

    def body(i, _):
        rows = ds(i * half, half)
        n1t = n1[rows, :].T
        for p, acc in enumerate(accs):
            acc[...] += dot(n1t, dmix[rows, p * HW : (p + 1) * HW])
        return 0

    lax.fori_loop(0, 8, body, 0)
    for p, acc in enumerate(accs):
        gq[:, p * HW : (p + 1) * HW] = acc[...].astype(BF)
    redq.send()

    def early():
        va[0, 0:8, :] = vgf[...] + vd0[...]
        va[0, 8:16, :] = vf1[...] + vd1[...]
        redq.step(0)
        vr_.send(0)
        redq.step(1)
        vr_.add(0, va.at[1])
        vr_.send(1)

    sc.run(lambda r0, i: back_tail(r0, half, dmix, xf, e2, wqkv, vecs.at[0], part, vgf), early)
    for d in range(2, dp - 1):
        redq.step(d)
    vr_.add(1, va.at[2])
    vr_.send(2)

    def write(n, i, value):
        dx[sc.side(n), ds(i * SUB, SUB), :] = value

    def leave(n):
        if n == 0:
            xs.far().start()
        else:
            xs.start_here()

    grad_out(sc, lambda n, i: dh[sc.side(n), ds(i * SUB, SUB), :], xf, vecs.at[0], write, leave)
    redq.step(dp - 1)
    vr_.add(2, vout)
    vec_o[...] = jnp.where(me.s == 0, vout[0:8, :], vout[8:16, :])
    redr.collect()
    redq.collect()

    @pl.when(me.s == 1)
    def _():
        for c in old:
            c.wait()

    ends = [pltpu.make_async_copy(fr, fr_o, lsem.at[0]), pltpu.make_async_copy(fq, fq_o, lsem.at[1])]
    for c in ends:
        c.start()
    redr.finish()
    redq.finish()
    vr_.finish()
    sc.finish()
    @pl.when(me.s == 1)
    def _():
        dh_over.wait()

    xs.wait()
    for c in ends:
        c.wait()


def layer_last(cfg, q, k, v, o, do, lse, sr, kc, tab, e2, dh, xf, n1, w0, vecs, vf1, vd1, vd0, gr0, out1, outq):
    seq, model = xf.shape
    dp, tensor, ff = cfg["dp"], cfg["tensor"], cfg["ff"]
    rows, nr, nq = model // dp, 2 * ff + HW, 3 * HW
    nv = dp + tensor - 1
    wide, owned, heads = pltpu.VMEM((seq, model), BF), pltpu.VMEM((2, seq // 8, model), BF), pltpu.VMEM((seq, HW), BF)
    return pl.pallas_call(
        functools.partial(last_kernel, cfg),
        out_shape=(sds((seq // 4, model), BF), sds((2, 2, seq // 8, model), BF), sds((rows, nq), F32), sds((rows, nr), F32), sds((8, model), F32)),
        in_specs=[ANY] * 5 + [VMEM] * 3 + [ANY] * 6 + [VMEM] * 4 + [ANY] * 3,
        out_specs=(ANY, ANY, ANY, ANY, VMEM),
        scratch_shapes=[
            heads, heads, heads, heads, heads, pltpu.VMEM(tab.shape, F32), pltpu.VMEM((HW, seq), BF),
            pltpu.VMEM((seq, HW), F32), pltpu.VMEM((seq, HW), F32), pltpu.VMEM((seq, nq), BF), owned, owned,
            wide, wide, wide, pltpu.VMEM((model, nq), BF),
            pltpu.VMEM((model, nq), BF), pltpu.VMEM((model, nq), BF), pltpu.VMEM((model, nq), BF),
            pltpu.VMEM((dp - 1, rows, nq), BF), pltpu.VMEM((dp - 1, rows, nq), BF),
            pltpu.VMEM((model, nr), BF), pltpu.VMEM((model, nr), BF),
            pltpu.VMEM((dp - 1, rows, nr), BF), pltpu.VMEM((dp - 1, rows, nr), BF),
            pltpu.VMEM((rows, nq), F32), pltpu.VMEM((rows, nr), F32),
            pltpu.VMEM((8, model), F32), pltpu.VMEM((3, 16, model), F32), pltpu.VMEM((nv, 16, model), F32),
            pltpu.VMEM((16, model), F32),
        ]
        + scatter_scratch(seq, model)
        + [DMA((17,)), DMA((nv,)), DMA((nv,)), DMA((3,)), DMA((4,))]
        + GradReduce.scratch(dp) * 2,
        compiler_params=params(6),
        cost_estimate=cost(80),
        name="layer_last",
    )(q, k, v, o, do, lse, sr, kc, tab, e2, dh, xf, n1, w0, vecs, vf1, vd1, vd0, gr0, out1, outq)


def finish_kernel(
    cfg, hf, hx, yx, dhf, dhx, dxx, fq_in, fr_in, vec, so, ig, bg1, bb1, gqkv, bqkv, gout, bdy, bdy2, bg2, bb2, gfc1, bfc1, gfc2,
    a, b, fq, fr, lsem, msem, osem,
):
    heads, ff, own, qw, fw = cfg["heads"], cfg["ff"], cfg["own"], cfg["qw"], cfg["fw"]
    me = Mesh(cfg["dp"], cfg["tensor"])
    loads = load([(fr_in, fr), (fq_in, fq)], lsem)
    half = a.shape[2]
    mine = [ref.at[pl.ds(pl.multiple_of((2 * me.t + n) * half, half), half)] for ref in (hf, dhf) for n in range(2)]

    def sources(core):
        if core == 0:
            first, second = [mine[0:2], [hx.at[pl.ds(n * half, half)] for n in range(2)]], None
        else:
            first, second = None, [mine[2:4], [dhx.at[pl.ds(n * half, half)] for n in range(2)]]
        whole = yx if core else dxx
        third = [[whole.at[me.y, n] for n in range(2)], [whole.at[1 - me.y, n] for n in range(2)]]
        return (first or third), (second or third)

    def moves(core):
        out = []
        for o, (ref, src) in enumerate(zip((a, b), sources(core))):
            for m in range(2):
                for n in range(2):
                    dst = ref.at[me.y if m == 0 else 1 - me.y, n]
                    out.append(pltpu.make_async_copy(src[m][n], dst, msem.at[4 * o + 2 * m + n]))
        return out

    for core in range(2):

        @pl.when(me.s == core)
        def _(core=core):
            for c in moves(core):
                c.start()

    model = vec.shape[1]
    short = pltpu.roll(vec[...], (model - (me.z * me.tensor + me.t) * own) % model, 1)
    for row, ref in ((0, bg1), (1, bb1), (2, bdy), (2, bdy2), (3, bg2), (4, bb2)):
        ref[...] = short[row : row + 1, 0:own]
    for h in range(heads):
        parts = [vec[6:7, p * HW + h * HD : p * HW + (h + 1) * HD] for p in range(3)]
        one = jnp.concatenate(parts + [jnp.zeros((1, HW - 3 * HD), F32)], axis=1)
        one = jnp.broadcast_to(one, (8, HW))
        bqkv[h] = pltpu.roll(one, (HW - me.z * qw) % HW, 1)[0:1, 0:qw]
        wide = ff // heads
        one = jnp.broadcast_to(vec[7:8, h * wide : (h + 1) * wide], (8, wide))
        bfc1[h] = pltpu.roll(one, (wide - me.z * fw) % wide, 1)[0:1, 0:fw]
    loads[0].wait()
    gfc1[0] = fr[:, 0:ff]
    gfc2[...] = fr[:, ff : 2 * ff]
    gout[0] = fr[:, 2 * ff : 2 * ff + HW].T[0 : heads * HD, :]
    for core in range(2):

        @pl.when(me.s == core)
        def _(core=core):
            for c in moves(core):
                c.wait()

    outs = []
    for o, (ref, dst) in enumerate(((a, so), (b, ig))):
        for m in range(2):
            for n in range(2):
                place = dst.at[0, m, 0, pl.ds(n * half, half)]
                outs.append(pltpu.make_async_copy(ref.at[m, n], place, osem.at[4 * o + 2 * m + n]))
    for c in outs:
        c.start()
    loads[1].wait()
    pieces = [fq[:, p * HW + h * HD : p * HW + (h + 1) * HD] for h in range(heads) for p in range(3)]
    gqkv[0] = jnp.concatenate(pieces, axis=1)
    for c in outs:
        c.wait()


def finish(cfg, hf, hx, yx, dhf, dhx, dxx, fq, fr, vec):
    heads, ff, rows = cfg["heads"], cfg["ff"], fq.shape[0]
    line = sds((1, cfg["own"]), F32)
    both = sds((1, 2, 1) + hx.shape, BF)
    return pl.pallas_call(
        functools.partial(finish_kernel, cfg),
        out_shape=(both, both, line, line, sds((1, rows, heads * 3 * HD), F32),
                   sds((heads, 1, cfg["qw"]), F32), sds((1, heads * HD, rows), F32), line, line, line, line,
                   sds((1, rows, ff), F32), sds((heads, 1, cfg["fw"]), F32), sds((rows, ff), F32)),
        in_specs=[ANY] * 8 + [VMEM],
        out_specs=(ANY, ANY) + (VMEM,) * 12,
        scratch_shapes=[
            pltpu.VMEM(yx.shape, BF), pltpu.VMEM(yx.shape, BF), pltpu.VMEM(fq.shape, F32), pltpu.VMEM(fr.shape, F32),
            DMA((2,)), DMA((8,)), DMA((8,)),
        ],
        compiler_params=pltpu.CompilerParams(vmem_limit_bytes=67043328),
        cost_estimate=cost(5),
        name="finish",
    )(hf, hx, yx, dhf, dhx, dxx, fq, fr, vec)


def by_part(w):
    rows = w.shape[0]
    heads = w.shape[1] // (3 * HD)
    w = w.reshape(rows, heads, 3, HD).transpose(0, 2, 1, 3).reshape(rows, 3, heads * HD)
    return jnp.pad(w, ((0, 0), (0, 0), (0, HW - heads * HD))).reshape(rows, 3 * HW)


def shards(
    dp, tensor, inputs, cotangent, segments, live_blocks, ln1_gain, ln1_bias, qkv_weight, qkv_bias,
    out_weight, out_bias, ln2_gain, ln2_bias, fc1_weight, fc1_bias, fc2_weight, fc2_bias,
):
    live_blocks = live_blocks.T
    model = inputs.shape[-1]
    ff = fc1_weight.shape[2]
    heads = qkv_bias.shape[1]
    col = columns(model, ff)
    wout = jnp.pad(out_weight[0].T, ((0, 0), (0, HW - heads * HD)))
    w = jnp.concatenate([by_part(qkv_weight[0]), fc1_weight[0], fc2_weight[0].T, wout], axis=1)
    small = jnp.stack([ln1_gain[0], ln1_bias[0], out_bias[0], ln2_gain[0], ln2_bias[0], fc2_bias[0]])

    def lanes(a):
        return jnp.pad(a.astype(F32), ((0, 0), (0, 128 - a.shape[1])))

    sv = jnp.concatenate([lanes(small), lanes(qkv_bias[0]), lanes(fc1_bias[0])], axis=0)
    sv = jnp.pad(sv, ((0, -sv.shape[0] % 8), (0, 0)))
    fr = np.float32(10000.0) ** (-(np.arange(ROT // 2, dtype=np.float32) * np.float32(2.0 / ROT)))
    fr = jnp.asarray(np.broadcast_to(fr[:, None], (ROT // 2, 128)).astype(np.float32))
    cfg = {
        "col": col, "ff": ff, "heads": heads, "dp": dp, "tensor": tensor, "own": small.shape[1],
        "qw": qkv_bias.shape[2], "fw": fc1_bias.shape[2],
        "groups": [(0, col["fc1"]), (col["fc1"], col["fc2"]), (col["fc2"], col["out"]), (col["out"], col["end"])],
    }

    xf, n1a, n2a, ga, gpa, tab, w0, qa, ka, va, cf, vecs, sr, kc = layer_in(
        cfg, inputs, cotangent, segments, live_blocks, w, sv, fr
    )
    oa, lsea, hf, n1b, n2b, gb, gpb, w1, qb, kb, vb = layer_mid(cfg, qa, ka, va, sr, kc, ga, xf, w, w0, vecs, tab)
    ob, lseb = attn_fwd(heads, segments, live_blocks, qb, kb, vb, sr, kc)
    y, dob, e2b, grb, hx, cy, vdb = layer_turn(cfg, ob, gb, hf, cf, cotangent, w1, vecs, n2b, gpb)
    dmb = attn_bwd(heads, segments, live_blocks, qb, kb, vb, ob, dob, lseb, sr, kc, tab)
    dhf, e2a, doa, vfb, vda, out1, outq, gra, yx = layer_back(
        cfg, dmb, e2b, cf, cy, hf, n1b, w1, w0, vecs, xf, ga, gpa, n2a, oa, grb, y
    )
    dhx, dxx, fq, fr_, gv = layer_last(
        cfg, qa, ka, va, oa, doa, lsea, sr, kc, tab, e2a, dhf, xf, n1a, w0, vecs, vfb, vdb, vda, gra, out1, outq
    )
    last_part = finish(cfg, hf, hx, yx, dhf, dhx, dxx, fq, fr_, gv)
    so, ig, bg1, bb1, gqkv, bqkv, gout, bdy, bdy2, bg2, bb2, gfc1, bfc1, gfc2 = last_part
    bqkv, bfc1, gfc2 = bqkv.transpose(1, 0, 2), bfc1.transpose(1, 0, 2), gfc2.T[None]
    return (so, ig, bg1, bb1, gqkv, bqkv, gout, bdy, bg2, bb2, gfc1, bfc1, gfc2, bdy2)


def solution(mesh):
    both = ("dp", "tensor")
    in_specs = (
        P(None, "dp", "tensor", None),
        P(None, "dp", "tensor", None),
        P(None, "dp", None),
        P(None, "dp"),
        P("section", both),
        P("section", both),
        P("section", "dp", "tensor"),
        P("section", "tensor", "dp"),
        P("section", "tensor", "dp"),
        P("section", both),
        P("section", both),
        P("section", both),
        P("section", "dp", "tensor"),
        P("section", "tensor", "dp"),
        P("section", "tensor", "dp"),
        P("section", both),
    )
    out_specs = (
        P("section", None, "dp", "tensor", None),
        P("section", None, "dp", "tensor", None),
        P("section", both),
        P("section", both),
        P("section", "dp", "tensor"),
        P("section", "tensor", "dp"),
        P("section", "tensor", "dp"),
        P("section", both),
        P("section", both),
        P("section", both),
        P("section", "dp", "tensor"),
        P("section", "tensor", "dp"),
        P("section", "tensor", "dp"),
        P("section", both),
    )
    body = functools.partial(shards, mesh.shape["dp"], mesh.shape["tensor"])
    return jax.shard_map(body, mesh=mesh, in_specs=in_specs, out_specs=out_specs, check_vma=False)
```

```python
import functools

import jax
import jax.numpy as jnp
import numpy as np
from jax import lax
from jax.experimental import pallas as pl
from jax.experimental.pallas import tpu as pltpu
from jax.sharding import PartitionSpec as P

F32 = jnp.float32
BF = jnp.bfloat16
MESH = pl.DeviceIdType.MESH
HD = 64
ROT = 16
LIVE = 128
DOCS = 4
DOC_MAX = 1024
QB = 256
HW = 256
SUB = 256
EPS = 1e-05
NEG = -1e30
VMEM = pl.BlockSpec(memory_space=pltpu.VMEM)
ANY = pl.BlockSpec(memory_space=pltpu.HBM)
SMEM = pl.BlockSpec(memory_space=pltpu.SMEM)
DMA = pltpu.SemaphoreType.DMA


def sds(shape, dtype):
    return jax.ShapeDtypeStruct(shape, dtype)


def dg(a, b, ca, cb):
    return lax.dot_general(a, b, (((ca,), (cb,)), ((), ())), preferred_element_type=F32)


def dot(a, b):
    return jnp.dot(a, b, preferred_element_type=F32)


def ds(start, size):
    return pl.ds(pl.multiple_of(start, size), size)


def norm_stats(x):
    mu = jnp.mean(x, axis=-1, keepdims=True)
    xc = x - mu
    var = jnp.mean(xc * xc, axis=-1, keepdims=True)
    return xc, lax.rsqrt(var + EPS)


def head_lanes(width, heads):
    lane = lax.broadcasted_iota(jnp.int32, (1, width), 1)
    return [(lane >= h * HD) & (lane < (h + 1) * HD) for h in range(heads)]


def allow_mask(kc, sq, diag):
    m = kc == sq
    if diag:
        r = lax.broadcasted_iota(jnp.int32, (QB, QB), 0)
        c = lax.broadcasted_iota(jnp.int32, (QB, QB), 1)
        m = (m & (r <= c)) | (r == c)
    return m


def block_bounds(seg, live, i, n):
    s = lax.axis_index("tensor") // 2
    doc = seg[s, 0, i * QB]

    def body(j, count):
        return count + jnp.where((j < i) & (seg[s, 0, (j + 1) * QB - 1] == doc), 1, 0)

    hi = jnp.minimum(i, (live[0, s] * LIVE + QB - 1) // QB)
    return jnp.minimum(i - lax.fori_loop(0, n, body, 0), hi), hi


def turn_blocks(src, dst):
    def turn(i, _):
        dst[:, ds(i * QB, QB)] = src[ds(i * QB, QB), :].T
        return 0

    lax.fori_loop(0, src.shape[0] // QB, turn, 0)


def attn_fwd_block(i, lo, hi, heads, q_ref, k_ref, vt, sr_ref, kc_ref, s_scr, o_ref, lse_ref):
    width = q_ref.shape[1]
    qi = ds(i * QB, QB)
    q = q_ref[qi, :]
    qm = [jnp.where(m, q, jnp.zeros_like(q)) for m in head_lanes(width, heads)]
    sq = sr_ref[0:1, qi]

    def scores(j, slot, ms, diag):
        kj = ds(j * QB, QB)
        k = k_ref[kj, :]
        mask = allow_mask(kc_ref[kj, 0:1], sq, diag)
        out = []
        for h in range(heads):
            s = jnp.where(mask, dg(k, qm[h], 1, 1), NEG)
            s_scr[h, ds(slot * QB, QB), :] = s
            out.append(jnp.maximum(ms[h], jnp.max(s, axis=0, keepdims=True)))
        return tuple(out)

    ms = tuple(jnp.full((1, QB), NEG, F32) for _ in range(heads))
    ms = scores(i, 0, ms, True)
    ms = lax.fori_loop(lo, hi, lambda j, ms: scores(j, j - lo + 1, ms, False), ms)

    def weigh(j, slot, st):
        kj = ds(j * QB, QB)
        out = []
        for h in range(heads):
            total, acc = st[h]
            p = jnp.exp(s_scr[h, ds(slot * QB, QB), :] - ms[h])
            total = total + jnp.sum(p, axis=0, keepdims=True)
            acc = acc + dot(vt[h * HD : (h + 1) * HD, kj], p.astype(BF))
            out.append((total, acc))
        return tuple(out)

    st = tuple((jnp.zeros((1, QB), F32), jnp.zeros((HD, QB), F32)) for _ in range(heads))
    st = weigh(i, 0, st)
    st = lax.fori_loop(lo, hi, lambda j, st: weigh(j, j - lo + 1, st), st)
    ot = [st[h][1] * (1.0 / st[h][0]) for h in range(heads)]
    ot = jnp.concatenate(ot + [jnp.zeros((width - heads * HD, QB), F32)], axis=0)
    o_ref[qi, :] = ot.T.astype(BF)
    lse = [ms[h] + jnp.log(st[h][0]) for h in range(heads)]
    lse_ref[:, qi] = jnp.concatenate(lse + [jnp.zeros((8 - heads, QB), F32)], axis=0)


def attn_fwd_kernel(heads, seg, live, q_in, k_in, v_in, sr_ref, kc_ref, o_out, lse_ref, q, k, v, o, vt, s_scr, lsem, osem):
    n = q.shape[0] // QB
    loads = load([(v_in, v), (q_in, q), (k_in, k)], lsem)
    loads[0].wait()
    turn_blocks(v, vt)
    loads[1].wait()
    loads[2].wait()

    def out(i):
        rows = ds(i * QB, QB)
        return pltpu.make_async_copy(o.at[rows], o_out.at[rows], osem.at[i])

    def qloop(i, _):
        lo, hi = block_bounds(seg, live, i, n)
        attn_fwd_block(i, lo, hi, heads, q, k, vt, sr_ref, kc_ref, s_scr, o, lse_ref)
        out(i).start()
        return 0

    lax.fori_loop(0, n, qloop, 0)

    def drain(i, _):
        out(i).wait()
        return 0

    lax.fori_loop(0, n, drain, 0)


def attn_fwd(heads, seg, live, q, k, v, sr, kc):
    rows, width = q.shape
    buf = pltpu.VMEM((rows, width), BF)
    return pl.pallas_call(
        functools.partial(attn_fwd_kernel, heads),
        out_shape=(sds((rows, width), BF), sds((8, rows), F32)),
        in_specs=[SMEM, SMEM, ANY, ANY, ANY, VMEM, VMEM],
        out_specs=(ANY, VMEM),
        scratch_shapes=[buf, buf, buf, buf, pltpu.VMEM((width, rows), BF), pltpu.VMEM((heads, rows + QB, QB), F32),
                        DMA((3,)), DMA((rows // QB,))],
        compiler_params=pltpu.CompilerParams(vmem_limit_bytes=67043328),
        cost_estimate=cost(12),
        name="attn_fwd",
    )(seg, live, q, k, v, sr, kc)


def turn_lanes(x, tab, sign):
    width = x.shape[1]
    c, sn = [jnp.concatenate([tab[:, a * 128 : (a + 1) * 128]] * (width // 128), axis=1) for a in range(2)]
    lane = lax.broadcasted_iota(jnp.int32, (1, width), 1) % HD
    moved = jnp.where(lane < ROT // 2, pltpu.roll(x, width - ROT // 2, 1), pltpu.roll(x, ROT // 2, 1)) * sn
    return x * c + moved if sign > 0 else x * c - moved


def attn_bwd_block(i, lo, hi, heads, q_ref, k_ref, v_ref, o_ref, do_ref, kt, lse_ref, sr_ref, kc_ref, tab, dk, dv, out):
    width = q_ref.shape[1]
    hm = head_lanes(width, heads)
    rowid = lax.broadcasted_iota(jnp.int32, (8, width), 0)
    lane = lax.broadcasted_iota(jnp.int32, (8, width), 1)
    sel = ((lane >= rowid * HD) & (lane < (rowid + 1) * HD)).astype(F32).astype(BF)
    qi = ds(i * QB, QB)
    q = q_ref[qi, :]
    do = do_ref[qi, :]
    z = jnp.zeros_like(q)
    qm = [jnp.where(hm[h], q, z) for h in range(heads)]
    dom = [jnp.where(hm[h], do, z) for h in range(heads)]
    qcat = jnp.concatenate(qm, axis=0)
    docat = jnp.concatenate(dom, axis=0)
    prod = do.astype(F32) * o_ref[qi, :].astype(F32)
    high = prod.astype(BF)
    low = (prod - high.astype(F32)).astype(BF)
    delta = dg(sel, high, 1, 1) + dg(sel, low, 1, 1)
    lse = lse_ref[:, qi]
    sq = sr_ref[0:1, qi]

    def step(j, dqs, diag):
        kj = ds(j * QB, QB)
        k = k_ref[kj, :]
        v = v_ref[kj, :]
        mask = allow_mask(kc_ref[kj, 0:1], sq, diag)
        ps, dss, res = [], [], []
        for h in range(heads):
            s = dg(k, qm[h], 1, 1)
            dp = dg(v, dom[h], 1, 1)
            p = jnp.exp(jnp.where(mask, s - lse[h : h + 1, :], NEG))
            score_grad = (p * (dp - delta[h : h + 1, :])).astype(BF)
            ps.append(p.astype(BF))
            dss.append(score_grad)
            res.append(dqs[h] + dot(kt[h * HD : (h + 1) * HD, kj], score_grad))
        dv[kj, :] += dot(jnp.concatenate(ps, axis=1), docat)
        dk[kj, :] += dot(jnp.concatenate(dss, axis=1), qcat)
        return tuple(res)

    dqs = tuple(jnp.zeros((HD, QB), F32) for _ in range(heads))
    dqs = step(i, dqs, True)
    dqs = lax.fori_loop(lo, hi, lambda j, d: step(j, d, False), dqs)
    dq = jnp.concatenate(list(dqs) + [jnp.zeros((width - heads * HD, QB), F32)], axis=0).T * 0.125
    out[qi, 0:width] = turn_lanes(dq, tab[qi, :], -1).astype(BF)


def attn_bwd_kernel(
    heads, seg, live, q_in, k_in, v_in, o_in, do_in, lse_ref, sr_ref, kc_ref, tab_in, out_ref,
    q, k, v, o, do, tab, out, kt, dk, dv, lsem, osem,
):
    rows, width = q.shape
    n = rows // QB
    loads = load([(k_in, k), (q_in, q), (v_in, v), (do_in, do), (o_in, o), (tab_in, tab)], lsem)
    dk[...] = jnp.zeros_like(dk)
    dv[...] = jnp.zeros_like(dv)
    loads[0].wait()
    turn_blocks(k, kt)
    for c in loads[1:]:
        c.wait()

    def qloop(i, _):
        lo, hi = block_bounds(seg, live, i, n)
        attn_bwd_block(i, lo, hi, heads, q, k, v, o, do, kt, lse_ref, sr_ref, kc_ref, tab, dk, dv, out)
        return 0

    lax.fori_loop(0, n, qloop, 0)

    def leave(i):
        rr = ds(i * QB, QB)
        return pltpu.make_async_copy(out.at[rr], out_ref.at[rr], osem.at[i])

    def finish(i, _):
        ii = ds(i * QB, QB)
        out[ii, width : 2 * width] = turn_lanes(dk[ii, :], tab[ii, :], -1).astype(BF)
        out[ii, 2 * width : 3 * width] = dv[ii, :].astype(BF)
        leave(i).start()
        return 0

    lax.fori_loop(0, n, finish, 0)

    def drain(i, _):
        leave(i).wait()
        return 0

    lax.fori_loop(0, n, drain, 0)


def attn_bwd(heads, seg, live, q, k, v, o, do, lse, sr, kc, tab):
    rows, width = q.shape
    buf = pltpu.VMEM((rows, width), BF)
    return pl.pallas_call(
        functools.partial(attn_bwd_kernel, heads),
        out_shape=sds((rows, 3 * width), BF),
        in_specs=[SMEM, SMEM] + [ANY] * 5 + [VMEM] * 3 + [ANY],
        out_specs=ANY,
        scratch_shapes=[buf, buf, buf, buf, buf, pltpu.VMEM(tab.shape, F32), pltpu.VMEM((rows, 3 * width), BF),
                        pltpu.VMEM((width, rows), BF), pltpu.VMEM((rows, width), F32), pltpu.VMEM((rows, width), F32),
                        DMA((6,)), DMA((rows // QB,))],
        compiler_params=pltpu.CompilerParams(vmem_limit_bytes=67043328),
        cost_estimate=cost(26),
        name="attn_bwd",
    )(seg, live, q, k, v, o, do, lse, sr, kc, tab)


class Mesh:
    def __init__(self, dp, tensor):
        self.dp, self.tensor = dp, tensor
        self.s, self.z, self.t = lax.axis_index("section"), lax.axis_index("dp"), lax.axis_index("tensor")
        self.x, self.y = self.t % 2, self.t // 2
        self.px, self.py = 2 * self.y + (1 - self.x), 2 * (1 - self.y) + self.x
        self.mate = {"section": 1 - self.s}
        self.beside = {"tensor": self.px}
        self.beside_mate = {"tensor": self.px, "section": 1 - self.s}
        self.across = {"tensor": self.py}
        self.across_mate = {"tensor": self.py, "section": 1 - self.s}
        self.ring = [{"dp": (self.z + d) % dp} for d in range(1, dp)]
        self.group = [{"tensor": (self.t + d) % tensor} for d in range(1, tensor)]
        self.quarter = 2 * self.s + self.x

    def across_core(self, core):
        return {"tensor": self.py, "section": core}


def greet(peers):
    bar = pltpu.get_barrier_semaphore()
    for peer in peers:
        pl.semaphore_signal(bar, inc=1, device_id=peer, device_id_type=MESH)
    pl.semaphore_wait(bar, len(peers))


def push(src, dst, ssem, rsem, peer):
    return pltpu.make_async_remote_copy(
        src_ref=src, dst_ref=dst, send_sem=ssem, recv_sem=rsem, device_id=peer, device_id_type=MESH
    )


def pick(i, values):
    out = values[-1]
    for n in range(len(values) - 2, -1, -1):
        out = jnp.where(i == n, values[n], out)
    return out


class Tokens:
    def __init__(self, me, seq):
        self.me, self.half = me, seq // 8

    def start_of(self, a, b, h):
        return (4 * a + 2 * b + h) * self.half

    def rows(self, a, b, h):
        return ds(self.start_of(a, b, h), self.half)

    def own(self, a):
        return self.start_of(a, self.me.x, self.me.s)


class Gather(Tokens):
    def __init__(self, me, full, ssem, rsem, first=0):
        super().__init__(me, full.shape[0])
        self.full, self.ssem, self.rsem, self.first = full, ssem, rsem, first

    def side(self, n):
        return self.first if n == 0 else 1 - self.first

    def plan(self, i):
        me, a = self.me, self.side(i % 2)
        ref = self.full.at[self.rows(a, (1 - me.x) if i >= 4 else me.x, me.s)]
        return push(ref, ref, self.ssem.at[i], self.rsem.at[i], me.beside if i in (2, 3) else me.mate)

    def start(self, n):
        self.plan(n).start()
        self.plan(2 + n).start()

    def order(self, i):
        me = self.me
        a = pick(i, [self.side(n) for n in (0, 1, 0, 1, 0, 0, 1, 1)])
        b = jnp.where(i < 4, me.x, 1 - me.x)
        h = pick(i, [me.s, me.s, 1 - me.s, 1 - me.s, me.s, 1 - me.s, me.s, 1 - me.s])
        return self.start_of(a, b, h)

    def step(self, i):
        if i in (2, 3):
            self.plan(i - 2).wait_recv()
        if i in (4, 6):
            n = i // 2 - 2
            self.plan(2 + n).wait_recv()
            self.plan(4 + n).start()
        if i in (5, 7):
            self.plan(4 + i // 2 - 2).wait_recv()

    def arrive(self, i):
        for n in range(2, 8):

            @pl.when(i == n)
            def _(n=n):
                self.step(n)

    def finish(self):
        for i in range(6):
            self.plan(i).wait_send()

    def run(self, work):
        def body(i, _):
            self.arrive(i)
            work(self.order(i), i)
            return 0

        lax.fori_loop(0, 8, body, 0)
        self.finish()


class Scatter(Tokens):
    def __init__(self, me, part, mr, xr, ssem, rsem, first=0):
        super().__init__(me, part.shape[0])
        self.part, self.mr, self.xr, self.ssem, self.rsem, self.first = part, mr, xr, ssem, rsem, first

    def side(self, n):
        return self.first if n == 0 else 1 - self.first

    def plan(self, i):
        me = self.me
        if i < 4:
            b = (1 - me.x) if i < 2 else me.x
            src, dst, peer = self.rows(self.side(i % 2), b, 1 - me.s), self.mr.at[i], me.mate
        else:
            src, dst, peer = self.rows(self.side(i - 4), 1 - me.x, me.s), self.xr.at[i - 4], me.beside
        return push(self.part.at[src], dst, self.ssem.at[i], self.rsem.at[i], peer)

    def run(self, work, early=None):
        me = self.me

        def body(i, _):
            k = i // 2
            b = jnp.where(k < 2, 1 - me.x, me.x)
            h = jnp.where(i % 2 == 0, 1 - me.s, me.s)
            work(self.start_of(jnp.where(k % 2 == 0, self.side(0), self.side(1)), b, h), i)
            for n in range(4):

                @pl.when(i == 2 * n)
                def _(n=n):
                    self.plan(n).start()

            for n in range(2):

                @pl.when(i == 2 * n + 1)
                def _(n=n):
                    self.plan(n).wait_recv()
                    base = self.start_of(self.side(n), 1 - me.x, me.s)

                    def add(j, _):
                        rr = ds(base + j * SUB, SUB)
                        got = self.mr[n, ds(j * SUB, SUB), :].astype(F32)
                        self.part[rr, :] = (self.part[rr, :].astype(F32) + got).astype(BF)
                        return 0

                    lax.fori_loop(0, self.half // SUB, add, 0)
                    self.plan(4 + n).start()

            return 0

        lax.fori_loop(0, 8, body, 0)
        if early is not None:
            early()

    def arrive(self, n):
        self.plan(2 + n).wait_recv()
        self.plan(4 + n).wait_recv()

    def total(self, n, i):
        rr = ds(self.own(self.side(n)) + i * SUB, SUB)
        sub = ds(i * SUB, SUB)
        return self.part[rr, :].astype(F32) + self.mr[2 + n, sub, :].astype(F32) + self.xr[n, sub, :].astype(F32)

    def finish(self):
        for i in range(6):
            self.plan(i).wait_send()


def scatter_scratch(rows, width):
    half = rows // 8
    return [
        pltpu.VMEM((rows, width), BF),
        pltpu.VMEM((4, half, width), BF),
        pltpu.VMEM((2, half, width), BF),
        DMA((6,)),
        DMA((6,)),
    ]


class WeightGather:
    def __init__(self, me, layer, shard, full, gat, groups, sems):
        self.me, self.layer, self.shard, self.full, self.gat, self.groups = me, layer, shard, full, gat, groups
        self.own, self.wss, self.wrs, self.fss, self.frs, self.yss, self.yrs = sems
        self.rows = shard.shape[0]
        self.collects = me.s == layer
        self.keeps = me.y == layer

    def block(self, ref, zz, g):
        a, b = self.groups[g]
        return ref.at[ds(zz * self.rows, self.rows), a:b]

    def mine(self, g):
        a, b = self.groups[g]
        return self.shard.at[:, a:b]

    def local(self, g):
        return pltpu.make_async_copy(self.mine(g), self.block(self.full, self.me.z, g), self.own.at[g])

    def out(self, g, d, ref):
        dst = self.block(ref, self.me.z, g)
        return push(self.mine(g), dst, self.wss.at[g, d], self.wrs.at[g, d], self.me.ring[d])

    def hand(self, g, d, ref, across):
        zz = (self.me.z + self.me.dp - d) % self.me.dp
        src = self.mine(g) if d == 0 else self.block(ref, zz, g)
        ss, rs = (self.yss, self.yrs) if across else (self.fss, self.frs)
        peer = self.me.across_core(self.me.y) if across else self.me.mate
        return push(src, self.block(self.full, zz, g), ss.at[g, d], rs.at[g, d], peer)

    def both(self, do):
        @pl.when(self.collects & self.keeps)
        def _():
            do(self.full, True)

        @pl.when(self.collects & jnp.logical_not(self.keeps))
        def _():
            do(self.gat, False)

    def send_ring(self):
        def do(ref, keeps):
            for g in range(len(self.groups)):
                for d in range(self.me.dp - 1):
                    self.out(g, d, ref).start()

        self.both(do)

    def send_own(self, g):
        def do(ref, keeps):
            self.hand(g, 0, ref, True).start()
            if keeps:
                self.local(g).start()
            else:
                self.hand(g, 0, ref, False).start()

        self.both(do)

    def forward(self, g, blocks=None):
        def do(ref, keeps):
            for d in range(self.me.dp - 1) if blocks is None else blocks:
                self.out(g, d, ref).wait_recv()
                self.hand(g, d + 1, ref, True).start()
                if not keeps:
                    self.hand(g, d + 1, ref, False).start()

        self.both(do)

    def ready(self, g):
        me = self.me

        @pl.when(self.collects & self.keeps)
        def _():
            self.local(g).wait()

        @pl.when(me.s != me.y)
        def _():
            for d in range(me.dp):
                self.hand(g, d, self.full, True).wait_recv()

        @pl.when((me.s == me.y) & jnp.logical_not(self.collects))
        def _():
            for d in range(me.dp):
                self.hand(g, d, self.full, False).wait_recv()

    def finish(self):
        def do(ref, keeps):
            for g in range(len(self.groups)):
                for d in range(self.me.dp - 1):
                    self.out(g, d, ref).wait_send()
                for d in range(self.me.dp):
                    self.hand(g, d, ref, True).wait_send()
                    if not keeps:
                        self.hand(g, d, ref, False).wait_send()

        self.both(do)

    @staticmethod
    def scratch(dp, n):
        return [DMA((n,)), DMA((n, dp - 1)), DMA((n, dp - 1))] + [DMA((n, dp))] * 4


class GradReduce:
    def __init__(self, me, layer, src, mine, got, across, sb, rb, own, sems):
        self.me, self.layer, self.src, self.mine, self.got, self.across = me, layer, src, mine, got, across
        self.sb, self.rb, self.own = sb, rb, own
        self.hss, self.hrs, self.yss, self.yrs, self.pss, self.prs = sems
        self.rows = own.shape[0]
        self.some = 96 if self.rows % 96 == 0 else 48
        self.sums = me.s == layer
        self.holds = me.y == layer

    @staticmethod
    def scratch(dp):
        return [DMA((1,)), DMA((1,)), DMA((dp,)), DMA((dp,)), DMA((dp - 1,)), DMA((dp - 1,))]

    def hand(self):
        return push(self.src, self.got, self.hss.at[0], self.hrs.at[0], self.me.mate)

    def zz(self, d):
        return (self.me.z + d + 1) % self.me.dp

    def over(self, d):
        rr = ds(self.zz(d) * self.rows, self.rows)
        peer = self.me.across_core(self.layer)
        return push(self.src.at[rr], self.across.at[rr], self.yss.at[d], self.yrs.at[d], peer)

    def out(self, d):
        return push(self.sb.at[d], self.rb.at[d], self.pss.at[d], self.prs.at[d], self.me.ring[d])

    def send(self):
        me = self.me

        @pl.when(me.s != me.y)
        def _():
            for d in range(me.dp):
                self.over(d).start()

        @pl.when((me.s == me.y) & jnp.logical_not(self.sums))
        def _():
            self.hand().start()

    def step(self, d):
        me = self.me

        @pl.when(self.sums)
        def _():
            if d == 0:

                @pl.when(jnp.logical_not(self.holds))
                def _():
                    self.hand().wait_recv()

            self.over(d).wait_recv()
            last = d == me.dp - 1
            step = self.some

            def add(ref):
                def body(i, _):
                    rr = ds(self.zz(d) * self.rows + i * step, step)
                    value = ref[rr, :].astype(F32) + self.across[rr, :].astype(F32)
                    if last:
                        self.own[ds(i * step, step), :] = value
                    else:
                        self.sb[d, ds(i * step, step), :] = value.astype(BF)
                    return 0

                lax.fori_loop(0, self.rows // step, body, 0)

            if self.mine is self.got:
                add(self.mine)
            else:

                @pl.when(self.holds)
                def _():
                    add(self.mine)

                @pl.when(jnp.logical_not(self.holds))
                def _():
                    add(self.got)

            if not last:
                self.out(d).start()

    def collect(self):
        me = self.me

        @pl.when(self.sums)
        def _():
            for d in range(me.dp - 1):
                self.out(d).wait_recv()

                def add(i, _, d=d):
                    rr = ds(i * self.some, self.some)
                    self.own[rr, :] += self.rb[d, rr, :].astype(F32)
                    return 0

                lax.fori_loop(0, self.rows // self.some, add, 0)
            for d in range(me.dp - 1):
                self.out(d).wait_send()

    def finish(self):
        me = self.me

        @pl.when(me.s != me.y)
        def _():
            for d in range(me.dp):
                self.over(d).wait_send()

        @pl.when((me.s == me.y) & jnp.logical_not(self.sums))
        def _():
            self.hand().wait_send()


class VectorGather:
    def __init__(self, me, sv, buf, ss, rs, own):
        self.me, self.sv, self.buf, self.ss, self.rs, self.own = me, sv, buf, ss, rs, own

    def local(self):
        me = self.me
        return pltpu.make_async_copy(self.sv, self.buf.at[me.s, me.t, me.z], self.own)

    def stage(self, n):
        me = self.me
        if n == 0:
            dst = self.buf.at[me.s, me.t, me.z]
            return [push(self.sv, dst, self.ss.at[d], self.rs.at[d], peer) for d, peer in enumerate(me.ring)]
        base = me.dp - 1
        if n == 1:
            ref = self.buf.at[me.s, me.t]
            return [
                push(ref, ref, self.ss.at[base + d], self.rs.at[base + d], peer) for d, peer in enumerate(me.group)
            ]
        i = base + me.tensor - 1
        ref = self.buf.at[me.s]
        return [push(ref, ref, self.ss.at[i], self.rs.at[i], me.mate)]

    def send(self, n):
        if n == 0:
            self.local().start()
        for c in self.stage(n):
            c.start()

    def wait(self, n):
        if n == 0:
            self.local().wait()
        for c in self.stage(n):
            c.wait_recv()

    def finish(self):
        for n in range(3):
            for c in self.stage(n):
                c.wait_send()

    def build(self, vecs, heads, own, qw, fw):
        me, buf = self.me, self.buf
        for layer in range(2):
            wide = [buf[layer, tt, zz, 0:8, :][:, 0:own] for zz in range(me.dp) for tt in range(me.tensor)]
            vecs[layer, 0:8, :] = jnp.concatenate(wide, axis=1)
            here = [buf[layer, me.quarter, zz] for zz in range(me.dp)]
            by = [jnp.concatenate([p[6 + h : 7 + h, 0:qw] for p in here], axis=1) for h in range(heads)]
            qb = []
            for part in range(3):
                qb += [b[:, part * HD : (part + 1) * HD] for b in by] + [jnp.zeros((1, HW - heads * HD), F32)]
            vecs[layer, 6:7, :] = jnp.concatenate(qb, axis=1)
            fb = [p[6 + heads + h : 7 + heads + h, 0:fw] for h in range(heads) for p in here]
            vecs[layer, 7:8, :] = jnp.concatenate(fb, axis=1)


class VectorReduce:
    def __init__(self, me, va, vr, ss, rs):
        self.me, self.va, self.vr, self.ss, self.rs = me, va, vr, ss, rs

    def stage(self, n):
        me, va, vr, ss, rs = self.me, self.va, self.vr, self.ss, self.rs
        peers, base = [([me.across], 0), (me.ring, 1), ([me.mate, me.beside, me.beside_mate], me.dp)][n]
        return [push(va.at[n], vr.at[base + d], ss.at[base + d], rs.at[base + d], p) for d, p in enumerate(peers)]

    def send(self, n):
        for c in self.stage(n):
            c.start()

    def add(self, n, out):
        base = [0, 1, self.me.dp][n]
        for c in self.stage(n):
            c.wait_recv()
        if n < 2:
            total = self.va[n]
            for d in range(len(self.stage(n))):
                total = total + self.vr[base + d]
            out[...] = total
            return
        mine, mate = self.va[2], self.vr[base]
        row = lax.broadcasted_iota(jnp.int32, mine.shape, 0)
        quarter = jnp.where(self.me.s == self.me.y, mine, mate)
        out[...] = jnp.where(row % 8 < 6, mine + mate + self.vr[base + 1] + self.vr[base + 2], quarter)

    def finish(self):
        for n in range(3):
            for c in self.stage(n):
                c.wait_send()


def document_tables(seg, live, fr_ref, tab, srow, kcol):
    seq = seg.shape[1]
    count = lax.broadcasted_iota(jnp.int32, seg.shape, 1)
    start = jnp.zeros_like(seg)
    for doc in range(DOCS - 1):
        before = jnp.sum(jnp.where(seg == doc, 1.0, 0.0), axis=1, keepdims=True).astype(jnp.int32)
        start = start + jnp.where(seg > doc, before, 0)
    ang = fr_ref[:, 0:1] * (count - start).astype(F32)
    cs, sn = jnp.cos(ang), jnp.sin(ang)
    one = jnp.ones((HD - ROT, seq), F32)
    tab[:, 0:128] = jnp.concatenate([cs, cs, one] * 2, axis=0).T
    tab[:, 128:256] = jnp.concatenate([-sn, sn, jnp.zeros_like(one)] * 2, axis=0).T
    srow[...] = jnp.broadcast_to(seg, srow.shape)
    keys = jnp.where(count < live * LIVE, seg, -1).astype(F32)
    for b in range(seq // QB):
        part = jnp.broadcast_to(keys[:, b * QB : (b + 1) * QB], (128, QB))
        kcol[b * QB : (b + 1) * QB, :] = part.T.astype(jnp.int32)


QKV, FC1, FC2, OUT = 0, 1, 2, 3


def columns(model, ff):
    return {"qkv": 0, "fc1": 3 * HW, "fc2": 3 * HW + ff, "out": 3 * HW + 2 * ff, "end": 3 * HW + 2 * ff + HW}


def project_norm(r0, half, hf, vec, n1, n2):
    rows = ds(r0, half)
    xc, r = norm_stats(hf[rows, :].astype(F32))
    xh = xc * r
    n1[rows, :] = (xh * vec[0:1, :] + vec[1:2, :]).astype(BF)
    n2[rows, :] = (xh * vec[3:4, :] + vec[4:5, :]).astype(BF)


def project_qkv(r0, half, wqkv, vec, tab, n1, q, k, v):
    rows = ds(r0, half)
    a = n1[rows, :]
    for part, dst in enumerate((q, k, v)):
        cols = slice(part * HW, (part + 1) * HW)
        y = dot(a, wqkv[:, cols]) + vec[6:7, cols]
        if part < 2:
            y = turn_lanes(y, tab[rows, :], 1)
        if part == 0:
            y = y * 0.125
        dst[rows, :] = y.astype(BF)


def project_fc1(r0, half, wfc1, vec, n2, g, gp):
    rows = ds(r0, half)
    a = n2[rows, :]
    for b in range(wfc1.shape[1] // 256):
        cols = slice(b * 256, (b + 1) * 256)
        y = dot(a, wfc1[:, cols]) + vec[7:8, cols]
        cdf = 0.5 + 0.5 * lax.erf(y * 0.7071067811865476)
        g[rows, cols] = (y * cdf).astype(BF)
        gp[rows, cols] = (cdf + y * jnp.exp(-0.5 * y * y) * 0.3989422804014327).astype(BF)


def branch_out(r0, half, o, g, wout, wfc2, part):
    rows = ds(r0, half)
    for b in range(part.shape[1] // 256):
        cols = slice(b * 256, (b + 1) * 256)
        y = dg(o[rows, :], wout[cols, :], 1, 1) + dg(g[rows, :], wfc2[cols, :], 1, 1)
        part[rows, cols] = y.astype(BF)


def back_head(r0, half, dyf, hf, g, gp, n2, o, wfc1, wfc2, wout, vec, do, e2, da, acc, vg):
    rows = ds(r0, half)
    model, ff = wfc1.shape
    dy = dyf[rows, :]
    for b in range(ff // 256):
        cols = slice(b * 256, (b + 1) * 256)
        y = dot(dy, wfc2[:, cols]) * gp[rows, cols].astype(F32)
        low = y.astype(BF)
        da[:, cols] = low
        vg[7:8, cols] += jnp.sum(low.astype(F32), axis=0, keepdims=True)
    do[rows, :] = dot(dy, wout[...]).astype(BF)
    xc, r = norm_stats(hf[rows, :].astype(F32))
    xh = xc * r
    for b in range(model // 256):
        cols = slice(b * 256, (b + 1) * 256)
        dn = dg(da[...], wfc1[cols, :], 1, 1)
        vg[3:4, cols] += jnp.sum(dn * xh[:, cols], axis=0, keepdims=True)
        vg[4:5, cols] += jnp.sum(dn, axis=0, keepdims=True)
        e2[rows, cols] = (dn * vec[3:4, cols]).astype(BF)
    n2t = n2[rows, :].T
    dyt = dy.T
    for b in range(ff // 256):
        cols = slice(b * 256, (b + 1) * 256)
        acc[:, cols] += dot(n2t, da[:, cols])
        acc[:, ff + b * 256 : ff + (b + 1) * 256] += dot(dyt, g[rows, cols])
    acc[:, 2 * ff :] += dot(dyt, o[rows, :])


def back_tail(r0, half, dmix, hf, e2, wqkv, vec, part, vg):
    rows = ds(r0, half)
    dm = dmix[rows, :]
    vg[6:7, :] += jnp.sum(dm.astype(F32), axis=0, keepdims=True)
    xc, r = norm_stats(hf[rows, :].astype(F32))
    xh = xc * r
    for b in range(part.shape[1] // 256):
        cols = slice(b * 256, (b + 1) * 256)
        dn = dg(dm, wqkv[cols, :], 1, 1)
        vg[0:1, cols] += jnp.sum(dn * xh[:, cols], axis=0, keepdims=True)
        vg[1:2, cols] += jnp.sum(dn, axis=0, keepdims=True)
        part[rows, cols] = (dn * vec[0:1, cols] + e2[rows, cols].astype(F32)).astype(BF)


def qkv_grad(n1, dmix, acc, half):
    acc[...] = jnp.zeros_like(acc)

    def body(i, _):
        rows = ds(i * half, half)
        n1t = n1[rows, :].T
        for b in range(3):
            cols = slice(b * HW, (b + 1) * HW)
            acc[:, cols] += dot(n1t, dmix[rows, cols])
        return 0

    lax.fori_loop(0, n1.shape[0] // half, body, 0)


def store_low(acc, out):
    def body(i, _):
        rr = ds(i * SUB, SUB)
        out[rr, :] = acc[rr, :].astype(BF)
        return 0

    lax.fori_loop(0, acc.shape[0] // SUB, body, 0)


def residual_out(sc, own, vec, write, after=None):
    for a in range(2):
        sc.arrive(a)

        def body(i, _, a=a):
            base = own[ds(sc.own(sc.side(a)) + i * SUB, SUB), :].astype(F32)
            write(a, i, (base + sc.total(a, i) + vec[2:3, :] + vec[5:6, :]).astype(BF))
            return 0

        lax.fori_loop(0, sc.half // SUB, body, 0)
        if after is not None:
            after(a)


def grad_out(sc, dy, hf, vec, write, after=None):
    for a in range(2):
        sc.arrive(a)

        def body(i, _, a=a):
            rr = ds(sc.own(sc.side(a)) + i * SUB, SUB)
            xc, r = norm_stats(hf[rr, :].astype(F32))
            xh = xc * r
            e = sc.total(a, i)
            m1 = jnp.mean(e, axis=-1, keepdims=True)
            m2 = jnp.mean(e * xh, axis=-1, keepdims=True)
            write(a, i, (dy(a, i).astype(F32) + r * (e - m1 - xh * m2)).astype(BF))
            return 0

        lax.fori_loop(0, sc.half // SUB, body, 0)
        if after is not None:
            after(a)


def column_sum(tok, ref, vg, row):
    total = jnp.zeros((1, ref.shape[1]), F32)
    for a in range(2):

        def body(i, acc, a=a):
            return acc + jnp.sum(ref[ds(tok.own(a) + i * SUB, SUB), :].astype(F32), axis=0, keepdims=True)

        total = lax.fori_loop(0, tok.half // SUB, body, total)
    vg[row : row + 1, :] = total


def load(pairs, sem):
    copies = [pltpu.make_async_copy(a, b, sem.at[i]) for i, (a, b) in enumerate(pairs)]
    for c in copies:
        c.start()
    return copies


def params(cid):
    return pltpu.CompilerParams(collective_id=cid, has_side_effects=True, vmem_limit_bytes=67043328)


def cost(us):
    return pl.CostEstimate(flops=int(us * 8e8), bytes_accessed=0, transcendentals=0)


class OwnedOut:
    def __init__(self, me, src, dst, core, ss, rs, local):
        self.me, self.src, self.dst, self.core, self.ss, self.rs, self.local = me, src, dst, core, ss, rs, local

    def place(self):
        return self.dst.at[self.me.y, self.me.s]

    def far(self):
        me = self.me
        return push(self.src.at[1 - me.y], self.place(), self.ss.at[0], self.rs.at[me.s], me.across_core(self.core))

    def mate(self):
        return push(self.src.at[self.me.y], self.place(), self.ss.at[1], self.rs.at[2], self.me.mate)

    def here(self):
        return pltpu.make_async_copy(self.src.at[self.me.y], self.place(), self.local)

    def start_here(self):
        @pl.when(self.me.s == self.core)
        def _():
            self.here().start()

        @pl.when(self.me.s != self.core)
        def _():
            self.mate().start()

    def wait(self):
        me = self.me
        self.far().wait_send()

        @pl.when(me.s == self.core)
        def _():
            self.here().wait()
            self.mate().wait_recv()
            for n in range(2):
                place = self.dst.at[1 - me.y, n]
                push(self.src.at[0], place, self.ss.at[0], self.rs.at[n], me.across_core(self.core)).wait_recv()

        @pl.when(me.s != self.core)
        def _():
            self.mate().wait_send()


class Stores:
    def __init__(self, pairs, half, sem):
        self.pairs, self.half, self.sem = pairs, half, sem

    def copy(self, n, r0, i):
        src, dst = self.pairs[n]
        rows = ds(r0, self.half)
        return pltpu.make_async_copy(src.at[rows], dst.at[rows], self.sem.at[n, i])

    def start(self, which, r0, i):
        for n in which:
            self.copy(n, r0, i).start()

    def finish(self):
        def body(i, _):
            for n in range(len(self.pairs)):
                self.copy(n, i * self.half, i).wait()
            return 0

        lax.fori_loop(0, 8, body, 0)


def in_kernel(
    cfg, in_ref, cot_ref, seg_ref, live, w_ref, sv_ref, fr_ref,
    hf_o, n1_o, n2_o, g_o, gp_o, tab_o, w_o, q_o, k_o, v_o, cf_o, vecs, srow, kcol,
    hf, n1, n2, g, gp, tab, q, k, v, wfull, gat, vb, cot, gss, grs, css, crs, yss, yrs, lsem, ssem, vss, vrs, *wsems,
):
    col, dp, tensor = cfg["col"], cfg["dp"], cfg["tensor"]
    me = Mesh(dp, tensor)
    ga = Gather(me, hf, gss, grs, me.y)
    gc = Gather(me, cf_o, css, crs, me.y)
    half = ga.half
    part = ds(me.s * half, half)
    first = pltpu.make_async_copy(in_ref.at[me.y, 0, part], hf.at[ds(ga.own(me.y), half)], lsem.at[0])
    first.start()
    up = pltpu.make_async_copy(cot_ref.at[me.y, 0, part], cot, lsem.at[4])
    up.start()
    greet([me.mate, me.across_mate] + me.ring + me.group)
    over = push(in_ref.at[1 - me.y, 0, part], hf.at[ds(ga.own(me.y), half)], yss.at[0], yrs.at[0], me.across)
    wg = WeightGather(me, 0, w_ref, wfull, gat, cfg["groups"], wsems)
    vg = VectorGather(me, sv_ref, vb, vss, vrs, lsem.at[1])
    st = Stores([(hf, hf_o), (n1, n1_o), (n2, n2_o), (g, g_o), (gp, gp_o), (q, q_o), (k, k_o), (v, v_o)], half, ssem)
    vg.send(0)
    wg.send_ring()
    first.wait()
    document_tables(seg_ref[me.y], live[0, me.y], fr_ref, tab, srow, kcol)
    vg.wait(0)
    vg.send(1)
    ga.start(0)
    over.start()
    wg.send_own(0)
    tab_out = pltpu.make_async_copy(tab, tab_o, lsem.at[2])
    tab_out.start()
    vg.wait(1)
    vg.send(2)
    up.wait()
    cot_out = pltpu.make_async_copy(cot, cf_o.at[ds(gc.own(me.y), half)], lsem.at[5])
    cot_out.start()
    vg.wait(2)
    vg.build(vecs, cfg["heads"], cfg["own"], cfg["qw"], cfg["fw"])
    vec = vecs.at[0]

    def norm(r0, i):
        project_norm(r0, half, hf, vec, n1, n2)
        st.start((0, 1, 2), r0, i)

        @pl.when(i == 0)
        def _():
            over.wait_recv()
            ga.start(1)

        @pl.when(i == 1)
        def _():
            wg.forward(0)
            wg.send_own(1)

    ga.run(norm)
    cot_out.wait()
    gc.plan(0).start()
    gc.plan(2).start()
    wg.ready(0)

    def qkv(i, _):
        r0 = ga.order(i)
        project_qkv(r0, half, wfull.at[:, 0 : col["fc1"]], vec, tab, n1, q, k, v)
        st.start((5, 6, 7), r0, i)
        return 0

    lax.fori_loop(0, 8, qkv, 0)
    wg.forward(1)
    wg.send_own(2)
    wg.send_own(3)
    wg.ready(1)
    wg.forward(2)

    def fc1(i, _):
        r0 = ga.order(i)
        project_fc1(r0, half, wfull.at[:, col["fc1"] : col["fc2"]], vec, n2, g, gp)
        st.start((3, 4), r0, i)

        @pl.when(i == 5)
        def _():
            wg.forward(3)

        return 0

    lax.fori_loop(0, 8, fc1, 0)
    gc.step(2)
    gc.step(4)
    gc.step(5)
    st.finish()
    tab_out.wait()
    wg.ready(2)
    wg.ready(3)
    w_out = pltpu.make_async_copy(wfull, w_o, lsem.at[3])
    w_out.start()
    wg.finish()
    vg.finish()
    for n in (0, 2, 4):
        gc.plan(n).wait_send()
    over.wait_send()
    w_out.wait()


def layer_in(cfg, inputs, cotangent, segments, live, w, sv, fr):
    seq, model, ff = segments.shape[2], inputs.shape[3], cfg["ff"]
    dp, tensor = cfg["dp"], cfg["tensor"]
    rows, hidden = sds((seq, model), BF), sds((seq, ff), BF)
    heads = sds((seq, HW), BF)
    nv = dp - 1 + tensor
    wide, wide_h, wide_q = pltpu.VMEM((seq, model), BF), pltpu.VMEM((seq, ff), BF), pltpu.VMEM((seq, HW), BF)
    weights = pltpu.VMEM((model, w.shape[1]), BF)
    return pl.pallas_call(
        functools.partial(in_kernel, cfg),
        out_shape=(rows, rows, rows, hidden, hidden, sds((seq, 256), F32), sds((model, w.shape[1]), BF),
                   heads, heads, heads, rows,
                   sds((2, 8, model), F32), sds((8, seq), jnp.int32), sds((seq, 128), jnp.int32)),
        in_specs=[ANY, ANY, VMEM, SMEM, VMEM, VMEM, VMEM],
        out_specs=(ANY,) * 11 + (VMEM,) * 3,
        scratch_shapes=[
            wide, wide, wide, wide_h, wide_h, pltpu.VMEM((seq, 256), F32), wide_q, wide_q, wide_q,
            weights, weights, pltpu.VMEM((2, tensor, dp) + sv.shape, F32),
            pltpu.VMEM((seq // 8, model), BF),
            DMA((6,)), DMA((6,)), DMA((6,)), DMA((6,)), DMA((1,)), DMA((1,)), DMA((6,)), DMA((8, 8)),
            DMA((nv,)), DMA((nv,)),
        ]
        + WeightGather.scratch(dp, 4),
        compiler_params=params(2),
        cost_estimate=cost(45),
        name="layer_in",
    )(inputs, cotangent, segments, live, w, sv, fr)


def mid_kernel(
    cfg, q_in, k_in, v_in, srow, kcol, g_in, x_in, cot_ref, w_ref, w0, vecs, tab_in,
    o_o, lse, hf_o, n1_o, n2_o, g_o, gp_o, w_o, q_o, k_o, v_o, cy,
    wout, wfc2, hf, n1, n2, g, gp, tab, wfull, gat, q, k, v, o, vt, s_scr,
    part, mr, xr, sss, srs, gss, grs, lsem, ssem, osem, yss, yrs, *wsems,
):
    col, heads = cfg["col"], cfg["heads"]
    me = Mesh(cfg["dp"], cfg["tensor"])
    sc = Scatter(me, part, mr, xr, sss, srs)
    ga = Gather(me, hf, gss, grs)
    half = sc.half
    loads = load(
        [
            (v_in, v),
            (q_in, q),
            (k_in, k),
            (w0.at[:, col["out"] : col["end"]], wout),
            (w0.at[:, col["fc2"] : col["out"]], wfc2),
            (g_in, g),
            (tab_in, tab),
        ]
        + [(x_in.at[ds(sc.own(a), half)], hf.at[ds(sc.own(a), half)]) for a in range(2)],
        lsem,
    )
    greet([me.mate, me.beside, me.across, me.across_mate] + me.ring)
    wg = WeightGather(me, 1, w_ref, wfull, gat, cfg["groups"], wsems)
    over = push(cot_ref.at[1 - me.y, 0, ds(me.s * half, half)], cy, yss.at[0], yrs.at[0], me.across)
    wg.send_ring()
    for n in range(4):
        wg.send_own(n)
    loads[0].wait()
    turn_blocks(v, vt)
    for c in loads[1:]:
        c.wait()
    st = Stores([(hf, hf_o), (n1, n1_o), (n2, n2_o), (g, g_o), (gp, gp_o), (q, q_o), (k, k_o), (v, v_o)], half, ssem)
    st_o = Stores([(o, o_o)], half, osem)

    def out(r0, i):
        b = r0 // QB
        attn_fwd_block(b, jnp.maximum(b - DOC_MAX // QB, 0), b, heads, q, k, vt, srow, kcol, s_scr, o, lse)
        st_o.start((0,), r0, i)
        branch_out(r0, half, o, g, wout, wfc2, part)

        @pl.when(i == 6)
        def _():
            wg.forward(0)

    sc.run(out)

    def write(a, i, value):
        hf[ds(sc.own(a) + i * SUB, SUB), :] = value

    residual_out(sc, hf, vecs.at[0], write, ga.start)
    wg.forward(1)
    vec = vecs.at[1]

    def fc1(i):
        r0 = ga.order(i)
        project_fc1(r0, half, wfull.at[:, col["fc1"] : col["fc2"]], vec, n2, g, gp)
        st.start((3, 4), r0, i)

    def work(r0, i):
        project_norm(r0, half, hf, vec, n1, n2)

        @pl.when(i == 0)
        def _():
            wg.ready(0)

        project_qkv(r0, half, wfull.at[:, 0 : col["fc1"]], vec, tab, n1, q, k, v)
        st.start((0, 1, 2, 5, 6, 7), r0, i)

        @pl.when(i == 4)
        def _():
            wg.ready(1)

        @pl.when(i >= 4)
        def _():
            fc1(i - 4)

        @pl.when(i == 5)
        def _():
            wg.forward(2)

        @pl.when(i == 7)
        def _():
            wg.forward(3)
            over.start()

    ga.run(work)

    def late(i, _):
        fc1(i)
        return 0

    lax.fori_loop(4, 8, late, 0)
    st.finish()
    wg.ready(2)
    wg.ready(3)
    w_out = pltpu.make_async_copy(wfull, w_o, lsem.at[0])
    w_out.start()
    sc.finish()
    wg.finish()
    st_o.finish()
    over.wait()
    w_out.wait()


def layer_mid(cfg, q, k, v, srow, kcol, g, xf, cotangent, w, w0, vecs, tab):
    seq, model, ff = tab.shape[0], xf.shape[1], cfg["ff"]
    rows, hidden, heads = sds((seq, model), BF), sds((seq, ff), BF), sds((seq, HW), BF)
    wide, wide_h, wide_q = pltpu.VMEM((seq, model), BF), pltpu.VMEM((seq, ff), BF), pltpu.VMEM((seq, HW), BF)
    return pl.pallas_call(
        functools.partial(mid_kernel, cfg),
        out_shape=(heads, sds((8, seq), F32), rows, rows, rows, hidden, hidden, sds(w0.shape, BF), heads, heads, heads,
                   sds((seq // 8, model), BF)),
        in_specs=[ANY, ANY, ANY, VMEM, VMEM, ANY, ANY, ANY, VMEM, ANY, VMEM, ANY],
        out_specs=(ANY, VMEM) + (ANY,) * 10,
        scratch_shapes=[
            pltpu.VMEM((model, HW), BF), pltpu.VMEM((model, ff), BF),
            wide, wide, wide, wide_h, wide_h, pltpu.VMEM((seq, 256), F32),
            pltpu.VMEM(w0.shape, BF), pltpu.VMEM(w0.shape, BF),
            wide_q, wide_q, wide_q, wide_q, pltpu.VMEM((HW, seq), BF),
            pltpu.VMEM((cfg["heads"], DOC_MAX + QB, QB), F32),
        ]
        + scatter_scratch(seq, model)
        + [DMA((6,)), DMA((6,)), DMA((9,)), DMA((8, 8)), DMA((1, 8)), DMA((1,)), DMA((1,))]
        + WeightGather.scratch(cfg["dp"], 4),
        compiler_params=params(3),
        cost_estimate=cost(70),
        name="layer_mid",
    )(q, k, v, srow, kcol, g, xf, cotangent, w, w0, vecs, tab)


def turn_kernel(
    cfg, o_in, g_in, hf_in, cf, cy, w1, vecs, n2_in, gp_in, y_o, do_o, e2_o, gr_o, hx, vg,
    o, g, hf, dyf, n2, gp, e2, do, y, gr, wout, wfc2, wfc1, da, acc,
    part, mr, xr, sss, srs, gss, grs, yss, yrs, lsem, ssem,
):
    col = cfg["col"]
    me = Mesh(cfg["dp"], cfg["tensor"])
    sc = Scatter(me, part, mr, xr, sss, srs)
    half = sc.half
    gt = Gather(me, dyf, gss, grs, me.y)
    near = ds(4 * me.y * half, 4 * half)
    loads = load(
        [
            (cy, dyf.at[ds(gt.own(1 - me.y), half)]),
            (w1.at[:, col["out"] : col["end"]], wout),
            (w1.at[:, col["fc2"] : col["out"]], wfc2),
            (o_in, o),
            (g_in, g),
            (w1.at[:, col["fc1"] : col["fc2"]], wfc1),
            (cf.at[near], dyf.at[near]),
            (gp_in, gp),
            (hf_in, hf),
            (n2_in, n2),
        ],
        lsem,
    )
    greet([me.mate, me.beside, me.across])
    loads[0].wait()
    gt.start(1)
    h_over = push(hf_in.at[ds(me.py * 2 * half, 2 * half)], hx, yss.at[0], yrs.at[0], me.across)

    @pl.when(me.s == 0)
    def _():
        h_over.start()

    for c in loads[1:5]:
        c.wait()
    vec = vecs.at[1]
    st = Stores([(e2, e2_o), (do, do_o)], half, ssem)

    def early():
        vg[...] = jnp.zeros_like(vg)
        acc[...] = jnp.zeros_like(acc)
        for c in loads[5:]:
            c.wait()

        def head(i, _):
            for n, step in ((5, 3), (6, 6), (7, 7)):

                @pl.when(i == n)
                def _(step=step):
                    gt.step(step)

            far_b = jnp.where(i < 6, me.x, 1 - me.x)
            far_h = jnp.where(i % 2 == 0, me.s, 1 - me.s)
            r0 = jnp.where(i < 4, (4 * me.y + i) * half, gt.start_of(1 - me.y, far_b, far_h))
            back_head(r0, half, dyf, hf, g, gp, n2, o, wfc1, wfc2, wout, vec, do, e2, da, acc, vg)
            st.start((0, 1), r0, i)
            return 0

        lax.fori_loop(0, 8, head, 0)

    sc.run(lambda r0, i: branch_out(r0, half, o, g, wout, wfc2, part), early)
    column_sum(sc, dyf, vg, 2)
    store_low(acc, gr)
    gr_out = pltpu.make_async_copy(gr, gr_o, lsem.at[0])
    gr_out.start()

    def write(a, i, value):
        y[a, ds(i * SUB, SUB), :] = value

    residual_out(sc, hf, vec, write)
    y_out = pltpu.make_async_copy(y, y_o, lsem.at[1])
    y_out.start()
    sc.finish()
    st.finish()
    for n in (1, 3, 5):
        gt.plan(n).wait_send()

    @pl.when(me.s == 0)
    def _():
        h_over.wait()

    gr_out.wait()
    y_out.wait()


def layer_turn(cfg, o, g, hf, cf, cy, w1, vecs, n2, gp):
    seq, model = hf.shape
    ff = cfg["ff"]
    wide, hidden, heads = pltpu.VMEM((seq, model), BF), pltpu.VMEM((seq, ff), BF), pltpu.VMEM((seq, HW), BF)
    owned = (2, seq // 8, model)
    return pl.pallas_call(
        functools.partial(turn_kernel, cfg),
        out_shape=(
            sds(owned, BF),
            sds((seq, HW), BF),
            sds((seq, model), BF),
            sds((model, 2 * ff + HW), BF),
            sds((seq // 4, model), BF),
            sds((8, model), F32),
        ),
        in_specs=[ANY] * 6 + [VMEM, ANY, ANY],
        out_specs=(ANY,) * 5 + (VMEM,),
        scratch_shapes=[
            heads, hidden, wide, wide, wide, hidden, wide, heads, pltpu.VMEM(owned, BF),
            pltpu.VMEM((model, 2 * ff + HW), BF),
            pltpu.VMEM((model, HW), BF), pltpu.VMEM((model, ff), BF), pltpu.VMEM((model, ff), BF),
            pltpu.VMEM((seq // 8, ff), BF), pltpu.VMEM((model, 2 * ff + HW), F32),
        ]
        + scatter_scratch(seq, model)
        + [DMA((6,)), DMA((6,)), DMA((1,)), DMA((1,)), DMA((10,)), DMA((2, 8))],
        compiler_params=params(4),
        cost_estimate=cost(40),
        name="layer_turn",
    )(o, g, hf, cf, cy, w1, vecs, n2, gp)


def back_kernel(
    cfg, dm_in, e2_in, cf, cy, hf_in, n1_in, w1, w0, vecs, xf_in, g_in, gp_in, n2_in, o_in, gr1, y_in,
    dh_o, e2_o, do_o, vgf, vgd, out1_o, outq_o, gr_o, yx,
    dmix, o, do, a, b, e2, g, gp, wqkv, wout, wfc2, wfc1, dhf, da, acc, gq, gr, got, gotq, acrq,
    sb, rb, sbq, rbq, out1, outq, part, mr, xr, sss, srs, gss, grs, lsem, ssem, oss, ors, osem, *rsems,
):
    col, dp = cfg["col"], cfg["dp"]
    me = Mesh(dp, cfg["tensor"])
    ga = Gather(me, dhf, gss, grs)
    sc = Scatter(me, part, mr, xr, sss, srs)
    half = sc.half
    loads = load(
        [
            (w1.at[:, col["qkv"] : col["fc1"]], wqkv),
            (dm_in, dmix),
            (hf_in, a),
            (e2_in, e2),
            (n1_in, b),
            (w0.at[:, col["out"] : col["end"]], wout),
            (w0.at[:, col["fc2"] : col["out"]], wfc2),
            (w0.at[:, col["fc1"] : col["fc2"]], wfc1),
            (g_in, g),
            (gp_in, gp),
            (o_in, o),
        ]
        + [(cf.at[ds(sc.own(me.y), half)], dhf.at[ds(sc.own(me.y), half)]), (cy, dhf.at[ds(sc.own(1 - me.y), half)])],
        lsem,
    )
    gr_load = pltpu.make_async_copy(gr1, gr, lsem.at[13])
    holds = (me.s == 1) & (me.y == 1)

    @pl.when(holds)
    def _():
        gr_load.start()

    greet([me.mate, me.beside, me.across, me.across_mate] + me.ring)
    red1 = GradReduce(me, 1, gr1, gr, gr, got, sb, rb, out1, rsems[:6])
    redq = GradReduce(me, 1, gq, gq, gotq, acrq, sbq, rbq, outq, rsems[6:])
    st = Stores([(e2, e2_o), (do, do_o), (dhf, dh_o)], half, ssem)
    ys = OwnedOut(me, y_in, yx, 1, oss, ors, osem.at[0])
    red1.send()
    vgf[...] = jnp.zeros_like(vgf)
    vgd[...] = jnp.zeros_like(vgd)
    for c in loads[:4]:
        c.wait()

    def early():
        loads[4].wait()
        small = acc.at[:, 0 : 3 * HW]
        qkv_grad(b, dmix, small, half)
        store_low(small, gq)
        redq.send()
        ys.far().start()
        ys.start_here()

        @pl.when(holds)
        def _():
            gr_load.wait()

        red1.step(0)

    sc.run(lambda r0, i: back_tail(r0, half, dmix, a, e2, wqkv, vecs.at[1], part, vgf), early)
    acc[...] = jnp.zeros_like(acc)
    again = pltpu.make_async_copy(n2_in, b, lsem.at[14])
    again.start()
    for c in loads[5:]:
        c.wait()
    for d in range(1, dp // 2):
        red1.step(d)

    def write(n, i, value):
        dhf[ds(sc.own(n) + i * SUB, SUB), :] = value

    grad_out(sc, lambda n, i: dhf[ds(sc.own(n) + i * SUB, SUB), :], a, vecs.at[1], write, ga.start)
    other = pltpu.make_async_copy(xf_in, a, lsem.at[15])
    other.start()
    again.wait()
    other.wait()

    def work(r0, i):
        back_head(r0, half, dhf, a, g, gp, b, o, wfc1, wfc2, wout, vecs.at[0], do, e2, da, acc, vgd)
        st.start((0, 1, 2), r0, i)

        @pl.when(i == 1)
        def _():
            for d in range(dp // 2, dp - 1):
                red1.step(d)

        @pl.when(i == 3)
        def _():
            red1.step(dp - 1)

        @pl.when(i == 5)
        def _():
            redq.step(0)

    ga.run(work)
    for d in range(1, dp):
        redq.step(d)
    store_low(acc, gr)
    gr_out = pltpu.make_async_copy(gr, gr_o, lsem.at[0])
    gr_out.start()
    column_sum(sc, dhf, vgd, 2)
    red1.collect()
    redq.collect()
    outs = [pltpu.make_async_copy(out1, out1_o, lsem.at[1]), pltpu.make_async_copy(outq, outq_o, lsem.at[2])]
    for c in outs:
        c.start()
    red1.finish()
    redq.finish()
    sc.finish()
    st.finish()
    gr_out.wait()
    ys.wait()
    for c in outs:
        c.wait()


def layer_back(cfg, dmix, e2, cf, cy, hf, n1, w1, w0, vecs, xf, g, gp, n2, o, gr1, y):
    seq, model = hf.shape
    ff, dp = cfg["ff"], cfg["dp"]
    rows, nr, nq = model // dp, 2 * ff + HW, 3 * HW
    wide, hidden, heads = pltpu.VMEM((seq, model), BF), pltpu.VMEM((seq, ff), BF), pltpu.VMEM((seq, HW), BF)
    return pl.pallas_call(
        functools.partial(back_kernel, cfg),
        out_shape=(
            sds((seq, model), BF),
            sds((seq, model), BF),
            sds((seq, HW), BF),
            sds((8, model), F32),
            sds((8, model), F32),
            sds((rows, nr), F32),
            sds((rows, nq), F32),
            sds((model, nr), BF),
            sds((2,) + y.shape, BF),
        ),
        in_specs=[ANY] * 8 + [VMEM] + [ANY] * 7,
        out_specs=(ANY, ANY, ANY, VMEM, VMEM, ANY, ANY, ANY, ANY),
        scratch_shapes=[
            pltpu.VMEM((seq, nq), BF), heads, heads, wide, wide, wide, hidden, hidden,
            pltpu.VMEM((model, nq), BF), pltpu.VMEM((model, HW), BF), pltpu.VMEM((model, ff), BF),
            pltpu.VMEM((model, ff), BF), wide, pltpu.VMEM((seq // 8, ff), BF), pltpu.VMEM((model, nr), F32),
            pltpu.VMEM((model, nq), BF), pltpu.VMEM((model, nr), BF), pltpu.VMEM((model, nr), BF),
            pltpu.VMEM((model, nq), BF), pltpu.VMEM((model, nq), BF),
            pltpu.VMEM((dp - 1, rows, nr), BF), pltpu.VMEM((dp - 1, rows, nr), BF),
            pltpu.VMEM((dp - 1, rows, nq), BF), pltpu.VMEM((dp - 1, rows, nq), BF),
            pltpu.VMEM((rows, nr), F32), pltpu.VMEM((rows, nq), F32),
        ]
        + scatter_scratch(seq, model)
        + [DMA((6,)), DMA((6,)), DMA((16,)), DMA((3, 8)), DMA((2,)), DMA((3,)), DMA((1,))]
        + GradReduce.scratch(dp) * 2,
        compiler_params=params(5),
        cost_estimate=cost(70),
        name="layer_back",
    )(dmix, e2, cf, cy, hf, n1, w1, w0, vecs, xf, g, gp, n2, o, gr1, y)


def last_kernel(
    cfg, q_in, k_in, v_in, o_in, do_in, lse, srow, kcol, tab_in, e2_in, dh_in, xf_in, n1_in, w0, vecs, vf1, vd1, vd0,
    gr0, out1, outq, dhx, dxx, fq_o, fr_o, vec_o,
    q, k, v, o, do, tab, kt, dk, dv, dmix, dh, dx, xf, n1, e2, wqkv, gq, gotq, acrq, sbq, rbq, gr, got, sb, rb, fq, fr,
    vgf, va, vr, vout, part, mr, xr, sss, srs, lsem, vss, vrs, oss, ors, *rsems,
):
    col, heads, dp = cfg["col"], cfg["heads"], cfg["dp"]
    me = Mesh(dp, cfg["tensor"])
    sc = Scatter(me, part, mr, xr, sss, srs, 1 - me.y)
    half = sc.half
    seq = xf.shape[0]
    width = q.shape[1]
    own = [ds(sc.own(n), half) for n in range(2)]
    loads = load(
        [
            (k_in, k),
            (q_in, q),
            (v_in, v),
            (do_in, do),
            (o_in, o),
            (tab_in, tab),
            (w0.at[:, col["qkv"] : col["fc1"]], wqkv),
            (xf_in, xf),
            (e2_in, e2),
            (n1_in, n1),
        ]
        + [(dh_in.at[rr], dh.at[n]) for n, rr in enumerate(own)],
        lsem,
    )
    gr_load = pltpu.make_async_copy(gr0, gr, lsem.at[12])
    holds = (me.s == 0) & (me.y == 0)

    @pl.when(holds)
    def _():
        gr_load.start()

    greet([me.mate, me.beside, me.beside_mate, me.across, me.across_mate] + me.ring)
    redr = GradReduce(me, 0, gr0, gr, gr, got, sb, rb, fr, rsems[:6])
    redq = GradReduce(me, 0, gq, gq, gotq, acrq, sbq, rbq, fq, rsems[6:])
    vr_ = VectorReduce(me, va, vr, vss, vrs)
    redr.send()

    dh_over = push(dh_in.at[ds(me.py * 2 * half, 2 * half)], dhx, oss.at[2], ors.at[3], me.across)

    xs = OwnedOut(me, dx, dxx, 0, oss, ors, lsem.at[14])
    old = [pltpu.make_async_copy(out1, fr, lsem.at[15]), pltpu.make_async_copy(outq, fq, lsem.at[16])]

    @pl.when(me.s == 1)
    def _():
        for c in old:
            c.start()

    vgf[...] = jnp.zeros_like(vgf)
    dk[...] = jnp.zeros_like(dk)
    dv[...] = jnp.zeros_like(dv)
    loads[0].wait()
    turn_blocks(k, kt)
    for c in loads[1:6]:
        c.wait()

    @pl.when(holds)
    def _():
        gr_load.wait()

    n_blocks = seq // QB

    def qloop(i, _):
        lo = jnp.maximum(i - DOC_MAX // QB, 0)

        @pl.when((i == n_blocks // 2 + 1) & (me.s == 1))
        def _():
            dh_over.start()

        attn_bwd_block(i, lo, i, heads, q, k, v, o, do, kt, lse, srow, kcol, tab, dk, dv, dmix)
        for at_block, steps in (
            (n_blocks // 2 - 1, range(0, 1)),
            (n_blocks // 2, range(1, dp // 2)),
            (n_blocks // 2 + 1, range(dp // 2, dp - 1)),
            (n_blocks - 2, range(dp - 1, dp)),
        ):

            @pl.when(i == at_block)
            def _(steps=steps):
                for d in steps:
                    redr.step(d)

        return 0

    lax.fori_loop(0, n_blocks, qloop, 0)

    def close(i, _):
        ii = ds(i * QB, QB)
        dmix[ii, width : 2 * width] = turn_lanes(dk[ii, :], tab[ii, :], -1).astype(BF)
        dmix[ii, 2 * width : 3 * width] = dv[ii, :].astype(BF)
        return 0

    lax.fori_loop(0, n_blocks, close, 0)
    for c in loads[6:]:
        c.wait()

    def early():
        va[0, 0:8, :] = vgf[...] + vd0[...]
        va[0, 8:16, :] = vf1[...] + vd1[...]
        vr_.send(0)
        nf = gq.shape[0]
        accs = [dk.at[0:nf], dk.at[nf : 2 * nf], dv.at[0:nf]]
        for acc in accs:
            acc[...] = jnp.zeros_like(acc)

        def body(i, _):
            rows = ds(i * half, half)
            n1t = n1[rows, :].T
            for p, acc in enumerate(accs):
                acc[...] += dot(n1t, dmix[rows, p * HW : (p + 1) * HW])
            return 0

        lax.fori_loop(0, 8, body, 0)
        for p, acc in enumerate(accs):
            gq[:, p * HW : (p + 1) * HW] = acc[...].astype(BF)
        vr_.add(0, va.at[1])
        vr_.send(1)
        redq.send()
        vr_.add(1, va.at[2])
        vr_.send(2)
        redq.step(0)

    sc.run(lambda r0, i: back_tail(r0, half, dmix, xf, e2, wqkv, vecs.at[0], part, vgf), early)
    for d in range(1, dp - 1):
        redq.step(d)

    def write(n, i, value):
        dx[sc.side(n), ds(i * SUB, SUB), :] = value

    def leave(n):
        if n == 0:
            xs.far().start()
        else:
            xs.start_here()

    grad_out(sc, lambda n, i: dh[sc.side(n), ds(i * SUB, SUB), :], xf, vecs.at[0], write, leave)
    redq.step(dp - 1)
    vr_.add(2, vout)
    vec_o[...] = jnp.where(me.s == 0, vout[0:8, :], vout[8:16, :])
    redr.collect()
    redq.collect()

    @pl.when(me.s == 1)
    def _():
        for c in old:
            c.wait()

    ends = [pltpu.make_async_copy(fr, fr_o, lsem.at[0]), pltpu.make_async_copy(fq, fq_o, lsem.at[1])]
    for c in ends:
        c.start()
    redr.finish()
    redq.finish()
    vr_.finish()
    sc.finish()
    @pl.when(me.s == 1)
    def _():
        dh_over.wait()

    xs.wait()
    for c in ends:
        c.wait()


def layer_last(cfg, q, k, v, o, do, lse, sr, kc, tab, e2, dh, xf, n1, w0, vecs, vf1, vd1, vd0, gr0, out1, outq):
    seq, model = xf.shape
    dp, tensor, ff = cfg["dp"], cfg["tensor"], cfg["ff"]
    rows, nr, nq = model // dp, 2 * ff + HW, 3 * HW
    nv = dp + tensor - 1
    wide, owned, heads = pltpu.VMEM((seq, model), BF), pltpu.VMEM((2, seq // 8, model), BF), pltpu.VMEM((seq, HW), BF)
    return pl.pallas_call(
        functools.partial(last_kernel, cfg),
        out_shape=(sds((seq // 4, model), BF), sds((2, 2, seq // 8, model), BF), sds((rows, nq), F32), sds((rows, nr), F32), sds((8, model), F32)),
        in_specs=[ANY] * 5 + [VMEM] * 3 + [ANY] * 6 + [VMEM] * 4 + [ANY] * 3,
        out_specs=(ANY, ANY, ANY, ANY, VMEM),
        scratch_shapes=[
            heads, heads, heads, heads, heads, pltpu.VMEM(tab.shape, F32), pltpu.VMEM((HW, seq), BF),
            pltpu.VMEM((seq, HW), F32), pltpu.VMEM((seq, HW), F32), pltpu.VMEM((seq, nq), BF), owned, owned,
            wide, wide, wide, pltpu.VMEM((model, nq), BF),
            pltpu.VMEM((model, nq), BF), pltpu.VMEM((model, nq), BF), pltpu.VMEM((model, nq), BF),
            pltpu.VMEM((dp - 1, rows, nq), BF), pltpu.VMEM((dp - 1, rows, nq), BF),
            pltpu.VMEM((model, nr), BF), pltpu.VMEM((model, nr), BF),
            pltpu.VMEM((dp - 1, rows, nr), BF), pltpu.VMEM((dp - 1, rows, nr), BF),
            pltpu.VMEM((rows, nq), F32), pltpu.VMEM((rows, nr), F32),
            pltpu.VMEM((8, model), F32), pltpu.VMEM((3, 16, model), F32), pltpu.VMEM((nv, 16, model), F32),
            pltpu.VMEM((16, model), F32),
        ]
        + scatter_scratch(seq, model)
        + [DMA((17,)), DMA((nv,)), DMA((nv,)), DMA((3,)), DMA((4,))]
        + GradReduce.scratch(dp) * 2,
        compiler_params=params(6),
        cost_estimate=cost(80),
        name="layer_last",
    )(q, k, v, o, do, lse, sr, kc, tab, e2, dh, xf, n1, w0, vecs, vf1, vd1, vd0, gr0, out1, outq)


def finish_kernel(
    cfg, hf, hx, yx, dhf, dhx, dxx, fq_in, fr_in, vec, so, ig, bg1, bb1, gqkv, bqkv, gout, bdy, bdy2, bg2, bb2, gfc1, bfc1, gfc2,
    a, b, fq, fr, lsem, msem, osem,
):
    heads, ff, own, qw, fw = cfg["heads"], cfg["ff"], cfg["own"], cfg["qw"], cfg["fw"]
    me = Mesh(cfg["dp"], cfg["tensor"])
    loads = load([(fr_in, fr), (fq_in, fq)], lsem)
    half = a.shape[2]
    mine = [ref.at[pl.ds(pl.multiple_of((2 * me.t + n) * half, half), half)] for ref in (hf, dhf) for n in range(2)]

    def sources(core):
        if core == 0:
            first, second = [mine[0:2], [hx.at[pl.ds(n * half, half)] for n in range(2)]], None
        else:
            first, second = None, [mine[2:4], [dhx.at[pl.ds(n * half, half)] for n in range(2)]]
        whole = yx if core else dxx
        third = [[whole.at[me.y, n] for n in range(2)], [whole.at[1 - me.y, n] for n in range(2)]]
        return (first or third), (second or third)

    def moves(core):
        out = []
        for o, (ref, src) in enumerate(zip((a, b), sources(core))):
            for m in range(2):
                for n in range(2):
                    dst = ref.at[me.y if m == 0 else 1 - me.y, n]
                    out.append(pltpu.make_async_copy(src[m][n], dst, msem.at[4 * o + 2 * m + n]))
        return out

    for core in range(2):

        @pl.when(me.s == core)
        def _(core=core):
            for c in moves(core):
                c.start()

    model = vec.shape[1]
    short = pltpu.roll(vec[...], (model - (me.z * me.tensor + me.t) * own) % model, 1)
    for row, ref in ((0, bg1), (1, bb1), (2, bdy), (2, bdy2), (3, bg2), (4, bb2)):
        ref[...] = short[row : row + 1, 0:own]
    for h in range(heads):
        parts = [vec[6:7, p * HW + h * HD : p * HW + (h + 1) * HD] for p in range(3)]
        one = jnp.concatenate(parts + [jnp.zeros((1, HW - 3 * HD), F32)], axis=1)
        one = jnp.broadcast_to(one, (8, HW))
        bqkv[h] = pltpu.roll(one, (HW - me.z * qw) % HW, 1)[0:1, 0:qw]
        wide = ff // heads
        one = jnp.broadcast_to(vec[7:8, h * wide : (h + 1) * wide], (8, wide))
        bfc1[h] = pltpu.roll(one, (wide - me.z * fw) % wide, 1)[0:1, 0:fw]
    loads[0].wait()
    gfc1[0] = fr[:, 0:ff]
    gfc2[...] = fr[:, ff : 2 * ff]
    gout[0] = fr[:, 2 * ff : 2 * ff + HW].T[0 : heads * HD, :]
    for core in range(2):

        @pl.when(me.s == core)
        def _(core=core):
            for c in moves(core):
                c.wait()

    outs = []
    for o, (ref, dst) in enumerate(((a, so), (b, ig))):
        for m in range(2):
            for n in range(2):
                place = dst.at[0, m, 0, pl.ds(n * half, half)]
                outs.append(pltpu.make_async_copy(ref.at[m, n], place, osem.at[4 * o + 2 * m + n]))
    for c in outs:
        c.start()
    loads[1].wait()
    pieces = [fq[:, p * HW + h * HD : p * HW + (h + 1) * HD] for h in range(heads) for p in range(3)]
    gqkv[0] = jnp.concatenate(pieces, axis=1)
    for c in outs:
        c.wait()


def finish(cfg, hf, hx, yx, dhf, dhx, dxx, fq, fr, vec):
    heads, ff, rows = cfg["heads"], cfg["ff"], fq.shape[0]
    line = sds((1, cfg["own"]), F32)
    both = sds((1, 2, 1) + hx.shape, BF)
    return pl.pallas_call(
        functools.partial(finish_kernel, cfg),
        out_shape=(both, both, line, line, sds((1, rows, heads * 3 * HD), F32),
                   sds((heads, 1, cfg["qw"]), F32), sds((1, heads * HD, rows), F32), line, line, line, line,
                   sds((1, rows, ff), F32), sds((heads, 1, cfg["fw"]), F32), sds((rows, ff), F32)),
        in_specs=[ANY] * 8 + [VMEM],
        out_specs=(ANY, ANY) + (VMEM,) * 12,
        scratch_shapes=[
            pltpu.VMEM(yx.shape, BF), pltpu.VMEM(yx.shape, BF), pltpu.VMEM(fq.shape, F32), pltpu.VMEM(fr.shape, F32),
            DMA((2,)), DMA((8,)), DMA((8,)),
        ],
        compiler_params=pltpu.CompilerParams(vmem_limit_bytes=67043328),
        cost_estimate=cost(5),
        name="finish",
    )(hf, hx, yx, dhf, dhx, dxx, fq, fr, vec)


def by_part(w):
    rows = w.shape[0]
    heads = w.shape[1] // (3 * HD)
    w = w.reshape(rows, heads, 3, HD).transpose(0, 2, 1, 3).reshape(rows, 3, heads * HD)
    return jnp.pad(w, ((0, 0), (0, 0), (0, HW - heads * HD))).reshape(rows, 3 * HW)


def shards(
    dp, tensor, inputs, cotangent, segments, live_blocks, ln1_gain, ln1_bias, qkv_weight, qkv_bias,
    out_weight, out_bias, ln2_gain, ln2_bias, fc1_weight, fc1_bias, fc2_weight, fc2_bias,
):
    live_blocks = live_blocks.T
    model = inputs.shape[-1]
    ff = fc1_weight.shape[2]
    heads = qkv_bias.shape[1]
    col = columns(model, ff)
    wout = jnp.pad(out_weight[0].T, ((0, 0), (0, HW - heads * HD)))
    w = jnp.concatenate([by_part(qkv_weight[0]), fc1_weight[0], fc2_weight[0].T, wout], axis=1)
    small = jnp.stack([ln1_gain[0], ln1_bias[0], out_bias[0], ln2_gain[0], ln2_bias[0], fc2_bias[0]])

    def lanes(a):
        return jnp.pad(a.astype(F32), ((0, 0), (0, 128 - a.shape[1])))

    sv = jnp.concatenate([lanes(small), lanes(qkv_bias[0]), lanes(fc1_bias[0])], axis=0)
    sv = jnp.pad(sv, ((0, -sv.shape[0] % 8), (0, 0)))
    fr = np.float32(10000.0) ** (-(np.arange(ROT // 2, dtype=np.float32) * np.float32(2.0 / ROT)))
    fr = jnp.asarray(np.broadcast_to(fr[:, None], (ROT // 2, 128)).astype(np.float32))
    cfg = {
        "col": col, "ff": ff, "heads": heads, "dp": dp, "tensor": tensor, "own": small.shape[1],
        "qw": qkv_bias.shape[2], "fw": fc1_bias.shape[2],
        "groups": [(0, col["fc1"]), (col["fc1"], col["fc2"]), (col["fc2"], col["out"]), (col["out"], col["end"])],
    }

    xf, n1a, n2a, ga, gpa, tab, w0, qa, ka, va, cf, vecs, sr, kc = layer_in(
        cfg, inputs, cotangent, segments, live_blocks, w, sv, fr
    )
    oa, lsea, hf, n1b, n2b, gb, gpb, w1, qb, kb, vb, cy = layer_mid(
        cfg, qa, ka, va, sr, kc, ga, xf, cotangent, w, w0, vecs, tab
    )
    ob, lseb = attn_fwd(heads, segments, live_blocks, qb, kb, vb, sr, kc)
    y, dob, e2b, grb, hx, vdb = layer_turn(cfg, ob, gb, hf, cf, cy, w1, vecs, n2b, gpb)
    dmb = attn_bwd(heads, segments, live_blocks, qb, kb, vb, ob, dob, lseb, sr, kc, tab)
    dhf, e2a, doa, vfb, vda, out1, outq, gra, yx = layer_back(
        cfg, dmb, e2b, cf, cy, hf, n1b, w1, w0, vecs, xf, ga, gpa, n2a, oa, grb, y
    )
    dhx, dxx, fq, fr_, gv = layer_last(
        cfg, qa, ka, va, oa, doa, lsea, sr, kc, tab, e2a, dhf, xf, n1a, w0, vecs, vfb, vdb, vda, gra, out1, outq
    )
    last_part = finish(cfg, hf, hx, yx, dhf, dhx, dxx, fq, fr_, gv)
    so, ig, bg1, bb1, gqkv, bqkv, gout, bdy, bdy2, bg2, bb2, gfc1, bfc1, gfc2 = last_part
    bqkv, bfc1, gfc2 = bqkv.transpose(1, 0, 2), bfc1.transpose(1, 0, 2), gfc2.T[None]
    return (so, ig, bg1, bb1, gqkv, bqkv, gout, bdy, bg2, bb2, gfc1, bfc1, gfc2, bdy2)


def solution(mesh):
    both = ("dp", "tensor")
    in_specs = (
        P(None, "dp", "tensor", None),
        P(None, "dp", "tensor", None),
        P(None, "dp", None),
        P(None, "dp"),
        P("section", both),
        P("section", both),
        P("section", "dp", "tensor"),
        P("section", "tensor", "dp"),
        P("section", "tensor", "dp"),
        P("section", both),
        P("section", both),
        P("section", both),
        P("section", "dp", "tensor"),
        P("section", "tensor", "dp"),
        P("section", "tensor", "dp"),
        P("section", both),
    )
    out_specs = (
        P("section", None, "dp", "tensor", None),
        P("section", None, "dp", "tensor", None),
        P("section", both),
        P("section", both),
        P("section", "dp", "tensor"),
        P("section", "tensor", "dp"),
        P("section", "tensor", "dp"),
        P("section", both),
        P("section", both),
        P("section", both),
        P("section", "dp", "tensor"),
        P("section", "tensor", "dp"),
        P("section", "tensor", "dp"),
        P("section", both),
    )
    body = functools.partial(shards, mesh.shape["dp"], mesh.shape["tensor"])
    return jax.shard_map(body, mesh=mesh, in_specs=in_specs, out_specs=out_specs, check_vma=False)
```

```python
import functools

import jax
import jax.numpy as jnp
import numpy as np
from jax import lax
from jax.experimental import pallas as pl
from jax.experimental.pallas import tpu as pltpu
from jax.sharding import PartitionSpec as P

F32 = jnp.float32
BF = jnp.bfloat16
MESH = pl.DeviceIdType.MESH
HD = 64
ROT = 16
LIVE = 128
DOCS = 4
DOC_MAX = 1024
QB = 256
HW = 256
SUB = 256
EPS = 1e-05
NEG = -1e30
VMEM = pl.BlockSpec(memory_space=pltpu.VMEM)
ANY = pl.BlockSpec(memory_space=pltpu.HBM)
SMEM = pl.BlockSpec(memory_space=pltpu.SMEM)
DMA = pltpu.SemaphoreType.DMA


def sds(shape, dtype):
    return jax.ShapeDtypeStruct(shape, dtype)


def dg(a, b, ca, cb):
    return lax.dot_general(a, b, (((ca,), (cb,)), ((), ())), preferred_element_type=F32)


def dot(a, b):
    return jnp.dot(a, b, preferred_element_type=F32)


def ds(start, size):
    return pl.ds(pl.multiple_of(start, size), size)


def norm_stats(x):
    mu = jnp.mean(x, axis=-1, keepdims=True)
    xc = x - mu
    var = jnp.mean(xc * xc, axis=-1, keepdims=True)
    return xc, lax.rsqrt(var + EPS)


def head_lanes(width, heads):
    lane = lax.broadcasted_iota(jnp.int32, (1, width), 1)
    return [(lane >= h * HD) & (lane < (h + 1) * HD) for h in range(heads)]


def allow_mask(kc, sq, diag):
    m = kc == sq
    if diag:
        r = lax.broadcasted_iota(jnp.int32, (QB, QB), 0)
        c = lax.broadcasted_iota(jnp.int32, (QB, QB), 1)
        m = (m & (r <= c)) | (r == c)
    return m


def block_bounds(seg, live, i, n):
    s = lax.axis_index("tensor") // 2
    doc = seg[s, 0, i * QB]

    def body(j, count):
        return count + jnp.where((j < i) & (seg[s, 0, (j + 1) * QB - 1] == doc), 1, 0)

    hi = jnp.minimum(i, (live[0, s] * LIVE + QB - 1) // QB)
    return jnp.minimum(i - lax.fori_loop(0, n, body, 0), hi), hi


def turn_blocks(src, dst):
    def turn(i, _):
        dst[:, ds(i * QB, QB)] = src[ds(i * QB, QB), :].T
        return 0

    lax.fori_loop(0, src.shape[0] // QB, turn, 0)


def attn_fwd_block(i, lo, hi, heads, q_ref, k_ref, vt, sr_ref, kc_ref, s_scr, o_ref, lse_ref):
    width = q_ref.shape[1]
    qi = ds(i * QB, QB)
    q = q_ref[qi, :]
    qm = [jnp.where(m, q, jnp.zeros_like(q)) for m in head_lanes(width, heads)]
    sq = sr_ref[0:1, qi]

    def scores(j, slot, ms, diag):
        kj = ds(j * QB, QB)
        k = k_ref[kj, :]
        mask = allow_mask(kc_ref[kj, 0:1], sq, diag)
        out = []
        for h in range(heads):
            s = jnp.where(mask, dg(k, qm[h], 1, 1), NEG)
            s_scr[h, ds(slot * QB, QB), :] = s
            out.append(jnp.maximum(ms[h], jnp.max(s, axis=0, keepdims=True)))
        return tuple(out)

    ms = tuple(jnp.full((1, QB), NEG, F32) for _ in range(heads))
    ms = scores(i, 0, ms, True)
    ms = lax.fori_loop(lo, hi, lambda j, ms: scores(j, j - lo + 1, ms, False), ms)

    def weigh(j, slot, st):
        kj = ds(j * QB, QB)
        out = []
        for h in range(heads):
            total, acc = st[h]
            p = jnp.exp(s_scr[h, ds(slot * QB, QB), :] - ms[h])
            total = total + jnp.sum(p, axis=0, keepdims=True)
            acc = acc + dot(vt[h * HD : (h + 1) * HD, kj], p.astype(BF))
            out.append((total, acc))
        return tuple(out)

    st = tuple((jnp.zeros((1, QB), F32), jnp.zeros((HD, QB), F32)) for _ in range(heads))
    st = weigh(i, 0, st)
    st = lax.fori_loop(lo, hi, lambda j, st: weigh(j, j - lo + 1, st), st)
    ot = [st[h][1] * (1.0 / st[h][0]) for h in range(heads)]
    ot = jnp.concatenate(ot + [jnp.zeros((width - heads * HD, QB), F32)], axis=0)
    o_ref[qi, :] = ot.T.astype(BF)
    lse = [ms[h] + jnp.log(st[h][0]) for h in range(heads)]
    lse_ref[:, qi] = jnp.concatenate(lse + [jnp.zeros((8 - heads, QB), F32)], axis=0)


def attn_fwd_kernel(heads, seg, live, q_in, k_in, v_in, sr_ref, kc_ref, o_out, lse_ref, q, k, v, o, vt, s_scr, lsem, osem):
    n = q.shape[0] // QB
    loads = load([(v_in, v), (q_in, q), (k_in, k)], lsem)
    loads[0].wait()
    turn_blocks(v, vt)
    loads[1].wait()
    loads[2].wait()

    def out(i):
        rows = ds(i * QB, QB)
        return pltpu.make_async_copy(o.at[rows], o_out.at[rows], osem.at[i])

    def qloop(i, _):
        lo, hi = block_bounds(seg, live, i, n)
        attn_fwd_block(i, lo, hi, heads, q, k, vt, sr_ref, kc_ref, s_scr, o, lse_ref)
        out(i).start()
        return 0

    lax.fori_loop(0, n, qloop, 0)

    def drain(i, _):
        out(i).wait()
        return 0

    lax.fori_loop(0, n, drain, 0)


def attn_fwd(heads, seg, live, q, k, v, sr, kc):
    rows, width = q.shape
    buf = pltpu.VMEM((rows, width), BF)
    return pl.pallas_call(
        functools.partial(attn_fwd_kernel, heads),
        out_shape=(sds((rows, width), BF), sds((8, rows), F32)),
        in_specs=[SMEM, SMEM, ANY, ANY, ANY, VMEM, VMEM],
        out_specs=(ANY, VMEM),
        scratch_shapes=[buf, buf, buf, buf, pltpu.VMEM((width, rows), BF), pltpu.VMEM((heads, rows + QB, QB), F32),
                        DMA((3,)), DMA((rows // QB,))],
        compiler_params=pltpu.CompilerParams(vmem_limit_bytes=67043328),
        cost_estimate=cost(12),
        name="attn_fwd",
    )(seg, live, q, k, v, sr, kc)


def turn_lanes(x, tab, sign):
    width = x.shape[1]
    c, sn = [jnp.concatenate([tab[:, a * 128 : (a + 1) * 128]] * (width // 128), axis=1) for a in range(2)]
    lane = lax.broadcasted_iota(jnp.int32, (1, width), 1) % HD
    moved = jnp.where(lane < ROT // 2, pltpu.roll(x, width - ROT // 2, 1), pltpu.roll(x, ROT // 2, 1)) * sn
    return x * c + moved if sign > 0 else x * c - moved


def attn_bwd_block(i, lo, hi, heads, q_ref, k_ref, v_ref, o_ref, do_ref, kt, lse_ref, sr_ref, kc_ref, tab, dk, dv, out):
    width = q_ref.shape[1]
    hm = head_lanes(width, heads)
    rowid = lax.broadcasted_iota(jnp.int32, (8, width), 0)
    lane = lax.broadcasted_iota(jnp.int32, (8, width), 1)
    sel = ((lane >= rowid * HD) & (lane < (rowid + 1) * HD)).astype(F32).astype(BF)
    qi = ds(i * QB, QB)
    q = q_ref[qi, :]
    do = do_ref[qi, :]
    z = jnp.zeros_like(q)
    qm = [jnp.where(hm[h], q, z) for h in range(heads)]
    dom = [jnp.where(hm[h], do, z) for h in range(heads)]
    qcat = jnp.concatenate(qm, axis=0)
    docat = jnp.concatenate(dom, axis=0)
    prod = do.astype(F32) * o_ref[qi, :].astype(F32)
    high = prod.astype(BF)
    low = (prod - high.astype(F32)).astype(BF)
    delta = dg(sel, high, 1, 1) + dg(sel, low, 1, 1)
    lse = lse_ref[:, qi]
    sq = sr_ref[0:1, qi]

    def step(j, dqs, diag):
        kj = ds(j * QB, QB)
        k = k_ref[kj, :]
        v = v_ref[kj, :]
        mask = allow_mask(kc_ref[kj, 0:1], sq, diag)
        ps, dss, res = [], [], []
        for h in range(heads):
            s = dg(k, qm[h], 1, 1)
            dp = dg(v, dom[h], 1, 1)
            p = jnp.exp(jnp.where(mask, s - lse[h : h + 1, :], NEG))
            score_grad = (p * (dp - delta[h : h + 1, :])).astype(BF)
            ps.append(p.astype(BF))
            dss.append(score_grad)
            res.append(dqs[h] + dot(kt[h * HD : (h + 1) * HD, kj], score_grad))
        dv[kj, :] += dot(jnp.concatenate(ps, axis=1), docat)
        dk[kj, :] += dot(jnp.concatenate(dss, axis=1), qcat)
        return tuple(res)

    dqs = tuple(jnp.zeros((HD, QB), F32) for _ in range(heads))
    dqs = step(i, dqs, True)
    dqs = lax.fori_loop(lo, hi, lambda j, d: step(j, d, False), dqs)
    dq = jnp.concatenate(list(dqs) + [jnp.zeros((width - heads * HD, QB), F32)], axis=0).T * 0.125
    out[qi, 0:width] = turn_lanes(dq, tab[qi, :], -1).astype(BF)


def attn_bwd_kernel(
    heads, seg, live, q_in, k_in, v_in, o_in, do_in, lse_ref, sr_ref, kc_ref, tab_in, out_ref,
    q, k, v, o, do, tab, out, kt, dk, dv, lsem, osem,
):
    rows, width = q.shape
    n = rows // QB
    loads = load([(k_in, k), (q_in, q), (v_in, v), (do_in, do), (o_in, o), (tab_in, tab)], lsem)
    dk[...] = jnp.zeros_like(dk)
    dv[...] = jnp.zeros_like(dv)
    loads[0].wait()
    turn_blocks(k, kt)
    for c in loads[1:]:
        c.wait()

    def qloop(i, _):
        lo, hi = block_bounds(seg, live, i, n)
        attn_bwd_block(i, lo, hi, heads, q, k, v, o, do, kt, lse_ref, sr_ref, kc_ref, tab, dk, dv, out)
        return 0

    lax.fori_loop(0, n, qloop, 0)

    def leave(i):
        rr = ds(i * QB, QB)
        return pltpu.make_async_copy(out.at[rr], out_ref.at[rr], osem.at[i])

    def finish(i, _):
        ii = ds(i * QB, QB)
        out[ii, width : 2 * width] = turn_lanes(dk[ii, :], tab[ii, :], -1).astype(BF)
        out[ii, 2 * width : 3 * width] = dv[ii, :].astype(BF)
        leave(i).start()
        return 0

    lax.fori_loop(0, n, finish, 0)

    def drain(i, _):
        leave(i).wait()
        return 0

    lax.fori_loop(0, n, drain, 0)


def attn_bwd(heads, seg, live, q, k, v, o, do, lse, sr, kc, tab):
    rows, width = q.shape
    buf = pltpu.VMEM((rows, width), BF)
    return pl.pallas_call(
        functools.partial(attn_bwd_kernel, heads),
        out_shape=sds((rows, 3 * width), BF),
        in_specs=[SMEM, SMEM] + [ANY] * 5 + [VMEM] * 3 + [ANY],
        out_specs=ANY,
        scratch_shapes=[buf, buf, buf, buf, buf, pltpu.VMEM(tab.shape, F32), pltpu.VMEM((rows, 3 * width), BF),
                        pltpu.VMEM((width, rows), BF), pltpu.VMEM((rows, width), F32), pltpu.VMEM((rows, width), F32),
                        DMA((6,)), DMA((rows // QB,))],
        compiler_params=pltpu.CompilerParams(vmem_limit_bytes=67043328),
        cost_estimate=cost(26),
        name="attn_bwd",
    )(seg, live, q, k, v, o, do, lse, sr, kc, tab)


class Mesh:
    def __init__(self, dp, tensor):
        self.dp, self.tensor = dp, tensor
        self.s, self.z, self.t = lax.axis_index("section"), lax.axis_index("dp"), lax.axis_index("tensor")
        self.x, self.y = self.t % 2, self.t // 2
        self.px, self.py = 2 * self.y + (1 - self.x), 2 * (1 - self.y) + self.x
        self.mate = {"section": 1 - self.s}
        self.beside = {"tensor": self.px}
        self.beside_mate = {"tensor": self.px, "section": 1 - self.s}
        self.across = {"tensor": self.py}
        self.across_mate = {"tensor": self.py, "section": 1 - self.s}
        self.ring = [{"dp": (self.z + d) % dp} for d in range(1, dp)]
        self.group = [{"tensor": (self.t + d) % tensor} for d in range(1, tensor)]
        self.quarter = 2 * self.s + self.x

    def across_core(self, core):
        return {"tensor": self.py, "section": core}


def greet(peers):
    bar = pltpu.get_barrier_semaphore()
    for peer in peers:
        pl.semaphore_signal(bar, inc=1, device_id=peer, device_id_type=MESH)
    pl.semaphore_wait(bar, len(peers))


def push(src, dst, ssem, rsem, peer):
    return pltpu.make_async_remote_copy(
        src_ref=src, dst_ref=dst, send_sem=ssem, recv_sem=rsem, device_id=peer, device_id_type=MESH
    )


def pick(i, values):
    out = values[-1]
    for n in range(len(values) - 2, -1, -1):
        out = jnp.where(i == n, values[n], out)
    return out


class Tokens:
    def __init__(self, me, seq):
        self.me, self.half = me, seq // 8

    def start_of(self, a, b, h):
        return (4 * a + 2 * b + h) * self.half

    def rows(self, a, b, h):
        return ds(self.start_of(a, b, h), self.half)

    def own(self, a):
        return self.start_of(a, self.me.x, self.me.s)


class Gather(Tokens):
    def __init__(self, me, full, ssem, rsem, first=0):
        super().__init__(me, full.shape[0])
        self.full, self.ssem, self.rsem, self.first = full, ssem, rsem, first

    def side(self, n):
        return self.first if n == 0 else 1 - self.first

    def plan(self, i):
        me, a = self.me, self.side(i % 2)
        ref = self.full.at[self.rows(a, (1 - me.x) if i >= 4 else me.x, me.s)]
        return push(ref, ref, self.ssem.at[i], self.rsem.at[i], me.beside if i in (2, 3) else me.mate)

    def start(self, n):
        self.plan(n).start()
        self.plan(2 + n).start()

    def order(self, i):
        me = self.me
        a = pick(i, [self.side(n) for n in (0, 1, 0, 1, 0, 0, 1, 1)])
        b = jnp.where(i < 4, me.x, 1 - me.x)
        h = pick(i, [me.s, me.s, 1 - me.s, 1 - me.s, me.s, 1 - me.s, me.s, 1 - me.s])
        return self.start_of(a, b, h)

    def step(self, i):
        if i in (2, 3):
            self.plan(i - 2).wait_recv()
        if i in (4, 6):
            n = i // 2 - 2
            self.plan(2 + n).wait_recv()
            self.plan(4 + n).start()
        if i in (5, 7):
            self.plan(4 + i // 2 - 2).wait_recv()

    def arrive(self, i):
        for n in range(2, 8):

            @pl.when(i == n)
            def _(n=n):
                self.step(n)

    def finish(self):
        for i in range(6):
            self.plan(i).wait_send()

    def run(self, work):
        def body(i, _):
            self.arrive(i)
            work(self.order(i), i)
            return 0

        lax.fori_loop(0, 8, body, 0)
        self.finish()


class Scatter(Tokens):
    def __init__(self, me, part, mr, xr, ssem, rsem, first=0):
        super().__init__(me, part.shape[0])
        self.part, self.mr, self.xr, self.ssem, self.rsem, self.first = part, mr, xr, ssem, rsem, first

    def side(self, n):
        return self.first if n == 0 else 1 - self.first

    def plan(self, i):
        me = self.me
        if i < 4:
            b = (1 - me.x) if i < 2 else me.x
            src, dst, peer = self.rows(self.side(i % 2), b, 1 - me.s), self.mr.at[i], me.mate
        else:
            src, dst, peer = self.rows(self.side(i - 4), 1 - me.x, me.s), self.xr.at[i - 4], me.beside
        return push(self.part.at[src], dst, self.ssem.at[i], self.rsem.at[i], peer)

    def run(self, work, early=None):
        me = self.me

        def body(i, _):
            k = i // 2
            b = jnp.where(k < 2, 1 - me.x, me.x)
            h = jnp.where(i % 2 == 0, 1 - me.s, me.s)
            work(self.start_of(jnp.where(k % 2 == 0, self.side(0), self.side(1)), b, h), i)
            for n in range(4):

                @pl.when(i == 2 * n)
                def _(n=n):
                    self.plan(n).start()

            for n in range(2):

                @pl.when(i == 2 * n + 1)
                def _(n=n):
                    self.plan(n).wait_recv()
                    base = self.start_of(self.side(n), 1 - me.x, me.s)

                    def add(j, _):
                        rr = ds(base + j * SUB, SUB)
                        got = self.mr[n, ds(j * SUB, SUB), :].astype(F32)
                        self.part[rr, :] = (self.part[rr, :].astype(F32) + got).astype(BF)
                        return 0

                    lax.fori_loop(0, self.half // SUB, add, 0)
                    self.plan(4 + n).start()

            return 0

        lax.fori_loop(0, 8, body, 0)
        if early is not None:
            early()

    def arrive(self, n):
        self.plan(2 + n).wait_recv()
        self.plan(4 + n).wait_recv()

    def total(self, n, i):
        rr = ds(self.own(self.side(n)) + i * SUB, SUB)
        sub = ds(i * SUB, SUB)
        return self.part[rr, :].astype(F32) + self.mr[2 + n, sub, :].astype(F32) + self.xr[n, sub, :].astype(F32)

    def finish(self):
        for i in range(6):
            self.plan(i).wait_send()


def scatter_scratch(rows, width):
    half = rows // 8
    return [
        pltpu.VMEM((rows, width), BF),
        pltpu.VMEM((4, half, width), BF),
        pltpu.VMEM((2, half, width), BF),
        DMA((6,)),
        DMA((6,)),
    ]


class WeightGather:
    def __init__(self, me, layer, shard, full, gat, groups, sems):
        self.me, self.layer, self.shard, self.full, self.gat, self.groups = me, layer, shard, full, gat, groups
        self.own, self.wss, self.wrs, self.fss, self.frs, self.yss, self.yrs = sems
        self.rows = shard.shape[0]
        self.collects = me.s == layer
        self.keeps = me.y == layer

    def block(self, ref, zz, g):
        a, b = self.groups[g]
        return ref.at[ds(zz * self.rows, self.rows), a:b]

    def mine(self, g):
        a, b = self.groups[g]
        return self.shard.at[:, a:b]

    def local(self, g):
        return pltpu.make_async_copy(self.mine(g), self.block(self.full, self.me.z, g), self.own.at[g])

    def out(self, g, d, ref):
        dst = self.block(ref, self.me.z, g)
        return push(self.mine(g), dst, self.wss.at[g, d], self.wrs.at[g, d], self.me.ring[d])

    def hand(self, g, d, ref, across):
        zz = (self.me.z + self.me.dp - d) % self.me.dp
        src = self.mine(g) if d == 0 else self.block(ref, zz, g)
        ss, rs = (self.yss, self.yrs) if across else (self.fss, self.frs)
        peer = self.me.across_core(self.me.y) if across else self.me.mate
        return push(src, self.block(self.full, zz, g), ss.at[g, d], rs.at[g, d], peer)

    def both(self, do):
        @pl.when(self.collects & self.keeps)
        def _():
            do(self.full, True)

        @pl.when(self.collects & jnp.logical_not(self.keeps))
        def _():
            do(self.gat, False)

    def send_ring(self):
        def do(ref, keeps):
            for g in range(len(self.groups)):
                for d in range(self.me.dp - 1):
                    self.out(g, d, ref).start()

        self.both(do)

    def send_own(self, g):
        def do(ref, keeps):
            self.hand(g, 0, ref, True).start()
            if keeps:
                self.local(g).start()
            else:
                self.hand(g, 0, ref, False).start()

        self.both(do)

    def forward(self, g, blocks=None):
        def do(ref, keeps):
            for d in range(self.me.dp - 1) if blocks is None else blocks:
                self.out(g, d, ref).wait_recv()
                self.hand(g, d + 1, ref, True).start()
                if not keeps:
                    self.hand(g, d + 1, ref, False).start()

        self.both(do)

    def ready(self, g):
        me = self.me

        @pl.when(self.collects & self.keeps)
        def _():
            self.local(g).wait()

        @pl.when(me.s != me.y)
        def _():
            for d in range(me.dp):
                self.hand(g, d, self.full, True).wait_recv()

        @pl.when((me.s == me.y) & jnp.logical_not(self.collects))
        def _():
            for d in range(me.dp):
                self.hand(g, d, self.full, False).wait_recv()

    def finish(self):
        def do(ref, keeps):
            for g in range(len(self.groups)):
                for d in range(self.me.dp - 1):
                    self.out(g, d, ref).wait_send()
                for d in range(self.me.dp):
                    self.hand(g, d, ref, True).wait_send()
                    if not keeps:
                        self.hand(g, d, ref, False).wait_send()

        self.both(do)

    @staticmethod
    def scratch(dp, n):
        return [DMA((n,)), DMA((n, dp - 1)), DMA((n, dp - 1))] + [DMA((n, dp))] * 4


class GradReduce:
    def __init__(self, me, layer, src, mine, got, across, sb, rb, own, sems):
        self.me, self.layer, self.src, self.mine, self.got, self.across = me, layer, src, mine, got, across
        self.sb, self.rb, self.own = sb, rb, own
        self.hss, self.hrs, self.yss, self.yrs, self.pss, self.prs = sems
        self.rows = own.shape[0]
        self.some = 96 if self.rows % 96 == 0 else 48
        self.sums = me.s == layer
        self.holds = me.y == layer

    @staticmethod
    def scratch(dp):
        return [DMA((1,)), DMA((1,)), DMA((dp,)), DMA((dp,)), DMA((dp - 1,)), DMA((dp - 1,))]

    def hand(self):
        return push(self.src, self.got, self.hss.at[0], self.hrs.at[0], self.me.mate)

    def zz(self, d):
        return (self.me.z + d + 1) % self.me.dp

    def over(self, d):
        rr = ds(self.zz(d) * self.rows, self.rows)
        peer = self.me.across_core(self.layer)
        return push(self.src.at[rr], self.across.at[rr], self.yss.at[d], self.yrs.at[d], peer)

    def out(self, d):
        return push(self.sb.at[d], self.rb.at[d], self.pss.at[d], self.prs.at[d], self.me.ring[d])

    def send(self):
        me = self.me

        @pl.when(me.s != me.y)
        def _():
            for d in range(me.dp):
                self.over(d).start()

        @pl.when((me.s == me.y) & jnp.logical_not(self.sums))
        def _():
            self.hand().start()

    def step(self, d):
        me = self.me

        @pl.when(self.sums)
        def _():
            if d == 0:

                @pl.when(jnp.logical_not(self.holds))
                def _():
                    self.hand().wait_recv()

            self.over(d).wait_recv()
            last = d == me.dp - 1
            step = self.some

            def add(ref):
                def body(i, _):
                    rr = ds(self.zz(d) * self.rows + i * step, step)
                    value = ref[rr, :].astype(F32) + self.across[rr, :].astype(F32)
                    if last:
                        self.own[ds(i * step, step), :] = value
                    else:
                        self.sb[d, ds(i * step, step), :] = value.astype(BF)
                    return 0

                lax.fori_loop(0, self.rows // step, body, 0)

            if self.mine is self.got:
                add(self.mine)
            else:

                @pl.when(self.holds)
                def _():
                    add(self.mine)

                @pl.when(jnp.logical_not(self.holds))
                def _():
                    add(self.got)

            if not last:
                self.out(d).start()

    def collect(self):
        me = self.me

        @pl.when(self.sums)
        def _():
            for d in range(me.dp - 1):
                self.out(d).wait_recv()

                def add(i, _, d=d):
                    rr = ds(i * self.some, self.some)
                    self.own[rr, :] += self.rb[d, rr, :].astype(F32)
                    return 0

                lax.fori_loop(0, self.rows // self.some, add, 0)
            for d in range(me.dp - 1):
                self.out(d).wait_send()

    def finish(self):
        me = self.me

        @pl.when(me.s != me.y)
        def _():
            for d in range(me.dp):
                self.over(d).wait_send()

        @pl.when((me.s == me.y) & jnp.logical_not(self.sums))
        def _():
            self.hand().wait_send()


class VectorGather:
    def __init__(self, me, sv, buf, ss, rs, own):
        self.me, self.sv, self.buf, self.ss, self.rs, self.own = me, sv, buf, ss, rs, own

    def local(self):
        me = self.me
        return pltpu.make_async_copy(self.sv, self.buf.at[me.s, me.t, me.z], self.own)

    def stage(self, n):
        me = self.me
        if n == 0:
            dst = self.buf.at[me.s, me.t, me.z]
            return [push(self.sv, dst, self.ss.at[d], self.rs.at[d], peer) for d, peer in enumerate(me.ring)]
        base = me.dp - 1
        if n == 1:
            ref = self.buf.at[me.s, me.t]
            return [
                push(ref, ref, self.ss.at[base + d], self.rs.at[base + d], peer) for d, peer in enumerate(me.group)
            ]
        i = base + me.tensor - 1
        ref = self.buf.at[me.s]
        return [push(ref, ref, self.ss.at[i], self.rs.at[i], me.mate)]

    def send(self, n):
        if n == 0:
            self.local().start()
        for c in self.stage(n):
            c.start()

    def wait(self, n):
        if n == 0:
            self.local().wait()
        for c in self.stage(n):
            c.wait_recv()

    def finish(self):
        for n in range(3):
            for c in self.stage(n):
                c.wait_send()

    def build(self, vecs, heads, own, qw, fw):
        me, buf = self.me, self.buf
        for layer in range(2):
            wide = [buf[layer, tt, zz, 0:8, :][:, 0:own] for zz in range(me.dp) for tt in range(me.tensor)]
            vecs[layer, 0:8, :] = jnp.concatenate(wide, axis=1)
            here = [buf[layer, me.quarter, zz] for zz in range(me.dp)]
            by = [jnp.concatenate([p[6 + h : 7 + h, 0:qw] for p in here], axis=1) for h in range(heads)]
            qb = []
            for part in range(3):
                qb += [b[:, part * HD : (part + 1) * HD] for b in by] + [jnp.zeros((1, HW - heads * HD), F32)]
            vecs[layer, 6:7, :] = jnp.concatenate(qb, axis=1)
            fb = [p[6 + heads + h : 7 + heads + h, 0:fw] for h in range(heads) for p in here]
            vecs[layer, 7:8, :] = jnp.concatenate(fb, axis=1)


class VectorReduce:
    def __init__(self, me, va, vr, ss, rs):
        self.me, self.va, self.vr, self.ss, self.rs = me, va, vr, ss, rs

    def stage(self, n):
        me, va, vr, ss, rs = self.me, self.va, self.vr, self.ss, self.rs
        peers, base = [([me.across], 0), (me.ring, 1), ([me.mate, me.beside, me.beside_mate], me.dp)][n]
        return [push(va.at[n], vr.at[base + d], ss.at[base + d], rs.at[base + d], p) for d, p in enumerate(peers)]

    def send(self, n):
        for c in self.stage(n):
            c.start()

    def add(self, n, out):
        base = [0, 1, self.me.dp][n]
        for c in self.stage(n):
            c.wait_recv()
        if n < 2:
            total = self.va[n]
            for d in range(len(self.stage(n))):
                total = total + self.vr[base + d]
            out[...] = total
            return
        mine, mate = self.va[2], self.vr[base]
        row = lax.broadcasted_iota(jnp.int32, mine.shape, 0)
        quarter = jnp.where(self.me.s == self.me.y, mine, mate)
        out[...] = jnp.where(row % 8 < 6, mine + mate + self.vr[base + 1] + self.vr[base + 2], quarter)

    def finish(self):
        for n in range(3):
            for c in self.stage(n):
                c.wait_send()


def document_tables(seg, live, fr_ref, tab, srow, kcol):
    seq = seg.shape[1]
    count = lax.broadcasted_iota(jnp.int32, seg.shape, 1)
    start = jnp.zeros_like(seg)
    for doc in range(DOCS - 1):
        before = jnp.sum(jnp.where(seg == doc, 1.0, 0.0), axis=1, keepdims=True).astype(jnp.int32)
        start = start + jnp.where(seg > doc, before, 0)
    ang = fr_ref[:, 0:1] * (count - start).astype(F32)
    cs, sn = jnp.cos(ang), jnp.sin(ang)
    one = jnp.ones((HD - ROT, seq), F32)
    tab[:, 0:128] = jnp.concatenate([cs, cs, one] * 2, axis=0).T
    tab[:, 128:256] = jnp.concatenate([-sn, sn, jnp.zeros_like(one)] * 2, axis=0).T
    srow[...] = jnp.broadcast_to(seg, srow.shape)
    keys = jnp.where(count < live * LIVE, seg, -1).astype(F32)
    for b in range(seq // QB):
        part = jnp.broadcast_to(keys[:, b * QB : (b + 1) * QB], (128, QB))
        kcol[b * QB : (b + 1) * QB, :] = part.T.astype(jnp.int32)


QKV, FC1, FC2, OUT = 0, 1, 2, 3


def columns(model, ff):
    return {"qkv": 0, "fc1": 3 * HW, "fc2": 3 * HW + ff, "out": 3 * HW + 2 * ff, "end": 3 * HW + 2 * ff + HW}


def project_norm(r0, half, hf, vec, n1, n2):
    rows = ds(r0, half)
    xc, r = norm_stats(hf[rows, :].astype(F32))
    xh = xc * r
    n1[rows, :] = (xh * vec[0:1, :] + vec[1:2, :]).astype(BF)
    n2[rows, :] = (xh * vec[3:4, :] + vec[4:5, :]).astype(BF)


def project_qkv(r0, half, wqkv, vec, tab, n1, q, k, v):
    rows = ds(r0, half)
    a = n1[rows, :]
    for part, dst in enumerate((q, k, v)):
        cols = slice(part * HW, (part + 1) * HW)
        y = dot(a, wqkv[:, cols]) + vec[6:7, cols]
        if part < 2:
            y = turn_lanes(y, tab[rows, :], 1)
        if part == 0:
            y = y * 0.125
        dst[rows, :] = y.astype(BF)


def project_fc1(r0, half, wfc1, vec, n2, g, gp):
    rows = ds(r0, half)
    a = n2[rows, :]
    for b in range(wfc1.shape[1] // 256):
        cols = slice(b * 256, (b + 1) * 256)
        y = dot(a, wfc1[:, cols]) + vec[7:8, cols]
        cdf = 0.5 + 0.5 * lax.erf(y * 0.7071067811865476)
        g[rows, cols] = (y * cdf).astype(BF)
        gp[rows, cols] = (cdf + y * jnp.exp(-0.5 * y * y) * 0.3989422804014327).astype(BF)


def branch_out(r0, half, o, g, wout, wfc2, part):
    rows = ds(r0, half)
    for b in range(part.shape[1] // 256):
        cols = slice(b * 256, (b + 1) * 256)
        y = dg(o[rows, :], wout[cols, :], 1, 1) + dg(g[rows, :], wfc2[cols, :], 1, 1)
        part[rows, cols] = y.astype(BF)


def back_head(r0, half, dyf, hf, g, gp, n2, o, wfc1, wfc2, wout, vec, do, e2, da, acc, vg):
    rows = ds(r0, half)
    model, ff = wfc1.shape
    dy = dyf[rows, :]
    for b in range(ff // 256):
        cols = slice(b * 256, (b + 1) * 256)
        y = dot(dy, wfc2[:, cols]) * gp[rows, cols].astype(F32)
        low = y.astype(BF)
        da[:, cols] = low
        vg[7:8, cols] += jnp.sum(low.astype(F32), axis=0, keepdims=True)
    do[rows, :] = dot(dy, wout[...]).astype(BF)
    xc, r = norm_stats(hf[rows, :].astype(F32))
    xh = xc * r
    for b in range(model // 256):
        cols = slice(b * 256, (b + 1) * 256)
        dn = dg(da[...], wfc1[cols, :], 1, 1)
        vg[3:4, cols] += jnp.sum(dn * xh[:, cols], axis=0, keepdims=True)
        vg[4:5, cols] += jnp.sum(dn, axis=0, keepdims=True)
        e2[rows, cols] = (dn * vec[3:4, cols]).astype(BF)
    n2t = n2[rows, :].T
    dyt = dy.T
    for b in range(ff // 256):
        cols = slice(b * 256, (b + 1) * 256)
        acc[:, cols] += dot(n2t, da[:, cols])
        acc[:, ff + b * 256 : ff + (b + 1) * 256] += dot(dyt, g[rows, cols])
    acc[:, 2 * ff :] += dot(dyt, o[rows, :])


def back_tail(r0, half, dmix, hf, e2, wqkv, vec, part, vg):
    rows = ds(r0, half)
    dm = dmix[rows, :]
    vg[6:7, :] += jnp.sum(dm.astype(F32), axis=0, keepdims=True)
    xc, r = norm_stats(hf[rows, :].astype(F32))
    xh = xc * r
    for b in range(part.shape[1] // 256):
        cols = slice(b * 256, (b + 1) * 256)
        dn = dg(dm, wqkv[cols, :], 1, 1)
        vg[0:1, cols] += jnp.sum(dn * xh[:, cols], axis=0, keepdims=True)
        vg[1:2, cols] += jnp.sum(dn, axis=0, keepdims=True)
        part[rows, cols] = (dn * vec[0:1, cols] + e2[rows, cols].astype(F32)).astype(BF)


def qkv_grad(n1, dmix, acc, half):
    acc[...] = jnp.zeros_like(acc)

    def body(i, _):
        rows = ds(i * half, half)
        n1t = n1[rows, :].T
        for b in range(3):
            cols = slice(b * HW, (b + 1) * HW)
            acc[:, cols] += dot(n1t, dmix[rows, cols])
        return 0

    lax.fori_loop(0, n1.shape[0] // half, body, 0)


def store_low(acc, out):
    def body(i, _):
        rr = ds(i * SUB, SUB)
        out[rr, :] = acc[rr, :].astype(BF)
        return 0

    lax.fori_loop(0, acc.shape[0] // SUB, body, 0)


def residual_out(sc, own, vec, write, after=None):
    for a in range(2):
        sc.arrive(a)

        def body(i, _, a=a):
            base = own[ds(sc.own(sc.side(a)) + i * SUB, SUB), :].astype(F32)
            write(a, i, (base + sc.total(a, i) + vec[2:3, :] + vec[5:6, :]).astype(BF))
            return 0

        lax.fori_loop(0, sc.half // SUB, body, 0)
        if after is not None:
            after(a)


def grad_out(sc, dy, hf, vec, write, after=None):
    for a in range(2):
        sc.arrive(a)

        def body(i, _, a=a):
            rr = ds(sc.own(sc.side(a)) + i * SUB, SUB)
            xc, r = norm_stats(hf[rr, :].astype(F32))
            xh = xc * r
            e = sc.total(a, i)
            m1 = jnp.mean(e, axis=-1, keepdims=True)
            m2 = jnp.mean(e * xh, axis=-1, keepdims=True)
            write(a, i, (dy(a, i).astype(F32) + r * (e - m1 - xh * m2)).astype(BF))
            return 0

        lax.fori_loop(0, sc.half // SUB, body, 0)
        if after is not None:
            after(a)


def column_sum(tok, ref, vg, row):
    total = jnp.zeros((1, ref.shape[1]), F32)
    for a in range(2):

        def body(i, acc, a=a):
            return acc + jnp.sum(ref[ds(tok.own(a) + i * SUB, SUB), :].astype(F32), axis=0, keepdims=True)

        total = lax.fori_loop(0, tok.half // SUB, body, total)
    vg[row : row + 1, :] = total


def load(pairs, sem):
    copies = [pltpu.make_async_copy(a, b, sem.at[i]) for i, (a, b) in enumerate(pairs)]
    for c in copies:
        c.start()
    return copies


def params(cid):
    return pltpu.CompilerParams(collective_id=cid, has_side_effects=True, vmem_limit_bytes=67043328)


def cost(us):
    return pl.CostEstimate(flops=int(us * 8e8), bytes_accessed=0, transcendentals=0)


class OwnedOut:
    def __init__(self, me, src, dst, core, ss, rs, local):
        self.me, self.src, self.dst, self.core, self.ss, self.rs, self.local = me, src, dst, core, ss, rs, local

    def place(self):
        return self.dst.at[self.me.y, self.me.s]

    def far(self):
        me = self.me
        return push(self.src.at[1 - me.y], self.place(), self.ss.at[0], self.rs.at[me.s], me.across_core(self.core))

    def mate(self):
        return push(self.src.at[self.me.y], self.place(), self.ss.at[1], self.rs.at[2], self.me.mate)

    def here(self):
        return pltpu.make_async_copy(self.src.at[self.me.y], self.place(), self.local)

    def start_here(self):
        @pl.when(self.me.s == self.core)
        def _():
            self.here().start()

        @pl.when(self.me.s != self.core)
        def _():
            self.mate().start()

    def wait(self):
        me = self.me
        self.far().wait_send()

        @pl.when(me.s == self.core)
        def _():
            self.here().wait()
            self.mate().wait_recv()
            for n in range(2):
                place = self.dst.at[1 - me.y, n]
                push(self.src.at[0], place, self.ss.at[0], self.rs.at[n], me.across_core(self.core)).wait_recv()

        @pl.when(me.s != self.core)
        def _():
            self.mate().wait_send()


class Stores:
    def __init__(self, pairs, half, sem):
        self.pairs, self.half, self.sem = pairs, half, sem

    def copy(self, n, r0, i):
        src, dst = self.pairs[n]
        rows = ds(r0, self.half)
        return pltpu.make_async_copy(src.at[rows], dst.at[rows], self.sem.at[n, i])

    def start(self, which, r0, i):
        for n in which:
            self.copy(n, r0, i).start()

    def finish(self):
        def body(i, _):
            for n in range(len(self.pairs)):
                self.copy(n, i * self.half, i).wait()
            return 0

        lax.fori_loop(0, 8, body, 0)


def in_kernel(
    cfg, in_ref, cot_ref, seg_ref, live, w_ref, sv_ref, fr_ref,
    hf_o, n1_o, n2_o, g_o, gp_o, tab_o, w_o, q_o, k_o, v_o, cf_o, vecs, srow, kcol,
    hf, n1, n2, g, gp, tab, q, k, v, wfull, gat, vb, cot, gss, grs, css, crs, yss, yrs, lsem, ssem, vss, vrs, *wsems,
):
    col, dp, tensor = cfg["col"], cfg["dp"], cfg["tensor"]
    me = Mesh(dp, tensor)
    ga = Gather(me, hf, gss, grs, me.y)
    gc = Gather(me, cf_o, css, crs, me.y)
    half = ga.half
    part = ds(me.s * half, half)
    first = pltpu.make_async_copy(in_ref.at[me.y, 0, part], hf.at[ds(ga.own(me.y), half)], lsem.at[0])
    first.start()
    up = pltpu.make_async_copy(cot_ref.at[me.y, 0, part], cot, lsem.at[4])
    up.start()
    greet([me.mate, me.across_mate] + me.ring + me.group)
    over = [
        push(ref.at[1 - me.y, 0, part], full.at[ds(ga.own(me.y), half)], yss.at[n], yrs.at[n], me.across)
        for n, (ref, full) in enumerate(((in_ref, hf), (cot_ref, cf_o)))
    ]
    wg = WeightGather(me, 0, w_ref, wfull, gat, cfg["groups"], wsems)
    vg = VectorGather(me, sv_ref, vb, vss, vrs, lsem.at[1])
    st = Stores([(hf, hf_o), (n1, n1_o), (n2, n2_o), (g, g_o), (gp, gp_o), (q, q_o), (k, k_o), (v, v_o)], half, ssem)
    vg.send(0)
    wg.send_ring()
    first.wait()
    document_tables(seg_ref[me.y], live[0, me.y], fr_ref, tab, srow, kcol)
    vg.wait(0)
    vg.send(1)
    ga.start(0)
    over[0].start()
    wg.send_own(0)
    tab_out = pltpu.make_async_copy(tab, tab_o, lsem.at[2])
    tab_out.start()
    vg.wait(1)
    vg.send(2)
    up.wait()
    cot_out = pltpu.make_async_copy(cot, cf_o.at[ds(gc.own(me.y), half)], lsem.at[5])
    cot_out.start()
    vg.wait(2)
    vg.build(vecs, cfg["heads"], cfg["own"], cfg["qw"], cfg["fw"])
    vec = vecs.at[0]

    def norm(r0, i):
        project_norm(r0, half, hf, vec, n1, n2)
        st.start((0, 1, 2), r0, i)

        @pl.when(i == 0)
        def _():
            over[0].wait_recv()
            ga.start(1)

        @pl.when(i == 1)
        def _():
            wg.forward(0)
            wg.send_own(1)

    ga.run(norm)
    cot_out.wait()
    gc.start(0)
    wg.ready(0)

    def qkv(i, _):
        r0 = ga.order(i)
        project_qkv(r0, half, wfull.at[:, 0 : col["fc1"]], vec, tab, n1, q, k, v)
        st.start((5, 6, 7), r0, i)
        return 0

    lax.fori_loop(0, 8, qkv, 0)
    wg.forward(1)
    wg.send_own(2)
    wg.send_own(3)
    wg.ready(1)
    wg.forward(2)

    def fc1(i, _):
        r0 = ga.order(i)
        project_fc1(r0, half, wfull.at[:, col["fc1"] : col["fc2"]], vec, n2, g, gp)
        st.start((3, 4), r0, i)

        @pl.when(i == 5)
        def _():
            wg.forward(3)
            over[1].start()

        return 0

    lax.fori_loop(0, 8, fc1, 0)
    gc.step(2)
    gc.step(4)
    gc.step(5)
    st.finish()
    tab_out.wait()
    wg.ready(2)
    wg.ready(3)
    w_out = pltpu.make_async_copy(wfull, w_o, lsem.at[3])
    w_out.start()
    over[1].wait_recv()
    gc.start(1)
    for n in (3, 6, 7):
        gc.step(n)
    wg.finish()
    vg.finish()
    gc.finish()
    for c in over:
        c.wait_send()
    w_out.wait()


def layer_in(cfg, inputs, cotangent, segments, live, w, sv, fr):
    seq, model, ff = segments.shape[2], inputs.shape[3], cfg["ff"]
    dp, tensor = cfg["dp"], cfg["tensor"]
    rows, hidden = sds((seq, model), BF), sds((seq, ff), BF)
    heads = sds((seq, HW), BF)
    nv = dp - 1 + tensor
    wide, wide_h, wide_q = pltpu.VMEM((seq, model), BF), pltpu.VMEM((seq, ff), BF), pltpu.VMEM((seq, HW), BF)
    weights = pltpu.VMEM((model, w.shape[1]), BF)
    return pl.pallas_call(
        functools.partial(in_kernel, cfg),
        out_shape=(rows, rows, rows, hidden, hidden, sds((seq, 256), F32), sds((model, w.shape[1]), BF),
                   heads, heads, heads, rows,
                   sds((2, 8, model), F32), sds((8, seq), jnp.int32), sds((seq, 128), jnp.int32)),
        in_specs=[ANY, ANY, VMEM, SMEM, VMEM, VMEM, VMEM],
        out_specs=(ANY,) * 11 + (VMEM,) * 3,
        scratch_shapes=[
            wide, wide, wide, wide_h, wide_h, pltpu.VMEM((seq, 256), F32), wide_q, wide_q, wide_q,
            weights, weights, pltpu.VMEM((2, tensor, dp) + sv.shape, F32),
            pltpu.VMEM((seq // 8, model), BF),
            DMA((6,)), DMA((6,)), DMA((6,)), DMA((6,)), DMA((2,)), DMA((2,)), DMA((6,)), DMA((8, 8)),
            DMA((nv,)), DMA((nv,)),
        ]
        + WeightGather.scratch(dp, 4),
        compiler_params=params(2),
        cost_estimate=cost(45),
        name="layer_in",
    )(inputs, cotangent, segments, live, w, sv, fr)


def mid_kernel(
    cfg, q_in, k_in, v_in, srow, kcol, g_in, x_in, w_ref, w0, vecs, tab_in,
    o_o, lse, hf_o, n1_o, n2_o, g_o, gp_o, w_o, q_o, k_o, v_o,
    wout, wfc2, hf, n1, n2, g, gp, tab, wfull, gat, q, k, v, o, vt, s_scr,
    part, mr, xr, sss, srs, gss, grs, lsem, ssem, osem, *wsems,
):
    col, heads = cfg["col"], cfg["heads"]
    me = Mesh(cfg["dp"], cfg["tensor"])
    sc = Scatter(me, part, mr, xr, sss, srs)
    ga = Gather(me, hf, gss, grs)
    half = sc.half
    loads = load(
        [
            (v_in, v),
            (q_in, q),
            (k_in, k),
            (w0.at[:, col["out"] : col["end"]], wout),
            (w0.at[:, col["fc2"] : col["out"]], wfc2),
            (g_in, g),
            (tab_in, tab),
        ]
        + [(x_in.at[ds(sc.own(a), half)], hf.at[ds(sc.own(a), half)]) for a in range(2)],
        lsem,
    )
    greet([me.mate, me.beside, me.across, me.across_mate] + me.ring)
    wg = WeightGather(me, 1, w_ref, wfull, gat, cfg["groups"], wsems)
    wg.send_ring()
    for n in range(4):
        wg.send_own(n)
    loads[0].wait()
    turn_blocks(v, vt)
    for c in loads[1:]:
        c.wait()
    st = Stores([(hf, hf_o), (n1, n1_o), (n2, n2_o), (g, g_o), (gp, gp_o), (q, q_o), (k, k_o), (v, v_o)], half, ssem)
    st_o = Stores([(o, o_o)], half, osem)

    def out(r0, i):
        b = r0 // QB
        attn_fwd_block(b, jnp.maximum(b - DOC_MAX // QB, 0), b, heads, q, k, vt, srow, kcol, s_scr, o, lse)
        st_o.start((0,), r0, i)
        branch_out(r0, half, o, g, wout, wfc2, part)

        @pl.when(i == 6)
        def _():
            wg.forward(0)

    sc.run(out)

    def write(a, i, value):
        hf[ds(sc.own(a) + i * SUB, SUB), :] = value

    residual_out(sc, hf, vecs.at[0], write, ga.start)
    wg.forward(1)
    vec = vecs.at[1]

    def fc1(i):
        r0 = ga.order(i)
        project_fc1(r0, half, wfull.at[:, col["fc1"] : col["fc2"]], vec, n2, g, gp)
        st.start((3, 4), r0, i)

    def work(r0, i):
        project_norm(r0, half, hf, vec, n1, n2)

        @pl.when(i == 0)
        def _():
            wg.ready(0)

        project_qkv(r0, half, wfull.at[:, 0 : col["fc1"]], vec, tab, n1, q, k, v)
        st.start((0, 1, 2, 5, 6, 7), r0, i)

        @pl.when(i == 4)
        def _():
            wg.ready(1)

        @pl.when(i >= 4)
        def _():
            fc1(i - 4)

        @pl.when(i == 5)
        def _():
            wg.forward(2)

        @pl.when(i == 7)
        def _():
            wg.forward(3)

    ga.run(work)

    def late(i, _):
        fc1(i)
        return 0

    lax.fori_loop(4, 8, late, 0)
    st.finish()
    wg.ready(2)
    wg.ready(3)
    w_out = pltpu.make_async_copy(wfull, w_o, lsem.at[0])
    w_out.start()
    sc.finish()
    wg.finish()
    st_o.finish()
    w_out.wait()


def layer_mid(cfg, q, k, v, srow, kcol, g, xf, w, w0, vecs, tab):
    seq, model, ff = tab.shape[0], xf.shape[1], cfg["ff"]
    rows, hidden, heads = sds((seq, model), BF), sds((seq, ff), BF), sds((seq, HW), BF)
    wide, wide_h, wide_q = pltpu.VMEM((seq, model), BF), pltpu.VMEM((seq, ff), BF), pltpu.VMEM((seq, HW), BF)
    return pl.pallas_call(
        functools.partial(mid_kernel, cfg),
        out_shape=(heads, sds((8, seq), F32), rows, rows, rows, hidden, hidden, sds(w0.shape, BF), heads, heads, heads),
        in_specs=[ANY, ANY, ANY, VMEM, VMEM, ANY, ANY, VMEM, ANY, VMEM, ANY],
        out_specs=(ANY, VMEM) + (ANY,) * 9,
        scratch_shapes=[
            pltpu.VMEM((model, HW), BF), pltpu.VMEM((model, ff), BF),
            wide, wide, wide, wide_h, wide_h, pltpu.VMEM((seq, 256), F32),
            pltpu.VMEM(w0.shape, BF), pltpu.VMEM(w0.shape, BF),
            wide_q, wide_q, wide_q, wide_q, pltpu.VMEM((HW, seq), BF),
            pltpu.VMEM((cfg["heads"], DOC_MAX + QB, QB), F32),
        ]
        + scatter_scratch(seq, model)
        + [DMA((6,)), DMA((6,)), DMA((9,)), DMA((8, 8)), DMA((1, 8))]
        + WeightGather.scratch(cfg["dp"], 4),
        compiler_params=params(3),
        cost_estimate=cost(70),
        name="layer_mid",
    )(q, k, v, srow, kcol, g, xf, w, w0, vecs, tab)


def turn_kernel(
    cfg, o_in, g_in, hf_in, cf, w1, vecs, n2_in, gp_in, y_o, do_o, e2_o, gr_o, hx, vg,
    o, g, hf, dyf, n2, gp, e2, do, y, gr, wout, wfc2, wfc1, da, acc,
    part, mr, xr, sss, srs, yss, yrs, lsem, ssem,
):
    col = cfg["col"]
    me = Mesh(cfg["dp"], cfg["tensor"])
    sc = Scatter(me, part, mr, xr, sss, srs)
    half = sc.half
    loads = load(
        [
            (w1.at[:, col["out"] : col["end"]], wout),
            (w1.at[:, col["fc2"] : col["out"]], wfc2),
            (o_in, o),
            (g_in, g),
            (w1.at[:, col["fc1"] : col["fc2"]], wfc1),
            (cf, dyf),
            (gp_in, gp),
            (hf_in, hf),
            (n2_in, n2),
        ],
        lsem,
    )
    greet([me.mate, me.beside, me.across])
    h_over = push(hf_in.at[ds(me.py * 2 * half, 2 * half)], hx, yss.at[0], yrs.at[0], me.across)

    @pl.when(me.s == 0)
    def _():
        h_over.start()

    for c in loads[:4]:
        c.wait()
    vec = vecs.at[1]
    st = Stores([(e2, e2_o), (do, do_o)], half, ssem)

    def early():
        vg[...] = jnp.zeros_like(vg)
        acc[...] = jnp.zeros_like(acc)
        for c in loads[4:]:
            c.wait()

        def head(i, _):
            r0 = i * half
            back_head(r0, half, dyf, hf, g, gp, n2, o, wfc1, wfc2, wout, vec, do, e2, da, acc, vg)
            st.start((0, 1), r0, i)
            return 0

        lax.fori_loop(0, 8, head, 0)

    sc.run(lambda r0, i: branch_out(r0, half, o, g, wout, wfc2, part), early)
    column_sum(sc, dyf, vg, 2)
    store_low(acc, gr)
    gr_out = pltpu.make_async_copy(gr, gr_o, lsem.at[0])
    gr_out.start()

    def write(a, i, value):
        y[a, ds(i * SUB, SUB), :] = value

    residual_out(sc, hf, vec, write)
    y_out = pltpu.make_async_copy(y, y_o, lsem.at[1])
    y_out.start()
    sc.finish()
    st.finish()

    @pl.when(me.s == 0)
    def _():
        h_over.wait()

    gr_out.wait()
    y_out.wait()


def layer_turn(cfg, o, g, hf, cf, w1, vecs, n2, gp):
    seq, model = hf.shape
    ff = cfg["ff"]
    wide, hidden, heads = pltpu.VMEM((seq, model), BF), pltpu.VMEM((seq, ff), BF), pltpu.VMEM((seq, HW), BF)
    owned = (2, seq // 8, model)
    return pl.pallas_call(
        functools.partial(turn_kernel, cfg),
        out_shape=(
            sds(owned, BF),
            sds((seq, HW), BF),
            sds((seq, model), BF),
            sds((model, 2 * ff + HW), BF),
            sds((seq // 4, model), BF),
            sds((8, model), F32),
        ),
        in_specs=[ANY] * 5 + [VMEM, ANY, ANY],
        out_specs=(ANY,) * 5 + (VMEM,),
        scratch_shapes=[
            heads, hidden, wide, wide, wide, hidden, wide, heads, pltpu.VMEM(owned, BF),
            pltpu.VMEM((model, 2 * ff + HW), BF),
            pltpu.VMEM((model, HW), BF), pltpu.VMEM((model, ff), BF), pltpu.VMEM((model, ff), BF),
            pltpu.VMEM((seq // 8, ff), BF), pltpu.VMEM((model, 2 * ff + HW), F32),
        ]
        + scatter_scratch(seq, model)
        + [DMA((1,)), DMA((1,)), DMA((9,)), DMA((2, 8))],
        compiler_params=params(4),
        cost_estimate=cost(40),
        name="layer_turn",
    )(o, g, hf, cf, w1, vecs, n2, gp)


def back_kernel(
    cfg, dm_in, e2_in, cf, hf_in, n1_in, w1, w0, vecs, xf_in, g_in, gp_in, n2_in, o_in, gr1, y_in,
    dh_o, e2_o, do_o, vgf, vgd, out1_o, outq_o, gr_o, yx,
    dmix, o, do, a, b, e2, g, gp, wqkv, wout, wfc2, wfc1, dhf, da, acc, gq, gr, got, gotq, acrq,
    sb, rb, sbq, rbq, out1, outq, part, mr, xr, sss, srs, gss, grs, lsem, ssem, oss, ors, osem, *rsems,
):
    col, dp = cfg["col"], cfg["dp"]
    me = Mesh(dp, cfg["tensor"])
    ga = Gather(me, dhf, gss, grs)
    sc = Scatter(me, part, mr, xr, sss, srs)
    half = sc.half
    loads = load(
        [
            (w1.at[:, col["qkv"] : col["fc1"]], wqkv),
            (dm_in, dmix),
            (hf_in, a),
            (e2_in, e2),
            (n1_in, b),
            (w0.at[:, col["out"] : col["end"]], wout),
            (w0.at[:, col["fc2"] : col["out"]], wfc2),
            (w0.at[:, col["fc1"] : col["fc2"]], wfc1),
            (g_in, g),
            (gp_in, gp),
            (o_in, o),
        ]
        + [(cf.at[ds(sc.own(n), half)], dhf.at[ds(sc.own(n), half)]) for n in range(2)],
        lsem,
    )
    gr_load = pltpu.make_async_copy(gr1, gr, lsem.at[13])
    holds = (me.s == 1) & (me.y == 1)

    @pl.when(holds)
    def _():
        gr_load.start()

    greet([me.mate, me.beside, me.across, me.across_mate] + me.ring)
    red1 = GradReduce(me, 1, gr1, gr, gr, got, sb, rb, out1, rsems[:6])
    redq = GradReduce(me, 1, gq, gq, gotq, acrq, sbq, rbq, outq, rsems[6:])
    st = Stores([(e2, e2_o), (do, do_o), (dhf, dh_o)], half, ssem)
    ys = OwnedOut(me, y_in, yx, 1, oss, ors, osem.at[0])
    red1.send()
    vgf[...] = jnp.zeros_like(vgf)
    vgd[...] = jnp.zeros_like(vgd)
    for c in loads[:4]:
        c.wait()

    def early():
        loads[4].wait()
        small = acc.at[:, 0 : 3 * HW]
        qkv_grad(b, dmix, small, half)
        store_low(small, gq)
        redq.send()
        ys.far().start()
        ys.start_here()

        @pl.when(holds)
        def _():
            gr_load.wait()

        red1.step(0)

    sc.run(lambda r0, i: back_tail(r0, half, dmix, a, e2, wqkv, vecs.at[1], part, vgf), early)
    acc[...] = jnp.zeros_like(acc)
    again = pltpu.make_async_copy(n2_in, b, lsem.at[14])
    again.start()
    for c in loads[5:]:
        c.wait()
    for d in range(1, dp // 2):
        red1.step(d)

    def write(n, i, value):
        dhf[ds(sc.own(n) + i * SUB, SUB), :] = value

    grad_out(sc, lambda n, i: dhf[ds(sc.own(n) + i * SUB, SUB), :], a, vecs.at[1], write, ga.start)
    other = pltpu.make_async_copy(xf_in, a, lsem.at[15])
    other.start()
    again.wait()
    other.wait()

    def work(r0, i):
        back_head(r0, half, dhf, a, g, gp, b, o, wfc1, wfc2, wout, vecs.at[0], do, e2, da, acc, vgd)
        st.start((0, 1, 2), r0, i)

        @pl.when(i == 1)
        def _():
            for d in range(dp // 2, dp - 1):
                red1.step(d)

        @pl.when(i == 3)
        def _():
            red1.step(dp - 1)

        @pl.when(i == 5)
        def _():
            redq.step(0)

    ga.run(work)
    for d in range(1, dp):
        redq.step(d)
    store_low(acc, gr)
    gr_out = pltpu.make_async_copy(gr, gr_o, lsem.at[0])
    gr_out.start()
    column_sum(sc, dhf, vgd, 2)
    red1.collect()
    redq.collect()
    outs = [pltpu.make_async_copy(out1, out1_o, lsem.at[1]), pltpu.make_async_copy(outq, outq_o, lsem.at[2])]
    for c in outs:
        c.start()
    red1.finish()
    redq.finish()
    sc.finish()
    st.finish()
    gr_out.wait()
    ys.wait()
    for c in outs:
        c.wait()


def layer_back(cfg, dmix, e2, cf, hf, n1, w1, w0, vecs, xf, g, gp, n2, o, gr1, y):
    seq, model = hf.shape
    ff, dp = cfg["ff"], cfg["dp"]
    rows, nr, nq = model // dp, 2 * ff + HW, 3 * HW
    wide, hidden, heads = pltpu.VMEM((seq, model), BF), pltpu.VMEM((seq, ff), BF), pltpu.VMEM((seq, HW), BF)
    return pl.pallas_call(
        functools.partial(back_kernel, cfg),
        out_shape=(
            sds((seq, model), BF),
            sds((seq, model), BF),
            sds((seq, HW), BF),
            sds((8, model), F32),
            sds((8, model), F32),
            sds((rows, nr), F32),
            sds((rows, nq), F32),
            sds((model, nr), BF),
            sds((2,) + y.shape, BF),
        ),
        in_specs=[ANY] * 7 + [VMEM] + [ANY] * 7,
        out_specs=(ANY, ANY, ANY, VMEM, VMEM, ANY, ANY, ANY, ANY),
        scratch_shapes=[
            pltpu.VMEM((seq, nq), BF), heads, heads, wide, wide, wide, hidden, hidden,
            pltpu.VMEM((model, nq), BF), pltpu.VMEM((model, HW), BF), pltpu.VMEM((model, ff), BF),
            pltpu.VMEM((model, ff), BF), wide, pltpu.VMEM((seq // 8, ff), BF), pltpu.VMEM((model, nr), F32),
            pltpu.VMEM((model, nq), BF), pltpu.VMEM((model, nr), BF), pltpu.VMEM((model, nr), BF),
            pltpu.VMEM((model, nq), BF), pltpu.VMEM((model, nq), BF),
            pltpu.VMEM((dp - 1, rows, nr), BF), pltpu.VMEM((dp - 1, rows, nr), BF),
            pltpu.VMEM((dp - 1, rows, nq), BF), pltpu.VMEM((dp - 1, rows, nq), BF),
            pltpu.VMEM((rows, nr), F32), pltpu.VMEM((rows, nq), F32),
        ]
        + scatter_scratch(seq, model)
        + [DMA((6,)), DMA((6,)), DMA((16,)), DMA((3, 8)), DMA((2,)), DMA((3,)), DMA((1,))]
        + GradReduce.scratch(dp) * 2,
        compiler_params=params(5),
        cost_estimate=cost(70),
        name="layer_back",
    )(dmix, e2, cf, hf, n1, w1, w0, vecs, xf, g, gp, n2, o, gr1, y)


def last_kernel(
    cfg, q_in, k_in, v_in, o_in, do_in, lse, srow, kcol, tab_in, e2_in, dh_in, xf_in, n1_in, w0, vecs, vf1, vd1, vd0,
    gr0, out1, outq, dhx, dxx, fq_o, fr_o, vec_o,
    q, k, v, o, do, tab, kt, dk, dv, dmix, dh, dx, xf, n1, e2, wqkv, gq, gotq, acrq, sbq, rbq, gr, got, sb, rb, fq, fr,
    vgf, va, vr, vout, part, mr, xr, sss, srs, lsem, vss, vrs, oss, ors, *rsems,
):
    col, heads, dp = cfg["col"], cfg["heads"], cfg["dp"]
    me = Mesh(dp, cfg["tensor"])
    sc = Scatter(me, part, mr, xr, sss, srs, 1 - me.y)
    half = sc.half
    seq = xf.shape[0]
    width = q.shape[1]
    own = [ds(sc.own(n), half) for n in range(2)]
    loads = load(
        [
            (k_in, k),
            (q_in, q),
            (v_in, v),
            (do_in, do),
            (o_in, o),
            (tab_in, tab),
            (w0.at[:, col["qkv"] : col["fc1"]], wqkv),
            (xf_in, xf),
            (e2_in, e2),
            (n1_in, n1),
        ]
        + [(dh_in.at[rr], dh.at[n]) for n, rr in enumerate(own)],
        lsem,
    )
    gr_load = pltpu.make_async_copy(gr0, gr, lsem.at[12])
    holds = (me.s == 0) & (me.y == 0)

    @pl.when(holds)
    def _():
        gr_load.start()

    greet([me.mate, me.beside, me.beside_mate, me.across, me.across_mate] + me.ring)
    redr = GradReduce(me, 0, gr0, gr, gr, got, sb, rb, fr, rsems[:6])
    redq = GradReduce(me, 0, gq, gq, gotq, acrq, sbq, rbq, fq, rsems[6:])
    vr_ = VectorReduce(me, va, vr, vss, vrs)
    redr.send()

    dh_over = push(dh_in.at[ds(me.py * 2 * half, 2 * half)], dhx, oss.at[2], ors.at[3], me.across)

    xs = OwnedOut(me, dx, dxx, 0, oss, ors, lsem.at[14])
    old = [pltpu.make_async_copy(out1, fr, lsem.at[15]), pltpu.make_async_copy(outq, fq, lsem.at[16])]

    @pl.when(me.s == 1)
    def _():
        for c in old:
            c.start()

    vgf[...] = jnp.zeros_like(vgf)
    dk[...] = jnp.zeros_like(dk)
    dv[...] = jnp.zeros_like(dv)
    loads[0].wait()
    turn_blocks(k, kt)
    for c in loads[1:6]:
        c.wait()

    @pl.when(holds)
    def _():
        gr_load.wait()

    n_blocks = seq // QB

    def qloop(i, _):
        lo = jnp.maximum(i - DOC_MAX // QB, 0)

        @pl.when((i == n_blocks // 2 + 1) & (me.s == 1))
        def _():
            dh_over.start()

        attn_bwd_block(i, lo, i, heads, q, k, v, o, do, kt, lse, srow, kcol, tab, dk, dv, dmix)
        for at_block, steps in (
            (n_blocks // 2 - 1, range(0, 1)),
            (n_blocks // 2, range(1, dp // 2)),
            (n_blocks // 2 + 1, range(dp // 2, dp - 1)),
            (n_blocks - 2, range(dp - 1, dp)),
        ):

            @pl.when(i == at_block)
            def _(steps=steps):
                for d in steps:
                    redr.step(d)

        return 0

    lax.fori_loop(0, n_blocks, qloop, 0)

    def close(i, _):
        ii = ds(i * QB, QB)
        dmix[ii, width : 2 * width] = turn_lanes(dk[ii, :], tab[ii, :], -1).astype(BF)
        dmix[ii, 2 * width : 3 * width] = dv[ii, :].astype(BF)
        return 0

    lax.fori_loop(0, n_blocks, close, 0)
    for c in loads[6:]:
        c.wait()

    def early():
        va[0, 0:8, :] = vgf[...] + vd0[...]
        va[0, 8:16, :] = vf1[...] + vd1[...]
        vr_.send(0)
        nf = gq.shape[0]
        accs = [dk.at[0:nf], dk.at[nf : 2 * nf], dv.at[0:nf]]
        for acc in accs:
            acc[...] = jnp.zeros_like(acc)

        def body(i, _):
            rows = ds(i * half, half)
            n1t = n1[rows, :].T
            for p, acc in enumerate(accs):
                acc[...] += dot(n1t, dmix[rows, p * HW : (p + 1) * HW])
            return 0

        lax.fori_loop(0, 8, body, 0)
        for p, acc in enumerate(accs):
            gq[:, p * HW : (p + 1) * HW] = acc[...].astype(BF)
        vr_.add(0, va.at[1])
        vr_.send(1)
        redq.send()
        vr_.add(1, va.at[2])
        vr_.send(2)
        redq.step(0)

    sc.run(lambda r0, i: back_tail(r0, half, dmix, xf, e2, wqkv, vecs.at[0], part, vgf), early)
    for d in range(1, dp - 1):
        redq.step(d)

    def write(n, i, value):
        dx[sc.side(n), ds(i * SUB, SUB), :] = value

    def leave(n):
        if n == 0:
            xs.far().start()
        else:
            xs.start_here()

    grad_out(sc, lambda n, i: dh[sc.side(n), ds(i * SUB, SUB), :], xf, vecs.at[0], write, leave)
    redq.step(dp - 1)
    vr_.add(2, vout)
    vec_o[...] = jnp.where(me.s == 0, vout[0:8, :], vout[8:16, :])
    redr.collect()
    redq.collect()

    @pl.when(me.s == 1)
    def _():
        for c in old:
            c.wait()

    ends = [pltpu.make_async_copy(fr, fr_o, lsem.at[0]), pltpu.make_async_copy(fq, fq_o, lsem.at[1])]
    for c in ends:
        c.start()
    redr.finish()
    redq.finish()
    vr_.finish()
    sc.finish()
    @pl.when(me.s == 1)
    def _():
        dh_over.wait()

    xs.wait()
    for c in ends:
        c.wait()


def layer_last(cfg, q, k, v, o, do, lse, sr, kc, tab, e2, dh, xf, n1, w0, vecs, vf1, vd1, vd0, gr0, out1, outq):
    seq, model = xf.shape
    dp, tensor, ff = cfg["dp"], cfg["tensor"], cfg["ff"]
    rows, nr, nq = model // dp, 2 * ff + HW, 3 * HW
    nv = dp + tensor - 1
    wide, owned, heads = pltpu.VMEM((seq, model), BF), pltpu.VMEM((2, seq // 8, model), BF), pltpu.VMEM((seq, HW), BF)
    return pl.pallas_call(
        functools.partial(last_kernel, cfg),
        out_shape=(sds((seq // 4, model), BF), sds((2, 2, seq // 8, model), BF), sds((rows, nq), F32), sds((rows, nr), F32), sds((8, model), F32)),
        in_specs=[ANY] * 5 + [VMEM] * 3 + [ANY] * 6 + [VMEM] * 4 + [ANY] * 3,
        out_specs=(ANY, ANY, ANY, ANY, VMEM),
        scratch_shapes=[
            heads, heads, heads, heads, heads, pltpu.VMEM(tab.shape, F32), pltpu.VMEM((HW, seq), BF),
            pltpu.VMEM((seq, HW), F32), pltpu.VMEM((seq, HW), F32), pltpu.VMEM((seq, nq), BF), owned, owned,
            wide, wide, wide, pltpu.VMEM((model, nq), BF),
            pltpu.VMEM((model, nq), BF), pltpu.VMEM((model, nq), BF), pltpu.VMEM((model, nq), BF),
            pltpu.VMEM((dp - 1, rows, nq), BF), pltpu.VMEM((dp - 1, rows, nq), BF),
            pltpu.VMEM((model, nr), BF), pltpu.VMEM((model, nr), BF),
            pltpu.VMEM((dp - 1, rows, nr), BF), pltpu.VMEM((dp - 1, rows, nr), BF),
            pltpu.VMEM((rows, nq), F32), pltpu.VMEM((rows, nr), F32),
            pltpu.VMEM((8, model), F32), pltpu.VMEM((3, 16, model), F32), pltpu.VMEM((nv, 16, model), F32),
            pltpu.VMEM((16, model), F32),
        ]
        + scatter_scratch(seq, model)
        + [DMA((17,)), DMA((nv,)), DMA((nv,)), DMA((3,)), DMA((4,))]
        + GradReduce.scratch(dp) * 2,
        compiler_params=params(6),
        cost_estimate=cost(80),
        name="layer_last",
    )(q, k, v, o, do, lse, sr, kc, tab, e2, dh, xf, n1, w0, vecs, vf1, vd1, vd0, gr0, out1, outq)


def finish_kernel(
    cfg, hf, hx, yx, dhf, dhx, dxx, fq_in, fr_in, vec, so, ig, bg1, bb1, gqkv, bqkv, gout, bdy, bdy2, bg2, bb2, gfc1, bfc1, gfc2,
    a, b, fq, fr, lsem, msem, osem,
):
    heads, ff, own, qw, fw = cfg["heads"], cfg["ff"], cfg["own"], cfg["qw"], cfg["fw"]
    me = Mesh(cfg["dp"], cfg["tensor"])
    loads = load([(fr_in, fr), (fq_in, fq)], lsem)
    half = a.shape[2]
    mine = [ref.at[pl.ds(pl.multiple_of((2 * me.t + n) * half, half), half)] for ref in (hf, dhf) for n in range(2)]

    def sources(core):
        if core == 0:
            first, second = [mine[0:2], [hx.at[pl.ds(n * half, half)] for n in range(2)]], None
        else:
            first, second = None, [mine[2:4], [dhx.at[pl.ds(n * half, half)] for n in range(2)]]
        whole = yx if core else dxx
        third = [[whole.at[me.y, n] for n in range(2)], [whole.at[1 - me.y, n] for n in range(2)]]
        return (first or third), (second or third)

    def moves(core):
        out = []
        for o, (ref, src) in enumerate(zip((a, b), sources(core))):
            for m in range(2):
                for n in range(2):
                    dst = ref.at[me.y if m == 0 else 1 - me.y, n]
                    out.append(pltpu.make_async_copy(src[m][n], dst, msem.at[4 * o + 2 * m + n]))
        return out

    for core in range(2):

        @pl.when(me.s == core)
        def _(core=core):
            for c in moves(core):
                c.start()

    model = vec.shape[1]
    short = pltpu.roll(vec[...], (model - (me.z * me.tensor + me.t) * own) % model, 1)
    for row, ref in ((0, bg1), (1, bb1), (2, bdy), (2, bdy2), (3, bg2), (4, bb2)):
        ref[...] = short[row : row + 1, 0:own]
    for h in range(heads):
        parts = [vec[6:7, p * HW + h * HD : p * HW + (h + 1) * HD] for p in range(3)]
        one = jnp.concatenate(parts + [jnp.zeros((1, HW - 3 * HD), F32)], axis=1)
        one = jnp.broadcast_to(one, (8, HW))
        bqkv[h] = pltpu.roll(one, (HW - me.z * qw) % HW, 1)[0:1, 0:qw]
        wide = ff // heads
        one = jnp.broadcast_to(vec[7:8, h * wide : (h + 1) * wide], (8, wide))
        bfc1[h] = pltpu.roll(one, (wide - me.z * fw) % wide, 1)[0:1, 0:fw]
    loads[0].wait()
    gfc1[0] = fr[:, 0:ff]
    gfc2[...] = fr[:, ff : 2 * ff]
    gout[0] = fr[:, 2 * ff : 2 * ff + HW].T[0 : heads * HD, :]
    for core in range(2):

        @pl.when(me.s == core)
        def _(core=core):
            for c in moves(core):
                c.wait()

    outs = []
    for o, (ref, dst) in enumerate(((a, so), (b, ig))):
        for m in range(2):
            for n in range(2):
                place = dst.at[0, m, 0, pl.ds(n * half, half)]
                outs.append(pltpu.make_async_copy(ref.at[m, n], place, osem.at[4 * o + 2 * m + n]))
    for c in outs:
        c.start()
    loads[1].wait()
    pieces = [fq[:, p * HW + h * HD : p * HW + (h + 1) * HD] for h in range(heads) for p in range(3)]
    gqkv[0] = jnp.concatenate(pieces, axis=1)
    for c in outs:
        c.wait()


def finish(cfg, hf, hx, yx, dhf, dhx, dxx, fq, fr, vec):
    heads, ff, rows = cfg["heads"], cfg["ff"], fq.shape[0]
    line = sds((1, cfg["own"]), F32)
    both = sds((1, 2, 1) + hx.shape, BF)
    return pl.pallas_call(
        functools.partial(finish_kernel, cfg),
        out_shape=(both, both, line, line, sds((1, rows, heads * 3 * HD), F32),
                   sds((heads, 1, cfg["qw"]), F32), sds((1, heads * HD, rows), F32), line, line, line, line,
                   sds((1, rows, ff), F32), sds((heads, 1, cfg["fw"]), F32), sds((rows, ff), F32)),
        in_specs=[ANY] * 8 + [VMEM],
        out_specs=(ANY, ANY) + (VMEM,) * 12,
        scratch_shapes=[
            pltpu.VMEM(yx.shape, BF), pltpu.VMEM(yx.shape, BF), pltpu.VMEM(fq.shape, F32), pltpu.VMEM(fr.shape, F32),
            DMA((2,)), DMA((8,)), DMA((8,)),
        ],
        compiler_params=pltpu.CompilerParams(vmem_limit_bytes=67043328),
        cost_estimate=cost(5),
        name="finish",
    )(hf, hx, yx, dhf, dhx, dxx, fq, fr, vec)


def by_part(w):
    rows = w.shape[0]
    heads = w.shape[1] // (3 * HD)
    w = w.reshape(rows, heads, 3, HD).transpose(0, 2, 1, 3).reshape(rows, 3, heads * HD)
    return jnp.pad(w, ((0, 0), (0, 0), (0, HW - heads * HD))).reshape(rows, 3 * HW)


def shards(
    dp, tensor, inputs, cotangent, segments, live_blocks, ln1_gain, ln1_bias, qkv_weight, qkv_bias,
    out_weight, out_bias, ln2_gain, ln2_bias, fc1_weight, fc1_bias, fc2_weight, fc2_bias,
):
    live_blocks = live_blocks.T
    model = inputs.shape[-1]
    ff = fc1_weight.shape[2]
    heads = qkv_bias.shape[1]
    col = columns(model, ff)
    wout = jnp.pad(out_weight[0].T, ((0, 0), (0, HW - heads * HD)))
    w = jnp.concatenate([by_part(qkv_weight[0]), fc1_weight[0], fc2_weight[0].T, wout], axis=1)
    small = jnp.stack([ln1_gain[0], ln1_bias[0], out_bias[0], ln2_gain[0], ln2_bias[0], fc2_bias[0]])

    def lanes(a):
        return jnp.pad(a.astype(F32), ((0, 0), (0, 128 - a.shape[1])))

    sv = jnp.concatenate([lanes(small), lanes(qkv_bias[0]), lanes(fc1_bias[0])], axis=0)
    sv = jnp.pad(sv, ((0, -sv.shape[0] % 8), (0, 0)))
    fr = np.float32(10000.0) ** (-(np.arange(ROT // 2, dtype=np.float32) * np.float32(2.0 / ROT)))
    fr = jnp.asarray(np.broadcast_to(fr[:, None], (ROT // 2, 128)).astype(np.float32))
    cfg = {
        "col": col, "ff": ff, "heads": heads, "dp": dp, "tensor": tensor, "own": small.shape[1],
        "qw": qkv_bias.shape[2], "fw": fc1_bias.shape[2],
        "groups": [(0, col["fc1"]), (col["fc1"], col["fc2"]), (col["fc2"], col["out"]), (col["out"], col["end"])],
    }

    xf, n1a, n2a, ga, gpa, tab, w0, qa, ka, va, cf, vecs, sr, kc = layer_in(
        cfg, inputs, cotangent, segments, live_blocks, w, sv, fr
    )
    oa, lsea, hf, n1b, n2b, gb, gpb, w1, qb, kb, vb = layer_mid(cfg, qa, ka, va, sr, kc, ga, xf, w, w0, vecs, tab)
    ob, lseb = attn_fwd(heads, segments, live_blocks, qb, kb, vb, sr, kc)
    y, dob, e2b, grb, hx, vdb = layer_turn(cfg, ob, gb, hf, cf, w1, vecs, n2b, gpb)
    dmb = attn_bwd(heads, segments, live_blocks, qb, kb, vb, ob, dob, lseb, sr, kc, tab)
    dhf, e2a, doa, vfb, vda, out1, outq, gra, yx = layer_back(
        cfg, dmb, e2b, cf, hf, n1b, w1, w0, vecs, xf, ga, gpa, n2a, oa, grb, y
    )
    dhx, dxx, fq, fr_, gv = layer_last(
        cfg, qa, ka, va, oa, doa, lsea, sr, kc, tab, e2a, dhf, xf, n1a, w0, vecs, vfb, vdb, vda, gra, out1, outq
    )
    last_part = finish(cfg, hf, hx, yx, dhf, dhx, dxx, fq, fr_, gv)
    so, ig, bg1, bb1, gqkv, bqkv, gout, bdy, bdy2, bg2, bb2, gfc1, bfc1, gfc2 = last_part
    bqkv, bfc1, gfc2 = bqkv.transpose(1, 0, 2), bfc1.transpose(1, 0, 2), gfc2.T[None]
    return (so, ig, bg1, bb1, gqkv, bqkv, gout, bdy, bg2, bb2, gfc1, bfc1, gfc2, bdy2)


def solution(mesh):
    both = ("dp", "tensor")
    in_specs = (
        P(None, "dp", "tensor", None),
        P(None, "dp", "tensor", None),
        P(None, "dp", None),
        P(None, "dp"),
        P("section", both),
        P("section", both),
        P("section", "dp", "tensor"),
        P("section", "tensor", "dp"),
        P("section", "tensor", "dp"),
        P("section", both),
        P("section", both),
        P("section", both),
        P("section", "dp", "tensor"),
        P("section", "tensor", "dp"),
        P("section", "tensor", "dp"),
        P("section", both),
    )
    out_specs = (
        P("section", None, "dp", "tensor", None),
        P("section", None, "dp", "tensor", None),
        P("section", both),
        P("section", both),
        P("section", "dp", "tensor"),
        P("section", "tensor", "dp"),
        P("section", "tensor", "dp"),
        P("section", both),
        P("section", both),
        P("section", both),
        P("section", "dp", "tensor"),
        P("section", "tensor", "dp"),
        P("section", "tensor", "dp"),
        P("section", both),
    )
    body = functools.partial(shards, mesh.shape["dp"], mesh.shape["tensor"])
    return jax.shard_map(body, mesh=mesh, in_specs=in_specs, out_specs=out_specs, check_vma=False)
```

```python
import functools

import jax
import jax.numpy as jnp
import numpy as np
from jax import lax
from jax.experimental import pallas as pl
from jax.experimental.pallas import tpu as pltpu
from jax.sharding import PartitionSpec as P

F32 = jnp.float32
BF = jnp.bfloat16
MESH = pl.DeviceIdType.MESH
HD = 64
ROT = 16
LIVE = 128
DOCS = 4
DOC_MAX = 1024
QB = 256
HW = 256
SUB = 256
EPS = 1e-05
NEG = -1e30
VMEM = pl.BlockSpec(memory_space=pltpu.VMEM)
ANY = pl.BlockSpec(memory_space=pltpu.HBM)
SMEM = pl.BlockSpec(memory_space=pltpu.SMEM)
DMA = pltpu.SemaphoreType.DMA


def sds(shape, dtype):
    return jax.ShapeDtypeStruct(shape, dtype)


def dg(a, b, ca, cb):
    return lax.dot_general(a, b, (((ca,), (cb,)), ((), ())), preferred_element_type=F32)


def dot(a, b):
    return jnp.dot(a, b, preferred_element_type=F32)


def ds(start, size):
    return pl.ds(pl.multiple_of(start, size), size)


def norm_stats(x):
    mu = jnp.mean(x, axis=-1, keepdims=True)
    xc = x - mu
    var = jnp.mean(xc * xc, axis=-1, keepdims=True)
    return xc, lax.rsqrt(var + EPS)


def head_lanes(width, heads):
    lane = lax.broadcasted_iota(jnp.int32, (1, width), 1)
    return [(lane >= h * HD) & (lane < (h + 1) * HD) for h in range(heads)]


def allow_mask(kc, sq, diag):
    m = kc == sq
    if diag:
        r = lax.broadcasted_iota(jnp.int32, (QB, QB), 0)
        c = lax.broadcasted_iota(jnp.int32, (QB, QB), 1)
        m = (m & (r <= c)) | (r == c)
    return m


def block_bounds(seg, live, i, n):
    s = lax.axis_index("tensor") // 2
    doc = seg[s, 0, i * QB]

    def body(j, count):
        return count + jnp.where((j < i) & (seg[s, 0, (j + 1) * QB - 1] == doc), 1, 0)

    hi = jnp.minimum(i, (live[0, s] * LIVE + QB - 1) // QB)
    return jnp.minimum(i - lax.fori_loop(0, n, body, 0), hi), hi


def turn_blocks(src, dst):
    def turn(i, _):
        dst[:, ds(i * QB, QB)] = src[ds(i * QB, QB), :].T
        return 0

    lax.fori_loop(0, src.shape[0] // QB, turn, 0)


def attn_fwd_block(i, lo, hi, heads, q_ref, k_ref, vt, sr_ref, kc_ref, s_scr, o_ref, lse_ref):
    width = q_ref.shape[1]
    qi = ds(i * QB, QB)
    q = q_ref[qi, :]
    qm = [jnp.where(m, q, jnp.zeros_like(q)) for m in head_lanes(width, heads)]
    sq = sr_ref[0:1, qi]

    def scores(j, slot, ms, diag):
        kj = ds(j * QB, QB)
        k = k_ref[kj, :]
        mask = allow_mask(kc_ref[kj, 0:1], sq, diag)
        out = []
        for h in range(heads):
            s = jnp.where(mask, dg(k, qm[h], 1, 1), NEG)
            s_scr[h, ds(slot * QB, QB), :] = s
            out.append(jnp.maximum(ms[h], jnp.max(s, axis=0, keepdims=True)))
        return tuple(out)

    ms = tuple(jnp.full((1, QB), NEG, F32) for _ in range(heads))
    ms = scores(i, 0, ms, True)
    ms = lax.fori_loop(lo, hi, lambda j, ms: scores(j, j - lo + 1, ms, False), ms)

    def weigh(j, slot, st):
        kj = ds(j * QB, QB)
        out = []
        for h in range(heads):
            total, acc = st[h]
            p = jnp.exp(s_scr[h, ds(slot * QB, QB), :] - ms[h])
            total = total + jnp.sum(p, axis=0, keepdims=True)
            acc = acc + dot(vt[h * HD : (h + 1) * HD, kj], p.astype(BF))
            out.append((total, acc))
        return tuple(out)

    st = tuple((jnp.zeros((1, QB), F32), jnp.zeros((HD, QB), F32)) for _ in range(heads))
    st = weigh(i, 0, st)
    st = lax.fori_loop(lo, hi, lambda j, st: weigh(j, j - lo + 1, st), st)
    ot = [st[h][1] * (1.0 / st[h][0]) for h in range(heads)]
    ot = jnp.concatenate(ot + [jnp.zeros((width - heads * HD, QB), F32)], axis=0)
    o_ref[qi, :] = ot.T.astype(BF)
    lse = [ms[h] + jnp.log(st[h][0]) for h in range(heads)]
    lse_ref[:, qi] = jnp.concatenate(lse + [jnp.zeros((8 - heads, QB), F32)], axis=0)


def attn_fwd_kernel(heads, seg, live, q_in, k_in, v_in, sr_ref, kc_ref, o_out, lse_ref, q, k, v, o, vt, s_scr, lsem, osem):
    n = q.shape[0] // QB
    loads = load([(v_in, v), (q_in, q), (k_in, k)], lsem)
    loads[0].wait()
    turn_blocks(v, vt)
    loads[1].wait()
    loads[2].wait()

    def out(i):
        rows = ds(i * QB, QB)
        return pltpu.make_async_copy(o.at[rows], o_out.at[rows], osem.at[i])

    def qloop(i, _):
        lo, hi = block_bounds(seg, live, i, n)
        attn_fwd_block(i, lo, hi, heads, q, k, vt, sr_ref, kc_ref, s_scr, o, lse_ref)
        out(i).start()
        return 0

    lax.fori_loop(0, n, qloop, 0)

    def drain(i, _):
        out(i).wait()
        return 0

    lax.fori_loop(0, n, drain, 0)


def attn_fwd(heads, seg, live, q, k, v, sr, kc):
    rows, width = q.shape
    buf = pltpu.VMEM((rows, width), BF)
    return pl.pallas_call(
        functools.partial(attn_fwd_kernel, heads),
        out_shape=(sds((rows, width), BF), sds((8, rows), F32)),
        in_specs=[SMEM, SMEM, ANY, ANY, ANY, VMEM, VMEM],
        out_specs=(ANY, VMEM),
        scratch_shapes=[buf, buf, buf, buf, pltpu.VMEM((width, rows), BF), pltpu.VMEM((heads, rows + QB, QB), F32),
                        DMA((3,)), DMA((rows // QB,))],
        compiler_params=pltpu.CompilerParams(vmem_limit_bytes=67043328),
        cost_estimate=cost(12),
        name="attn_fwd",
    )(seg, live, q, k, v, sr, kc)


def turn_lanes(x, tab, sign):
    width = x.shape[1]
    c, sn = [jnp.concatenate([tab[:, a * 128 : (a + 1) * 128]] * (width // 128), axis=1) for a in range(2)]
    lane = lax.broadcasted_iota(jnp.int32, (1, width), 1) % HD
    moved = jnp.where(lane < ROT // 2, pltpu.roll(x, width - ROT // 2, 1), pltpu.roll(x, ROT // 2, 1)) * sn
    return x * c + moved if sign > 0 else x * c - moved


def attn_bwd_block(i, lo, hi, heads, q_ref, k_ref, v_ref, o_ref, do_ref, kt, lse_ref, sr_ref, kc_ref, tab, dk, dv, out):
    width = q_ref.shape[1]
    hm = head_lanes(width, heads)
    rowid = lax.broadcasted_iota(jnp.int32, (8, width), 0)
    lane = lax.broadcasted_iota(jnp.int32, (8, width), 1)
    sel = ((lane >= rowid * HD) & (lane < (rowid + 1) * HD)).astype(F32).astype(BF)
    qi = ds(i * QB, QB)
    q = q_ref[qi, :]
    do = do_ref[qi, :]
    z = jnp.zeros_like(q)
    qm = [jnp.where(hm[h], q, z) for h in range(heads)]
    dom = [jnp.where(hm[h], do, z) for h in range(heads)]
    qcat = jnp.concatenate(qm, axis=0)
    docat = jnp.concatenate(dom, axis=0)
    prod = do.astype(F32) * o_ref[qi, :].astype(F32)
    high = prod.astype(BF)
    low = (prod - high.astype(F32)).astype(BF)
    delta = dg(sel, high, 1, 1) + dg(sel, low, 1, 1)
    lse = lse_ref[:, qi]
    sq = sr_ref[0:1, qi]

    def step(j, dqs, diag):
        kj = ds(j * QB, QB)
        k = k_ref[kj, :]
        v = v_ref[kj, :]
        mask = allow_mask(kc_ref[kj, 0:1], sq, diag)
        ps, dss, res = [], [], []
        for h in range(heads):
            s = dg(k, qm[h], 1, 1)
            dp = dg(v, dom[h], 1, 1)
            p = jnp.exp(jnp.where(mask, s - lse[h : h + 1, :], NEG))
            score_grad = (p * (dp - delta[h : h + 1, :])).astype(BF)
            ps.append(p.astype(BF))
            dss.append(score_grad)
            res.append(dqs[h] + dot(kt[h * HD : (h + 1) * HD, kj], score_grad))
        dv[kj, :] += dot(jnp.concatenate(ps, axis=1), docat)
        dk[kj, :] += dot(jnp.concatenate(dss, axis=1), qcat)
        return tuple(res)

    dqs = tuple(jnp.zeros((HD, QB), F32) for _ in range(heads))
    dqs = step(i, dqs, True)
    dqs = lax.fori_loop(lo, hi, lambda j, d: step(j, d, False), dqs)
    dq = jnp.concatenate(list(dqs) + [jnp.zeros((width - heads * HD, QB), F32)], axis=0).T * 0.125
    out[qi, 0:width] = turn_lanes(dq, tab[qi, :], -1).astype(BF)


def attn_bwd_kernel(
    heads, seg, live, q_in, k_in, v_in, o_in, do_in, lse_ref, sr_ref, kc_ref, tab_in, out_ref,
    q, k, v, o, do, tab, out, kt, dk, dv, lsem, osem,
):
    rows, width = q.shape
    n = rows // QB
    loads = load([(k_in, k), (q_in, q), (v_in, v), (do_in, do), (o_in, o), (tab_in, tab)], lsem)
    dk[...] = jnp.zeros_like(dk)
    dv[...] = jnp.zeros_like(dv)
    loads[0].wait()
    turn_blocks(k, kt)
    for c in loads[1:]:
        c.wait()

    def qloop(i, _):
        lo, hi = block_bounds(seg, live, i, n)
        attn_bwd_block(i, lo, hi, heads, q, k, v, o, do, kt, lse_ref, sr_ref, kc_ref, tab, dk, dv, out)
        return 0

    lax.fori_loop(0, n, qloop, 0)

    def leave(i):
        rr = ds(i * QB, QB)
        return pltpu.make_async_copy(out.at[rr], out_ref.at[rr], osem.at[i])

    def finish(i, _):
        ii = ds(i * QB, QB)
        out[ii, width : 2 * width] = turn_lanes(dk[ii, :], tab[ii, :], -1).astype(BF)
        out[ii, 2 * width : 3 * width] = dv[ii, :].astype(BF)
        leave(i).start()
        return 0

    lax.fori_loop(0, n, finish, 0)

    def drain(i, _):
        leave(i).wait()
        return 0

    lax.fori_loop(0, n, drain, 0)


def attn_bwd(heads, seg, live, q, k, v, o, do, lse, sr, kc, tab):
    rows, width = q.shape
    buf = pltpu.VMEM((rows, width), BF)
    return pl.pallas_call(
        functools.partial(attn_bwd_kernel, heads),
        out_shape=sds((rows, 3 * width), BF),
        in_specs=[SMEM, SMEM] + [ANY] * 5 + [VMEM] * 3 + [ANY],
        out_specs=ANY,
        scratch_shapes=[buf, buf, buf, buf, buf, pltpu.VMEM(tab.shape, F32), pltpu.VMEM((rows, 3 * width), BF),
                        pltpu.VMEM((width, rows), BF), pltpu.VMEM((rows, width), F32), pltpu.VMEM((rows, width), F32),
                        DMA((6,)), DMA((rows // QB,))],
        compiler_params=pltpu.CompilerParams(vmem_limit_bytes=67043328),
        cost_estimate=cost(26),
        name="attn_bwd",
    )(seg, live, q, k, v, o, do, lse, sr, kc, tab)


class Mesh:
    def __init__(self, dp, tensor):
        self.dp, self.tensor = dp, tensor
        self.s, self.z, self.t = lax.axis_index("section"), lax.axis_index("dp"), lax.axis_index("tensor")
        self.x, self.y = self.t % 2, self.t // 2
        self.px, self.py = 2 * self.y + (1 - self.x), 2 * (1 - self.y) + self.x
        self.mate = {"section": 1 - self.s}
        self.beside = {"tensor": self.px}
        self.beside_mate = {"tensor": self.px, "section": 1 - self.s}
        self.across = {"tensor": self.py}
        self.across_mate = {"tensor": self.py, "section": 1 - self.s}
        self.ring = [{"dp": (self.z + d) % dp} for d in range(1, dp)]
        self.group = [{"tensor": (self.t + d) % tensor} for d in range(1, tensor)]
        self.quarter = 2 * self.s + self.x

    def across_core(self, core):
        return {"tensor": self.py, "section": core}


def greet(peers):
    bar = pltpu.get_barrier_semaphore()
    for peer in peers:
        pl.semaphore_signal(bar, inc=1, device_id=peer, device_id_type=MESH)
    pl.semaphore_wait(bar, len(peers))


def push(src, dst, ssem, rsem, peer):
    return pltpu.make_async_remote_copy(
        src_ref=src, dst_ref=dst, send_sem=ssem, recv_sem=rsem, device_id=peer, device_id_type=MESH
    )


def pick(i, values):
    out = values[-1]
    for n in range(len(values) - 2, -1, -1):
        out = jnp.where(i == n, values[n], out)
    return out


class Tokens:
    def __init__(self, me, seq):
        self.me, self.half = me, seq // 8

    def start_of(self, a, b, h):
        return (4 * a + 2 * b + h) * self.half

    def rows(self, a, b, h):
        return ds(self.start_of(a, b, h), self.half)

    def own(self, a):
        return self.start_of(a, self.me.x, self.me.s)


class Gather(Tokens):
    def __init__(self, me, full, ssem, rsem, first=0):
        super().__init__(me, full.shape[0])
        self.full, self.ssem, self.rsem, self.first = full, ssem, rsem, first

    def side(self, n):
        return self.first if n == 0 else 1 - self.first

    def plan(self, i):
        me, a = self.me, self.side(i % 2)
        ref = self.full.at[self.rows(a, (1 - me.x) if i >= 4 else me.x, me.s)]
        return push(ref, ref, self.ssem.at[i], self.rsem.at[i], me.beside if i in (2, 3) else me.mate)

    def start(self, n):
        self.plan(n).start()
        self.plan(2 + n).start()

    def order(self, i):
        me = self.me
        a = pick(i, [self.side(n) for n in (0, 1, 0, 1, 0, 0, 1, 1)])
        b = jnp.where(i < 4, me.x, 1 - me.x)
        h = pick(i, [me.s, me.s, 1 - me.s, 1 - me.s, me.s, 1 - me.s, me.s, 1 - me.s])
        return self.start_of(a, b, h)

    def step(self, i):
        if i in (2, 3):
            self.plan(i - 2).wait_recv()
        if i in (4, 6):
            n = i // 2 - 2
            self.plan(2 + n).wait_recv()
            self.plan(4 + n).start()
        if i in (5, 7):
            self.plan(4 + i // 2 - 2).wait_recv()

    def arrive(self, i):
        for n in range(2, 8):

            @pl.when(i == n)
            def _(n=n):
                self.step(n)

    def finish(self):
        for i in range(6):
            self.plan(i).wait_send()

    def run(self, work):
        def body(i, _):
            self.arrive(i)
            work(self.order(i), i)
            return 0

        lax.fori_loop(0, 8, body, 0)
        self.finish()


class Scatter(Tokens):
    def __init__(self, me, part, mr, xr, ssem, rsem, first=0):
        super().__init__(me, part.shape[0])
        self.part, self.mr, self.xr, self.ssem, self.rsem, self.first = part, mr, xr, ssem, rsem, first

    def side(self, n):
        return self.first if n == 0 else 1 - self.first

    def plan(self, i):
        me = self.me
        if i < 4:
            b = (1 - me.x) if i < 2 else me.x
            src, dst, peer = self.rows(self.side(i % 2), b, 1 - me.s), self.mr.at[i], me.mate
        else:
            src, dst, peer = self.rows(self.side(i - 4), 1 - me.x, me.s), self.xr.at[i - 4], me.beside
        return push(self.part.at[src], dst, self.ssem.at[i], self.rsem.at[i], peer)

    def run(self, work, early=None):
        me = self.me

        def body(i, _):
            k = i // 2
            b = jnp.where(k < 2, 1 - me.x, me.x)
            h = jnp.where(i % 2 == 0, 1 - me.s, me.s)
            work(self.start_of(jnp.where(k % 2 == 0, self.side(0), self.side(1)), b, h), i)
            for n in range(4):

                @pl.when(i == 2 * n)
                def _(n=n):
                    self.plan(n).start()

            for n in range(2):

                @pl.when(i == 2 * n + 1)
                def _(n=n):
                    self.plan(n).wait_recv()
                    base = self.start_of(self.side(n), 1 - me.x, me.s)

                    def add(j, _):
                        rr = ds(base + j * SUB, SUB)
                        got = self.mr[n, ds(j * SUB, SUB), :].astype(F32)
                        self.part[rr, :] = (self.part[rr, :].astype(F32) + got).astype(BF)
                        return 0

                    lax.fori_loop(0, self.half // SUB, add, 0)
                    self.plan(4 + n).start()

            return 0

        lax.fori_loop(0, 8, body, 0)
        if early is not None:
            early()

    def arrive(self, n):
        self.plan(2 + n).wait_recv()
        self.plan(4 + n).wait_recv()

    def total(self, n, i):
        rr = ds(self.own(self.side(n)) + i * SUB, SUB)
        sub = ds(i * SUB, SUB)
        return self.part[rr, :].astype(F32) + self.mr[2 + n, sub, :].astype(F32) + self.xr[n, sub, :].astype(F32)

    def finish(self):
        for i in range(6):
            self.plan(i).wait_send()


def scatter_scratch(rows, width):
    half = rows // 8
    return [
        pltpu.VMEM((rows, width), BF),
        pltpu.VMEM((4, half, width), BF),
        pltpu.VMEM((2, half, width), BF),
        DMA((6,)),
        DMA((6,)),
    ]


class WeightGather:
    def __init__(self, me, layer, shard, full, gat, groups, sems):
        self.me, self.layer, self.shard, self.full, self.gat, self.groups = me, layer, shard, full, gat, groups
        self.own, self.wss, self.wrs, self.fss, self.frs, self.yss, self.yrs = sems
        self.rows = shard.shape[0]
        self.collects = me.s == layer
        self.keeps = me.y == layer

    def block(self, ref, zz, g):
        a, b = self.groups[g]
        return ref.at[ds(zz * self.rows, self.rows), a:b]

    def mine(self, g):
        a, b = self.groups[g]
        return self.shard.at[:, a:b]

    def local(self, g):
        return pltpu.make_async_copy(self.mine(g), self.block(self.full, self.me.z, g), self.own.at[g])

    def out(self, g, d, ref):
        dst = self.block(ref, self.me.z, g)
        return push(self.mine(g), dst, self.wss.at[g, d], self.wrs.at[g, d], self.me.ring[d])

    def hand(self, g, d, ref, across):
        zz = (self.me.z + self.me.dp - d) % self.me.dp
        src = self.mine(g) if d == 0 else self.block(ref, zz, g)
        ss, rs = (self.yss, self.yrs) if across else (self.fss, self.frs)
        peer = self.me.across_core(self.me.y) if across else self.me.mate
        return push(src, self.block(self.full, zz, g), ss.at[g, d], rs.at[g, d], peer)

    def both(self, do):
        @pl.when(self.collects & self.keeps)
        def _():
            do(self.full, True)

        @pl.when(self.collects & jnp.logical_not(self.keeps))
        def _():
            do(self.gat, False)

    def send_ring(self):
        def do(ref, keeps):
            for g in range(len(self.groups)):
                for d in range(self.me.dp - 1):
                    self.out(g, d, ref).start()

        self.both(do)

    def send_own(self, g):
        def do(ref, keeps):
            self.hand(g, 0, ref, True).start()
            if keeps:
                self.local(g).start()
            else:
                self.hand(g, 0, ref, False).start()

        self.both(do)

    def forward(self, g, blocks=None):
        def do(ref, keeps):
            for d in range(self.me.dp - 1) if blocks is None else blocks:
                self.out(g, d, ref).wait_recv()
                self.hand(g, d + 1, ref, True).start()
                if not keeps:
                    self.hand(g, d + 1, ref, False).start()

        self.both(do)

    def ready(self, g):
        me = self.me

        @pl.when(self.collects & self.keeps)
        def _():
            self.local(g).wait()

        @pl.when(me.s != me.y)
        def _():
            for d in range(me.dp):
                self.hand(g, d, self.full, True).wait_recv()

        @pl.when((me.s == me.y) & jnp.logical_not(self.collects))
        def _():
            for d in range(me.dp):
                self.hand(g, d, self.full, False).wait_recv()

    def finish(self):
        def do(ref, keeps):
            for g in range(len(self.groups)):
                for d in range(self.me.dp - 1):
                    self.out(g, d, ref).wait_send()
                for d in range(self.me.dp):
                    self.hand(g, d, ref, True).wait_send()
                    if not keeps:
                        self.hand(g, d, ref, False).wait_send()

        self.both(do)

    @staticmethod
    def scratch(dp, n):
        return [DMA((n,)), DMA((n, dp - 1)), DMA((n, dp - 1))] + [DMA((n, dp))] * 4


class GradReduce:
    def __init__(self, me, layer, src, mine, got, across, sb, rb, own, sems):
        self.me, self.layer, self.src, self.mine, self.got, self.across = me, layer, src, mine, got, across
        self.sb, self.rb, self.own = sb, rb, own
        self.hss, self.hrs, self.yss, self.yrs, self.pss, self.prs = sems
        self.rows = own.shape[0]
        self.some = 96 if self.rows % 96 == 0 else 48
        self.sums = me.s == layer
        self.holds = me.y == layer

    @staticmethod
    def scratch(dp):
        return [DMA((1,)), DMA((1,)), DMA((dp,)), DMA((dp,)), DMA((dp - 1,)), DMA((dp - 1,))]

    def hand(self):
        return push(self.src, self.got, self.hss.at[0], self.hrs.at[0], self.me.mate)

    def zz(self, d):
        return (self.me.z + d + 1) % self.me.dp

    def over(self, d):
        rr = ds(self.zz(d) * self.rows, self.rows)
        peer = self.me.across_core(self.layer)
        return push(self.src.at[rr], self.across.at[rr], self.yss.at[d], self.yrs.at[d], peer)

    def out(self, d):
        return push(self.sb.at[d], self.rb.at[d], self.pss.at[d], self.prs.at[d], self.me.ring[d])

    def send(self):
        me = self.me

        @pl.when(me.s != me.y)
        def _():
            for d in range(me.dp):
                self.over(d).start()

        @pl.when((me.s == me.y) & jnp.logical_not(self.sums))
        def _():
            self.hand().start()

    def step(self, d):
        me = self.me

        @pl.when(self.sums)
        def _():
            if d == 0:

                @pl.when(jnp.logical_not(self.holds))
                def _():
                    self.hand().wait_recv()

            self.over(d).wait_recv()
            last = d == me.dp - 1
            step = self.some

            def add(ref):
                def body(i, _):
                    rr = ds(self.zz(d) * self.rows + i * step, step)
                    value = ref[rr, :].astype(F32) + self.across[rr, :].astype(F32)
                    if last:
                        self.own[ds(i * step, step), :] = value
                    else:
                        self.sb[d, ds(i * step, step), :] = value.astype(BF)
                    return 0

                lax.fori_loop(0, self.rows // step, body, 0)

            if self.mine is self.got:
                add(self.mine)
            else:

                @pl.when(self.holds)
                def _():
                    add(self.mine)

                @pl.when(jnp.logical_not(self.holds))
                def _():
                    add(self.got)

            if not last:
                self.out(d).start()

    def collect(self):
        me = self.me

        @pl.when(self.sums)
        def _():
            for d in range(me.dp - 1):
                self.out(d).wait_recv()

                def add(i, _, d=d):
                    rr = ds(i * self.some, self.some)
                    self.own[rr, :] += self.rb[d, rr, :].astype(F32)
                    return 0

                lax.fori_loop(0, self.rows // self.some, add, 0)
            for d in range(me.dp - 1):
                self.out(d).wait_send()

    def finish(self):
        me = self.me

        @pl.when(me.s != me.y)
        def _():
            for d in range(me.dp):
                self.over(d).wait_send()

        @pl.when((me.s == me.y) & jnp.logical_not(self.sums))
        def _():
            self.hand().wait_send()


class VectorGather:
    def __init__(self, me, sv, buf, ss, rs, own):
        self.me, self.sv, self.buf, self.ss, self.rs, self.own = me, sv, buf, ss, rs, own

    def local(self):
        me = self.me
        return pltpu.make_async_copy(self.sv, self.buf.at[me.s, me.t, me.z], self.own)

    def stage(self, n):
        me = self.me
        if n == 0:
            dst = self.buf.at[me.s, me.t, me.z]
            return [push(self.sv, dst, self.ss.at[d], self.rs.at[d], peer) for d, peer in enumerate(me.ring)]
        base = me.dp - 1
        if n == 1:
            ref = self.buf.at[me.s, me.t]
            return [
                push(ref, ref, self.ss.at[base + d], self.rs.at[base + d], peer) for d, peer in enumerate(me.group)
            ]
        i = base + me.tensor - 1
        ref = self.buf.at[me.s]
        return [push(ref, ref, self.ss.at[i], self.rs.at[i], me.mate)]

    def send(self, n):
        if n == 0:
            self.local().start()
        for c in self.stage(n):
            c.start()

    def wait(self, n):
        if n == 0:
            self.local().wait()
        for c in self.stage(n):
            c.wait_recv()

    def finish(self):
        for n in range(3):
            for c in self.stage(n):
                c.wait_send()

    def build(self, vecs, heads, own, qw, fw):
        me, buf = self.me, self.buf
        for layer in range(2):
            wide = [buf[layer, tt, zz, 0:8, :][:, 0:own] for zz in range(me.dp) for tt in range(me.tensor)]
            vecs[layer, 0:8, :] = jnp.concatenate(wide, axis=1)
            here = [buf[layer, me.quarter, zz] for zz in range(me.dp)]
            by = [jnp.concatenate([p[6 + h : 7 + h, 0:qw] for p in here], axis=1) for h in range(heads)]
            qb = []
            for part in range(3):
                qb += [b[:, part * HD : (part + 1) * HD] for b in by] + [jnp.zeros((1, HW - heads * HD), F32)]
            vecs[layer, 6:7, :] = jnp.concatenate(qb, axis=1)
            fb = [p[6 + heads + h : 7 + heads + h, 0:fw] for h in range(heads) for p in here]
            vecs[layer, 7:8, :] = jnp.concatenate(fb, axis=1)


class VectorReduce:
    def __init__(self, me, va, vr, ss, rs):
        self.me, self.va, self.vr, self.ss, self.rs = me, va, vr, ss, rs

    def stage(self, n):
        me, va, vr, ss, rs = self.me, self.va, self.vr, self.ss, self.rs
        peers, base = [([me.across], 0), (me.ring, 1), ([me.mate, me.beside, me.beside_mate], me.dp)][n]
        return [push(va.at[n], vr.at[base + d], ss.at[base + d], rs.at[base + d], p) for d, p in enumerate(peers)]

    def send(self, n):
        for c in self.stage(n):
            c.start()

    def add(self, n, out):
        base = [0, 1, self.me.dp][n]
        for c in self.stage(n):
            c.wait_recv()
        if n < 2:
            total = self.va[n]
            for d in range(len(self.stage(n))):
                total = total + self.vr[base + d]
            out[...] = total
            return
        mine, mate = self.va[2], self.vr[base]
        row = lax.broadcasted_iota(jnp.int32, mine.shape, 0)
        quarter = jnp.where(self.me.s == self.me.y, mine, mate)
        out[...] = jnp.where(row % 8 < 6, mine + mate + self.vr[base + 1] + self.vr[base + 2], quarter)

    def finish(self):
        for n in range(3):
            for c in self.stage(n):
                c.wait_send()


def document_tables(seg, live, fr_ref, tab, srow, kcol):
    seq = seg.shape[1]
    count = lax.broadcasted_iota(jnp.int32, seg.shape, 1)
    start = jnp.zeros_like(seg)
    for doc in range(DOCS - 1):
        before = jnp.sum(jnp.where(seg == doc, 1.0, 0.0), axis=1, keepdims=True).astype(jnp.int32)
        start = start + jnp.where(seg > doc, before, 0)
    ang = fr_ref[:, 0:1] * (count - start).astype(F32)
    cs, sn = jnp.cos(ang), jnp.sin(ang)
    one = jnp.ones((HD - ROT, seq), F32)
    tab[:, 0:128] = jnp.concatenate([cs, cs, one] * 2, axis=0).T
    tab[:, 128:256] = jnp.concatenate([-sn, sn, jnp.zeros_like(one)] * 2, axis=0).T
    srow[...] = jnp.broadcast_to(seg, srow.shape)
    keys = jnp.where(count < live * LIVE, seg, -1).astype(F32)
    for b in range(seq // QB):
        part = jnp.broadcast_to(keys[:, b * QB : (b + 1) * QB], (128, QB))
        kcol[b * QB : (b + 1) * QB, :] = part.T.astype(jnp.int32)


QKV, FC1, FC2, OUT = 0, 1, 2, 3


def columns(model, ff):
    return {"qkv": 0, "fc1": 3 * HW, "fc2": 3 * HW + ff, "out": 3 * HW + 2 * ff, "end": 3 * HW + 2 * ff + HW}


def project_norm(r0, half, hf, vec, n1, n2):
    rows = ds(r0, half)
    xc, r = norm_stats(hf[rows, :].astype(F32))
    xh = xc * r
    n1[rows, :] = (xh * vec[0:1, :] + vec[1:2, :]).astype(BF)
    n2[rows, :] = (xh * vec[3:4, :] + vec[4:5, :]).astype(BF)


def project_qkv(r0, half, wqkv, vec, tab, n1, q, k, v):
    rows = ds(r0, half)
    a = n1[rows, :]
    for part, dst in enumerate((q, k, v)):
        cols = slice(part * HW, (part + 1) * HW)
        y = dot(a, wqkv[:, cols]) + vec[6:7, cols]
        if part < 2:
            y = turn_lanes(y, tab[rows, :], 1)
        if part == 0:
            y = y * 0.125
        dst[rows, :] = y.astype(BF)


def project_fc1(r0, half, wfc1, vec, n2, g, gp):
    rows = ds(r0, half)
    a = n2[rows, :]
    for b in range(wfc1.shape[1] // 256):
        cols = slice(b * 256, (b + 1) * 256)
        y = dot(a, wfc1[:, cols]) + vec[7:8, cols]
        cdf = 0.5 + 0.5 * lax.erf(y * 0.7071067811865476)
        g[rows, cols] = (y * cdf).astype(BF)
        gp[rows, cols] = (cdf + y * jnp.exp(-0.5 * y * y) * 0.3989422804014327).astype(BF)


def branch_out(r0, half, o, g, wout, wfc2, part):
    rows = ds(r0, half)
    for b in range(part.shape[1] // 256):
        cols = slice(b * 256, (b + 1) * 256)
        y = dg(o[rows, :], wout[cols, :], 1, 1) + dg(g[rows, :], wfc2[cols, :], 1, 1)
        part[rows, cols] = y.astype(BF)


def back_head(r0, half, dyf, hf, g, gp, n2, o, wfc1, wfc2, wout, vec, do, e2, da, acc, vg):
    rows = ds(r0, half)
    model, ff = wfc1.shape
    dy = dyf[rows, :]
    for b in range(ff // 256):
        cols = slice(b * 256, (b + 1) * 256)
        y = dot(dy, wfc2[:, cols]) * gp[rows, cols].astype(F32)
        low = y.astype(BF)
        da[:, cols] = low
        vg[7:8, cols] += jnp.sum(low.astype(F32), axis=0, keepdims=True)
    do[rows, :] = dot(dy, wout[...]).astype(BF)
    xc, r = norm_stats(hf[rows, :].astype(F32))
    xh = xc * r
    for b in range(model // 256):
        cols = slice(b * 256, (b + 1) * 256)
        dn = dg(da[...], wfc1[cols, :], 1, 1)
        vg[3:4, cols] += jnp.sum(dn * xh[:, cols], axis=0, keepdims=True)
        vg[4:5, cols] += jnp.sum(dn, axis=0, keepdims=True)
        e2[rows, cols] = (dn * vec[3:4, cols]).astype(BF)
    n2t = n2[rows, :].T
    dyt = dy.T
    for b in range(ff // 256):
        cols = slice(b * 256, (b + 1) * 256)
        acc[:, cols] += dot(n2t, da[:, cols])
        acc[:, ff + b * 256 : ff + (b + 1) * 256] += dot(dyt, g[rows, cols])
    acc[:, 2 * ff :] += dot(dyt, o[rows, :])


def back_tail(r0, half, dmix, hf, e2, wqkv, vec, part, vg):
    rows = ds(r0, half)
    dm = dmix[rows, :]
    vg[6:7, :] += jnp.sum(dm.astype(F32), axis=0, keepdims=True)
    xc, r = norm_stats(hf[rows, :].astype(F32))
    xh = xc * r
    for b in range(part.shape[1] // 256):
        cols = slice(b * 256, (b + 1) * 256)
        dn = dg(dm, wqkv[cols, :], 1, 1)
        vg[0:1, cols] += jnp.sum(dn * xh[:, cols], axis=0, keepdims=True)
        vg[1:2, cols] += jnp.sum(dn, axis=0, keepdims=True)
        part[rows, cols] = (dn * vec[0:1, cols] + e2[rows, cols].astype(F32)).astype(BF)


def qkv_grad(n1, dmix, acc, half):
    acc[...] = jnp.zeros_like(acc)

    def body(i, _):
        rows = ds(i * half, half)
        n1t = n1[rows, :].T
        for b in range(3):
            cols = slice(b * HW, (b + 1) * HW)
            acc[:, cols] += dot(n1t, dmix[rows, cols])
        return 0

    lax.fori_loop(0, n1.shape[0] // half, body, 0)


def store_low(acc, out):
    def body(i, _):
        rr = ds(i * SUB, SUB)
        out[rr, :] = acc[rr, :].astype(BF)
        return 0

    lax.fori_loop(0, acc.shape[0] // SUB, body, 0)


def residual_out(sc, own, vec, write, after=None):
    for a in range(2):
        sc.arrive(a)

        def body(i, _, a=a):
            base = own[ds(sc.own(sc.side(a)) + i * SUB, SUB), :].astype(F32)
            write(a, i, (base + sc.total(a, i) + vec[2:3, :] + vec[5:6, :]).astype(BF))
            return 0

        lax.fori_loop(0, sc.half // SUB, body, 0)
        if after is not None:
            after(a)


def grad_out(sc, dy, hf, vec, write, after=None):
    for a in range(2):
        sc.arrive(a)

        def body(i, _, a=a):
            rr = ds(sc.own(sc.side(a)) + i * SUB, SUB)
            xc, r = norm_stats(hf[rr, :].astype(F32))
            xh = xc * r
            e = sc.total(a, i)
            m1 = jnp.mean(e, axis=-1, keepdims=True)
            m2 = jnp.mean(e * xh, axis=-1, keepdims=True)
            write(a, i, (dy(a, i).astype(F32) + r * (e - m1 - xh * m2)).astype(BF))
            return 0

        lax.fori_loop(0, sc.half // SUB, body, 0)
        if after is not None:
            after(a)


def column_sum(tok, ref, vg, row):
    total = jnp.zeros((1, ref.shape[1]), F32)
    for a in range(2):

        def body(i, acc, a=a):
            return acc + jnp.sum(ref[ds(tok.own(a) + i * SUB, SUB), :].astype(F32), axis=0, keepdims=True)

        total = lax.fori_loop(0, tok.half // SUB, body, total)
    vg[row : row + 1, :] = total


def load(pairs, sem):
    copies = [pltpu.make_async_copy(a, b, sem.at[i]) for i, (a, b) in enumerate(pairs)]
    for c in copies:
        c.start()
    return copies


def params(cid):
    return pltpu.CompilerParams(collective_id=cid, has_side_effects=True, vmem_limit_bytes=67043328)


def cost(us):
    return pl.CostEstimate(flops=int(us * 8e8), bytes_accessed=0, transcendentals=0)


class Stores:
    def __init__(self, pairs, half, sem):
        self.pairs, self.half, self.sem = pairs, half, sem

    def copy(self, n, r0, i):
        src, dst = self.pairs[n]
        rows = ds(r0, self.half)
        return pltpu.make_async_copy(src.at[rows], dst.at[rows], self.sem.at[n, i])

    def start(self, which, r0, i):
        for n in which:
            self.copy(n, r0, i).start()

    def finish(self):
        def body(i, _):
            for n in range(len(self.pairs)):
                self.copy(n, i * self.half, i).wait()
            return 0

        lax.fori_loop(0, 8, body, 0)


def in_kernel(
    cfg, in_ref, cot_ref, seg_ref, live, w_ref, sv_ref, fr_ref,
    hf_o, n1_o, n2_o, g_o, gp_o, tab_o, w_o, q_o, k_o, v_o, cf_o, vecs, srow, kcol,
    hf, n1, n2, g, gp, tab, q, k, v, wfull, gat, vb, cot, gss, grs, css, crs, yss, yrs, lsem, ssem, vss, vrs, *wsems,
):
    col, dp, tensor = cfg["col"], cfg["dp"], cfg["tensor"]
    me = Mesh(dp, tensor)
    ga = Gather(me, hf, gss, grs, me.y)
    gc = Gather(me, cf_o, css, crs, me.y)
    half = ga.half
    part = ds(me.s * half, half)
    first = pltpu.make_async_copy(in_ref.at[me.y, 0, part], hf.at[ds(ga.own(me.y), half)], lsem.at[0])
    first.start()
    up = pltpu.make_async_copy(cot_ref.at[me.y, 0, part], cot, lsem.at[4])
    up.start()
    greet([me.mate, me.across_mate] + me.ring + me.group)
    over = [
        push(ref.at[1 - me.y, 0, part], full.at[ds(ga.own(me.y), half)], yss.at[n], yrs.at[n], me.across)
        for n, (ref, full) in enumerate(((in_ref, hf), (cot_ref, cf_o)))
    ]
    wg = WeightGather(me, 0, w_ref, wfull, gat, cfg["groups"], wsems)
    vg = VectorGather(me, sv_ref, vb, vss, vrs, lsem.at[1])
    st = Stores([(hf, hf_o), (n1, n1_o), (n2, n2_o), (g, g_o), (gp, gp_o), (q, q_o), (k, k_o), (v, v_o)], half, ssem)
    vg.send(0)
    wg.send_ring()
    first.wait()
    document_tables(seg_ref[me.y], live[0, me.y], fr_ref, tab, srow, kcol)
    vg.wait(0)
    vg.send(1)
    ga.start(0)
    over[0].start()
    wg.send_own(0)
    tab_out = pltpu.make_async_copy(tab, tab_o, lsem.at[2])
    tab_out.start()
    vg.wait(1)
    vg.send(2)
    up.wait()
    cot_out = pltpu.make_async_copy(cot, cf_o.at[ds(gc.own(me.y), half)], lsem.at[5])
    cot_out.start()
    vg.wait(2)
    vg.build(vecs, cfg["heads"], cfg["own"], cfg["qw"], cfg["fw"])
    vec = vecs.at[0]

    def norm(r0, i):
        project_norm(r0, half, hf, vec, n1, n2)
        st.start((0, 1, 2), r0, i)

        @pl.when(i == 0)
        def _():
            over[0].wait_recv()
            ga.start(1)

        @pl.when(i == 1)
        def _():
            wg.forward(0)
            wg.send_own(1)
            wg.send_own(2)

    ga.run(norm)
    cot_out.wait()
    gc.start(0)
    wg.ready(0)

    def qkv(i, _):
        r0 = ga.order(i)
        project_qkv(r0, half, wfull.at[:, 0 : col["fc1"]], vec, tab, n1, q, k, v)
        st.start((5, 6, 7), r0, i)
        return 0

    lax.fori_loop(0, 8, qkv, 0)
    wg.forward(1)
    over[1].start()
    wg.ready(1)

    def fc1(i, _):
        r0 = ga.order(i)
        project_fc1(r0, half, wfull.at[:, col["fc1"] : col["fc2"]], vec, n2, g, gp)
        st.start((3, 4), r0, i)

        @pl.when(i == 6)
        def _():
            wg.forward(2)

        return 0

    lax.fori_loop(0, 8, fc1, 0)
    gc.step(2)
    gc.step(4)
    over[1].wait_recv()
    gc.start(1)
    st.finish()
    tab_out.wait()
    wg.ready(2)
    w_out = pltpu.make_async_copy(wfull, w_o, lsem.at[3])
    w_out.start()
    for n in (3, 5, 6, 7):
        gc.step(n)
    wg.finish()
    vg.finish()
    gc.finish()
    for c in over:
        c.wait_send()
    w_out.wait()


def layer_in(cfg, inputs, cotangent, segments, live, w, sv, fr):
    seq, model, ff = segments.shape[2], inputs.shape[3], cfg["ff"]
    dp, tensor = cfg["dp"], cfg["tensor"]
    rows, hidden = sds((seq, model), BF), sds((seq, ff), BF)
    heads = sds((seq, HW), BF)
    nv = dp - 1 + tensor
    wide, wide_h, wide_q = pltpu.VMEM((seq, model), BF), pltpu.VMEM((seq, ff), BF), pltpu.VMEM((seq, HW), BF)
    weights = pltpu.VMEM((model, w.shape[1]), BF)
    return pl.pallas_call(
        functools.partial(in_kernel, cfg),
        out_shape=(rows, rows, rows, hidden, hidden, sds((seq, 256), F32), sds((model, w.shape[1]), BF),
                   heads, heads, heads, rows,
                   sds((2, 8, model), F32), sds((8, seq), jnp.int32), sds((seq, 128), jnp.int32)),
        in_specs=[ANY, ANY, VMEM, SMEM, VMEM, VMEM, VMEM],
        out_specs=(ANY,) * 11 + (VMEM,) * 3,
        scratch_shapes=[
            wide, wide, wide, wide_h, wide_h, pltpu.VMEM((seq, 256), F32), wide_q, wide_q, wide_q,
            weights, weights, pltpu.VMEM((2, tensor, dp) + sv.shape, F32),
            pltpu.VMEM((seq // 8, model), BF),
            DMA((6,)), DMA((6,)), DMA((6,)), DMA((6,)), DMA((2,)), DMA((2,)), DMA((6,)), DMA((8, 8)),
            DMA((nv,)), DMA((nv,)),
        ]
        + WeightGather.scratch(dp, 3),
        compiler_params=params(2),
        cost_estimate=cost(45),
        name="layer_in",
    )(inputs, cotangent, segments, live, w, sv, fr)


def mid_kernel(
    cfg, q_in, k_in, v_in, srow, kcol, g_in, x_in, w_ref, w0, vecs, tab_in,
    o_o, lse, hf_o, n1_o, n2_o, g_o, gp_o, w_o, q_o, k_o, v_o,
    wout, wfc2, hf, n1, n2, g, gp, tab, wfull, gat, q, k, v, o, vt, s_scr,
    part, mr, xr, sss, srs, gss, grs, lsem, ssem, osem, *wsems,
):
    col, heads = cfg["col"], cfg["heads"]
    me = Mesh(cfg["dp"], cfg["tensor"])
    sc = Scatter(me, part, mr, xr, sss, srs)
    ga = Gather(me, hf, gss, grs)
    half = sc.half
    loads = load(
        [
            (v_in, v),
            (q_in, q),
            (k_in, k),
            (w0.at[:, col["out"] : col["end"]], wout),
            (w0.at[:, col["fc2"] : col["out"]], wfc2),
            (g_in, g),
            (tab_in, tab),
        ]
        + [(x_in.at[ds(sc.own(a), half)], hf.at[ds(sc.own(a), half)]) for a in range(2)],
        lsem,
    )
    greet([me.mate, me.beside, me.across, me.across_mate] + me.ring)
    wg = WeightGather(me, 1, w_ref, wfull, gat, cfg["groups"], wsems)
    wg.send_ring()
    for n in range(3):
        wg.send_own(n)
    loads[0].wait()
    turn_blocks(v, vt)
    for c in loads[1:]:
        c.wait()
    st = Stores([(hf, hf_o), (n1, n1_o), (n2, n2_o), (g, g_o), (gp, gp_o), (q, q_o), (k, k_o), (v, v_o)], half, ssem)
    st_o = Stores([(o, o_o)], half, osem)

    def out(r0, i):
        b = r0 // QB
        attn_fwd_block(b, jnp.maximum(b - DOC_MAX // QB, 0), b, heads, q, k, vt, srow, kcol, s_scr, o, lse)
        st_o.start((0,), r0, i)
        branch_out(r0, half, o, g, wout, wfc2, part)

        @pl.when(i == 6)
        def _():
            wg.forward(0)

    sc.run(out)

    def write(a, i, value):
        hf[ds(sc.own(a) + i * SUB, SUB), :] = value

    residual_out(sc, hf, vecs.at[0], write, ga.start)
    wg.forward(1)
    vec = vecs.at[1]

    def fc1(i):
        r0 = ga.order(i)
        project_fc1(r0, half, wfull.at[:, col["fc1"] : col["fc2"]], vec, n2, g, gp)
        st.start((3, 4), r0, i)

    def work(r0, i):
        project_norm(r0, half, hf, vec, n1, n2)

        @pl.when(i == 0)
        def _():
            wg.ready(0)

        project_qkv(r0, half, wfull.at[:, 0 : col["fc1"]], vec, tab, n1, q, k, v)
        st.start((0, 1, 2, 5, 6, 7), r0, i)

        @pl.when(i == 4)
        def _():
            wg.ready(1)

        @pl.when(i >= 4)
        def _():
            fc1(i - 4)

        @pl.when(i == 5)
        def _():
            wg.forward(2)

    ga.run(work)

    def late(i, _):
        fc1(i)
        return 0

    lax.fori_loop(4, 8, late, 0)
    st.finish()
    wg.ready(2)
    w_out = pltpu.make_async_copy(wfull, w_o, lsem.at[0])
    w_out.start()
    sc.finish()
    wg.finish()
    st_o.finish()
    w_out.wait()


def layer_mid(cfg, q, k, v, srow, kcol, g, xf, w, w0, vecs, tab):
    seq, model, ff = tab.shape[0], xf.shape[1], cfg["ff"]
    rows, hidden, heads = sds((seq, model), BF), sds((seq, ff), BF), sds((seq, HW), BF)
    wide, wide_h, wide_q = pltpu.VMEM((seq, model), BF), pltpu.VMEM((seq, ff), BF), pltpu.VMEM((seq, HW), BF)
    return pl.pallas_call(
        functools.partial(mid_kernel, cfg),
        out_shape=(heads, sds((8, seq), F32), rows, rows, rows, hidden, hidden, sds(w0.shape, BF), heads, heads, heads),
        in_specs=[ANY, ANY, ANY, VMEM, VMEM, ANY, ANY, VMEM, ANY, VMEM, ANY],
        out_specs=(ANY, VMEM) + (ANY,) * 9,
        scratch_shapes=[
            pltpu.VMEM((model, HW), BF), pltpu.VMEM((model, ff), BF),
            wide, wide, wide, wide_h, wide_h, pltpu.VMEM((seq, 256), F32),
            pltpu.VMEM(w0.shape, BF), pltpu.VMEM(w0.shape, BF),
            wide_q, wide_q, wide_q, wide_q, pltpu.VMEM((HW, seq), BF),
            pltpu.VMEM((cfg["heads"], DOC_MAX + QB, QB), F32),
        ]
        + scatter_scratch(seq, model)
        + [DMA((6,)), DMA((6,)), DMA((9,)), DMA((8, 8)), DMA((1, 8))]
        + WeightGather.scratch(cfg["dp"], 3),
        compiler_params=params(3),
        cost_estimate=cost(70),
        name="layer_mid",
    )(q, k, v, srow, kcol, g, xf, w, w0, vecs, tab)


def turn_kernel(
    cfg, o_in, g_in, hf_in, cf, w1, vecs, n2_in, gp_in, y_o, do_o, e2_o, gr_o, vg,
    o, g, hf, dyf, n2, gp, e2, do, y, gr, wout, wfc2, wfc1, da, acc,
    part, mr, xr, sss, srs, lsem, ssem,
):
    col = cfg["col"]
    me = Mesh(cfg["dp"], cfg["tensor"])
    sc = Scatter(me, part, mr, xr, sss, srs)
    half = sc.half
    loads = load(
        [
            (w1.at[:, col["out"] : col["end"]], wout),
            (w1.at[:, col["fc2"] : col["out"]], wfc2),
            (o_in, o),
            (g_in, g),
            (w1.at[:, col["fc1"] : col["fc2"]], wfc1),
            (cf, dyf),
            (gp_in, gp),
            (hf_in, hf),
            (n2_in, n2),
        ],
        lsem,
    )
    greet([me.mate, me.beside])
    for c in loads[:4]:
        c.wait()
    vec = vecs.at[1]
    st = Stores([(e2, e2_o), (do, do_o)], half, ssem)

    def early():
        vg[...] = jnp.zeros_like(vg)
        acc[...] = jnp.zeros_like(acc)
        for c in loads[4:]:
            c.wait()

        def head(i, _):
            r0 = i * half
            back_head(r0, half, dyf, hf, g, gp, n2, o, wfc1, wfc2, wout, vec, do, e2, da, acc, vg)
            st.start((0, 1), r0, i)
            return 0

        lax.fori_loop(0, 8, head, 0)

    sc.run(lambda r0, i: branch_out(r0, half, o, g, wout, wfc2, part), early)
    column_sum(sc, dyf, vg, 2)
    store_low(acc, gr)
    gr_out = pltpu.make_async_copy(gr, gr_o, lsem.at[0])
    gr_out.start()

    def write(a, i, value):
        y[a, ds(i * SUB, SUB), :] = value

    residual_out(sc, hf, vec, write)
    y_out = pltpu.make_async_copy(y, y_o, lsem.at[1])
    y_out.start()
    sc.finish()
    st.finish()
    gr_out.wait()
    y_out.wait()


def layer_turn(cfg, o, g, hf, cf, w1, vecs, n2, gp):
    seq, model = hf.shape
    ff = cfg["ff"]
    wide, hidden, heads = pltpu.VMEM((seq, model), BF), pltpu.VMEM((seq, ff), BF), pltpu.VMEM((seq, HW), BF)
    owned = (2, seq // 8, model)
    return pl.pallas_call(
        functools.partial(turn_kernel, cfg),
        out_shape=(
            sds(owned, BF),
            sds((seq, HW), BF),
            sds((seq, model), BF),
            sds((model, 2 * ff + HW), BF),
            sds((8, model), F32),
        ),
        in_specs=[ANY] * 5 + [VMEM, ANY, ANY],
        out_specs=(ANY,) * 4 + (VMEM,),
        scratch_shapes=[
            heads, hidden, wide, wide, wide, hidden, wide, heads, pltpu.VMEM(owned, BF),
            pltpu.VMEM((model, 2 * ff + HW), BF),
            pltpu.VMEM((model, HW), BF), pltpu.VMEM((model, ff), BF), pltpu.VMEM((model, ff), BF),
            pltpu.VMEM((seq // 8, ff), BF), pltpu.VMEM((model, 2 * ff + HW), F32),
        ]
        + scatter_scratch(seq, model)
        + [DMA((9,)), DMA((2, 8))],
        compiler_params=params(4),
        cost_estimate=cost(40),
        name="layer_turn",
    )(o, g, hf, cf, w1, vecs, n2, gp)


def back_kernel(
    cfg, dm_in, e2_in, cf, hf_in, n1_in, w1, w0, vecs, xf_in, g_in, gp_in, n2_in, o_in, gr1,
    dh_o, e2_o, do_o, vgf, vgd, out1_o, outq_o, gr_o,
    dmix, o, do, a, b, e2, g, gp, wqkv, wout, wfc2, wfc1, dhf, da, acc, gq, gr, got, gotq, acrq,
    sb, rb, sbq, rbq, out1, outq, part, mr, xr, sss, srs, gss, grs, lsem, ssem, *rsems,
):
    col, dp = cfg["col"], cfg["dp"]
    me = Mesh(dp, cfg["tensor"])
    ga = Gather(me, dhf, gss, grs)
    sc = Scatter(me, part, mr, xr, sss, srs)
    half = sc.half
    own = [ds(sc.own(n), half) for n in range(2)]
    loads = load(
        [
            (w1.at[:, col["qkv"] : col["fc1"]], wqkv),
            (dm_in, dmix),
            (hf_in, a),
            (e2_in, e2),
            (n1_in, b),
            (w0.at[:, col["out"] : col["end"]], wout),
            (w0.at[:, col["fc2"] : col["out"]], wfc2),
            (w0.at[:, col["fc1"] : col["fc2"]], wfc1),
            (g_in, g),
            (gp_in, gp),
            (o_in, o),
        ]
        + [(cf.at[rr], dhf.at[rr]) for rr in own],
        lsem,
    )
    gr_load = pltpu.make_async_copy(gr1, gr, lsem.at[13])
    holds = (me.s == 1) & (me.y == 1)

    @pl.when(holds)
    def _():
        gr_load.start()

    greet([me.mate, me.beside, me.across, me.across_mate] + me.ring)
    red1 = GradReduce(me, 1, gr1, gr, gr, got, sb, rb, out1, rsems[:6])
    redq = GradReduce(me, 1, gq, gq, gotq, acrq, sbq, rbq, outq, rsems[6:])
    st = Stores([(e2, e2_o), (do, do_o), (dhf, dh_o)], half, ssem)
    red1.send()
    vgf[...] = jnp.zeros_like(vgf)
    vgd[...] = jnp.zeros_like(vgd)
    for c in loads[:4]:
        c.wait()

    def early():
        loads[4].wait()
        small = acc.at[:, 0 : 3 * HW]
        qkv_grad(b, dmix, small, half)
        store_low(small, gq)
        redq.send()

        @pl.when(holds)
        def _():
            gr_load.wait()

        red1.step(0)

    sc.run(lambda r0, i: back_tail(r0, half, dmix, a, e2, wqkv, vecs.at[1], part, vgf), early)
    acc[...] = jnp.zeros_like(acc)
    again = pltpu.make_async_copy(n2_in, b, lsem.at[14])
    again.start()
    for c in loads[5:]:
        c.wait()
    for d in range(1, dp // 2):
        red1.step(d)

    def write(n, i, value):
        dhf[ds(sc.own(n) + i * SUB, SUB), :] = value

    grad_out(sc, lambda n, i: dhf[ds(sc.own(n) + i * SUB, SUB), :], a, vecs.at[1], write, ga.start)
    other = pltpu.make_async_copy(xf_in, a, lsem.at[15])
    other.start()
    again.wait()
    other.wait()

    def work(r0, i):
        back_head(r0, half, dhf, a, g, gp, b, o, wfc1, wfc2, wout, vecs.at[0], do, e2, da, acc, vgd)
        st.start((0, 1, 2), r0, i)

        @pl.when(i == 1)
        def _():
            for d in range(dp // 2, dp - 1):
                red1.step(d)

        @pl.when(i == 3)
        def _():
            red1.step(dp - 1)

        @pl.when(i == 5)
        def _():
            redq.step(0)

    ga.run(work)
    for d in range(1, dp):
        redq.step(d)
    store_low(acc, gr)
    gr_out = pltpu.make_async_copy(gr, gr_o, lsem.at[0])
    gr_out.start()
    column_sum(sc, dhf, vgd, 2)
    red1.collect()
    redq.collect()
    outs = [pltpu.make_async_copy(out1, out1_o, lsem.at[1]), pltpu.make_async_copy(outq, outq_o, lsem.at[2])]
    for c in outs:
        c.start()
    red1.finish()
    redq.finish()
    sc.finish()
    st.finish()
    gr_out.wait()
    for c in outs:
        c.wait()


def layer_back(cfg, dmix, e2, cf, hf, n1, w1, w0, vecs, xf, g, gp, n2, o, gr1):
    seq, model = hf.shape
    ff, dp = cfg["ff"], cfg["dp"]
    rows, nr, nq = model // dp, 2 * ff + HW, 3 * HW
    wide, hidden, heads = pltpu.VMEM((seq, model), BF), pltpu.VMEM((seq, ff), BF), pltpu.VMEM((seq, HW), BF)
    return pl.pallas_call(
        functools.partial(back_kernel, cfg),
        out_shape=(
            sds((seq, model), BF),
            sds((seq, model), BF),
            sds((seq, HW), BF),
            sds((8, model), F32),
            sds((8, model), F32),
            sds((rows, nr), F32),
            sds((rows, nq), F32),
            sds((model, nr), BF),
        ),
        in_specs=[ANY] * 7 + [VMEM] + [ANY] * 6,
        out_specs=(ANY, ANY, ANY, VMEM, VMEM, ANY, ANY, ANY),
        scratch_shapes=[
            pltpu.VMEM((seq, nq), BF), heads, heads, wide, wide, wide, hidden, hidden,
            pltpu.VMEM((model, nq), BF), pltpu.VMEM((model, HW), BF), pltpu.VMEM((model, ff), BF),
            pltpu.VMEM((model, ff), BF), wide, pltpu.VMEM((seq // 8, ff), BF), pltpu.VMEM((model, nr), F32),
            pltpu.VMEM((model, nq), BF), pltpu.VMEM((model, nr), BF), pltpu.VMEM((model, nr), BF),
            pltpu.VMEM((model, nq), BF), pltpu.VMEM((model, nq), BF),
            pltpu.VMEM((dp - 1, rows, nr), BF), pltpu.VMEM((dp - 1, rows, nr), BF),
            pltpu.VMEM((dp - 1, rows, nq), BF), pltpu.VMEM((dp - 1, rows, nq), BF),
            pltpu.VMEM((rows, nr), F32), pltpu.VMEM((rows, nq), F32),
        ]
        + scatter_scratch(seq, model)
        + [DMA((6,)), DMA((6,)), DMA((16,)), DMA((3, 8))]
        + GradReduce.scratch(dp) * 2,
        compiler_params=params(5),
        cost_estimate=cost(70),
        name="layer_back",
    )(dmix, e2, cf, hf, n1, w1, w0, vecs, xf, g, gp, n2, o, gr1)


def last_kernel(
    cfg, q_in, k_in, v_in, o_in, do_in, lse, srow, kcol, tab_in, e2_in, dh_in, xf_in, n1_in, w0, vecs, vf1, vd1, vd0,
    gr0, out1, outq, hf_in, y_in, so, ig, fq_o, fr_o, vec_o,
    q, k, v, o, do, tab, kt, dk, dv, dmix, dh, dx, xf, n1, e2, wqkv, gq, gotq, acrq, sbq, rbq, gr, got, sb, rb, fq, fr,
    vgf, va, vr, vout, part, mr, xr, sss, srs, lsem, vss, vrs, oss, ors, *rsems,
):
    col, heads, dp = cfg["col"], cfg["heads"], cfg["dp"]
    me = Mesh(dp, cfg["tensor"])
    sc = Scatter(me, part, mr, xr, sss, srs, 1 - me.y)
    half = sc.half
    seq = xf.shape[0]
    width = q.shape[1]
    own = [ds(sc.own(n), half) for n in range(2)]
    loads = load(
        [
            (k_in, k),
            (q_in, q),
            (v_in, v),
            (do_in, do),
            (o_in, o),
            (tab_in, tab),
            (w0.at[:, col["qkv"] : col["fc1"]], wqkv),
            (xf_in, xf),
            (e2_in, e2),
            (n1_in, n1),
        ]
        + [(dh_in.at[rr], dh.at[n]) for n, rr in enumerate(own)],
        lsem,
    )
    gr_load = pltpu.make_async_copy(gr0, gr, lsem.at[12])
    holds = (me.s == 0) & (me.y == 0)

    @pl.when(holds)
    def _():
        gr_load.start()

    greet([me.mate, me.beside, me.beside_mate, me.across, me.across_mate] + me.ring)
    redr = GradReduce(me, 0, gr0, gr, gr, got, sb, rb, fr, rsems[:6])
    redq = GradReduce(me, 0, gq, gq, gotq, acrq, sbq, rbq, fq, rsems[6:])
    vr_ = VectorReduce(me, va, vr, vss, vrs)
    redr.send()

    def at(dst, h):
        return dst.at[0, me.y, 0, pl.ds(h * half, half)]

    def full_out(src, dst, i):
        chunk = 2 * half
        mine, theirs = ds(me.t * chunk, chunk), ds(me.py * chunk, chunk)
        return [
            pltpu.make_async_copy(src.at[mine], dst.at[0, me.y, 0], lsem.at[13]),
            push(src.at[theirs], dst.at[0, me.y, 0], oss.at[i], ors.at[i], me.across),
        ]

    def owned_out(src, dst, core, i):
        here, far = src.at[me.y], src.at[1 - me.y]
        place = dst.at[0, me.y, 0, ds(me.s * half, half)]
        across = push(far, place, oss.at[i], ors.at[i + me.s], me.across_core(core))
        local = pltpu.make_async_copy(here, place, lsem.at[14])
        mate = push(here, place, oss.at[i + 2], ors.at[i + 2], me.mate)
        return across, local, mate

    def whole(n):
        return full_out(hf_in, so, 0) if n == 0 else full_out(dh_in, ig, 0)

    def start_here(src, dst, core, i):
        across, local, mate = owned_out(src, dst, core, i)

        @pl.when(me.s == core)
        def _():
            local.start()

        @pl.when(me.s != core)
        def _():
            mate.start()

    def wait_owned(src, dst, core, i):
        across, local, mate = owned_out(src, dst, core, i)
        across.wait_send()

        @pl.when(me.s == core)
        def _():
            local.wait()
            mate.wait_recv()
            for n in range(2):
                push(src.at[0], at(dst, n), oss.at[i], ors.at[i + n], me.across_core(core)).wait_recv()

        @pl.when(me.s != core)
        def _():
            mate.wait_send()

    old = [pltpu.make_async_copy(out1, fr, lsem.at[15]), pltpu.make_async_copy(outq, fq, lsem.at[16])]

    @pl.when(me.s == 1)
    def _():
        for c in old:
            c.start()

    vgf[...] = jnp.zeros_like(vgf)
    dk[...] = jnp.zeros_like(dk)
    dv[...] = jnp.zeros_like(dv)
    loads[0].wait()
    turn_blocks(k, kt)
    for c in loads[1:6]:
        c.wait()

    @pl.when(holds)
    def _():
        gr_load.wait()

    n_blocks = seq // QB

    def qloop(i, _):
        lo = jnp.maximum(i - DOC_MAX // QB, 0)

        @pl.when(i == n_blocks - 2)
        def _():
            for n in range(2):

                @pl.when(me.s == n)
                def _(n=n):
                    for c in whole(n):
                        c.start()

            owned_out(y_in, so, 1, 1)[0].start()
            start_here(y_in, so, 1, 1)

        attn_bwd_block(i, lo, i, heads, q, k, v, o, do, kt, lse, srow, kcol, tab, dk, dv, dmix)
        for at_block, steps in (
            (n_blocks // 2 - 1, range(0, 1)),
            (n_blocks // 2, range(1, dp // 2)),
            (n_blocks // 2 + 1, range(dp // 2, dp - 1)),
            (n_blocks - 2, range(dp - 1, dp)),
        ):

            @pl.when(i == at_block)
            def _(steps=steps):
                for d in steps:
                    redr.step(d)

        return 0

    lax.fori_loop(0, n_blocks, qloop, 0)

    def close(i, _):
        ii = ds(i * QB, QB)
        dmix[ii, width : 2 * width] = turn_lanes(dk[ii, :], tab[ii, :], -1).astype(BF)
        dmix[ii, 2 * width : 3 * width] = dv[ii, :].astype(BF)
        return 0

    lax.fori_loop(0, n_blocks, close, 0)
    for c in loads[6:]:
        c.wait()

    def early():
        va[0, 0:8, :] = vgf[...] + vd0[...]
        va[0, 8:16, :] = vf1[...] + vd1[...]
        vr_.send(0)
        nf = gq.shape[0]
        accs = [dk.at[0:nf], dk.at[nf : 2 * nf], dv.at[0:nf]]
        for acc in accs:
            acc[...] = jnp.zeros_like(acc)

        def body(i, _):
            rows = ds(i * half, half)
            n1t = n1[rows, :].T
            for p, acc in enumerate(accs):
                acc[...] += dot(n1t, dmix[rows, p * HW : (p + 1) * HW])
            return 0

        lax.fori_loop(0, 8, body, 0)
        for p, acc in enumerate(accs):
            gq[:, p * HW : (p + 1) * HW] = acc[...].astype(BF)
        vr_.add(0, va.at[1])
        vr_.send(1)
        redq.send()
        vr_.add(1, va.at[2])
        vr_.send(2)
        redq.step(0)

    sc.run(lambda r0, i: back_tail(r0, half, dmix, xf, e2, wqkv, vecs.at[0], part, vgf), early)
    for d in range(1, dp - 1):
        redq.step(d)

    def write(n, i, value):
        dx[sc.side(n), ds(i * SUB, SUB), :] = value

    def leave(n):
        if n == 0:
            owned_out(dx, ig, 0, 4)[0].start()
        else:
            start_here(dx, ig, 0, 4)

    grad_out(sc, lambda n, i: dh[sc.side(n), ds(i * SUB, SUB), :], xf, vecs.at[0], write, leave)
    redq.step(dp - 1)
    vr_.add(2, vout)
    vec_o[...] = jnp.where(me.s == 0, vout[0:8, :], vout[8:16, :])
    redr.collect()
    redq.collect()

    @pl.when(me.s == 1)
    def _():
        for c in old:
            c.wait()

    ends = [pltpu.make_async_copy(fr, fr_o, lsem.at[0]), pltpu.make_async_copy(fq, fq_o, lsem.at[1])]
    for c in ends:
        c.start()
    redr.finish()
    redq.finish()
    vr_.finish()
    sc.finish()
    for n in range(2):

        @pl.when(me.s == n)
        def _(n=n):
            for c in whole(n):
                c.wait()

    wait_owned(y_in, so, 1, 1)
    wait_owned(dx, ig, 0, 4)
    for c in ends:
        c.wait()


def layer_last(cfg, q, k, v, o, do, lse, sr, kc, tab, e2, dh, xf, n1, w0, vecs, vf1, vd1, vd0, gr0, out1, outq, hf, y):
    seq, model = xf.shape
    dp, tensor, ff = cfg["dp"], cfg["tensor"], cfg["ff"]
    rows, nr, nq = model // dp, 2 * ff + HW, 3 * HW
    nv = dp + tensor - 1
    wide, owned, heads = pltpu.VMEM((seq, model), BF), pltpu.VMEM((2, seq // 8, model), BF), pltpu.VMEM((seq, HW), BF)
    both = sds((1, 2, 1, seq // 4, model), BF)
    return pl.pallas_call(
        functools.partial(last_kernel, cfg),
        out_shape=(both, both, sds((rows, nq), F32), sds((rows, nr), F32), sds((8, model), F32)),
        in_specs=[ANY] * 5 + [VMEM] * 3 + [ANY] * 6 + [VMEM] * 4 + [ANY] * 5,
        out_specs=(ANY, ANY, ANY, ANY, VMEM),
        scratch_shapes=[
            heads, heads, heads, heads, heads, pltpu.VMEM(tab.shape, F32), pltpu.VMEM((HW, seq), BF),
            pltpu.VMEM((seq, HW), F32), pltpu.VMEM((seq, HW), F32), pltpu.VMEM((seq, nq), BF), owned, owned,
            wide, wide, wide, pltpu.VMEM((model, nq), BF),
            pltpu.VMEM((model, nq), BF), pltpu.VMEM((model, nq), BF), pltpu.VMEM((model, nq), BF),
            pltpu.VMEM((dp - 1, rows, nq), BF), pltpu.VMEM((dp - 1, rows, nq), BF),
            pltpu.VMEM((model, nr), BF), pltpu.VMEM((model, nr), BF),
            pltpu.VMEM((dp - 1, rows, nr), BF), pltpu.VMEM((dp - 1, rows, nr), BF),
            pltpu.VMEM((rows, nq), F32), pltpu.VMEM((rows, nr), F32),
            pltpu.VMEM((8, model), F32), pltpu.VMEM((3, 16, model), F32), pltpu.VMEM((nv, 16, model), F32),
            pltpu.VMEM((16, model), F32),
        ]
        + scatter_scratch(seq, model)
        + [DMA((17,)), DMA((nv,)), DMA((nv,)), DMA((7,)), DMA((7,))]
        + GradReduce.scratch(dp) * 2,
        compiler_params=params(6),
        cost_estimate=cost(80),
        name="layer_last",
    )(q, k, v, o, do, lse, sr, kc, tab, e2, dh, xf, n1, w0, vecs, vf1, vd1, vd0, gr0, out1, outq, hf, y)


def finish_kernel(
    cfg, so_in, ig_in, fq_in, fr_in, vec, so, ig, bg1, bb1, gqkv, bqkv, gout, bdy, bdy2, bg2, bb2, gfc1, bfc1, gfc2,
    a, b, fq, fr, lsem, osem,
):
    heads, ff, own, qw, fw = cfg["heads"], cfg["ff"], cfg["own"], cfg["qw"], cfg["fw"]
    me = Mesh(cfg["dp"], cfg["tensor"])
    loads = load([(fr_in, fr), (fq_in, fq), (so_in, a), (ig_in, b)], lsem)
    model = vec.shape[1]
    short = pltpu.roll(vec[...], (model - (me.z * me.tensor + me.t) * own) % model, 1)
    for row, ref in ((0, bg1), (1, bb1), (2, bdy), (2, bdy2), (3, bg2), (4, bb2)):
        ref[...] = short[row : row + 1, 0:own]
    for h in range(heads):
        parts = [vec[6:7, p * HW + h * HD : p * HW + (h + 1) * HD] for p in range(3)]
        one = jnp.concatenate(parts + [jnp.zeros((1, HW - 3 * HD), F32)], axis=1)
        one = jnp.broadcast_to(one, (8, HW))
        bqkv[h] = pltpu.roll(one, (HW - me.z * qw) % HW, 1)[0:1, 0:qw]
        wide = ff // heads
        one = jnp.broadcast_to(vec[7:8, h * wide : (h + 1) * wide], (8, wide))
        bfc1[h] = pltpu.roll(one, (wide - me.z * fw) % wide, 1)[0:1, 0:fw]
    loads[0].wait()
    gfc1[0] = fr[:, 0:ff]
    gfc2[...] = fr[:, ff : 2 * ff]
    gout[0] = fr[:, 2 * ff : 2 * ff + HW].T[0 : heads * HD, :]
    loads[2].wait()
    loads[3].wait()
    outs = [pltpu.make_async_copy(a, so, osem.at[0]), pltpu.make_async_copy(b, ig, osem.at[1])]
    for c in outs:
        c.start()
    loads[1].wait()
    pieces = [fq[:, p * HW + h * HD : p * HW + (h + 1) * HD] for h in range(heads) for p in range(3)]
    gqkv[0] = jnp.concatenate(pieces, axis=1)
    for c in outs:
        c.wait()


def finish(cfg, so, ig, fq, fr, vec):
    heads, ff, rows = cfg["heads"], cfg["ff"], fq.shape[0]
    line = sds((1, cfg["own"]), F32)
    return pl.pallas_call(
        functools.partial(finish_kernel, cfg),
        out_shape=(sds(so.shape, BF), sds(ig.shape, BF), line, line, sds((1, rows, heads * 3 * HD), F32),
                   sds((heads, 1, cfg["qw"]), F32), sds((1, heads * HD, rows), F32), line, line, line, line,
                   sds((1, rows, ff), F32), sds((heads, 1, cfg["fw"]), F32), sds((rows, ff), F32)),
        in_specs=[ANY] * 4 + [VMEM],
        out_specs=(ANY, ANY) + (VMEM,) * 12,
        scratch_shapes=[
            pltpu.VMEM(so.shape, BF), pltpu.VMEM(ig.shape, BF), pltpu.VMEM(fq.shape, F32), pltpu.VMEM(fr.shape, F32),
            DMA((4,)), DMA((2,)),
        ],
        compiler_params=pltpu.CompilerParams(vmem_limit_bytes=67043328),
        cost_estimate=cost(5),
        name="finish",
    )(so, ig, fq, fr, vec)


def by_part(w):
    rows = w.shape[0]
    heads = w.shape[1] // (3 * HD)
    w = w.reshape(rows, heads, 3, HD).transpose(0, 2, 1, 3).reshape(rows, 3, heads * HD)
    return jnp.pad(w, ((0, 0), (0, 0), (0, HW - heads * HD))).reshape(rows, 3 * HW)


def shards(
    dp, tensor, inputs, cotangent, segments, live_blocks, ln1_gain, ln1_bias, qkv_weight, qkv_bias,
    out_weight, out_bias, ln2_gain, ln2_bias, fc1_weight, fc1_bias, fc2_weight, fc2_bias,
):
    live_blocks = live_blocks.T
    model = inputs.shape[-1]
    ff = fc1_weight.shape[2]
    heads = qkv_bias.shape[1]
    col = columns(model, ff)
    wout = jnp.pad(out_weight[0].T, ((0, 0), (0, HW - heads * HD)))
    w = jnp.concatenate([by_part(qkv_weight[0]), fc1_weight[0], fc2_weight[0].T, wout], axis=1)
    small = jnp.stack([ln1_gain[0], ln1_bias[0], out_bias[0], ln2_gain[0], ln2_bias[0], fc2_bias[0]])

    def lanes(a):
        return jnp.pad(a.astype(F32), ((0, 0), (0, 128 - a.shape[1])))

    sv = jnp.concatenate([lanes(small), lanes(qkv_bias[0]), lanes(fc1_bias[0])], axis=0)
    sv = jnp.pad(sv, ((0, -sv.shape[0] % 8), (0, 0)))
    fr = np.float32(10000.0) ** (-(np.arange(ROT // 2, dtype=np.float32) * np.float32(2.0 / ROT)))
    fr = jnp.asarray(np.broadcast_to(fr[:, None], (ROT // 2, 128)).astype(np.float32))
    cfg = {
        "col": col, "ff": ff, "heads": heads, "dp": dp, "tensor": tensor, "own": small.shape[1],
        "qw": qkv_bias.shape[2], "fw": fc1_bias.shape[2],
        "groups": [(0, col["fc1"]), (col["fc1"], col["fc2"]), (col["fc2"], col["end"])],
    }

    xf, n1a, n2a, ga, gpa, tab, w0, qa, ka, va, cf, vecs, sr, kc = layer_in(
        cfg, inputs, cotangent, segments, live_blocks, w, sv, fr
    )
    oa, lsea, hf, n1b, n2b, gb, gpb, w1, qb, kb, vb = layer_mid(cfg, qa, ka, va, sr, kc, ga, xf, w, w0, vecs, tab)
    ob, lseb = attn_fwd(heads, segments, live_blocks, qb, kb, vb, sr, kc)
    y, dob, e2b, grb, vdb = layer_turn(cfg, ob, gb, hf, cf, w1, vecs, n2b, gpb)
    dmb = attn_bwd(heads, segments, live_blocks, qb, kb, vb, ob, dob, lseb, sr, kc, tab)
    dhf, e2a, doa, vfb, vda, out1, outq, gra = layer_back(
        cfg, dmb, e2b, cf, hf, n1b, w1, w0, vecs, xf, ga, gpa, n2a, oa, grb
    )
    last_part = finish(
        cfg,
        *layer_last(
            cfg, qa, ka, va, oa, doa, lsea, sr, kc, tab, e2a, dhf, xf, n1a, w0, vecs, vfb, vdb, vda, gra, out1, outq, hf, y
        ),
    )
    so, ig, bg1, bb1, gqkv, bqkv, gout, bdy, bdy2, bg2, bb2, gfc1, bfc1, gfc2 = last_part
    bqkv, bfc1, gfc2 = bqkv.transpose(1, 0, 2), bfc1.transpose(1, 0, 2), gfc2.T[None]
    return (so, ig, bg1, bb1, gqkv, bqkv, gout, bdy, bg2, bb2, gfc1, bfc1, gfc2, bdy2)


def solution(mesh):
    both = ("dp", "tensor")
    in_specs = (
        P(None, "dp", "tensor", None),
        P(None, "dp", "tensor", None),
        P(None, "dp", None),
        P(None, "dp"),
        P("section", both),
        P("section", both),
        P("section", "dp", "tensor"),
        P("section", "tensor", "dp"),
        P("section", "tensor", "dp"),
        P("section", both),
        P("section", both),
        P("section", both),
        P("section", "dp", "tensor"),
        P("section", "tensor", "dp"),
        P("section", "tensor", "dp"),
        P("section", both),
    )
    out_specs = (
        P("section", None, "dp", "tensor", None),
        P("section", None, "dp", "tensor", None),
        P("section", both),
        P("section", both),
        P("section", "dp", "tensor"),
        P("section", "tensor", "dp"),
        P("section", "tensor", "dp"),
        P("section", both),
        P("section", both),
        P("section", both),
        P("section", "dp", "tensor"),
        P("section", "tensor", "dp"),
        P("section", "tensor", "dp"),
        P("section", both),
    )
    body = functools.partial(shards, mesh.shape["dp"], mesh.shape["tensor"])
    return jax.shard_map(body, mesh=mesh, in_specs=in_specs, out_specs=out_specs, check_vma=False)
```

```python
import functools

import jax
import jax.numpy as jnp
import numpy as np
from jax import lax
from jax.experimental import pallas as pl
from jax.experimental.pallas import tpu as pltpu
from jax.sharding import PartitionSpec as P

F32 = jnp.float32
BF = jnp.bfloat16
MESH = pl.DeviceIdType.MESH
HD = 64
ROT = 16
LIVE = 128
DOCS = 4
DOC_MAX = 1024
QB = 256
HW = 256
SUB = 256
EPS = 1e-05
NEG = -1e30
VMEM = pl.BlockSpec(memory_space=pltpu.VMEM)
ANY = pl.BlockSpec(memory_space=pltpu.HBM)
SMEM = pl.BlockSpec(memory_space=pltpu.SMEM)
DMA = pltpu.SemaphoreType.DMA


def sds(shape, dtype):
    return jax.ShapeDtypeStruct(shape, dtype)


def dg(a, b, ca, cb):
    return lax.dot_general(a, b, (((ca,), (cb,)), ((), ())), preferred_element_type=F32)


def dot(a, b):
    return jnp.dot(a, b, preferred_element_type=F32)


def ds(start, size):
    return pl.ds(pl.multiple_of(start, size), size)


def norm_stats(x):
    mu = jnp.mean(x, axis=-1, keepdims=True)
    xc = x - mu
    var = jnp.mean(xc * xc, axis=-1, keepdims=True)
    return xc, lax.rsqrt(var + EPS)


def head_lanes(width, heads):
    lane = lax.broadcasted_iota(jnp.int32, (1, width), 1)
    return [(lane >= h * HD) & (lane < (h + 1) * HD) for h in range(heads)]


def allow_mask(kc, sq, diag):
    m = kc == sq
    if diag:
        r = lax.broadcasted_iota(jnp.int32, (QB, QB), 0)
        c = lax.broadcasted_iota(jnp.int32, (QB, QB), 1)
        m = (m & (r <= c)) | (r == c)
    return m


def block_bounds(seg, live, i, n):
    s = lax.axis_index("tensor") // 2
    doc = seg[s, 0, i * QB]

    def body(j, count):
        return count + jnp.where((j < i) & (seg[s, 0, (j + 1) * QB - 1] == doc), 1, 0)

    hi = jnp.minimum(i, (live[0, s] * LIVE + QB - 1) // QB)
    return jnp.minimum(i - lax.fori_loop(0, n, body, 0), hi), hi


def turn_blocks(src, dst):
    def turn(i, _):
        dst[:, ds(i * QB, QB)] = src[ds(i * QB, QB), :].T
        return 0

    lax.fori_loop(0, src.shape[0] // QB, turn, 0)


def attn_fwd_block(i, lo, hi, heads, q_ref, k_ref, vt, sr_ref, kc_ref, s_scr, o_ref, lse_ref):
    width = q_ref.shape[1]
    qi = ds(i * QB, QB)
    q = q_ref[qi, :]
    qm = [jnp.where(m, q, jnp.zeros_like(q)) for m in head_lanes(width, heads)]
    sq = sr_ref[0:1, qi]

    def scores(j, slot, ms, diag):
        kj = ds(j * QB, QB)
        k = k_ref[kj, :]
        mask = allow_mask(kc_ref[kj, 0:1], sq, diag)
        out = []
        for h in range(heads):
            s = jnp.where(mask, dg(k, qm[h], 1, 1), NEG)
            s_scr[h, ds(slot * QB, QB), :] = s
            out.append(jnp.maximum(ms[h], jnp.max(s, axis=0, keepdims=True)))
        return tuple(out)

    ms = tuple(jnp.full((1, QB), NEG, F32) for _ in range(heads))
    ms = scores(i, 0, ms, True)
    ms = lax.fori_loop(lo, hi, lambda j, ms: scores(j, j - lo + 1, ms, False), ms)

    def weigh(j, slot, st):
        kj = ds(j * QB, QB)
        out = []
        for h in range(heads):
            total, acc = st[h]
            p = jnp.exp(s_scr[h, ds(slot * QB, QB), :] - ms[h])
            total = total + jnp.sum(p, axis=0, keepdims=True)
            acc = acc + dot(vt[h * HD : (h + 1) * HD, kj], p.astype(BF))
            out.append((total, acc))
        return tuple(out)

    st = tuple((jnp.zeros((1, QB), F32), jnp.zeros((HD, QB), F32)) for _ in range(heads))
    st = weigh(i, 0, st)
    st = lax.fori_loop(lo, hi, lambda j, st: weigh(j, j - lo + 1, st), st)
    ot = [st[h][1] * (1.0 / st[h][0]) for h in range(heads)]
    ot = jnp.concatenate(ot + [jnp.zeros((width - heads * HD, QB), F32)], axis=0)
    o_ref[qi, :] = ot.T.astype(BF)
    lse = [ms[h] + jnp.log(st[h][0]) for h in range(heads)]
    lse_ref[:, qi] = jnp.concatenate(lse + [jnp.zeros((8 - heads, QB), F32)], axis=0)


def attn_fwd_kernel(heads, seg, live, q_in, k_in, v_in, sr_ref, kc_ref, o_out, lse_ref, q, k, v, o, vt, s_scr, lsem, osem):
    n = q.shape[0] // QB
    loads = load([(v_in, v), (q_in, q), (k_in, k)], lsem)
    loads[0].wait()
    turn_blocks(v, vt)
    loads[1].wait()
    loads[2].wait()

    def out(i):
        rows = ds(i * QB, QB)
        return pltpu.make_async_copy(o.at[rows], o_out.at[rows], osem.at[i])

    def qloop(i, _):
        lo, hi = block_bounds(seg, live, i, n)
        attn_fwd_block(i, lo, hi, heads, q, k, vt, sr_ref, kc_ref, s_scr, o, lse_ref)
        out(i).start()
        return 0

    lax.fori_loop(0, n, qloop, 0)

    def drain(i, _):
        out(i).wait()
        return 0

    lax.fori_loop(0, n, drain, 0)


def attn_fwd(heads, seg, live, q, k, v, sr, kc):
    rows, width = q.shape
    buf = pltpu.VMEM((rows, width), BF)
    return pl.pallas_call(
        functools.partial(attn_fwd_kernel, heads),
        out_shape=(sds((rows, width), BF), sds((8, rows), F32)),
        in_specs=[SMEM, SMEM, ANY, ANY, ANY, VMEM, VMEM],
        out_specs=(ANY, VMEM),
        scratch_shapes=[buf, buf, buf, buf, pltpu.VMEM((width, rows), BF), pltpu.VMEM((heads, rows + QB, QB), F32),
                        DMA((3,)), DMA((rows // QB,))],
        compiler_params=pltpu.CompilerParams(vmem_limit_bytes=67043328),
        cost_estimate=cost(12),
        name="attn_fwd",
    )(seg, live, q, k, v, sr, kc)


def turn_lanes(x, tab, sign):
    width = x.shape[1]
    c, sn = [jnp.concatenate([tab[:, a * 128 : (a + 1) * 128]] * (width // 128), axis=1) for a in range(2)]
    lane = lax.broadcasted_iota(jnp.int32, (1, width), 1) % HD
    moved = jnp.where(lane < ROT // 2, pltpu.roll(x, width - ROT // 2, 1), pltpu.roll(x, ROT // 2, 1)) * sn
    return x * c + moved if sign > 0 else x * c - moved


def attn_bwd_block(i, lo, hi, heads, q_ref, k_ref, v_ref, o_ref, do_ref, kt, lse_ref, sr_ref, kc_ref, tab, dk, dv, out):
    width = q_ref.shape[1]
    hm = head_lanes(width, heads)
    rowid = lax.broadcasted_iota(jnp.int32, (8, width), 0)
    lane = lax.broadcasted_iota(jnp.int32, (8, width), 1)
    sel = ((lane >= rowid * HD) & (lane < (rowid + 1) * HD)).astype(F32).astype(BF)
    qi = ds(i * QB, QB)
    q = q_ref[qi, :]
    do = do_ref[qi, :]
    z = jnp.zeros_like(q)
    qm = [jnp.where(hm[h], q, z) for h in range(heads)]
    dom = [jnp.where(hm[h], do, z) for h in range(heads)]
    qcat = jnp.concatenate(qm, axis=0)
    docat = jnp.concatenate(dom, axis=0)
    prod = do.astype(F32) * o_ref[qi, :].astype(F32)
    high = prod.astype(BF)
    low = (prod - high.astype(F32)).astype(BF)
    delta = dg(sel, high, 1, 1) + dg(sel, low, 1, 1)
    lse = lse_ref[:, qi]
    sq = sr_ref[0:1, qi]

    def step(j, dqs, diag):
        kj = ds(j * QB, QB)
        k = k_ref[kj, :]
        v = v_ref[kj, :]
        mask = allow_mask(kc_ref[kj, 0:1], sq, diag)
        ps, dss, res = [], [], []
        for h in range(heads):
            s = dg(k, qm[h], 1, 1)
            dp = dg(v, dom[h], 1, 1)
            p = jnp.exp(jnp.where(mask, s - lse[h : h + 1, :], NEG))
            score_grad = (p * (dp - delta[h : h + 1, :])).astype(BF)
            ps.append(p.astype(BF))
            dss.append(score_grad)
            res.append(dqs[h] + dot(kt[h * HD : (h + 1) * HD, kj], score_grad))
        dv[kj, :] += dot(jnp.concatenate(ps, axis=1), docat)
        dk[kj, :] += dot(jnp.concatenate(dss, axis=1), qcat)
        return tuple(res)

    dqs = tuple(jnp.zeros((HD, QB), F32) for _ in range(heads))
    dqs = step(i, dqs, True)
    dqs = lax.fori_loop(lo, hi, lambda j, d: step(j, d, False), dqs)
    dq = jnp.concatenate(list(dqs) + [jnp.zeros((width - heads * HD, QB), F32)], axis=0).T * 0.125
    out[qi, 0:width] = turn_lanes(dq, tab[qi, :], -1).astype(BF)


def attn_bwd_kernel(
    heads, seg, live, q_in, k_in, v_in, o_in, do_in, lse_ref, sr_ref, kc_ref, tab_in, out_ref,
    q, k, v, o, do, tab, out, kt, dk, dv, lsem, osem,
):
    rows, width = q.shape
    n = rows // QB
    loads = load([(k_in, k), (q_in, q), (v_in, v), (do_in, do), (o_in, o), (tab_in, tab)], lsem)
    dk[...] = jnp.zeros_like(dk)
    dv[...] = jnp.zeros_like(dv)
    loads[0].wait()
    turn_blocks(k, kt)
    for c in loads[1:]:
        c.wait()

    def qloop(i, _):
        lo, hi = block_bounds(seg, live, i, n)
        attn_bwd_block(i, lo, hi, heads, q, k, v, o, do, kt, lse_ref, sr_ref, kc_ref, tab, dk, dv, out)
        return 0

    lax.fori_loop(0, n, qloop, 0)

    def leave(i):
        rr = ds(i * QB, QB)
        return pltpu.make_async_copy(out.at[rr], out_ref.at[rr], osem.at[i])

    def finish(i, _):
        ii = ds(i * QB, QB)
        out[ii, width : 2 * width] = turn_lanes(dk[ii, :], tab[ii, :], -1).astype(BF)
        out[ii, 2 * width : 3 * width] = dv[ii, :].astype(BF)
        leave(i).start()
        return 0

    lax.fori_loop(0, n, finish, 0)

    def drain(i, _):
        leave(i).wait()
        return 0

    lax.fori_loop(0, n, drain, 0)


def attn_bwd(heads, seg, live, q, k, v, o, do, lse, sr, kc, tab):
    rows, width = q.shape
    buf = pltpu.VMEM((rows, width), BF)
    return pl.pallas_call(
        functools.partial(attn_bwd_kernel, heads),
        out_shape=sds((rows, 3 * width), BF),
        in_specs=[SMEM, SMEM] + [ANY] * 5 + [VMEM] * 3 + [ANY],
        out_specs=ANY,
        scratch_shapes=[buf, buf, buf, buf, buf, pltpu.VMEM(tab.shape, F32), pltpu.VMEM((rows, 3 * width), BF),
                        pltpu.VMEM((width, rows), BF), pltpu.VMEM((rows, width), F32), pltpu.VMEM((rows, width), F32),
                        DMA((6,)), DMA((rows // QB,))],
        compiler_params=pltpu.CompilerParams(vmem_limit_bytes=67043328),
        cost_estimate=cost(26),
        name="attn_bwd",
    )(seg, live, q, k, v, o, do, lse, sr, kc, tab)


class Mesh:
    def __init__(self, dp, tensor):
        self.dp, self.tensor = dp, tensor
        self.s, self.z, self.t = lax.axis_index("section"), lax.axis_index("dp"), lax.axis_index("tensor")
        self.x, self.y = self.t % 2, self.t // 2
        self.px, self.py = 2 * self.y + (1 - self.x), 2 * (1 - self.y) + self.x
        self.mate = {"section": 1 - self.s}
        self.beside = {"tensor": self.px}
        self.beside_mate = {"tensor": self.px, "section": 1 - self.s}
        self.across = {"tensor": self.py}
        self.across_mate = {"tensor": self.py, "section": 1 - self.s}
        self.ring = [{"dp": (self.z + d) % dp} for d in range(1, dp)]
        self.group = [{"tensor": (self.t + d) % tensor} for d in range(1, tensor)]
        self.quarter = 2 * self.s + self.x

    def across_core(self, core):
        return {"tensor": self.py, "section": core}


def greet(peers):
    bar = pltpu.get_barrier_semaphore()
    for peer in peers:
        pl.semaphore_signal(bar, inc=1, device_id=peer, device_id_type=MESH)
    pl.semaphore_wait(bar, len(peers))


def push(src, dst, ssem, rsem, peer):
    return pltpu.make_async_remote_copy(
        src_ref=src, dst_ref=dst, send_sem=ssem, recv_sem=rsem, device_id=peer, device_id_type=MESH
    )


def pick(i, values):
    out = values[-1]
    for n in range(len(values) - 2, -1, -1):
        out = jnp.where(i == n, values[n], out)
    return out


class Tokens:
    def __init__(self, me, seq):
        self.me, self.half = me, seq // 8

    def start_of(self, a, b, h):
        return (4 * a + 2 * b + h) * self.half

    def rows(self, a, b, h):
        return ds(self.start_of(a, b, h), self.half)

    def own(self, a):
        return self.start_of(a, self.me.x, self.me.s)


class Gather(Tokens):
    def __init__(self, me, full, ssem, rsem, first=0):
        super().__init__(me, full.shape[0])
        self.full, self.ssem, self.rsem, self.first = full, ssem, rsem, first

    def side(self, n):
        return self.first if n == 0 else 1 - self.first

    def plan(self, i):
        me, a = self.me, self.side(i % 2)
        ref = self.full.at[self.rows(a, (1 - me.x) if i >= 4 else me.x, me.s)]
        return push(ref, ref, self.ssem.at[i], self.rsem.at[i], me.beside if i in (2, 3) else me.mate)

    def start(self, n):
        self.plan(n).start()
        self.plan(2 + n).start()

    def order(self, i):
        me = self.me
        a = pick(i, [self.side(n) for n in (0, 1, 0, 1, 0, 0, 1, 1)])
        b = jnp.where(i < 4, me.x, 1 - me.x)
        h = pick(i, [me.s, me.s, 1 - me.s, 1 - me.s, me.s, 1 - me.s, me.s, 1 - me.s])
        return self.start_of(a, b, h)

    def step(self, i):
        if i in (2, 3):
            self.plan(i - 2).wait_recv()
        if i in (4, 6):
            n = i // 2 - 2
            self.plan(2 + n).wait_recv()
            self.plan(4 + n).start()
        if i in (5, 7):
            self.plan(4 + i // 2 - 2).wait_recv()

    def arrive(self, i):
        for n in range(2, 8):

            @pl.when(i == n)
            def _(n=n):
                self.step(n)

    def finish(self):
        for i in range(6):
            self.plan(i).wait_send()

    def run(self, work):
        def body(i, _):
            self.arrive(i)
            work(self.order(i), i)
            return 0

        lax.fori_loop(0, 8, body, 0)
        self.finish()


class Scatter(Tokens):
    def __init__(self, me, part, mr, xr, ssem, rsem, first=0):
        super().__init__(me, part.shape[0])
        self.part, self.mr, self.xr, self.ssem, self.rsem, self.first = part, mr, xr, ssem, rsem, first

    def side(self, n):
        return self.first if n == 0 else 1 - self.first

    def plan(self, i):
        me = self.me
        if i < 4:
            b = (1 - me.x) if i < 2 else me.x
            src, dst, peer = self.rows(self.side(i % 2), b, 1 - me.s), self.mr.at[i], me.mate
        else:
            src, dst, peer = self.rows(self.side(i - 4), 1 - me.x, me.s), self.xr.at[i - 4], me.beside
        return push(self.part.at[src], dst, self.ssem.at[i], self.rsem.at[i], peer)

    def run(self, work, early=None):
        me = self.me

        def body(i, _):
            k = i // 2
            b = jnp.where(k < 2, 1 - me.x, me.x)
            h = jnp.where(i % 2 == 0, 1 - me.s, me.s)
            work(self.start_of(jnp.where(k % 2 == 0, self.side(0), self.side(1)), b, h), i)
            for n in range(4):

                @pl.when(i == 2 * n)
                def _(n=n):
                    self.plan(n).start()

            for n in range(2):

                @pl.when(i == 2 * n + 1)
                def _(n=n):
                    self.plan(n).wait_recv()
                    base = self.start_of(self.side(n), 1 - me.x, me.s)

                    def add(j, _):
                        rr = ds(base + j * SUB, SUB)
                        got = self.mr[n, ds(j * SUB, SUB), :].astype(F32)
                        self.part[rr, :] = (self.part[rr, :].astype(F32) + got).astype(BF)
                        return 0

                    lax.fori_loop(0, self.half // SUB, add, 0)
                    self.plan(4 + n).start()

            return 0

        lax.fori_loop(0, 8, body, 0)
        if early is not None:
            early()

    def arrive(self, n):
        self.plan(2 + n).wait_recv()
        self.plan(4 + n).wait_recv()

    def total(self, n, i):
        rr = ds(self.own(self.side(n)) + i * SUB, SUB)
        sub = ds(i * SUB, SUB)
        return self.part[rr, :].astype(F32) + self.mr[2 + n, sub, :].astype(F32) + self.xr[n, sub, :].astype(F32)

    def finish(self):
        for i in range(6):
            self.plan(i).wait_send()


def scatter_scratch(rows, width):
    half = rows // 8
    return [
        pltpu.VMEM((rows, width), BF),
        pltpu.VMEM((4, half, width), BF),
        pltpu.VMEM((2, half, width), BF),
        DMA((6,)),
        DMA((6,)),
    ]


class WeightGather:
    def __init__(self, me, layer, shard, full, gat, groups, sems):
        self.me, self.layer, self.shard, self.full, self.gat, self.groups = me, layer, shard, full, gat, groups
        self.own, self.wss, self.wrs, self.fss, self.frs, self.yss, self.yrs = sems
        self.rows = shard.shape[0]
        self.collects = me.s == layer
        self.keeps = me.y == layer

    def block(self, ref, zz, g):
        a, b = self.groups[g]
        return ref.at[ds(zz * self.rows, self.rows), a:b]

    def mine(self, g):
        a, b = self.groups[g]
        return self.shard.at[:, a:b]

    def local(self, g):
        return pltpu.make_async_copy(self.mine(g), self.block(self.full, self.me.z, g), self.own.at[g])

    def out(self, g, d, ref):
        dst = self.block(ref, self.me.z, g)
        return push(self.mine(g), dst, self.wss.at[g, d], self.wrs.at[g, d], self.me.ring[d])

    def hand(self, g, d, ref, across):
        zz = (self.me.z + self.me.dp - d) % self.me.dp
        src = self.mine(g) if d == 0 else self.block(ref, zz, g)
        ss, rs = (self.yss, self.yrs) if across else (self.fss, self.frs)
        peer = self.me.across_core(self.me.y) if across else self.me.mate
        return push(src, self.block(self.full, zz, g), ss.at[g, d], rs.at[g, d], peer)

    def both(self, do):
        @pl.when(self.collects & self.keeps)
        def _():
            do(self.full, True)

        @pl.when(self.collects & jnp.logical_not(self.keeps))
        def _():
            do(self.gat, False)

    def send_ring(self):
        def do(ref, keeps):
            for g in range(len(self.groups)):
                for d in range(self.me.dp - 1):
                    self.out(g, d, ref).start()

        self.both(do)

    def send_own(self, g):
        def do(ref, keeps):
            self.hand(g, 0, ref, True).start()
            if keeps:
                self.local(g).start()
            else:
                self.hand(g, 0, ref, False).start()

        self.both(do)

    def forward(self, g, blocks=None):
        def do(ref, keeps):
            for d in range(self.me.dp - 1) if blocks is None else blocks:
                self.out(g, d, ref).wait_recv()
                self.hand(g, d + 1, ref, True).start()
                if not keeps:
                    self.hand(g, d + 1, ref, False).start()

        self.both(do)

    def ready(self, g):
        me = self.me

        @pl.when(self.collects & self.keeps)
        def _():
            self.local(g).wait()

        @pl.when(me.s != me.y)
        def _():
            for d in range(me.dp):
                self.hand(g, d, self.full, True).wait_recv()

        @pl.when((me.s == me.y) & jnp.logical_not(self.collects))
        def _():
            for d in range(me.dp):
                self.hand(g, d, self.full, False).wait_recv()

    def finish(self):
        def do(ref, keeps):
            for g in range(len(self.groups)):
                for d in range(self.me.dp - 1):
                    self.out(g, d, ref).wait_send()
                for d in range(self.me.dp):
                    self.hand(g, d, ref, True).wait_send()
                    if not keeps:
                        self.hand(g, d, ref, False).wait_send()

        self.both(do)

    @staticmethod
    def scratch(dp, n):
        return [DMA((n,)), DMA((n, dp - 1)), DMA((n, dp - 1))] + [DMA((n, dp))] * 4


class GradReduce:
    def __init__(self, me, layer, src, mine, got, across, sb, rb, own, sems):
        self.me, self.layer, self.src, self.mine, self.got, self.across = me, layer, src, mine, got, across
        self.sb, self.rb, self.own = sb, rb, own
        self.hss, self.hrs, self.yss, self.yrs, self.pss, self.prs = sems
        self.rows = own.shape[0]
        self.some = 96 if self.rows % 96 == 0 else 48
        self.sums = me.s == layer
        self.holds = me.y == layer

    @staticmethod
    def scratch(dp):
        return [DMA((1,)), DMA((1,)), DMA((dp,)), DMA((dp,)), DMA((dp - 1,)), DMA((dp - 1,))]

    def hand(self):
        return push(self.src, self.got, self.hss.at[0], self.hrs.at[0], self.me.mate)

    def zz(self, d):
        return (self.me.z + d + 1) % self.me.dp

    def over(self, d):
        rr = ds(self.zz(d) * self.rows, self.rows)
        peer = self.me.across_core(self.layer)
        return push(self.src.at[rr], self.across.at[rr], self.yss.at[d], self.yrs.at[d], peer)

    def out(self, d):
        return push(self.sb.at[d], self.rb.at[d], self.pss.at[d], self.prs.at[d], self.me.ring[d])

    def send(self):
        me = self.me

        @pl.when(me.s != me.y)
        def _():
            for d in range(me.dp):
                self.over(d).start()

        @pl.when((me.s == me.y) & jnp.logical_not(self.sums))
        def _():
            self.hand().start()

    def step(self, d):
        me = self.me

        @pl.when(self.sums)
        def _():
            if d == 0:

                @pl.when(jnp.logical_not(self.holds))
                def _():
                    self.hand().wait_recv()

            self.over(d).wait_recv()
            last = d == me.dp - 1
            step = self.some

            def add(ref):
                def body(i, _):
                    rr = ds(self.zz(d) * self.rows + i * step, step)
                    value = ref[rr, :].astype(F32) + self.across[rr, :].astype(F32)
                    if last:
                        self.own[ds(i * step, step), :] = value
                    else:
                        self.sb[d, ds(i * step, step), :] = value.astype(BF)
                    return 0

                lax.fori_loop(0, self.rows // step, body, 0)

            if self.mine is self.got:
                add(self.mine)
            else:

                @pl.when(self.holds)
                def _():
                    add(self.mine)

                @pl.when(jnp.logical_not(self.holds))
                def _():
                    add(self.got)

            if not last:
                self.out(d).start()

    def collect(self):
        me = self.me

        @pl.when(self.sums)
        def _():
            for d in range(me.dp - 1):
                self.out(d).wait_recv()

                def add(i, _, d=d):
                    rr = ds(i * self.some, self.some)
                    self.own[rr, :] += self.rb[d, rr, :].astype(F32)
                    return 0

                lax.fori_loop(0, self.rows // self.some, add, 0)
            for d in range(me.dp - 1):
                self.out(d).wait_send()

    def finish(self):
        me = self.me

        @pl.when(me.s != me.y)
        def _():
            for d in range(me.dp):
                self.over(d).wait_send()

        @pl.when((me.s == me.y) & jnp.logical_not(self.sums))
        def _():
            self.hand().wait_send()


class VectorGather:
    def __init__(self, me, sv, buf, ss, rs, own):
        self.me, self.sv, self.buf, self.ss, self.rs, self.own = me, sv, buf, ss, rs, own

    def local(self):
        me = self.me
        return pltpu.make_async_copy(self.sv, self.buf.at[me.s, me.t, me.z], self.own)

    def stage(self, n):
        me = self.me
        if n == 0:
            dst = self.buf.at[me.s, me.t, me.z]
            return [push(self.sv, dst, self.ss.at[d], self.rs.at[d], peer) for d, peer in enumerate(me.ring)]
        base = me.dp - 1
        if n == 1:
            ref = self.buf.at[me.s, me.t]
            return [
                push(ref, ref, self.ss.at[base + d], self.rs.at[base + d], peer) for d, peer in enumerate(me.group)
            ]
        i = base + me.tensor - 1
        ref = self.buf.at[me.s]
        return [push(ref, ref, self.ss.at[i], self.rs.at[i], me.mate)]

    def send(self, n):
        if n == 0:
            self.local().start()
        for c in self.stage(n):
            c.start()

    def wait(self, n):
        if n == 0:
            self.local().wait()
        for c in self.stage(n):
            c.wait_recv()

    def finish(self):
        for n in range(3):
            for c in self.stage(n):
                c.wait_send()

    def build(self, vecs, heads, own, qw, fw):
        me, buf = self.me, self.buf
        for layer in range(2):
            wide = [buf[layer, tt, zz, 0:8, :][:, 0:own] for zz in range(me.dp) for tt in range(me.tensor)]
            vecs[layer, 0:8, :] = jnp.concatenate(wide, axis=1)
            here = [buf[layer, me.quarter, zz] for zz in range(me.dp)]
            by = [jnp.concatenate([p[6 + h : 7 + h, 0:qw] for p in here], axis=1) for h in range(heads)]
            qb = []
            for part in range(3):
                qb += [b[:, part * HD : (part + 1) * HD] for b in by] + [jnp.zeros((1, HW - heads * HD), F32)]
            vecs[layer, 6:7, :] = jnp.concatenate(qb, axis=1)
            fb = [p[6 + heads + h : 7 + heads + h, 0:fw] for h in range(heads) for p in here]
            vecs[layer, 7:8, :] = jnp.concatenate(fb, axis=1)


class VectorReduce:
    def __init__(self, me, va, vr, ss, rs):
        self.me, self.va, self.vr, self.ss, self.rs = me, va, vr, ss, rs

    def stage(self, n):
        me, va, vr, ss, rs = self.me, self.va, self.vr, self.ss, self.rs
        peers, base = [([me.across], 0), (me.ring, 1), ([me.mate, me.beside, me.beside_mate], me.dp)][n]
        return [push(va.at[n], vr.at[base + d], ss.at[base + d], rs.at[base + d], p) for d, p in enumerate(peers)]

    def send(self, n):
        for c in self.stage(n):
            c.start()

    def add(self, n, out):
        base = [0, 1, self.me.dp][n]
        for c in self.stage(n):
            c.wait_recv()
        if n < 2:
            total = self.va[n]
            for d in range(len(self.stage(n))):
                total = total + self.vr[base + d]
            out[...] = total
            return
        mine, mate = self.va[2], self.vr[base]
        row = lax.broadcasted_iota(jnp.int32, mine.shape, 0)
        quarter = jnp.where(self.me.s == self.me.y, mine, mate)
        out[...] = jnp.where(row % 8 < 6, mine + mate + self.vr[base + 1] + self.vr[base + 2], quarter)

    def finish(self):
        for n in range(3):
            for c in self.stage(n):
                c.wait_send()


def document_tables(seg, live, fr_ref, tab, srow, kcol):
    seq = seg.shape[1]
    count = lax.broadcasted_iota(jnp.int32, seg.shape, 1)
    start = jnp.zeros_like(seg)
    for doc in range(DOCS - 1):
        before = jnp.sum(jnp.where(seg == doc, 1.0, 0.0), axis=1, keepdims=True).astype(jnp.int32)
        start = start + jnp.where(seg > doc, before, 0)
    ang = fr_ref[:, 0:1] * (count - start).astype(F32)
    cs, sn = jnp.cos(ang), jnp.sin(ang)
    one = jnp.ones((HD - ROT, seq), F32)
    tab[:, 0:128] = jnp.concatenate([cs, cs, one] * 2, axis=0).T
    tab[:, 128:256] = jnp.concatenate([-sn, sn, jnp.zeros_like(one)] * 2, axis=0).T
    srow[...] = jnp.broadcast_to(seg, srow.shape)
    keys = jnp.where(count < live * LIVE, seg, -1).astype(F32)
    for b in range(seq // QB):
        part = jnp.broadcast_to(keys[:, b * QB : (b + 1) * QB], (128, QB))
        kcol[b * QB : (b + 1) * QB, :] = part.T.astype(jnp.int32)


QKV, FC1, FC2, OUT = 0, 1, 2, 3


def columns(model, ff):
    return {"qkv": 0, "fc1": 3 * HW, "fc2": 3 * HW + ff, "out": 3 * HW + 2 * ff, "end": 3 * HW + 2 * ff + HW}


def project_norm(r0, half, hf, vec, n1, n2):
    rows = ds(r0, half)
    xc, r = norm_stats(hf[rows, :].astype(F32))
    xh = xc * r
    n1[rows, :] = (xh * vec[0:1, :] + vec[1:2, :]).astype(BF)
    n2[rows, :] = (xh * vec[3:4, :] + vec[4:5, :]).astype(BF)


def project_qkv(r0, half, wqkv, vec, tab, n1, q, k, v):
    rows = ds(r0, half)
    a = n1[rows, :]
    for part, dst in enumerate((q, k, v)):
        cols = slice(part * HW, (part + 1) * HW)
        y = dot(a, wqkv[:, cols]) + vec[6:7, cols]
        if part < 2:
            y = turn_lanes(y, tab[rows, :], 1)
        if part == 0:
            y = y * 0.125
        dst[rows, :] = y.astype(BF)


def project_fc1(r0, half, wfc1, vec, n2, g, gp):
    rows = ds(r0, half)
    a = n2[rows, :]
    for b in range(wfc1.shape[1] // 256):
        cols = slice(b * 256, (b + 1) * 256)
        y = dot(a, wfc1[:, cols]) + vec[7:8, cols]
        cdf = 0.5 + 0.5 * lax.erf(y * 0.7071067811865476)
        g[rows, cols] = (y * cdf).astype(BF)
        gp[rows, cols] = (cdf + y * jnp.exp(-0.5 * y * y) * 0.3989422804014327).astype(BF)


def branch_out(r0, half, o, g, wout, wfc2, part):
    rows = ds(r0, half)
    for b in range(part.shape[1] // 256):
        cols = slice(b * 256, (b + 1) * 256)
        y = dg(o[rows, :], wout[cols, :], 1, 1) + dg(g[rows, :], wfc2[cols, :], 1, 1)
        part[rows, cols] = y.astype(BF)


def back_head(r0, half, dyf, hf, g, gp, n2, o, wfc1, wfc2, wout, vec, do, e2, da, acc, vg):
    rows = ds(r0, half)
    model, ff = wfc1.shape
    dy = dyf[rows, :]
    for b in range(ff // 256):
        cols = slice(b * 256, (b + 1) * 256)
        y = dot(dy, wfc2[:, cols]) * gp[rows, cols].astype(F32)
        low = y.astype(BF)
        da[:, cols] = low
        vg[7:8, cols] += jnp.sum(low.astype(F32), axis=0, keepdims=True)
    do[rows, :] = dot(dy, wout[...]).astype(BF)
    xc, r = norm_stats(hf[rows, :].astype(F32))
    xh = xc * r
    for b in range(model // 256):
        cols = slice(b * 256, (b + 1) * 256)
        dn = dg(da[...], wfc1[cols, :], 1, 1)
        vg[3:4, cols] += jnp.sum(dn * xh[:, cols], axis=0, keepdims=True)
        vg[4:5, cols] += jnp.sum(dn, axis=0, keepdims=True)
        e2[rows, cols] = (dn * vec[3:4, cols]).astype(BF)
    n2t = n2[rows, :].T
    dyt = dy.T
    for b in range(ff // 256):
        cols = slice(b * 256, (b + 1) * 256)
        acc[:, cols] += dot(n2t, da[:, cols])
        acc[:, ff + b * 256 : ff + (b + 1) * 256] += dot(dyt, g[rows, cols])
    acc[:, 2 * ff :] += dot(dyt, o[rows, :])


def back_tail(r0, half, dmix, hf, e2, wqkv, vec, part, vg):
    rows = ds(r0, half)
    dm = dmix[rows, :]
    vg[6:7, :] += jnp.sum(dm.astype(F32), axis=0, keepdims=True)
    xc, r = norm_stats(hf[rows, :].astype(F32))
    xh = xc * r
    for b in range(part.shape[1] // 256):
        cols = slice(b * 256, (b + 1) * 256)
        dn = dg(dm, wqkv[cols, :], 1, 1)
        vg[0:1, cols] += jnp.sum(dn * xh[:, cols], axis=0, keepdims=True)
        vg[1:2, cols] += jnp.sum(dn, axis=0, keepdims=True)
        part[rows, cols] = (dn * vec[0:1, cols] + e2[rows, cols].astype(F32)).astype(BF)


def qkv_grad(n1, dmix, acc, half):
    acc[...] = jnp.zeros_like(acc)

    def body(i, _):
        rows = ds(i * half, half)
        n1t = n1[rows, :].T
        for b in range(3):
            cols = slice(b * HW, (b + 1) * HW)
            acc[:, cols] += dot(n1t, dmix[rows, cols])
        return 0

    lax.fori_loop(0, n1.shape[0] // half, body, 0)


def store_low(acc, out):
    def body(i, _):
        rr = ds(i * SUB, SUB)
        out[rr, :] = acc[rr, :].astype(BF)
        return 0

    lax.fori_loop(0, acc.shape[0] // SUB, body, 0)


def residual_out(sc, own, vec, write, after=None):
    for a in range(2):
        sc.arrive(a)

        def body(i, _, a=a):
            base = own[ds(sc.own(sc.side(a)) + i * SUB, SUB), :].astype(F32)
            write(a, i, (base + sc.total(a, i) + vec[2:3, :] + vec[5:6, :]).astype(BF))
            return 0

        lax.fori_loop(0, sc.half // SUB, body, 0)
        if after is not None:
            after(a)


def grad_out(sc, dy, hf, vec, write, after=None):
    for a in range(2):
        sc.arrive(a)

        def body(i, _, a=a):
            rr = ds(sc.own(sc.side(a)) + i * SUB, SUB)
            xc, r = norm_stats(hf[rr, :].astype(F32))
            xh = xc * r
            e = sc.total(a, i)
            m1 = jnp.mean(e, axis=-1, keepdims=True)
            m2 = jnp.mean(e * xh, axis=-1, keepdims=True)
            write(a, i, (dy(a, i).astype(F32) + r * (e - m1 - xh * m2)).astype(BF))
            return 0

        lax.fori_loop(0, sc.half // SUB, body, 0)
        if after is not None:
            after(a)


def column_sum(tok, ref, vg, row):
    total = jnp.zeros((1, ref.shape[1]), F32)
    for a in range(2):

        def body(i, acc, a=a):
            return acc + jnp.sum(ref[ds(tok.own(a) + i * SUB, SUB), :].astype(F32), axis=0, keepdims=True)

        total = lax.fori_loop(0, tok.half // SUB, body, total)
    vg[row : row + 1, :] = total


def load(pairs, sem):
    copies = [pltpu.make_async_copy(a, b, sem.at[i]) for i, (a, b) in enumerate(pairs)]
    for c in copies:
        c.start()
    return copies


def params(cid):
    return pltpu.CompilerParams(collective_id=cid, has_side_effects=True, vmem_limit_bytes=67043328)


def cost(us):
    return pl.CostEstimate(flops=int(us * 8e8), bytes_accessed=0, transcendentals=0)


class Stores:
    def __init__(self, pairs, half, sem):
        self.pairs, self.half, self.sem = pairs, half, sem

    def copy(self, n, r0, i):
        src, dst = self.pairs[n]
        rows = ds(r0, self.half)
        return pltpu.make_async_copy(src.at[rows], dst.at[rows], self.sem.at[n, i])

    def start(self, which, r0, i):
        for n in which:
            self.copy(n, r0, i).start()

    def finish(self):
        def body(i, _):
            for n in range(len(self.pairs)):
                self.copy(n, i * self.half, i).wait()
            return 0

        lax.fori_loop(0, 8, body, 0)


def in_kernel(
    cfg, in_ref, cot_ref, seg_ref, live, w_ref, sv_ref, fr_ref,
    hf_o, n1_o, n2_o, g_o, gp_o, tab_o, w_o, q_o, k_o, v_o, cf_o, vecs, srow, kcol,
    hf, n1, n2, g, gp, tab, q, k, v, wfull, gat, vb, cot, gss, grs, css, crs, yss, yrs, lsem, ssem, vss, vrs, *wsems,
):
    col, dp, tensor = cfg["col"], cfg["dp"], cfg["tensor"]
    me = Mesh(dp, tensor)
    ga = Gather(me, hf, gss, grs, me.y)
    gc = Gather(me, cf_o, css, crs, me.y)
    half = ga.half
    part = ds(me.s * half, half)
    first = pltpu.make_async_copy(in_ref.at[me.y, 0, part], hf.at[ds(ga.own(me.y), half)], lsem.at[0])
    first.start()
    up = pltpu.make_async_copy(cot_ref.at[me.y, 0, part], cot, lsem.at[4])
    up.start()
    greet([me.mate, me.across_mate] + me.ring + me.group)
    over = [
        push(ref.at[1 - me.y, 0, part], full.at[ds(ga.own(me.y), half)], yss.at[n], yrs.at[n], me.across)
        for n, (ref, full) in enumerate(((in_ref, hf), (cot_ref, cf_o)))
    ]
    wg = WeightGather(me, 0, w_ref, wfull, gat, cfg["groups"], wsems)
    vg = VectorGather(me, sv_ref, vb, vss, vrs, lsem.at[1])
    st = Stores([(hf, hf_o), (n1, n1_o), (n2, n2_o), (g, g_o), (gp, gp_o), (q, q_o), (k, k_o), (v, v_o)], half, ssem)
    vg.send(0)
    wg.send_ring()
    first.wait()
    document_tables(seg_ref[me.y], live[0, me.y], fr_ref, tab, srow, kcol)
    vg.wait(0)
    vg.send(1)
    ga.start(0)
    over[0].start()
    wg.send_own(0)
    tab_out = pltpu.make_async_copy(tab, tab_o, lsem.at[2])
    tab_out.start()
    vg.wait(1)
    vg.send(2)
    up.wait()
    cot_out = pltpu.make_async_copy(cot, cf_o.at[ds(gc.own(me.y), half)], lsem.at[5])
    cot_out.start()
    vg.wait(2)
    vg.build(vecs, cfg["heads"], cfg["own"], cfg["qw"], cfg["fw"])
    vec = vecs.at[0]

    def norm(r0, i):
        project_norm(r0, half, hf, vec, n1, n2)
        st.start((0, 1, 2), r0, i)

        @pl.when(i == 0)
        def _():
            over[0].wait_recv()
            ga.start(1)

        @pl.when(i == 1)
        def _():
            wg.forward(0)
            wg.send_own(1)
            wg.send_own(2)

    ga.run(norm)
    cot_out.wait()
    gc.start(0)
    wg.ready(0)

    def qkv(i, _):
        r0 = ga.order(i)
        project_qkv(r0, half, wfull.at[:, 0 : col["fc1"]], vec, tab, n1, q, k, v)
        st.start((5, 6, 7), r0, i)
        return 0

    lax.fori_loop(0, 8, qkv, 0)
    wg.forward(1)
    over[1].start()
    wg.ready(1)

    def fc1(i, _):
        r0 = ga.order(i)
        project_fc1(r0, half, wfull.at[:, col["fc1"] : col["fc2"]], vec, n2, g, gp)
        st.start((3, 4), r0, i)

        @pl.when(i == 6)
        def _():
            wg.forward(2)

        return 0

    lax.fori_loop(0, 8, fc1, 0)
    gc.step(2)
    gc.step(4)
    over[1].wait_recv()
    gc.start(1)
    st.finish()
    tab_out.wait()
    wg.ready(2)
    w_out = pltpu.make_async_copy(wfull, w_o, lsem.at[3])
    w_out.start()
    for n in (3, 5, 6, 7):
        gc.step(n)
    wg.finish()
    vg.finish()
    gc.finish()
    for c in over:
        c.wait_send()
    w_out.wait()


def layer_in(cfg, inputs, cotangent, segments, live, w, sv, fr):
    seq, model, ff = segments.shape[2], inputs.shape[3], cfg["ff"]
    dp, tensor = cfg["dp"], cfg["tensor"]
    rows, hidden = sds((seq, model), BF), sds((seq, ff), BF)
    heads = sds((seq, HW), BF)
    nv = dp - 1 + tensor
    wide, wide_h, wide_q = pltpu.VMEM((seq, model), BF), pltpu.VMEM((seq, ff), BF), pltpu.VMEM((seq, HW), BF)
    weights = pltpu.VMEM((model, w.shape[1]), BF)
    return pl.pallas_call(
        functools.partial(in_kernel, cfg),
        out_shape=(rows, rows, rows, hidden, hidden, sds((seq, 256), F32), sds((model, w.shape[1]), BF),
                   heads, heads, heads, rows,
                   sds((2, 8, model), F32), sds((8, seq), jnp.int32), sds((seq, 128), jnp.int32)),
        in_specs=[ANY, ANY, VMEM, SMEM, VMEM, VMEM, VMEM],
        out_specs=(ANY,) * 11 + (VMEM,) * 3,
        scratch_shapes=[
            wide, wide, wide, wide_h, wide_h, pltpu.VMEM((seq, 256), F32), wide_q, wide_q, wide_q,
            weights, weights, pltpu.VMEM((2, tensor, dp) + sv.shape, F32),
            pltpu.VMEM((seq // 8, model), BF),
            DMA((6,)), DMA((6,)), DMA((6,)), DMA((6,)), DMA((2,)), DMA((2,)), DMA((6,)), DMA((8, 8)),
            DMA((nv,)), DMA((nv,)),
        ]
        + WeightGather.scratch(dp, 3),
        compiler_params=params(2),
        cost_estimate=cost(45),
        name="layer_in",
    )(inputs, cotangent, segments, live, w, sv, fr)


def mid_kernel(
    cfg, q_in, k_in, v_in, srow, kcol, g_in, x_in, w_ref, w0, vecs, tab_in,
    o_o, lse, hf_o, n1_o, n2_o, g_o, gp_o, w_o, q_o, k_o, v_o,
    wout, wfc2, hf, n1, n2, g, gp, tab, wfull, gat, q, k, v, o, vt, s_scr,
    part, mr, xr, sss, srs, gss, grs, lsem, ssem, osem, *wsems,
):
    col, heads = cfg["col"], cfg["heads"]
    me = Mesh(cfg["dp"], cfg["tensor"])
    sc = Scatter(me, part, mr, xr, sss, srs)
    ga = Gather(me, hf, gss, grs)
    half = sc.half
    loads = load(
        [
            (v_in, v),
            (q_in, q),
            (k_in, k),
            (w0.at[:, col["out"] : col["end"]], wout),
            (w0.at[:, col["fc2"] : col["out"]], wfc2),
            (g_in, g),
            (tab_in, tab),
        ]
        + [(x_in.at[ds(sc.own(a), half)], hf.at[ds(sc.own(a), half)]) for a in range(2)],
        lsem,
    )
    greet([me.mate, me.beside, me.across, me.across_mate] + me.ring)
    wg = WeightGather(me, 1, w_ref, wfull, gat, cfg["groups"], wsems)
    wg.send_ring()
    for n in range(3):
        wg.send_own(n)
    loads[0].wait()
    turn_blocks(v, vt)
    for c in loads[1:]:
        c.wait()
    st = Stores([(hf, hf_o), (n1, n1_o), (n2, n2_o), (g, g_o), (gp, gp_o), (q, q_o), (k, k_o), (v, v_o)], half, ssem)
    st_o = Stores([(o, o_o)], half, osem)

    def out(r0, i):
        b = r0 // QB
        attn_fwd_block(b, jnp.maximum(b - DOC_MAX // QB, 0), b, heads, q, k, vt, srow, kcol, s_scr, o, lse)
        st_o.start((0,), r0, i)
        branch_out(r0, half, o, g, wout, wfc2, part)

        @pl.when(i == 5)
        def _():
            wg.forward(0)

    sc.run(out)

    def write(a, i, value):
        hf[ds(sc.own(a) + i * SUB, SUB), :] = value

    residual_out(sc, hf, vecs.at[0], write, ga.start)
    wg.forward(1)
    vec = vecs.at[1]

    def fc1(i):
        r0 = ga.order(i)
        project_fc1(r0, half, wfull.at[:, col["fc1"] : col["fc2"]], vec, n2, g, gp)
        st.start((3, 4), r0, i)

    def work(r0, i):
        project_norm(r0, half, hf, vec, n1, n2)

        @pl.when(i == 0)
        def _():
            wg.ready(0)

        project_qkv(r0, half, wfull.at[:, 0 : col["fc1"]], vec, tab, n1, q, k, v)
        st.start((0, 1, 2, 5, 6, 7), r0, i)

        @pl.when(i == 4)
        def _():
            wg.ready(1)

        @pl.when(i >= 4)
        def _():
            fc1(i - 4)

        @pl.when(i == 5)
        def _():
            wg.forward(2)

    ga.run(work)

    def late(i, _):
        fc1(i)
        return 0

    lax.fori_loop(4, 8, late, 0)
    st.finish()
    wg.ready(2)
    w_out = pltpu.make_async_copy(wfull, w_o, lsem.at[0])
    w_out.start()
    sc.finish()
    wg.finish()
    st_o.finish()
    w_out.wait()


def layer_mid(cfg, q, k, v, srow, kcol, g, xf, w, w0, vecs, tab):
    seq, model, ff = tab.shape[0], xf.shape[1], cfg["ff"]
    rows, hidden, heads = sds((seq, model), BF), sds((seq, ff), BF), sds((seq, HW), BF)
    wide, wide_h, wide_q = pltpu.VMEM((seq, model), BF), pltpu.VMEM((seq, ff), BF), pltpu.VMEM((seq, HW), BF)
    return pl.pallas_call(
        functools.partial(mid_kernel, cfg),
        out_shape=(heads, sds((8, seq), F32), rows, rows, rows, hidden, hidden, sds(w0.shape, BF), heads, heads, heads),
        in_specs=[ANY, ANY, ANY, VMEM, VMEM, ANY, ANY, VMEM, ANY, VMEM, ANY],
        out_specs=(ANY, VMEM) + (ANY,) * 9,
        scratch_shapes=[
            pltpu.VMEM((model, HW), BF), pltpu.VMEM((model, ff), BF),
            wide, wide, wide, wide_h, wide_h, pltpu.VMEM((seq, 256), F32),
            pltpu.VMEM(w0.shape, BF), pltpu.VMEM(w0.shape, BF),
            wide_q, wide_q, wide_q, wide_q, pltpu.VMEM((HW, seq), BF),
            pltpu.VMEM((cfg["heads"], DOC_MAX + QB, QB), F32),
        ]
        + scatter_scratch(seq, model)
        + [DMA((6,)), DMA((6,)), DMA((9,)), DMA((8, 8)), DMA((1, 8))]
        + WeightGather.scratch(cfg["dp"], 3),
        compiler_params=params(3),
        cost_estimate=cost(70),
        name="layer_mid",
    )(q, k, v, srow, kcol, g, xf, w, w0, vecs, tab)


def turn_kernel(
    cfg, o_in, g_in, hf_in, cf, w1, vecs, n2_in, gp_in, y_o, do_o, e2_o, gr_o, vg,
    o, g, hf, dyf, n2, gp, e2, do, y, gr, wout, wfc2, wfc1, da, acc,
    part, mr, xr, sss, srs, lsem, ssem,
):
    col = cfg["col"]
    me = Mesh(cfg["dp"], cfg["tensor"])
    sc = Scatter(me, part, mr, xr, sss, srs)
    half = sc.half
    loads = load(
        [
            (w1.at[:, col["out"] : col["end"]], wout),
            (w1.at[:, col["fc2"] : col["out"]], wfc2),
            (o_in, o),
            (g_in, g),
            (w1.at[:, col["fc1"] : col["fc2"]], wfc1),
            (cf, dyf),
            (gp_in, gp),
            (hf_in, hf),
            (n2_in, n2),
        ],
        lsem,
    )
    greet([me.mate, me.beside])
    for c in loads[:4]:
        c.wait()
    vec = vecs.at[1]
    st = Stores([(e2, e2_o), (do, do_o)], half, ssem)

    def early():
        vg[...] = jnp.zeros_like(vg)
        acc[...] = jnp.zeros_like(acc)
        for c in loads[4:]:
            c.wait()

        def head(i, _):
            r0 = i * half
            back_head(r0, half, dyf, hf, g, gp, n2, o, wfc1, wfc2, wout, vec, do, e2, da, acc, vg)
            st.start((0, 1), r0, i)
            return 0

        lax.fori_loop(0, 8, head, 0)

    sc.run(lambda r0, i: branch_out(r0, half, o, g, wout, wfc2, part), early)
    column_sum(sc, dyf, vg, 2)
    store_low(acc, gr)
    gr_out = pltpu.make_async_copy(gr, gr_o, lsem.at[0])
    gr_out.start()

    def write(a, i, value):
        y[a, ds(i * SUB, SUB), :] = value

    residual_out(sc, hf, vec, write)
    y_out = pltpu.make_async_copy(y, y_o, lsem.at[1])
    y_out.start()
    sc.finish()
    st.finish()
    gr_out.wait()
    y_out.wait()


def layer_turn(cfg, o, g, hf, cf, w1, vecs, n2, gp):
    seq, model = hf.shape
    ff = cfg["ff"]
    wide, hidden, heads = pltpu.VMEM((seq, model), BF), pltpu.VMEM((seq, ff), BF), pltpu.VMEM((seq, HW), BF)
    owned = (2, seq // 8, model)
    return pl.pallas_call(
        functools.partial(turn_kernel, cfg),
        out_shape=(
            sds(owned, BF),
            sds((seq, HW), BF),
            sds((seq, model), BF),
            sds((model, 2 * ff + HW), BF),
            sds((8, model), F32),
        ),
        in_specs=[ANY] * 5 + [VMEM, ANY, ANY],
        out_specs=(ANY,) * 4 + (VMEM,),
        scratch_shapes=[
            heads, hidden, wide, wide, wide, hidden, wide, heads, pltpu.VMEM(owned, BF),
            pltpu.VMEM((model, 2 * ff + HW), BF),
            pltpu.VMEM((model, HW), BF), pltpu.VMEM((model, ff), BF), pltpu.VMEM((model, ff), BF),
            pltpu.VMEM((seq // 8, ff), BF), pltpu.VMEM((model, 2 * ff + HW), F32),
        ]
        + scatter_scratch(seq, model)
        + [DMA((9,)), DMA((2, 8))],
        compiler_params=params(4),
        cost_estimate=cost(40),
        name="layer_turn",
    )(o, g, hf, cf, w1, vecs, n2, gp)


def back_kernel(
    cfg, dm_in, e2_in, cf, hf_in, n1_in, w1, w0, vecs, xf_in, g_in, gp_in, n2_in, o_in, gr1,
    dh_o, e2_o, do_o, vgf, vgd, out1_o, outq_o, gr_o,
    dmix, o, do, a, b, e2, g, gp, wqkv, wout, wfc2, wfc1, dhf, da, acc, gq, gr, got, gotq, acrq,
    sb, rb, sbq, rbq, out1, outq, part, mr, xr, sss, srs, gss, grs, lsem, ssem, *rsems,
):
    col, dp = cfg["col"], cfg["dp"]
    me = Mesh(dp, cfg["tensor"])
    ga = Gather(me, dhf, gss, grs)
    sc = Scatter(me, part, mr, xr, sss, srs)
    half = sc.half
    own = [ds(sc.own(n), half) for n in range(2)]
    loads = load(
        [
            (w1.at[:, col["qkv"] : col["fc1"]], wqkv),
            (dm_in, dmix),
            (hf_in, a),
            (e2_in, e2),
            (n1_in, b),
            (w0.at[:, col["out"] : col["end"]], wout),
            (w0.at[:, col["fc2"] : col["out"]], wfc2),
            (w0.at[:, col["fc1"] : col["fc2"]], wfc1),
            (g_in, g),
            (gp_in, gp),
            (o_in, o),
        ]
        + [(cf.at[rr], dhf.at[rr]) for rr in own],
        lsem,
    )
    gr_load = pltpu.make_async_copy(gr1, gr, lsem.at[13])
    holds = (me.s == 1) & (me.y == 1)

    @pl.when(holds)
    def _():
        gr_load.start()

    greet([me.mate, me.beside, me.across, me.across_mate] + me.ring)
    red1 = GradReduce(me, 1, gr1, gr, gr, got, sb, rb, out1, rsems[:6])
    redq = GradReduce(me, 1, gq, gq, gotq, acrq, sbq, rbq, outq, rsems[6:])
    st = Stores([(e2, e2_o), (do, do_o), (dhf, dh_o)], half, ssem)
    red1.send()
    vgf[...] = jnp.zeros_like(vgf)
    vgd[...] = jnp.zeros_like(vgd)
    for c in loads[:4]:
        c.wait()

    def early():
        loads[4].wait()
        small = acc.at[:, 0 : 3 * HW]
        qkv_grad(b, dmix, small, half)
        store_low(small, gq)
        redq.send()

        @pl.when(holds)
        def _():
            gr_load.wait()

        red1.step(0)

    sc.run(lambda r0, i: back_tail(r0, half, dmix, a, e2, wqkv, vecs.at[1], part, vgf), early)
    acc[...] = jnp.zeros_like(acc)
    again = pltpu.make_async_copy(n2_in, b, lsem.at[14])
    again.start()
    for c in loads[5:]:
        c.wait()
    for d in range(1, dp // 2):
        red1.step(d)

    def write(n, i, value):
        dhf[ds(sc.own(n) + i * SUB, SUB), :] = value

    grad_out(sc, lambda n, i: dhf[ds(sc.own(n) + i * SUB, SUB), :], a, vecs.at[1], write, ga.start)
    other = pltpu.make_async_copy(xf_in, a, lsem.at[15])
    other.start()
    again.wait()
    other.wait()

    def work(r0, i):
        back_head(r0, half, dhf, a, g, gp, b, o, wfc1, wfc2, wout, vecs.at[0], do, e2, da, acc, vgd)
        st.start((0, 1, 2), r0, i)

        @pl.when(i == 1)
        def _():
            for d in range(dp // 2, dp - 1):
                red1.step(d)

        @pl.when(i == 3)
        def _():
            red1.step(dp - 1)

        @pl.when(i == 5)
        def _():
            redq.step(0)

    ga.run(work)
    for d in range(1, dp):
        redq.step(d)
    store_low(acc, gr)
    gr_out = pltpu.make_async_copy(gr, gr_o, lsem.at[0])
    gr_out.start()
    column_sum(sc, dhf, vgd, 2)
    red1.collect()
    redq.collect()
    outs = [pltpu.make_async_copy(out1, out1_o, lsem.at[1]), pltpu.make_async_copy(outq, outq_o, lsem.at[2])]
    for c in outs:
        c.start()
    red1.finish()
    redq.finish()
    sc.finish()
    st.finish()
    gr_out.wait()
    for c in outs:
        c.wait()


def layer_back(cfg, dmix, e2, cf, hf, n1, w1, w0, vecs, xf, g, gp, n2, o, gr1):
    seq, model = hf.shape
    ff, dp = cfg["ff"], cfg["dp"]
    rows, nr, nq = model // dp, 2 * ff + HW, 3 * HW
    wide, hidden, heads = pltpu.VMEM((seq, model), BF), pltpu.VMEM((seq, ff), BF), pltpu.VMEM((seq, HW), BF)
    return pl.pallas_call(
        functools.partial(back_kernel, cfg),
        out_shape=(
            sds((seq, model), BF),
            sds((seq, model), BF),
            sds((seq, HW), BF),
            sds((8, model), F32),
            sds((8, model), F32),
            sds((rows, nr), F32),
            sds((rows, nq), F32),
            sds((model, nr), BF),
        ),
        in_specs=[ANY] * 7 + [VMEM] + [ANY] * 6,
        out_specs=(ANY, ANY, ANY, VMEM, VMEM, ANY, ANY, ANY),
        scratch_shapes=[
            pltpu.VMEM((seq, nq), BF), heads, heads, wide, wide, wide, hidden, hidden,
            pltpu.VMEM((model, nq), BF), pltpu.VMEM((model, HW), BF), pltpu.VMEM((model, ff), BF),
            pltpu.VMEM((model, ff), BF), wide, pltpu.VMEM((seq // 8, ff), BF), pltpu.VMEM((model, nr), F32),
            pltpu.VMEM((model, nq), BF), pltpu.VMEM((model, nr), BF), pltpu.VMEM((model, nr), BF),
            pltpu.VMEM((model, nq), BF), pltpu.VMEM((model, nq), BF),
            pltpu.VMEM((dp - 1, rows, nr), BF), pltpu.VMEM((dp - 1, rows, nr), BF),
            pltpu.VMEM((dp - 1, rows, nq), BF), pltpu.VMEM((dp - 1, rows, nq), BF),
            pltpu.VMEM((rows, nr), F32), pltpu.VMEM((rows, nq), F32),
        ]
        + scatter_scratch(seq, model)
        + [DMA((6,)), DMA((6,)), DMA((16,)), DMA((3, 8))]
        + GradReduce.scratch(dp) * 2,
        compiler_params=params(5),
        cost_estimate=cost(70),
        name="layer_back",
    )(dmix, e2, cf, hf, n1, w1, w0, vecs, xf, g, gp, n2, o, gr1)


def last_kernel(
    cfg, q_in, k_in, v_in, o_in, do_in, lse, srow, kcol, tab_in, e2_in, dh_in, xf_in, n1_in, w0, vecs, vf1, vd1, vd0,
    gr0, out1, outq, hf_in, y_in, so, ig, fq_o, fr_o, vec_o,
    q, k, v, o, do, tab, kt, dk, dv, dmix, dh, dx, xf, n1, e2, wqkv, gq, gotq, acrq, sbq, rbq, gr, got, sb, rb, fq, fr,
    vgf, va, vr, vout, part, mr, xr, sss, srs, lsem, vss, vrs, oss, ors, *rsems,
):
    col, heads, dp = cfg["col"], cfg["heads"], cfg["dp"]
    me = Mesh(dp, cfg["tensor"])
    sc = Scatter(me, part, mr, xr, sss, srs, 1 - me.y)
    half = sc.half
    seq = xf.shape[0]
    width = q.shape[1]
    own = [ds(sc.own(n), half) for n in range(2)]
    loads = load(
        [
            (k_in, k),
            (q_in, q),
            (v_in, v),
            (do_in, do),
            (o_in, o),
            (tab_in, tab),
            (w0.at[:, col["qkv"] : col["fc1"]], wqkv),
            (xf_in, xf),
            (e2_in, e2),
            (n1_in, n1),
        ]
        + [(dh_in.at[rr], dh.at[n]) for n, rr in enumerate(own)],
        lsem,
    )
    gr_load = pltpu.make_async_copy(gr0, gr, lsem.at[12])
    holds = (me.s == 0) & (me.y == 0)

    @pl.when(holds)
    def _():
        gr_load.start()

    greet([me.mate, me.beside, me.beside_mate, me.across, me.across_mate] + me.ring)
    redr = GradReduce(me, 0, gr0, gr, gr, got, sb, rb, fr, rsems[:6])
    redq = GradReduce(me, 0, gq, gq, gotq, acrq, sbq, rbq, fq, rsems[6:])
    vr_ = VectorReduce(me, va, vr, vss, vrs)
    redr.send()

    def at(dst, h):
        return dst.at[0, me.y, 0, pl.ds(h * half, half)]

    def full_out(src, dst, i):
        chunk = 2 * half
        mine, theirs = ds(me.t * chunk, chunk), ds(me.py * chunk, chunk)
        return [
            pltpu.make_async_copy(src.at[mine], dst.at[0, me.y, 0], lsem.at[13]),
            push(src.at[theirs], dst.at[0, me.y, 0], oss.at[i], ors.at[i], me.across),
        ]

    def owned_out(src, dst, core, i):
        here, far = src.at[me.y], src.at[1 - me.y]
        place = dst.at[0, me.y, 0, ds(me.s * half, half)]
        across = push(far, place, oss.at[i], ors.at[i + me.s], me.across_core(core))
        local = pltpu.make_async_copy(here, place, lsem.at[14])
        mate = push(here, place, oss.at[i + 2], ors.at[i + 2], me.mate)
        return across, local, mate

    def whole(n):
        return full_out(hf_in, so, 0) if n == 0 else full_out(dh_in, ig, 0)

    def start_here(src, dst, core, i):
        across, local, mate = owned_out(src, dst, core, i)

        @pl.when(me.s == core)
        def _():
            local.start()

        @pl.when(me.s != core)
        def _():
            mate.start()

    def wait_owned(src, dst, core, i):
        across, local, mate = owned_out(src, dst, core, i)
        across.wait_send()

        @pl.when(me.s == core)
        def _():
            local.wait()
            mate.wait_recv()
            for n in range(2):
                push(src.at[0], at(dst, n), oss.at[i], ors.at[i + n], me.across_core(core)).wait_recv()

        @pl.when(me.s != core)
        def _():
            mate.wait_send()

    old = [pltpu.make_async_copy(out1, fr, lsem.at[15]), pltpu.make_async_copy(outq, fq, lsem.at[16])]

    @pl.when(me.s == 1)
    def _():
        for c in old:
            c.start()

    vgf[...] = jnp.zeros_like(vgf)
    dk[...] = jnp.zeros_like(dk)
    dv[...] = jnp.zeros_like(dv)
    loads[0].wait()
    turn_blocks(k, kt)
    for c in loads[1:6]:
        c.wait()

    @pl.when(holds)
    def _():
        gr_load.wait()

    n_blocks = seq // QB

    def qloop(i, _):
        lo = jnp.maximum(i - DOC_MAX // QB, 0)

        @pl.when(i == n_blocks - 2)
        def _():
            for n in range(2):

                @pl.when(me.s == n)
                def _(n=n):
                    for c in whole(n):
                        c.start()

            owned_out(y_in, so, 1, 1)[0].start()
            start_here(y_in, so, 1, 1)

        attn_bwd_block(i, lo, i, heads, q, k, v, o, do, kt, lse, srow, kcol, tab, dk, dv, dmix)
        for at_block, steps in (
            (n_blocks // 2 - 1, range(0, 1)),
            (n_blocks // 2, range(1, dp // 2)),
            (n_blocks // 2 + 1, range(dp // 2, dp - 1)),
            (n_blocks - 2, range(dp - 1, dp)),
        ):

            @pl.when(i == at_block)
            def _(steps=steps):
                for d in steps:
                    redr.step(d)

        return 0

    lax.fori_loop(0, n_blocks, qloop, 0)

    def close(i, _):
        ii = ds(i * QB, QB)
        dmix[ii, width : 2 * width] = turn_lanes(dk[ii, :], tab[ii, :], -1).astype(BF)
        dmix[ii, 2 * width : 3 * width] = dv[ii, :].astype(BF)
        return 0

    lax.fori_loop(0, n_blocks, close, 0)
    for c in loads[6:]:
        c.wait()

    def early():
        va[0, 0:8, :] = vgf[...] + vd0[...]
        va[0, 8:16, :] = vf1[...] + vd1[...]
        vr_.send(0)
        nf = gq.shape[0]
        accs = [dk.at[0:nf], dk.at[nf : 2 * nf], dv.at[0:nf]]
        for acc in accs:
            acc[...] = jnp.zeros_like(acc)

        def body(i, _):
            rows = ds(i * half, half)
            n1t = n1[rows, :].T
            for p, acc in enumerate(accs):
                acc[...] += dot(n1t, dmix[rows, p * HW : (p + 1) * HW])
            return 0

        lax.fori_loop(0, 8, body, 0)
        for p, acc in enumerate(accs):
            gq[:, p * HW : (p + 1) * HW] = acc[...].astype(BF)
        vr_.add(0, va.at[1])
        vr_.send(1)
        redq.send()
        vr_.add(1, va.at[2])
        vr_.send(2)
        redq.step(0)

    sc.run(lambda r0, i: back_tail(r0, half, dmix, xf, e2, wqkv, vecs.at[0], part, vgf), early)
    for d in range(1, dp - 1):
        redq.step(d)

    def write(n, i, value):
        dx[sc.side(n), ds(i * SUB, SUB), :] = value

    def leave(n):
        if n == 0:
            owned_out(dx, ig, 0, 4)[0].start()
        else:
            start_here(dx, ig, 0, 4)

    grad_out(sc, lambda n, i: dh[sc.side(n), ds(i * SUB, SUB), :], xf, vecs.at[0], write, leave)
    redq.step(dp - 1)
    vr_.add(2, vout)
    vec_o[...] = jnp.where(me.s == 0, vout[0:8, :], vout[8:16, :])
    redr.collect()
    redq.collect()

    @pl.when(me.s == 1)
    def _():
        for c in old:
            c.wait()

    ends = [pltpu.make_async_copy(fr, fr_o, lsem.at[0]), pltpu.make_async_copy(fq, fq_o, lsem.at[1])]
    for c in ends:
        c.start()
    redr.finish()
    redq.finish()
    vr_.finish()
    sc.finish()
    for n in range(2):

        @pl.when(me.s == n)
        def _(n=n):
            for c in whole(n):
                c.wait()

    wait_owned(y_in, so, 1, 1)
    wait_owned(dx, ig, 0, 4)
    for c in ends:
        c.wait()


def layer_last(cfg, q, k, v, o, do, lse, sr, kc, tab, e2, dh, xf, n1, w0, vecs, vf1, vd1, vd0, gr0, out1, outq, hf, y):
    seq, model = xf.shape
    dp, tensor, ff = cfg["dp"], cfg["tensor"], cfg["ff"]
    rows, nr, nq = model // dp, 2 * ff + HW, 3 * HW
    nv = dp + tensor - 1
    wide, owned, heads = pltpu.VMEM((seq, model), BF), pltpu.VMEM((2, seq // 8, model), BF), pltpu.VMEM((seq, HW), BF)
    both = sds((1, 2, 1, seq // 4, model), BF)
    return pl.pallas_call(
        functools.partial(last_kernel, cfg),
        out_shape=(both, both, sds((rows, nq), F32), sds((rows, nr), F32), sds((8, model), F32)),
        in_specs=[ANY] * 5 + [VMEM] * 3 + [ANY] * 6 + [VMEM] * 4 + [ANY] * 5,
        out_specs=(ANY, ANY, ANY, ANY, VMEM),
        scratch_shapes=[
            heads, heads, heads, heads, heads, pltpu.VMEM(tab.shape, F32), pltpu.VMEM((HW, seq), BF),
            pltpu.VMEM((seq, HW), F32), pltpu.VMEM((seq, HW), F32), pltpu.VMEM((seq, nq), BF), owned, owned,
            wide, wide, wide, pltpu.VMEM((model, nq), BF),
            pltpu.VMEM((model, nq), BF), pltpu.VMEM((model, nq), BF), pltpu.VMEM((model, nq), BF),
            pltpu.VMEM((dp - 1, rows, nq), BF), pltpu.VMEM((dp - 1, rows, nq), BF),
            pltpu.VMEM((model, nr), BF), pltpu.VMEM((model, nr), BF),
            pltpu.VMEM((dp - 1, rows, nr), BF), pltpu.VMEM((dp - 1, rows, nr), BF),
            pltpu.VMEM((rows, nq), F32), pltpu.VMEM((rows, nr), F32),
            pltpu.VMEM((8, model), F32), pltpu.VMEM((3, 16, model), F32), pltpu.VMEM((nv, 16, model), F32),
            pltpu.VMEM((16, model), F32),
        ]
        + scatter_scratch(seq, model)
        + [DMA((17,)), DMA((nv,)), DMA((nv,)), DMA((7,)), DMA((7,))]
        + GradReduce.scratch(dp) * 2,
        compiler_params=params(6),
        cost_estimate=cost(80),
        name="layer_last",
    )(q, k, v, o, do, lse, sr, kc, tab, e2, dh, xf, n1, w0, vecs, vf1, vd1, vd0, gr0, out1, outq, hf, y)


def finish_kernel(
    cfg, so_in, ig_in, fq_in, fr_in, vec, so, ig, bg1, bb1, gqkv, bqkv, gout, bdy, bdy2, bg2, bb2, gfc1, bfc1, gfc2,
    a, b, fq, fr, lsem, osem,
):
    heads, ff, own, qw, fw = cfg["heads"], cfg["ff"], cfg["own"], cfg["qw"], cfg["fw"]
    me = Mesh(cfg["dp"], cfg["tensor"])
    loads = load([(so_in, a), (ig_in, b), (fr_in, fr), (fq_in, fq)], lsem)
    model = vec.shape[1]
    short = pltpu.roll(vec[...], (model - (me.z * me.tensor + me.t) * own) % model, 1)
    for row, ref in ((0, bg1), (1, bb1), (2, bdy), (2, bdy2), (3, bg2), (4, bb2)):
        ref[...] = short[row : row + 1, 0:own]
    for h in range(heads):
        parts = [vec[6:7, p * HW + h * HD : p * HW + (h + 1) * HD] for p in range(3)]
        one = jnp.concatenate(parts + [jnp.zeros((1, HW - 3 * HD), F32)], axis=1)
        one = jnp.broadcast_to(one, (8, HW))
        bqkv[h] = pltpu.roll(one, (HW - me.z * qw) % HW, 1)[0:1, 0:qw]
        wide = ff // heads
        one = jnp.broadcast_to(vec[7:8, h * wide : (h + 1) * wide], (8, wide))
        bfc1[h] = pltpu.roll(one, (wide - me.z * fw) % wide, 1)[0:1, 0:fw]
    loads[0].wait()
    loads[1].wait()
    outs = [pltpu.make_async_copy(a, so, osem.at[0]), pltpu.make_async_copy(b, ig, osem.at[1])]
    for c in outs:
        c.start()
    loads[2].wait()
    gfc1[0] = fr[:, 0:ff]
    gfc2[...] = fr[:, ff : 2 * ff]
    gout[0] = fr[:, 2 * ff : 2 * ff + HW].T[0 : heads * HD, :]
    loads[3].wait()
    pieces = [fq[:, p * HW + h * HD : p * HW + (h + 1) * HD] for h in range(heads) for p in range(3)]
    gqkv[0] = jnp.concatenate(pieces, axis=1)
    for c in outs:
        c.wait()


def finish(cfg, so, ig, fq, fr, vec):
    heads, ff, rows = cfg["heads"], cfg["ff"], fq.shape[0]
    line = sds((1, cfg["own"]), F32)
    return pl.pallas_call(
        functools.partial(finish_kernel, cfg),
        out_shape=(sds(so.shape, BF), sds(ig.shape, BF), line, line, sds((1, rows, heads * 3 * HD), F32),
                   sds((heads, 1, cfg["qw"]), F32), sds((1, heads * HD, rows), F32), line, line, line, line,
                   sds((1, rows, ff), F32), sds((heads, 1, cfg["fw"]), F32), sds((rows, ff), F32)),
        in_specs=[ANY] * 4 + [VMEM],
        out_specs=(ANY, ANY) + (VMEM,) * 12,
        scratch_shapes=[
            pltpu.VMEM(so.shape, BF), pltpu.VMEM(ig.shape, BF), pltpu.VMEM(fq.shape, F32), pltpu.VMEM(fr.shape, F32),
            DMA((4,)), DMA((2,)),
        ],
        compiler_params=pltpu.CompilerParams(vmem_limit_bytes=67043328),
        cost_estimate=cost(5),
        name="finish",
    )(so, ig, fq, fr, vec)


def by_part(w):
    rows = w.shape[0]
    heads = w.shape[1] // (3 * HD)
    w = w.reshape(rows, heads, 3, HD).transpose(0, 2, 1, 3).reshape(rows, 3, heads * HD)
    return jnp.pad(w, ((0, 0), (0, 0), (0, HW - heads * HD))).reshape(rows, 3 * HW)


def shards(
    dp, tensor, inputs, cotangent, segments, live_blocks, ln1_gain, ln1_bias, qkv_weight, qkv_bias,
    out_weight, out_bias, ln2_gain, ln2_bias, fc1_weight, fc1_bias, fc2_weight, fc2_bias,
):
    live_blocks = live_blocks.T
    model = inputs.shape[-1]
    ff = fc1_weight.shape[2]
    heads = qkv_bias.shape[1]
    col = columns(model, ff)
    wout = jnp.pad(out_weight[0].T, ((0, 0), (0, HW - heads * HD)))
    w = jnp.concatenate([by_part(qkv_weight[0]), fc1_weight[0], fc2_weight[0].T, wout], axis=1)
    small = jnp.stack([ln1_gain[0], ln1_bias[0], out_bias[0], ln2_gain[0], ln2_bias[0], fc2_bias[0]])

    def lanes(a):
        return jnp.pad(a.astype(F32), ((0, 0), (0, 128 - a.shape[1])))

    sv = jnp.concatenate([lanes(small), lanes(qkv_bias[0]), lanes(fc1_bias[0])], axis=0)
    sv = jnp.pad(sv, ((0, -sv.shape[0] % 8), (0, 0)))
    fr = np.float32(10000.0) ** (-(np.arange(ROT // 2, dtype=np.float32) * np.float32(2.0 / ROT)))
    fr = jnp.asarray(np.broadcast_to(fr[:, None], (ROT // 2, 128)).astype(np.float32))
    cfg = {
        "col": col, "ff": ff, "heads": heads, "dp": dp, "tensor": tensor, "own": small.shape[1],
        "qw": qkv_bias.shape[2], "fw": fc1_bias.shape[2],
        "groups": [(0, col["fc1"]), (col["fc1"], col["fc2"]), (col["fc2"], col["end"])],
    }

    xf, n1a, n2a, ga, gpa, tab, w0, qa, ka, va, cf, vecs, sr, kc = layer_in(
        cfg, inputs, cotangent, segments, live_blocks, w, sv, fr
    )
    oa, lsea, hf, n1b, n2b, gb, gpb, w1, qb, kb, vb = layer_mid(cfg, qa, ka, va, sr, kc, ga, xf, w, w0, vecs, tab)
    ob, lseb = attn_fwd(heads, segments, live_blocks, qb, kb, vb, sr, kc)
    y, dob, e2b, grb, vdb = layer_turn(cfg, ob, gb, hf, cf, w1, vecs, n2b, gpb)
    dmb = attn_bwd(heads, segments, live_blocks, qb, kb, vb, ob, dob, lseb, sr, kc, tab)
    dhf, e2a, doa, vfb, vda, out1, outq, gra = layer_back(
        cfg, dmb, e2b, cf, hf, n1b, w1, w0, vecs, xf, ga, gpa, n2a, oa, grb
    )
    last_part = finish(
        cfg,
        *layer_last(
            cfg, qa, ka, va, oa, doa, lsea, sr, kc, tab, e2a, dhf, xf, n1a, w0, vecs, vfb, vdb, vda, gra, out1, outq, hf, y
        ),
    )
    so, ig, bg1, bb1, gqkv, bqkv, gout, bdy, bdy2, bg2, bb2, gfc1, bfc1, gfc2 = last_part
    bqkv, bfc1, gfc2 = bqkv.transpose(1, 0, 2), bfc1.transpose(1, 0, 2), gfc2.T[None]
    return (so, ig, bg1, bb1, gqkv, bqkv, gout, bdy, bg2, bb2, gfc1, bfc1, gfc2, bdy2)


def solution(mesh):
    both = ("dp", "tensor")
    in_specs = (
        P(None, "dp", "tensor", None),
        P(None, "dp", "tensor", None),
        P(None, "dp", None),
        P(None, "dp"),
        P("section", both),
        P("section", both),
        P("section", "dp", "tensor"),
        P("section", "tensor", "dp"),
        P("section", "tensor", "dp"),
        P("section", both),
        P("section", both),
        P("section", both),
        P("section", "dp", "tensor"),
        P("section", "tensor", "dp"),
        P("section", "tensor", "dp"),
        P("section", both),
    )
    out_specs = (
        P("section", None, "dp", "tensor", None),
        P("section", None, "dp", "tensor", None),
        P("section", both),
        P("section", both),
        P("section", "dp", "tensor"),
        P("section", "tensor", "dp"),
        P("section", "tensor", "dp"),
        P("section", both),
        P("section", both),
        P("section", both),
        P("section", "dp", "tensor"),
        P("section", "tensor", "dp"),
        P("section", "tensor", "dp"),
        P("section", both),
    )
    body = functools.partial(shards, mesh.shape["dp"], mesh.shape["tensor"])
    return jax.shard_map(body, mesh=mesh, in_specs=in_specs, out_specs=out_specs, check_vma=False)
```
